32 devices in a mesh: dp: 8 (over y, x, core), seq: 4 (over z).
Axes of the slice: x: 2, y: 2, z: 4, core: 2. Of those that a mesh axis runs over, the one named last changes fastest.
Arguments:
- block_input: bfloat16 [16, 512, 2048], P('dp', 'seq'), may hold values from -12 to 12
- segment_ids: int32 [16, 512], P('dp'), may hold values from 0 to 3, never falling along the last dimension, each value on 1 to 256 neighbouring positions
- cotangent: bfloat16 [16, 512, 2048], P('dp', 'seq'), may hold values from -6 to 6
- attn_gain: float32 [2048], P(('dp', 'seq')), may hold values from 0.5 to 1.5
- qkv_weight: float32 [2048, 3072], P('dp', 'seq'), may hold values from -1 to 1
- out_weight: float32 [2048, 2048], P('seq', 'dp'), may hold values from -0.75 to 0.75
- mlp_gain: float32 [2048], P(('dp', 'seq')), may hold values from 0.5 to 1.5
- gate_up_weight: float32 [2048, 2, 8192], P('dp', None, 'seq'), may hold values from -0.125 to 0.125
- down_weight: float32 [8192, 2048], P('seq', 'dp'), may hold values from -0.125 to 0.125
- first_attn_gain: float32 [2048], P(('dp', 'seq')), may hold values from -30 to 30
- first_qkv: float32 [2048, 3072], P('dp', 'seq'), may hold values from -30 to 30
- first_out: float32 [2048, 2048], P('seq', 'dp'), may hold values from -30 to 30
- first_mlp_gain: float32 [2048], P(('dp', 'seq')), may hold values from -30 to 30
- first_gate_up: float32 [2048, 2, 8192], P('dp', None, 'seq'), may hold values from -30 to 30
- first_down: float32 [8192, 2048], P('seq', 'dp'), may hold values from -30 to 30
- second_attn_gain: float32 [2048], P(('dp', 'seq')), may hold values from 100 to 300000
- second_qkv: float32 [2048, 3072], P('dp', 'seq'), may hold values from 100 to 30000
- second_out: float32 [2048, 2048], P('seq', 'dp'), may hold values from 50 to 500
- second_mlp_gain: float32 [2048], P(('dp', 'seq')), may hold values from 50 to 500
- second_gate_up: float32 [2048, 2, 8192], P('dp', None, 'seq'), may hold values from 50 to 500
- second_down: float32 [8192, 2048], P('seq', 'dp'), may hold values from 50 to 500
Outputs:
- output: bfloat16 [16, 512, 2048], P('dp', 'seq')
- input_grad: bfloat16 [16, 512, 2048], P('dp', 'seq')
- grad_attn_gain: float32 [2048], P(('dp', 'seq'))
- grad_qkv: float32 [2048, 3072], P('dp', 'seq')
- grad_out: float32 [2048, 2048], P('seq', 'dp')
- grad_mlp_gain: float32 [2048], P(('dp', 'seq'))
- grad_gate_up: float32 [2048, 2, 8192], P('dp', None, 'seq')
- grad_down: float32 [8192, 2048], P('seq', 'dp')
- new_attn_gain: float32 [2048], P(('dp', 'seq'))
- new_qkv: float32 [2048, 3072], P('dp', 'seq')
- new_out: float32 [2048, 2048], P('seq', 'dp')
- new_mlp_gain: float32 [2048], P(('dp', 'seq'))
- new_gate_up: float32 [2048, 2, 8192], P('dp', None, 'seq')
- new_down: float32 [8192, 2048], P('seq', 'dp')
- new_first_attn_gain: float32 [2048], P(('dp', 'seq'))
- new_first_qkv: float32 [2048, 3072], P('dp', 'seq')
- new_first_out: float32 [2048, 2048], P('seq', 'dp')
- new_first_mlp_gain: float32 [2048], P(('dp', 'seq'))
- new_first_gate_up: float32 [2048, 2, 8192], P('dp', None, 'seq')
- new_first_down: float32 [8192, 2048], P('seq', 'dp')
- new_second_attn_gain: float32 [2048], P(('dp', 'seq'))
- new_second_qkv: float32 [2048, 3072], P('dp', 'seq')
- new_second_out: float32 [2048, 2048], P('seq', 'dp')
- new_second_mlp_gain: float32 [2048], P(('dp', 'seq'))
- new_second_gate_up: float32 [2048, 2, 8192], P('dp', None, 'seq')
- new_second_down: float32 [8192, 2048], P('seq', 'dp')
The draws below stay inside these ranges and needn't reach their ends.
Inputs may be any that keep to these rules, and one draw needn't show every extreme that they name: `segment_ids`: in each sequence the numbers never fall, and each segment holds 1 to 256 consecutive positions, one of them exactly that many.
All inputs are finite; a program needn't handle non-finite values.
Results may differ from the reference program's by a relative error of at most 0.023.
Values may be sent and summed in bfloat16 or wider, within the bound.
A program may use at most 320 MiB of HBM per device.

```python
import math
import jax
import jax.numpy as jnp
import numpy as np
from jax import lax

D = 2048
FF = 8192
HEADS = 32
KV_HEADS = 8
HEAD_DIM = 64
LEN = 512
SEQS = 16
Q_WIDTH = 2048
QKV_WIDTH = 3072


def log_between(key, shape, low, high):
    fraction = jax.random.uniform(key, shape, dtype=jnp.float32)
    return jnp.exp(math.log(low) + fraction * (math.log(high) - math.log(low)))


def draw_block_input(key, part):
    noise_part = jnp.clip(jax.random.normal(jax.random.fold_in(key, 11), (SEQS, LEN, D), dtype=jnp.float32), -6.0, 6.0)
    return noise_part.astype(jnp.bfloat16)


def draw_qkv_weight(key, part):
    base_draw = jnp.clip(jax.random.normal(jax.random.fold_in(key, 21), (D, QKV_WIDTH), dtype=jnp.float32), -6.0, 6.0) * D ** (-0.5)
    return base_draw


def draw_second_attn_gain(key, part):
    return log_between(jax.random.fold_in(key, 32), (D,), 100.0, 30000.0)


def draw_second_qkv(key, part):
    return log_between(jax.random.fold_in(key, 44), (D, QKV_WIDTH), 100.0, 30000.0)


def shard_levels(own_key, dims, pieces, smallest, largest):
    def one(position, shards_of):
        steps = jax.random.uniform(jax.random.fold_in(jax.random.fold_in(own_key, 6), position), (shards_of,), jnp.float32, smallest / len(pieces), largest / len(pieces))
        return jnp.repeat(jnp.exp(steps), dims[position] // shards_of).reshape((-1,) + (1,) * (len(dims) - position - 1))

    level = one(*pieces[0])
    for cut in pieces[1:]:
        level = level * one(*cut)
    return level


def split_up(amount, total, limit, lean):
    loads = [(1 << 20) // math.isqrt(rank ** lean) + 1 for rank in range(2, amount + 1)]
    surplus, counts = total - limit - (amount - 1), [1] * (amount - 1)
    while surplus > 0:
        free = [i for i in range(amount - 1) if counts[i] < limit]
        whole, remaining = sum([loads[i] for i in free]), surplus
        for i in free:
            addition = min(limit - counts[i], max(1, remaining * loads[i] // whole), surplus)
            counts[i] = counts[i] + addition
            surplus = surplus - addition
    return np.array([limit] + counts)


def ragged(rng, count, total, reach, slope):
    if count == 2:
        one = jax.random.randint(rng, (), max(1, total - reach), min(reach, total - 1) + 1)
        return jnp.stack([one, total - one])
    lengths = jnp.asarray(split_up(count, total, reach, slope), jnp.int32)
    twos = (count - 1) // 2
    donor, taker = lengths[1:1 + 2 * twos:2], lengths[2:2 + 2 * twos:2]
    room = jnp.minimum(donor - 1, reach - taker)
    moved = jax.random.randint(jax.random.fold_in(rng, 1), (twos,), 0, 1 << 20) % (room + 1)
    lengths = lengths.at[1:1 + 2 * twos:2].set(donor - moved).at[2:2 + 2 * twos:2].set(taker + moved)
    return lengths[jax.random.permutation(jax.random.fold_in(rng, 2), count)]


def normal_values(own_key, dims, scale, reach, pieces=(), kind=jnp.bfloat16):
    result = scale * jax.random.normal(own_key, dims, jnp.float32)
    if pieces:
        result = result * shard_levels(own_key, dims, pieces, -0.22, 0.18)
    return jnp.clip(result, -reach, reach).astype(kind)


def setup_inputs(seed: int = 0) -> dict:
    key_of = jax.random.split(jax.random.key(seed), 22)
    return {
        "block_input": draw_block_input(jax.random.fold_in(key_of[21], 71), 0),
        "segment_ids": jax.vmap(lambda own: jnp.searchsorted(jnp.cumsum(ragged(own, 4, LEN, LEN // 2, 0)), jnp.arange(LEN), side="right"))(jax.random.split(key_of[1], SEQS)).reshape((SEQS, LEN)).astype(jnp.int32),
        "cotangent": normal_values(key_of[2], (SEQS, LEN, D), 1.0, 6.0, ((0, 8), (1, 4))),
        "attn_gain": jnp.clip(1.0 + 0.1 * jax.random.normal(key_of[3], (D,), jnp.float32), 0.5, 1.5),
        "qkv_weight": draw_qkv_weight(jax.random.fold_in(key_of[21], 71), 0),
        "out_weight": normal_values(key_of[5], (Q_WIDTH, D), (Q_WIDTH // 32) ** -0.5, 0.75, ((0, 4), (1, 8)), jnp.float32),
        "mlp_gain": jnp.clip(1.0 + 0.1 * jax.random.normal(key_of[6], (D,), jnp.float32), 0.5, 1.5),
        "gate_up_weight": normal_values(key_of[7], (D, 2, FF), D ** -0.5, 0.125, ((0, 8), (2, 4)), jnp.float32),
        "down_weight": normal_values(key_of[8], (FF, D), (FF // 4) ** -0.5, 0.125, ((0, 4), (1, 8)), jnp.float32),
        "first_attn_gain": normal_values(key_of[9], (D,), 5.0, 30.0, ((0, 32),), jnp.float32),
        "first_qkv": normal_values(key_of[10], (D, QKV_WIDTH), 5.0, 30.0, ((0, 8), (1, 4)), jnp.float32),
        "first_out": normal_values(key_of[11], (Q_WIDTH, D), 5.0, 30.0, ((0, 4), (1, 8)), jnp.float32),
        "first_mlp_gain": normal_values(key_of[12], (D,), 5.0, 30.0, ((0, 32),), jnp.float32),
        "first_gate_up": normal_values(key_of[13], (D, 2, FF), 5.0, 30.0, ((0, 8), (2, 4)), jnp.float32),
        "first_down": normal_values(key_of[14], (FF, D), 5.0, 30.0, ((0, 4), (1, 8)), jnp.float32),
        "second_attn_gain": draw_second_attn_gain(jax.random.fold_in(key_of[21], 71), 0),
        "second_qkv": draw_second_qkv(jax.random.fold_in(key_of[21], 71), 0),
        "second_out": jnp.clip(jnp.exp(math.log(500.0) - 2.3025851 * jax.random.uniform(key_of[17], (Q_WIDTH, D), jnp.float32) ** shard_levels(key_of[17], (Q_WIDTH, D), ((0, 4), (1, 8)), -0.2, 0.2)), 50.0, 500.0),
        "second_mlp_gain": jnp.clip(jnp.exp(math.log(500.0) - 2.3025851 * jax.random.uniform(key_of[18], (D,), jnp.float32) ** shard_levels(key_of[18], (D,), ((0, 32),), -0.2, 0.2)), 50.0, 500.0),
        "second_gate_up": jnp.clip(jnp.exp(math.log(500.0) - 2.3025851 * jax.random.uniform(key_of[19], (D, 2, FF), jnp.float32) ** shard_levels(key_of[19], (D, 2, FF), ((0, 8), (2, 4)), -0.2, 0.2)), 50.0, 500.0),
        "second_down": jnp.clip(jnp.exp(math.log(500.0) - 2.3025851 * jax.random.uniform(key_of[20], (FF, D), jnp.float32) ** shard_levels(key_of[20], (FF, D), ((0, 4), (1, 8)), -0.2, 0.2)), 50.0, 500.0),
    }


norm_eps = 1e-05
rope_base = 500000.0
beta_one = 0.9
beta_two = 0.95
learn_rate = 0.01
weight_decay = 0.1
adam_eps = 1e-08
step_count = 10.0
masked_score = -1e+30

def narrow(values):
    return lax.optimization_barrier(values.astype(jnp.bfloat16))

def segment_positions(segments):
    length_here = segments.shape[-1]
    earlier = (segments[..., None, :] < segments[..., :, None]).astype(jnp.int32)
    return jnp.arange(length_here, dtype=jnp.int32) - lax.optimization_barrier(jnp.sum(earlier, axis=-1, dtype=jnp.int32))

def rope_tables(positions, head_size):
    half_size = head_size // 2
    inverse = rope_base ** (-2.0 * jnp.arange(half_size, dtype=jnp.float32) / head_size)
    angles = positions.astype(jnp.float32)[..., None] * inverse
    return (jnp.cos(angles), jnp.sin(angles))

def rotate(vectors, cosine, sine):
    half_size = vectors.shape[-1] // 2
    first_half = vectors[..., :half_size]
    second_half = vectors[..., half_size:]
    cos_wide = cosine[..., None, :]
    sin_wide = sine[..., None, :]
    return jnp.concatenate([first_half * cos_wide - second_half * sin_wide, second_half * cos_wide + first_half * sin_wide], -1)

def unrotate(vectors, cosine, sine):
    half_size = vectors.shape[-1] // 2
    first_half = vectors[..., :half_size]
    second_half = vectors[..., half_size:]
    cos_wide = cosine[..., None, :]
    sin_wide = sine[..., None, :]
    return jnp.concatenate([first_half * cos_wide + second_half * sin_wide, second_half * cos_wide - first_half * sin_wide], -1)

def rms_forward(values, gain_wide):
    inverse = lax.rsqrt(lax.optimization_barrier(jnp.mean(values * values, axis=-1, keepdims=True)) + norm_eps)
    scaled = values * inverse
    return (scaled, inverse, (scaled * gain_wide).astype(jnp.bfloat16))

def rms_backward(d_normed, scaled, inverse, gain_wide):
    d_scaled = d_normed * gain_wide
    d_values = inverse * (d_scaled - scaled * lax.optimization_barrier(jnp.mean(d_scaled * scaled, axis=-1, keepdims=True)))
    return (d_values, lax.optimization_barrier(jnp.sum(d_normed * scaled, axis=0)))

def adam_update(weight, grad, first, second):
    new_first = beta_one * first + (1.0 - beta_one) * grad
    new_second = beta_two * second + (1.0 - beta_two) * grad * grad
    first_hat = new_first / (1.0 - beta_one ** step_count)
    second_hat = new_second / (1.0 - beta_two ** step_count)
    new_weight = weight - learn_rate * (first_hat / (jnp.sqrt(second_hat) + adam_eps) + weight_decay * weight)
    return (new_weight, new_first, new_second)

def layer_block(inputs16, segments, cotangent16, params):
    qkv16, gain_one, out16, gate_up16, gain_two, down16 = params
    block_seqs = inputs16.shape[0]
    total_rows = block_seqs * LEN
    groups = HEADS // KV_HEADS
    slot_count = groups + 2
    score_scale = HEAD_DIM ** (-0.5)
    gate_up_flat = gate_up16.reshape(D, 2 * FF)
    positions = segment_positions(segments)
    cosine, sine = rope_tables(positions, HEAD_DIM)
    index_line = jnp.arange(LEN, dtype=jnp.int32)
    allowed = (segments[:, :, None] == segments[:, None, :]) & (index_line[None, None, :] <= index_line[None, :, None])
    allowed = allowed[:, None, None, :, :]
    wide_input = inputs16.reshape(total_rows, D).astype(jnp.float32)
    scaled_one, inverse_one, normed_one = rms_forward(wide_input, gain_one)
    qkv = jnp.dot(normed_one, qkv16, preferred_element_type=jnp.float32).reshape(block_seqs, LEN, KV_HEADS, slot_count, HEAD_DIM)
    query = qkv[:, :, :, :groups].reshape(block_seqs, LEN, HEADS, HEAD_DIM)
    key_part = qkv[:, :, :, groups]
    value_wide = narrow(qkv[:, :, :, groups + 1]).astype(jnp.float32)
    query_wide = narrow(rotate(query, cosine, sine)).astype(jnp.float32).reshape(block_seqs, LEN, KV_HEADS, groups, HEAD_DIM)
    key_wide = narrow(rotate(key_part, cosine, sine)).astype(jnp.float32)
    raw_scores = jnp.einsum('sqgjd,skgd->sgjqk', query_wide, key_wide) * score_scale
    scores = jnp.where(allowed, raw_scores, masked_score)
    top_score = lax.optimization_barrier(jnp.max(scores, axis=-1, keepdims=True))
    log_total = top_score + jnp.log(lax.optimization_barrier(jnp.sum(jnp.exp(scores - top_score), axis=-1, keepdims=True)))
    probs = jnp.exp(scores - log_total)
    probs_wide = narrow(probs).astype(jnp.float32)
    attended16 = jnp.einsum('sgjqk,skgd->sqgjd', probs_wide, value_wide).reshape(total_rows, Q_WIDTH).astype(jnp.bfloat16)
    resid = wide_input + jnp.dot(attended16, out16, preferred_element_type=jnp.float32)
    scaled_two, inverse_two, normed_two = rms_forward(resid, gain_two)
    gate_up = jnp.dot(normed_two, gate_up_flat, preferred_element_type=jnp.float32)
    gate_part = gate_up[:, :FF]
    up_part = gate_up[:, FF:]
    sigmoid_gate = jax.nn.sigmoid(gate_part)
    active = gate_part * sigmoid_gate
    hidden16 = (active * up_part).astype(jnp.bfloat16)
    output = (resid + jnp.dot(hidden16, down16, preferred_element_type=jnp.float32)).astype(jnp.bfloat16)
    cot_rows = cotangent16.reshape(total_rows, D)
    grad_down = jnp.dot(hidden16.T, cot_rows, preferred_element_type=jnp.float32)
    d_hidden = jnp.dot(cot_rows, down16.T, preferred_element_type=jnp.float32)
    d_gate = d_hidden * up_part * sigmoid_gate * (1.0 + gate_part * (1.0 - sigmoid_gate))
    d_up = d_hidden * active
    d_gate_up16 = jnp.concatenate([d_gate, d_up], 1).astype(jnp.bfloat16)
    grad_gate_up = jnp.dot(normed_two.T, d_gate_up16, preferred_element_type=jnp.float32).reshape(D, 2, FF)
    d_normed_two = jnp.dot(d_gate_up16, gate_up_flat.T, preferred_element_type=jnp.float32)
    d_resid_part, grad_gain_two = rms_backward(d_normed_two, scaled_two, inverse_two, gain_two)
    d_resid = cot_rows.astype(jnp.float32) + d_resid_part
    d_resid16 = d_resid.astype(jnp.bfloat16)
    grad_out = jnp.dot(attended16.T, d_resid16, preferred_element_type=jnp.float32)
    d_attended = narrow(jnp.dot(d_resid16, out16.T, preferred_element_type=jnp.float32)).astype(jnp.float32)
    d_attended = d_attended.reshape(block_seqs, LEN, KV_HEADS, groups, HEAD_DIM)
    d_probs = jnp.einsum('sqgjd,skgd->sgjqk', d_attended, value_wide)
    delta = lax.optimization_barrier(jnp.sum(probs * d_probs, axis=-1, keepdims=True))
    d_scores = narrow(probs * (d_probs - delta) * score_scale).astype(jnp.float32)
    d_query = jnp.einsum('sgjqk,skgd->sqgjd', d_scores, key_wide).reshape(block_seqs, LEN, HEADS, HEAD_DIM)
    d_key = jnp.einsum('sgjqk,sqgjd->skgd', d_scores, query_wide)
    d_value = jnp.einsum('sgjqk,sqgjd->skgd', probs_wide, d_attended)
    d_query = unrotate(d_query, cosine, sine).reshape(block_seqs, LEN, KV_HEADS, groups, HEAD_DIM)
    d_key = unrotate(d_key, cosine, sine)
    d_qkv16 = jnp.concatenate([d_query, d_key[:, :, :, None], d_value[:, :, :, None]], 3)
    d_qkv16 = d_qkv16.reshape(total_rows, QKV_WIDTH).astype(jnp.bfloat16)
    grad_qkv = jnp.dot(normed_one.T, d_qkv16, preferred_element_type=jnp.float32)
    d_normed_one = jnp.dot(d_qkv16, qkv16.T, preferred_element_type=jnp.float32)
    d_input_part, grad_gain_one = rms_backward(d_normed_one, scaled_one, inverse_one, gain_one)
    input_grad = (d_resid + d_input_part).astype(jnp.bfloat16)
    grads = (grad_gain_one, grad_qkv, grad_out, grad_gain_two, grad_gate_up, grad_down)
    return (output.reshape(block_seqs, LEN, D), input_grad.reshape(block_seqs, LEN, D), grads)

def reference(block_input, segment_ids, cotangent, attn_gain, qkv_weight, out_weight, mlp_gain, gate_up_weight, down_weight, first_attn_gain, first_qkv, first_out, first_mlp_gain, first_gate_up, first_down, second_attn_gain, second_qkv, second_out, second_mlp_gain, second_gate_up, second_down):
    params = (qkv_weight.astype(jnp.bfloat16), narrow(attn_gain).astype(jnp.float32), out_weight.astype(jnp.bfloat16), gate_up_weight.astype(jnp.bfloat16), narrow(mlp_gain).astype(jnp.float32), down_weight.astype(jnp.bfloat16))
    block_seqs = math.gcd(SEQS, 8)
    block_count = SEQS // block_seqs
    inputs = (block_input.reshape(block_count, block_seqs, LEN, D), segment_ids.reshape(block_count, block_seqs, LEN), cotangent.reshape(block_count, block_seqs, LEN, D))
    zeros = (jnp.zeros((D,), jnp.float32), jnp.zeros((D, QKV_WIDTH), jnp.float32), jnp.zeros((Q_WIDTH, D), jnp.float32), jnp.zeros((D,), jnp.float32), jnp.zeros((D, 2, FF), jnp.float32), jnp.zeros((FF, D), jnp.float32))

    def one_block(carry, item):
        block_out, block_grad, grads = layer_block(item[0], item[1], item[2], params)
        return (jax.tree.map(jnp.add, carry, grads), (block_out, block_grad))
    grads, (outputs, input_grads) = lax.scan(one_block, zeros, inputs)
    output = outputs.reshape(SEQS, LEN, D)
    input_grad = input_grads.reshape(SEQS, LEN, D)
    g_one, g_qkv, g_out, g_two, g_gu, g_down = grads
    w_one, m_one, v_one = adam_update(attn_gain, g_one, first_attn_gain, second_attn_gain)
    w_qkv, m_qkv, v_qkv = adam_update(qkv_weight, g_qkv, first_qkv, second_qkv)
    w_out, m_out, v_out = adam_update(out_weight, g_out, first_out, second_out)
    w_two, m_two, v_two = adam_update(mlp_gain, g_two, first_mlp_gain, second_mlp_gain)
    w_gu, m_gu, v_gu = adam_update(gate_up_weight, g_gu, first_gate_up, second_gate_up)
    w_down, m_down, v_down = adam_update(down_weight, g_down, first_down, second_down)
    return (output, input_grad, g_one, g_qkv, g_out, g_two, g_gu, g_down, w_one, w_qkv, w_out, w_two, w_gu, w_down, m_one, m_qkv, m_out, m_two, m_gu, m_down, v_one, v_qkv, v_out, v_two, v_gu, v_down)
```

```python
import jax
import jax.numpy as jnp
from jax import lax
from jax.sharding import PartitionSpec as P

HEADS = 32
KV_HEADS = 8
HEAD_DIM = 64


norm_eps = 1e-05
rope_base = 500000.0
beta_one = 0.9
beta_two = 0.95
learn_rate = 0.01
weight_decay = 0.1
adam_eps = 1e-08
step_count = 10.0
masked_score = -1e30


def segment_positions(segments):
    length_here = segments.shape[-1]
    earlier = (segments[..., None, :] < segments[..., :, None]).astype(jnp.int32)
    return jnp.arange(length_here, dtype=jnp.int32) - jnp.sum(earlier, axis=-1, dtype=jnp.int32)


def rope_tables(positions, head_size):
    half_size = head_size // 2
    inverse = rope_base ** (-2.0 * jnp.arange(half_size, dtype=jnp.float32) / head_size)
    angles = positions.astype(jnp.float32)[..., None] * inverse
    return (jnp.cos(angles), jnp.sin(angles))


def rotate(vectors, cosine, sine):
    half_size = vectors.shape[-1] // 2
    first_half = vectors[..., :half_size]
    second_half = vectors[..., half_size:]
    cos_wide = cosine[..., None, :]
    sin_wide = sine[..., None, :]
    return jnp.concatenate(
        [
            first_half * cos_wide - second_half * sin_wide,
            second_half * cos_wide + first_half * sin_wide,
        ],
        -1,
    )


def unrotate(vectors, cosine, sine):
    half_size = vectors.shape[-1] // 2
    first_half = vectors[..., :half_size]
    second_half = vectors[..., half_size:]
    cos_wide = cosine[..., None, :]
    sin_wide = sine[..., None, :]
    return jnp.concatenate(
        [
            first_half * cos_wide + second_half * sin_wide,
            second_half * cos_wide - first_half * sin_wide,
        ],
        -1,
    )


def rms_forward(values, gain_wide):
    inverse = lax.rsqrt(jnp.mean(values * values, axis=-1, keepdims=True) + norm_eps)
    scaled = values * inverse
    return (scaled, inverse, (scaled * gain_wide).astype(jnp.bfloat16))


def rms_backward(d_normed, scaled, inverse, gain_wide):
    d_scaled = d_normed * gain_wide
    d_values = inverse * (d_scaled - scaled * jnp.mean(d_scaled * scaled, axis=-1, keepdims=True))
    return (d_values, jnp.sum(d_normed * scaled, axis=0))


def adam_update(weight, grad, first, second):
    new_first = beta_one * first + (1.0 - beta_one) * grad
    new_second = beta_two * second + (1.0 - beta_two) * grad * grad
    first_hat = new_first / (1.0 - beta_one**step_count)
    second_hat = new_second / (1.0 - beta_two**step_count)
    new_weight = weight - learn_rate * (
        first_hat / (jnp.sqrt(second_hat) + adam_eps) + weight_decay * weight
    )
    return (new_weight, new_first, new_second)


def contract_rows(left, right):
    return lax.dot_general(
        left, right, (((0,), (0,)), ((), ())), preferred_element_type=jnp.float32
    )


def times_transpose(left, right):
    return lax.dot_general(
        left, right, (((1,), (1,)), ((), ())), preferred_element_type=jnp.float32
    )


def per_device(
    block_input,
    segment_ids,
    cotangent,
    attn_gain,
    qkv_weight,
    out_weight,
    mlp_gain,
    gate_up_weight,
    down_weight,
    first_attn_gain,
    first_qkv,
    first_out,
    first_mlp_gain,
    first_gate_up,
    first_down,
    second_attn_gain,
    second_qkv,
    second_out,
    second_mlp_gain,
    second_gate_up,
    second_down,
):
    seqs_here, local_len, width = block_input.shape
    full_len = segment_ids.shape[1]
    total_rows = seqs_here * full_len
    groups = HEADS // KV_HEADS
    slot_count = groups + 2
    kv_local = qkv_weight.shape[1] // (slot_count * HEAD_DIM)
    query_cols = kv_local * groups * HEAD_DIM
    unit_count = down_weight.shape[0]
    score_scale = HEAD_DIM ** (-0.5)
    local_rows = seqs_here * local_len
    gain_pair = jnp.stack([attn_gain, mlp_gain]).astype(jnp.bfloat16)
    gain_block = lax.all_gather(gain_pair, ("dp", "seq"), axis=1, tiled=True)
    gain_one = gain_block[0].astype(jnp.float32)
    gain_two = gain_block[1].astype(jnp.float32)
    local_input = block_input.reshape(local_rows, width).astype(jnp.float32)
    scaled_one, inverse_one, normed_here = rms_forward(local_input, gain_one)
    normed_one = lax.all_gather(
        normed_here.reshape(seqs_here, local_len, width), "seq", axis=1, tiled=True
    ).reshape(total_rows, width)
    qkv_cols = lax.all_gather(qkv_weight.astype(jnp.bfloat16), "dp", axis=0, tiled=True)
    out_rows = lax.all_gather(out_weight.astype(jnp.bfloat16), "dp", axis=1, tiled=True)
    gate_up_cols = lax.all_gather(
        gate_up_weight.astype(jnp.bfloat16).reshape(-1, 2 * unit_count), "dp", axis=0, tiled=True
    )
    cot_all = lax.all_gather(cotangent, "seq", axis=1, tiled=True)
    down_rows = lax.all_gather(down_weight.astype(jnp.bfloat16), "dp", axis=1, tiled=True)
    positions = segment_positions(segment_ids)
    cosine, sine = rope_tables(positions, HEAD_DIM)
    index_line = jnp.arange(full_len, dtype=jnp.int32)
    allowed = (segment_ids[:, :, None] == segment_ids[:, None, :]) & (
        index_line[None, None, :] <= index_line[None, :, None]
    )
    allowed = allowed[:, None, None, :, :]
    qkv = jnp.dot(normed_one, qkv_cols, preferred_element_type=jnp.float32)
    qkv = qkv.reshape(seqs_here, full_len, kv_local, slot_count, HEAD_DIM)
    query = qkv[:, :, :, :groups].reshape(seqs_here, full_len, kv_local * groups, HEAD_DIM)
    query_groups = (
        rotate(query, cosine, sine)
        .astype(jnp.bfloat16)
        .reshape(seqs_here, full_len, kv_local, groups, HEAD_DIM)
    )
    key16 = rotate(qkv[:, :, :, groups], cosine, sine).astype(jnp.bfloat16)
    value16 = qkv[:, :, :, groups + 1].astype(jnp.bfloat16)

    def masked_scores():
        raw_scores = (
            jnp.einsum("sqgjd,skgd->sgjqk", query_groups, key16, preferred_element_type=jnp.float32)
            * score_scale
        )
        return jnp.where(allowed, raw_scores, masked_score)

    scores = masked_scores()
    top_score = jnp.max(scores, axis=-1, keepdims=True)
    log_total = top_score + jnp.log(jnp.sum(jnp.exp(scores - top_score), axis=-1, keepdims=True))
    probs16 = jnp.exp(scores - log_total).astype(jnp.bfloat16)
    attended16 = jnp.einsum(
        "sgjqk,skgd->sqgjd", probs16, value16, preferred_element_type=jnp.float32
    )
    attended16 = attended16.reshape(total_rows, query_cols).astype(jnp.bfloat16)
    attn_part = jnp.dot(attended16, out_rows, preferred_element_type=jnp.float32)

    def to_local(part):
        return (
            lax.psum_scatter(
                part.astype(jnp.bfloat16).reshape(seqs_here, full_len, width),
                "seq",
                scatter_dimension=1,
                tiled=True,
            )
            .astype(jnp.float32)
            .reshape(local_rows, width)
        )

    resid = local_input + to_local(attn_part)
    scaled_two, inverse_two, normed_two_here = rms_forward(resid, gain_two)
    normed_two = lax.all_gather(
        normed_two_here.reshape(seqs_here, local_len, width), "seq", axis=1, tiled=True
    ).reshape(total_rows, width)
    gate_up = jnp.dot(normed_two, gate_up_cols, preferred_element_type=jnp.float32)
    gate_part = gate_up[:, :unit_count]
    up_part = gate_up[:, unit_count:]
    sigmoid_gate = jax.nn.sigmoid(gate_part)
    active = gate_part * sigmoid_gate
    hidden16 = (active * up_part).astype(jnp.bfloat16)
    down_part = jnp.dot(hidden16, down_rows, preferred_element_type=jnp.float32)
    output = (resid + to_local(down_part)).astype(jnp.bfloat16).reshape(block_input.shape)
    cot_rows = cot_all.reshape(total_rows, width)
    d_hidden = times_transpose(cot_rows, down_rows)
    d_gate = d_hidden * up_part * sigmoid_gate * (1.0 + gate_part * (1.0 - sigmoid_gate))
    d_up = d_hidden * active
    d_gate_up16 = jnp.concatenate([d_gate, d_up], 1).astype(jnp.bfloat16)
    d_normed_two = to_local(times_transpose(d_gate_up16, gate_up_cols))
    down_term = contract_rows(cot_rows, hidden16)
    gate_up_term = contract_rows(normed_two, d_gate_up16)
    down_sum = lax.psum_scatter(
        down_term.astype(jnp.bfloat16), "dp", scatter_dimension=0, tiled=True
    ).astype(jnp.float32)
    grad_gate_up = (
        lax.psum_scatter(gate_up_term.astype(jnp.bfloat16), "dp", scatter_dimension=0, tiled=True)
        .reshape(gate_up_weight.shape)
        .astype(jnp.float32)
    )
    grad_down = down_sum.T
    resid_part, gain_two_term = rms_backward(d_normed_two, scaled_two, inverse_two, gain_two)
    d_resid = cotangent.reshape(local_rows, width).astype(jnp.float32) + resid_part
    d_resid16 = lax.all_gather(
        d_resid.astype(jnp.bfloat16).reshape(seqs_here, local_len, width),
        "seq",
        axis=1,
        tiled=True,
    ).reshape(total_rows, width)
    d_attended = times_transpose(d_resid16, out_rows).astype(jnp.bfloat16)
    d_attended = d_attended.reshape(seqs_here, full_len, kv_local, groups, HEAD_DIM)
    scores = masked_scores()
    probs = jnp.exp(scores - log_total)
    d_probs = jnp.einsum(
        "sqgjd,skgd->sgjqk", d_attended, value16, preferred_element_type=jnp.float32
    )
    delta = jnp.sum(probs * d_probs, axis=-1, keepdims=True)
    d_scores16 = (probs * (d_probs - delta) * score_scale).astype(jnp.bfloat16)
    d_query = jnp.einsum("sgjqk,skgd->sqgjd", d_scores16, key16, preferred_element_type=jnp.float32)
    d_key = jnp.einsum(
        "sgjqk,sqgjd->skgd", d_scores16, query_groups, preferred_element_type=jnp.float32
    )
    d_value = jnp.einsum(
        "sgjqk,sqgjd->skgd", probs16, d_attended, preferred_element_type=jnp.float32
    )
    d_query = unrotate(
        d_query.reshape(seqs_here, full_len, kv_local * groups, HEAD_DIM), cosine, sine
    )
    d_query = d_query.reshape(seqs_here, full_len, kv_local, groups, HEAD_DIM)
    d_key = unrotate(d_key, cosine, sine)
    d_qkv16 = jnp.concatenate([d_query, d_key[:, :, :, None], d_value[:, :, :, None]], 3)
    d_qkv16 = d_qkv16.reshape(total_rows, qkv_cols.shape[1]).astype(jnp.bfloat16)
    d_normed_one = to_local(times_transpose(d_qkv16, qkv_cols))
    qkv_term = contract_rows(normed_one, d_qkv16)
    out_term = contract_rows(d_resid16, attended16)
    grad_qkv = lax.psum_scatter(
        qkv_term.astype(jnp.bfloat16), "dp", scatter_dimension=0, tiled=True
    ).astype(jnp.float32)
    out_sum = lax.psum_scatter(
        out_term.astype(jnp.bfloat16), "dp", scatter_dimension=0, tiled=True
    ).astype(jnp.float32)
    grad_out = out_sum.T
    input_part, gain_one_term = rms_backward(d_normed_one, scaled_one, inverse_one, gain_one)
    input_grad = (d_resid + input_part).astype(jnp.bfloat16).reshape(block_input.shape)
    gain_grads = lax.psum_scatter(
        jnp.stack([gain_one_term, gain_two_term], 1), ("dp", "seq"), scatter_dimension=0, tiled=True
    )
    grad_gain_one = gain_grads[:, 0]
    grad_gain_two = gain_grads[:, 1]
    w_one, m_one, v_one = adam_update(attn_gain, grad_gain_one, first_attn_gain, second_attn_gain)
    w_qkv, m_qkv, v_qkv = adam_update(qkv_weight, grad_qkv, first_qkv, second_qkv)
    w_out, m_out, v_out = adam_update(out_weight, grad_out, first_out, second_out)
    w_two, m_two, v_two = adam_update(mlp_gain, grad_gain_two, first_mlp_gain, second_mlp_gain)
    w_gu, m_gu, v_gu = adam_update(gate_up_weight, grad_gate_up, first_gate_up, second_gate_up)
    w_down, m_down, v_down = adam_update(down_weight, grad_down, first_down, second_down)
    return (
        output,
        input_grad,
        grad_gain_one,
        grad_qkv,
        grad_out,
        grad_gain_two,
        grad_gate_up,
        grad_down,
        w_one,
        w_qkv,
        w_out,
        w_two,
        w_gu,
        w_down,
        m_one,
        m_qkv,
        m_out,
        m_two,
        m_gu,
        m_down,
        v_one,
        v_qkv,
        v_out,
        v_two,
        v_gu,
        v_down,
    )


def solution(mesh):
    in_specs = (
        P("dp", "seq", None),
        P("dp", None),
        P("dp", "seq", None),
        P(("dp", "seq")),
        P("dp", "seq"),
        P("seq", "dp"),
        P(("dp", "seq")),
        P("dp", None, "seq"),
        P("seq", "dp"),
        P(("dp", "seq")),
        P("dp", "seq"),
        P("seq", "dp"),
        P(("dp", "seq")),
        P("dp", None, "seq"),
        P("seq", "dp"),
        P(("dp", "seq")),
        P("dp", "seq"),
        P("seq", "dp"),
        P(("dp", "seq")),
        P("dp", None, "seq"),
        P("seq", "dp"),
    )
    out_specs = (
        P("dp", "seq", None),
        P("dp", "seq", None),
        P(("dp", "seq")),
        P("dp", "seq"),
        P("seq", "dp"),
        P(("dp", "seq")),
        P("dp", None, "seq"),
        P("seq", "dp"),
        P(("dp", "seq")),
        P("dp", "seq"),
        P("seq", "dp"),
        P(("dp", "seq")),
        P("dp", None, "seq"),
        P("seq", "dp"),
        P(("dp", "seq")),
        P("dp", "seq"),
        P("seq", "dp"),
        P(("dp", "seq")),
        P("dp", None, "seq"),
        P("seq", "dp"),
        P(("dp", "seq")),
        P("dp", "seq"),
        P("seq", "dp"),
        P(("dp", "seq")),
        P("dp", None, "seq"),
        P("seq", "dp"),
    )
    return jax.shard_map(
        per_device, mesh=mesh, in_specs=in_specs, out_specs=out_specs, check_vma=False
    )
```

```python
import functools

import jax
import jax.numpy as jnp
from jax import lax
from jax.experimental import pallas as pl
from jax.experimental.pallas import tpu as pltpu
from jax.sharding import PartitionSpec as P

HEADS = 32
KV_HEADS = 8
norm_eps = 1e-05
rope_base = 500000.0
beta_one = 0.9
beta_two = 0.95
learn_rate = 0.01
weight_decay = 0.1
adam_eps = 1e-08
step_count = 10.0
masked_score = -1e30


HEAD_DIM = 64
LANES = 128


def dot_t(a, b):
    return lax.dot_general(a, b, (((1,), (1,)), ((), ())), preferred_element_type=jnp.float32)


def dot_n(a, b):
    return lax.dot_general(a, b, (((1,), (0,)), ((), ())), preferred_element_type=jnp.float32)


def dot_c(a, b):
    return lax.dot_general(a, b, (((0,), (0,)), ((), ())), preferred_element_type=jnp.float32)


def swap_halves(u):
    lane = lax.broadcasted_iota(jnp.int32, u.shape, 1)
    return jnp.where(lane % 64 < 32, pltpu.roll(u, 96, 1), pltpu.roll(u, 32, 1))


def turn(u, cos_wide, sin_wide):
    return u * cos_wide + swap_halves(u) * sin_wide


def key_start(block, q_rows, reach):
    return max(0, (block * q_rows - reach + 1) // q_rows * q_rows)


def attn_forward_kernel(pairs, q_rows, reach, qkv_ref, cos_ref, sin_ref, seg_col_ref, seg_row_ref,
                        turned_ref, lse_ref, out_ref):
    full_len = qkv_ref.shape[0]
    lane = lax.broadcasted_iota(jnp.int32, (full_len, LANES), 1)
    low = lane < HEAD_DIM
    cos_q = cos_ref[...]
    sin_q = sin_ref[...]
    kv = qkv_ref[:, pairs * LANES:].astype(jnp.float32)
    kv16 = turn(kv, jnp.where(low, cos_q, 1.0), jnp.where(low, sin_q, 0.0)).astype(jnp.bfloat16)
    turned_ref[:, pairs * LANES:] = kv16
    kv32 = kv16.astype(jnp.float32)
    rolled = pltpu.roll(kv32, HEAD_DIM, 1)
    zero = jnp.zeros_like(kv32)
    keys = (jnp.where(low, kv32, zero).astype(jnp.bfloat16), jnp.where(low, zero, rolled).astype(jnp.bfloat16))
    vals = (jnp.where(low, rolled, zero).astype(jnp.bfloat16), jnp.where(low, zero, kv32).astype(jnp.bfloat16))
    for pair in range(pairs):
        cols = slice(pair * LANES, (pair + 1) * LANES)
        query = turn(qkv_ref[:, cols].astype(jnp.float32), cos_q, sin_q) .astype(jnp.bfloat16)
        turned_ref[:, cols] = query
    for block in range(full_len // q_rows):
        first = key_start(block, q_rows, reach)
        last = (block + 1) * q_rows
        rows = slice(block * q_rows, last)
        span = slice(first, last)
        i = lax.broadcasted_iota(jnp.int32, (q_rows, last - first), 0) + block * q_rows
        j = lax.broadcasted_iota(jnp.int32, (q_rows, last - first), 1) + first
        allowed = (j <= i) & (seg_col_ref[rows, :1] == seg_row_ref[:1, span])
        for pair in range(pairs):
            cols = slice(pair * LANES, (pair + 1) * LANES)
            query = turned_ref[rows, cols]
            total = None
            for half in range(2):
                scores = dot_t(query, keys[half][span]) * (HEAD_DIM ** -0.5)
                scores = jnp.where(allowed, scores, masked_score)
                top = jnp.max(scores, axis=1, keepdims=True)
                lse = top + jnp.log(jnp.sum(jnp.exp(scores - top), axis=1, keepdims=True))
                probs = jnp.exp(scores - lse).astype(jnp.bfloat16)
                part = dot_n(probs, vals[half][span])
                total = part if total is None else total + part
                head = 2 * pair + half
                lse_ref[rows, head:head + 1] = lse
            out_ref[rows, cols] = total.astype(jnp.bfloat16)


def attn_backward_kernel(pairs, q_rows, reach, turned_ref, d_out_ref, lse_ref, cos_ref, sin_ref, seg_col_ref,
                         seg_row_ref, grad_ref, dk_ref, dv_ref):
    full_len = turned_ref.shape[0]
    lane = lax.broadcasted_iota(jnp.int32, (full_len, LANES), 1)
    low = lane < HEAD_DIM
    kv32 = turned_ref[:, pairs * LANES:].astype(jnp.float32)
    rolled = pltpu.roll(kv32, HEAD_DIM, 1)
    zero = jnp.zeros_like(kv32)
    keys = (jnp.where(low, kv32, zero).astype(jnp.bfloat16), jnp.where(low, zero, rolled).astype(jnp.bfloat16))
    vals = (jnp.where(low, rolled, zero).astype(jnp.bfloat16), jnp.where(low, zero, kv32).astype(jnp.bfloat16))
    dk_ref[...] = jnp.zeros_like(dk_ref)
    dv_ref[...] = jnp.zeros_like(dv_ref)
    low_rows = low[:q_rows]
    scale = HEAD_DIM ** -0.5
    for block in range(full_len // q_rows):
        first = key_start(block, q_rows, reach)
        last = (block + 1) * q_rows
        rows = slice(block * q_rows, last)
        span = slice(first, last)
        i = lax.broadcasted_iota(jnp.int32, (q_rows, last - first), 0) + block * q_rows
        j = lax.broadcasted_iota(jnp.int32, (q_rows, last - first), 1) + first
        allowed = (j <= i) & (seg_col_ref[rows, :1] == seg_row_ref[:1, span])
        cos_q = cos_ref[rows]
        sin_q = sin_ref[rows]
        for pair in range(pairs):
            cols = slice(pair * LANES, (pair + 1) * LANES)
            query = turned_ref[rows, cols]
            d_out = d_out_ref[rows, cols]
            q32 = query.astype(jnp.float32)
            o32 = d_out.astype(jnp.float32)
            d_query = None
            d_key = None
            d_val = None
            for half in range(2):
                keep = low_rows if half == 0 else ~low_rows
                q_only = jnp.where(keep, q32, 0.0).astype(jnp.bfloat16)
                o_only = jnp.where(keep, o32, 0.0).astype(jnp.bfloat16)
                head = 2 * pair + half
                scores = dot_t(query, keys[half][span]) * scale
                scores = jnp.where(allowed, scores, masked_score)
                probs = jnp.exp(scores - lse_ref[rows, head:head + 1])
                d_probs = dot_t(d_out, vals[half][span])
                delta = jnp.sum(probs * d_probs, axis=1, keepdims=True)
                d_scores = (probs * (d_probs - delta) * scale).astype(jnp.bfloat16)
                probs16 = probs.astype(jnp.bfloat16)
                dq = dot_n(d_scores, keys[half][span])
                dk = dot_c(d_scores, q_only)
                dv = dot_c(probs16, o_only)
                d_query = dq if d_query is None else d_query + dq
                d_key = dk if d_key is None else d_key + dk
                d_val = dv if d_val is None else d_val + dv
            dk_ref[span] = dk_ref[span] + d_key
            dv_ref[span] = dv_ref[span] + d_val
            grad_ref[rows, cols] = turn(d_query, cos_q, -sin_q).astype(jnp.bfloat16)
    d_key = dk_ref[...]
    d_val = dv_ref[...]
    d_key = d_key + pltpu.roll(d_key, HEAD_DIM, 1)
    d_val = d_val + pltpu.roll(d_val, HEAD_DIM, 1)
    d_key = turn(d_key, cos_ref[...], -sin_ref[...])
    grad_ref[:, pairs * LANES:] = jnp.where(low, d_key, d_val).astype(jnp.bfloat16)


def attn_specs(full_len, width):
    line = pl.BlockSpec((full_len, width), lambda s, g: (s, g))
    table = pl.BlockSpec((full_len, LANES), lambda s, g: (s, 0))
    row = pl.BlockSpec((8, full_len), lambda s, g: (s, 0))
    return line, table, row


Q_ROWS = 128
REACH = 256


def attn_forward(qkv, cos, sin, seg_col, seg_row, full_len, groups):
    pairs = groups // 2
    width = (groups + 2) * HEAD_DIM
    seqs = qkv.shape[0] // full_len
    kv = qkv.shape[1] // width
    line, table, row = attn_specs(full_len, width)
    outw = pl.BlockSpec((full_len, groups * HEAD_DIM), lambda s, g: (s, g))
    rows = seqs * full_len
    return pl.pallas_call(
        functools.partial(attn_forward_kernel, pairs, Q_ROWS, REACH),
        grid=(seqs, kv),
        in_specs=[line, table, table, table, row],
        out_specs=[line, pl.BlockSpec((full_len, LANES), lambda s, g: (s, g)), outw],
        out_shape=[
            jax.ShapeDtypeStruct((rows, kv * width), jnp.bfloat16),
            jax.ShapeDtypeStruct((rows, kv * LANES), jnp.float32),
            jax.ShapeDtypeStruct((rows, kv * groups * HEAD_DIM), jnp.bfloat16),
        ],
        cost_estimate=pl.CostEstimate(flops=4 * rows * full_len * kv * LANES * groups, bytes_accessed=rows * kv * width * 6, transcendentals=0),
        name="attn_forward",
    )(qkv, cos, sin, seg_col, seg_row)


def attn_backward(turned, d_out, lse, cos, sin, seg_col, seg_row, full_len, groups):
    pairs = groups // 2
    width = (groups + 2) * HEAD_DIM
    seqs = turned.shape[0] // full_len
    kv = turned.shape[1] // width
    line, table, row = attn_specs(full_len, width)
    outw = pl.BlockSpec((full_len, groups * HEAD_DIM), lambda s, g: (s, g))
    rows = seqs * full_len
    return pl.pallas_call(
        functools.partial(attn_backward_kernel, pairs, Q_ROWS, REACH),
        grid=(seqs, kv),
        in_specs=[line, outw, pl.BlockSpec((full_len, LANES), lambda s, g: (s, g)), table, table, table, row],
        out_specs=line,
        out_shape=jax.ShapeDtypeStruct((rows, kv * width), jnp.bfloat16),
        scratch_shapes=[pltpu.VMEM((full_len, LANES), jnp.float32)] * 2,
        cost_estimate=pl.CostEstimate(flops=10 * rows * full_len * kv * LANES * groups, bytes_accessed=rows * kv * width * 6, transcendentals=0),
        name="attn_backward",
    )(turned, d_out, lse, cos, sin, seg_col, seg_row)


def attn_tables(segment_ids):
    seqs, full_len = segment_ids.shape
    earlier = (segment_ids[..., None, :] < segment_ids[..., :, None]).astype(jnp.int32)
    positions = jnp.arange(full_len, dtype=jnp.int32) - jnp.sum(earlier, axis=-1, dtype=jnp.int32)
    inverse = 500000.0 ** (-2.0 * jnp.arange(HEAD_DIM // 2, dtype=jnp.float32) / HEAD_DIM)
    angles = positions.astype(jnp.float32)[..., None] * inverse
    cos = jnp.cos(angles)
    sin = jnp.sin(angles)
    cos = jnp.concatenate([cos] * 4, -1).reshape(seqs * full_len, LANES)
    sin = jnp.concatenate([-sin, sin] * 2, -1).reshape(seqs * full_len, LANES)
    seg_col = jnp.broadcast_to(segment_ids[:, :, None], (seqs, full_len, LANES)).reshape(seqs * full_len, LANES)
    seg_row = jnp.broadcast_to(segment_ids[:, None, :], (seqs, 8, full_len)).reshape(seqs * 8, full_len)
    return cos, sin, seg_col, seg_row


MESH = pl.DeviceIdType.MESH
VMEM_SPEC = pl.BlockSpec(memory_space=pltpu.VMEM)
ANY_SPEC = pl.BlockSpec(memory_space=pl.ANY)
DMA = pltpu.SemaphoreType.DMA


def place():
    d = lax.axis_index("dp")
    z = lax.axis_index("seq")
    return d, z, d // 2, d % 2


def remote(src, dst, send, recv, dev):
    return pltpu.make_async_remote_copy(
        src_ref=src, dst_ref=dst, send_sem=send, recv_sem=recv, device_id=dev, device_id_type=MESH
    )


def greet_all(n_dp, n_z, d, z):
    barrier = pltpu.get_barrier_semaphore()
    me = d * n_z + z

    def one(o, carry):
        other = lax.rem(me + o, n_dp * n_z)
        pl.semaphore_signal(barrier, inc=1, device_id=(other // n_z, lax.rem(other, n_z)), device_id_type=MESH)
        return carry

    lax.fori_loop(1, n_dp * n_z, one, 0)
    pl.semaphore_wait(barrier, n_dp * n_z - 1)


def greet_line(n_z, d, z, extra=()):
    barrier = pltpu.get_barrier_semaphore()
    c = d % 2
    for o in range(n_z):
        zz = lax.rem(z + o, n_z)
        for core in range(2):
            if o == 0 and core == 0:
                continue
            pl.semaphore_signal(barrier, inc=1, device_id=(d - c + lax.rem(c + core, 2), zz), device_id_type=MESH)
    for dev in extra:
        pl.semaphore_signal(barrier, inc=1, device_id=dev, device_id_type=MESH)
    pl.semaphore_wait(barrier, 2 * n_z - 1 + len(extra))


def block_at(ref, shape, row, col):
    return ref.at[pl.ds(pl.multiple_of(row * shape[0], shape[0]), shape[0]),
                  pl.ds(pl.multiple_of(col * shape[1], shape[1]), shape[1])]


def gather_in_kernel(n_dp, n_z, x_ref, w_ref, g_ref, s_ref, xs, wq, ga, sg,
                     x_s, x_r, f_s, f_r, w_s, w_r, d_s, d_r, g_s, g_r, s_s, s_r, loc):
    d, z, pair, c = place()
    n_d = n_dp // 2
    me = d * n_z + z
    total = n_dp * n_z
    rows = x_ref.shape[1]
    half = rows // 2
    shape = w_ref.shape
    cz = z // 2
    greet_all(n_dp, n_z, d, z)

    my_block = block_at(wq, shape, d, z % 2)
    for o in range(n_z):
        zz = lax.rem(z + o, n_z)
        copy = remote(w_ref, my_block, w_s.at[o], w_r.at[c, z % 2], (2 * pair + cz, zz))
        if o == 0:
            pl.when(c != cz)(copy.start)
            pl.when(c == cz)(lambda: pltpu.make_async_copy(w_ref, my_block, loc.at[0]).start())
        else:
            copy.start()

    for i in range(2):
        for h in range(2):
            src = x_ref.at[i, pl.ds(h * half, half)]
            dst = xs.at[pl.ds(pl.multiple_of(z * rows + h * half, half), half)]
            zz = 2 * c + i
            mine = (h == c) & (zz == z)
            copy = remote(src, dst, x_s.at[i, h], x_r.at[z], (2 * pair + h, zz))
            pl.when(jnp.logical_not(mine))(copy.start)
            pl.when(mine)(lambda src=src, dst=dst: pltpu.make_async_copy(src, dst, loc.at[1]).start())

    seg_copy = remote(s_ref, sg.at[c], s_s, s_r, (2 * pair + 1 - c, z))
    seg_copy.start()
    own_seg = pltpu.make_async_copy(s_ref, sg.at[c], loc.at[2])
    own_seg.start()
    own_gain = pltpu.make_async_copy(g_ref, ga.at[me], loc.at[3])
    own_gain.start()

    def send_gain(o, carry):
        other = lax.rem(me + o, total)
        remote(g_ref, ga.at[me], g_s, g_r, (other // n_z, lax.rem(other, n_z))).start()
        return carry

    lax.fori_loop(1, total, send_gain, 0)

    first = jnp.where(c == cz, z % 2, 1 - c)
    for t in range(4):
        b = first if t < 2 else 1 - first
        core = t % 2
        blk = block_at(wq, shape, 2 * pair + core, b)
        mine = (core == c) & (2 * c + b == z)
        arrive = remote(w_ref, blk, w_s.at[0], w_r.at[core, b], (d, z))
        pl.when(jnp.logical_not(mine))(arrive.wait_recv)
        pl.when(mine)(lambda blk=blk: pltpu.make_async_copy(w_ref, blk, loc.at[0]).wait())
        for k in range(1, n_d):
            remote(blk, blk, d_s.at[k - 1, t], d_r.at[k - 1], (2 * (pair ^ k) + c, z)).start()

    for o in range(n_z):
        zs = lax.rem(z + o, n_z)
        src = xs.at[pl.ds(pl.multiple_of(zs * rows + c * half, half), half)]
        mine = (cz == c) & (zs == z)
        arrive = remote(src, src, x_s.at[0, 0], x_r.at[zs], (d, z))
        pl.when(jnp.logical_not(mine))(arrive.wait_recv)
        pl.when(mine)(lambda src=src: pltpu.make_async_copy(src, src, loc.at[1]).wait())
        remote(src, src, f_s.at[zs], f_r.at[zs], (2 * pair + 1 - c, z)).start()

    for o in range(n_z):
        copy = remote(w_ref, my_block, w_s.at[o], w_r.at[0, 0], (d, z))
        if o == 0:
            pl.when(c != cz)(copy.wait_send)
        else:
            copy.wait_send()
    for i in range(2):
        for h in range(2):
            src = x_ref.at[i, pl.ds(h * half, half)]
            mine = (h == c) & (2 * c + i == z)
            copy = remote(src, src, x_s.at[i, h], x_r.at[0], (d, z))
            pl.when(jnp.logical_not(mine))(copy.wait_send)
    for zs in range(n_z):
        src = xs.at[pl.ds(zs * rows, half)]
        copy = remote(src, src, f_s.at[zs], f_r.at[zs], (d, z))
        copy.wait_send()
        copy.wait_recv()
    seg_copy.wait_send()
    remote(s_ref, sg.at[1 - c], s_s, s_r, (d, z)).wait_recv()
    own_seg.wait()
    own_gain.wait()
    many = ga.at[pl.ds(0, total - 1)]
    gains = remote(many, many, g_s, g_r, (d, z))
    gains.wait_send()
    gains.wait_recv()
    blk = block_at(wq, shape, 0, 0)
    for k in range(1, n_d):
        for t in range(4):
            remote(blk, blk, d_s.at[k - 1, t], d_r.at[k - 1], (d, z)).wait_send()
        region = wq.at[pl.ds(0, 2 * shape[0])]
        remote(region, region, d_s.at[k - 1, 0], d_r.at[k - 1], (d, z)).wait_recv()


def gather_in(x_loc, w, gain_tile, seg_tile, n_dp, n_z):
    seqs, rows, width = x_loc.shape
    n_d = n_dp // 2
    total = n_dp * n_z
    return pl.pallas_call(
        functools.partial(gather_in_kernel, n_dp, n_z),
        in_specs=[VMEM_SPEC] * 4,
        out_specs=[ANY_SPEC] * 4,
        out_shape=[
            jax.ShapeDtypeStruct((rows * n_z, width), x_loc.dtype),
            jax.ShapeDtypeStruct((w.shape[0] * n_dp, 2 * w.shape[1]), w.dtype),
            jax.ShapeDtypeStruct((total,) + gain_tile.shape, gain_tile.dtype),
            jax.ShapeDtypeStruct((2,) + seg_tile.shape, seg_tile.dtype),
        ],
        scratch_shapes=[
            DMA((2, 2)), DMA((n_z,)), DMA((n_z,)), DMA((n_z,)), DMA((n_z,)), DMA((2, 2)),
            DMA((n_d - 1, 4)), DMA((n_d - 1,)), DMA, DMA, DMA, DMA, DMA((4,)),
        ],
        compiler_params=pltpu.CompilerParams(collective_id=1, has_side_effects=True),
        cost_estimate=pl.CostEstimate(flops=0, bytes_accessed=200_000_000, transcendentals=0),
        name="gather_in",
    )(x_loc, w, gain_tile, seg_tile)


def share_resid_kernel(n_z, part_ref, x_ref, out, got, buf, p_s, p_r, u_s, u_r, loc):
    d, z, pair, c = place()
    cz = z // 2
    full = x_ref.shape[0]
    half = full // 2
    unit = half // 2
    greet_line(n_z, d, z)
    mine = pl.ds(pl.multiple_of(c * half, half), half)
    theirs = pl.ds(pl.multiple_of((1 - c) * half, half), half)
    swap = remote(part_ref.at[theirs], got, p_s, p_r, (2 * pair + 1 - c, z))
    swap.start()
    swap.wait_recv()

    def add(r, carry):
        at = pl.ds(pl.multiple_of(r * 16, 16), 16)
        src = pl.ds(pl.multiple_of(c * half + r * 16, 16), 16)
        total = x_ref[src].astype(jnp.float32) + part_ref[src].astype(jnp.float32) + got[at].astype(jnp.float32)
        buf[at] = total.astype(jnp.bfloat16)
        return carry

    def spot(jl, h, k):
        return out.at[jl, pl.ds(pl.multiple_of(h * half + k * unit, unit), unit)]

    def sends(k, wait):
        src = buf.at[pl.ds(k * unit, unit)]
        dst = spot(z % 2, c, k)
        for o, zz in ((0, z), (1, z - 1), (2, z + 1)):
            copy = remote(src, dst, u_s.at[o, k], u_r.at[z % 2, c, k], (2 * pair + cz, zz))
            act = copy.wait_send if wait else copy.start
            if o == 0:
                keep = pltpu.make_async_copy(src, dst, loc.at[k])
                pl.when(c != cz)(act)
                pl.when(c == cz)(keep.wait if wait else keep.start)
            elif o == 1:
                pl.when(z > 0)(act)
            else:
                pl.when(z < n_z - 1)(act)

    per = unit // 16
    lax.fori_loop(0, per, add, 0)
    lax.fori_loop(per, per + per // 2, add, 0)
    sends(0, False)
    lax.fori_loop(per + per // 2, 2 * per, add, 0)
    swap.wait_send()
    sends(1, False)

    def relay(dist, sign, jl_wait):
        j = z + sign * dist
        ok = (j >= 2 * c) & (j <= 2 * c + 1)
        to = z - sign
        more = (to >= 0) & (to <= n_z - 1)
        jl = lax.rem(j + n_z, 2)

        @pl.when(ok)
        def _():
            for k in range(2):
                for h in range(2):
                    at = spot(jl, h, k)
                    copy = remote(at, at, u_s.at[3 + (0 if sign < 0 else 1), 4 * jl + 2 * h + k], u_r.at[jl, h, k], (2 * pair + c, to))
                    if jl_wait:
                        copy.wait_recv()
                        pl.when(more)(copy.start)
                    else:
                        pl.when(more)(copy.wait_send)

    order = [(dist, sign) for dist in range(1, n_z) for sign in (-1, 1)]
    for dist, sign in order:
        relay(dist, sign, True)
    @pl.when(c == cz)
    def _():
        for k in range(2):
            at = spot(z % 2, 1 - c, k)
            remote(at, at, u_s.at[0, 0], u_r.at[z % 2, 1 - c, k], (d, z)).wait_recv()
    for dist, sign in order:
        relay(dist, sign, False)
    sends(0, True)
    sends(1, True)


def share_resid(part, x, n_z):
    full, width = x.shape
    return pl.pallas_call(
        functools.partial(share_resid_kernel, n_z),
        in_specs=[VMEM_SPEC] * 2,
        out_specs=ANY_SPEC,
        out_shape=jax.ShapeDtypeStruct((2, full, width), jnp.bfloat16),
        scratch_shapes=[
            pltpu.VMEM((full // 2, width), jnp.bfloat16), pltpu.VMEM((full // 2, width), jnp.bfloat16),
            DMA, DMA, DMA((5, 8)), DMA((2, 2, 2)), DMA((2,)),
        ],
        compiler_params=pltpu.CompilerParams(collective_id=2, has_side_effects=True),
        cost_estimate=pl.CostEstimate(flops=0, bytes_accessed=200_000_000, transcendentals=0),
        name="share_resid",
    )(part, x)


CHUNKS = 8


def sum_line_kernel(n_z, part_ref, resid_all, cot_all, gain_ref, d_out, gain_out, got, buf, resid_ref, cot_ref,
                    s_s, s_r, p_s, p_r, loc, rows_sem):
    d, z, pair, c = place()
    cz = z // 2
    full, width = buf.shape
    rows = full // CHUNKS
    fetch = (
        pltpu.make_async_copy(resid_all.at[z % 2], resid_ref, rows_sem.at[0]),
        pltpu.make_async_copy(cot_all.at[z % 2], cot_ref, rows_sem.at[1]),
    )
    for one in fetch:
        one.start()
    greet_line(n_z, d, z)
    gain_out[...] = jnp.zeros_like(gain_out)
    own = c == cz
    steps = [(k, t) for k in range(CHUNKS) for t in range(2)]

    def where_is(k, t):
        jl = jnp.bitwise_xor(c, t)
        return jl, 2 * c + jl, pl.ds(k * rows, rows)

    def copy_on(k, t, side, src):
        jl, j, at = where_is(k, t)
        to = z + 1 if side == 0 else z - 1
        return remote(src, got.at[side, jl, at], s_s.at[t, k], s_r.at[side, jl, k], (2 * pair + c, to))

    def arrived(side, jl, k):
        at = got.at[side, jl, pl.ds(k * rows, rows)]
        return remote(at, at, s_s.at[0, 0], s_r.at[side, jl, k], (d, z))

    def add_in(side, jl, k):
        def one(r, carry):
            at = pl.ds(pl.multiple_of(k * rows + r * 16, 16), 16)
            got[side, jl, at] = (got[side, jl, at].astype(jnp.float32) + part_ref[jl, at].astype(jnp.float32)).astype(jnp.bfloat16)
            return carry
        lax.fori_loop(0, rows // 16, one, 0)

    def finish(jl, k):
        def one(r, carry):
            at = pl.ds(pl.multiple_of(k * rows + r * 16, 16), 16)
            total = part_ref[jl, at].astype(jnp.float32)
            left = got[0, jl, at].astype(jnp.float32)
            right = got[1, jl, at].astype(jnp.float32)
            total = total + jnp.where(z > 0, left, 0.0) + jnp.where(z < n_z - 1, right, 0.0)
            value = resid_ref[at].astype(jnp.float32)
            inverse = lax.rsqrt(jnp.mean(value * value, axis=-1, keepdims=True) + norm_eps)
            scaled = value * inverse
            d_scaled = total * gain_ref[...]
            mean = jnp.mean(d_scaled * scaled, axis=-1, keepdims=True)
            d_resid = cot_ref[at].astype(jnp.float32) + inverse * (d_scaled - scaled * mean)
            buf[at] = d_resid.astype(jnp.bfloat16)
            prod = total * scaled
            gain_out[...] = gain_out[...] + prod[:8] + prod[8:]
            return carry
        lax.fori_loop(0, rows // 16, one, 0)

    def to_partner(k):
        at = pl.ds(k * rows, rows)
        return remote(buf.at[at], d_out.at[at], p_s.at[k], p_r.at[k], (2 * pair + 1 - c, z))

    def keep(k):
        at = pl.ds(k * rows, rows)
        return pltpu.make_async_copy(buf.at[at], d_out.at[at], loc.at[k])

    def send_step(k, t, wait):
        jl, j, at = where_is(k, t)
        for side in range(2):
            going = (z < j) if side == 0 else (z > j)
            edge = (z == 0) if side == 0 else (z == n_z - 1)
            edge_copy = copy_on(k, t, side, part_ref.at[jl, at])
            inner_copy = copy_on(k, t, side, got.at[side, jl, at])
            pl.when(going & edge)(edge_copy.wait_send if wait else edge_copy.start)
            pl.when(going & jnp.logical_not(edge))(inner_copy.wait_send if wait else inner_copy.start)

    def publish(k, wait):
        @pl.when(own)
        def _():
            if wait:
                to_partner(k).wait_send()
                keep(k).wait()
            else:
                to_partner(k).start()
                keep(k).start()

    for n, (k, t) in enumerate(steps):
        jl, j, at = where_is(k, t)
        for side in range(2):
            going = (z < j) if side == 0 else (z > j)
            inner = (z > 0) if side == 0 else (z < n_z - 1)

            @pl.when(going & inner)
            def _():
                arrived(side, jl, k).wait_recv()
                add_in(side, jl, k)

        if n > 0:
            send_step(*steps[n - 1], False)
    send_step(*steps[-1], False)

    for one in fetch:
        one.wait()

    @pl.when(own)
    def _():
        jl = z % 2
        for k in range(CHUNKS):
            pl.when(z > 0)(arrived(0, jl, k).wait_recv)
            pl.when(z < n_z - 1)(arrived(1, jl, k).wait_recv)
            finish(jl, k)
            if k > 0:
                to_partner(k - 1).start()
                keep(k - 1).start()
        to_partner(CHUNKS - 1).start()
        keep(CHUNKS - 1).start()

    for k, t in steps:
        send_step(k, t, True)
    for k in range(CHUNKS):
        publish(k, True)
        at = d_out.at[pl.ds(k * rows, rows)]
        pl.when(jnp.logical_not(own))(remote(at, at, p_s.at[k], p_r.at[k], (d, z)).wait_recv)


def sum_line(part, resid, cot, gain, n_z):
    _, full, width = part.shape
    return pl.pallas_call(
        functools.partial(sum_line_kernel, n_z),
        in_specs=[VMEM_SPEC, ANY_SPEC, ANY_SPEC, VMEM_SPEC],
        out_specs=[ANY_SPEC, VMEM_SPEC],
        out_shape=[jax.ShapeDtypeStruct((full, width), jnp.bfloat16), jax.ShapeDtypeStruct((8, width), jnp.float32)],
        scratch_shapes=[
            pltpu.VMEM((2, 2, full, width), jnp.bfloat16), pltpu.VMEM((full, width), jnp.bfloat16),
            pltpu.VMEM((full, width), jnp.bfloat16), pltpu.VMEM((full, width), jnp.bfloat16),
            DMA((2, CHUNKS)), DMA((2, 2, CHUNKS)), DMA((CHUNKS,)), DMA((CHUNKS,)), DMA((CHUNKS,)), DMA((2,)),
        ],
        compiler_params=pltpu.CompilerParams(collective_id=3, has_side_effects=True, vmem_limit_bytes=56 * 1024 * 1024),
        cost_estimate=pl.CostEstimate(flops=0, bytes_accessed=200_000_000, transcendentals=0),
        name="sum_line",
    )(part, resid, cot, gain)


def gather_out_kernel(n_dp, n_z, w_ref, wo, w_s, w_r, d_s, d_r, loc):
    d, z, pair, c = place()
    n_d = n_dp // 2
    cz = z // 2
    shape = w_ref.shape
    greet_line(n_z, d, z, [(2 * (pair ^ k) + c, z) for k in range(1, n_d)])
    my_block = block_at(wo, shape, d, z % 2)
    for o in range(n_z):
        copy = remote(w_ref, my_block, w_s.at[o], w_r.at[c, z % 2], (2 * pair + cz, lax.rem(z + o, n_z)))
        if o == 0:
            pl.when(c != cz)(copy.start)
            pl.when(c == cz)(lambda: pltpu.make_async_copy(w_ref, my_block, loc).start())
        else:
            copy.start()
    first = jnp.where(c == cz, z % 2, 1 - c)
    for t in range(4):
        b = first if t < 2 else 1 - first
        core = t % 2
        blk = block_at(wo, shape, 2 * pair + core, b)
        mine = (core == c) & (2 * c + b == z)
        arrive = remote(w_ref, blk, w_s.at[0], w_r.at[core, b], (d, z))
        pl.when(jnp.logical_not(mine))(arrive.wait_recv)
        pl.when(mine)(lambda blk=blk: pltpu.make_async_copy(w_ref, blk, loc).wait())
        for k in range(1, n_d):
            remote(blk, blk, d_s.at[k - 1, t], d_r.at[k - 1], (2 * (pair ^ k) + c, z)).start()
    for o in range(n_z):
        copy = remote(w_ref, my_block, w_s.at[o], w_r.at[0, 0], (d, z))
        if o == 0:
            pl.when(c != cz)(copy.wait_send)
        else:
            copy.wait_send()
    blk = block_at(wo, shape, 0, 0)
    for k in range(1, n_d):
        for t in range(4):
            remote(blk, blk, d_s.at[k - 1, t], d_r.at[k - 1], (d, z)).wait_send()
        region = wo.at[pl.ds(0, 2 * shape[0])]
        remote(region, region, d_s.at[k - 1, 0], d_r.at[k - 1], (d, z)).wait_recv()


def gather_out(w, n_dp, n_z):
    n_d = n_dp // 2
    return pl.pallas_call(
        functools.partial(gather_out_kernel, n_dp, n_z),
        in_specs=[VMEM_SPEC],
        out_specs=ANY_SPEC,
        out_shape=jax.ShapeDtypeStruct((n_dp * w.shape[0], 2 * w.shape[1]), w.dtype),
        scratch_shapes=[DMA((n_z,)), DMA((2, 2)), DMA((n_d - 1, 4)), DMA((n_d - 1,)), DMA],
        compiler_params=pltpu.CompilerParams(collective_id=4, has_side_effects=True),
        cost_estimate=pl.CostEstimate(flops=0, bytes_accessed=100_000_000, transcendentals=0),
        name="gather_out",
    )(w)


def hand_out_kernel(n_dp, n_z, dn_ref, x_ref, dr_ref, gain_ref, gain2_ref, qt_ref, ot_ref,
                    ig, gq, go, gains, got, buf, q_got, q_own, q_put, q_fin, o_got, o_own, o_put, o_fin, g_src, g_all,
                    p_s, p_r, i_s, i_r, q_s, q_r, qf_s, qf_r, o_s, o_r, of_s, of_r, g_s, g_r, loc):
    d, z, pair, c = place()
    n_d = n_dp // 2
    total = n_dp * n_z
    me = d * n_z + z
    cz = z // 2
    full, width = x_ref.shape
    half = full // 2
    quarter = half // 2
    q_rows, q_cols = q_fin.shape[1:]
    o_rows, o_cols = o_fin.shape[1:]
    q_load = pltpu.make_async_copy(qt_ref.at[pl.ds(pl.multiple_of(pair * 2 * q_rows, 2 * q_rows), 2 * q_rows)], q_own, loc.at[0])
    o_load = pltpu.make_async_copy(ot_ref.at[pl.ds(pl.multiple_of(pair * 2 * o_rows, 2 * o_rows), 2 * o_rows)], o_own, loc.at[1])
    q_load.start()
    o_load.start()
    greet_all(n_dp, n_z, d, z)

    def q_send(k, b):
        other = pair ^ k
        src = qt_ref.at[pl.ds(pl.multiple_of(other * 2 * q_rows, 2 * q_rows), 2 * q_rows), pl.ds(b * q_cols, q_cols)]
        return remote(src, q_got.at[k - 1, :, pl.ds(b * q_cols, q_cols)], q_s.at[k - 1, b], q_r.at[k - 1, b], (2 * other + c, z))

    def o_send(k, b):
        other = pair ^ k
        src = ot_ref.at[pl.ds(pl.multiple_of(other * 2 * o_rows, 2 * o_rows), 2 * o_rows), pl.ds(b * o_cols, o_cols)]
        return remote(src, o_got.at[k - 1, :, pl.ds(b * o_cols, o_cols)], o_s.at[k - 1, b], o_r.at[k - 1, b], (2 * other + c, z))

    mine = pl.ds(pl.multiple_of(c * half, half), half)
    theirs = pl.ds(pl.multiple_of((1 - c) * half, half), half)
    swap = remote(dn_ref.at[theirs], got, p_s, p_r, (2 * pair + 1 - c, z))
    swap.start()
    for b in range(2):
        for k in range(1, n_d):
            o_send(k, b).start()
    for b in range(2):
        for k in range(1, n_d):
            q_send(k, b).start()

    g_src[pl.ds(0, 8)] = jnp.zeros((8, width), jnp.float32)
    g_src[pl.ds(8, 8)] = gain2_ref[...]
    swap.wait_recv()

    def rows_of(r, carry):
        at = pl.ds(pl.multiple_of(r * 16, 16), 16)
        src = pl.ds(pl.multiple_of(c * half + r * 16, 16), 16)
        d_normed = dn_ref[src].astype(jnp.float32) + got[at].astype(jnp.float32)
        value = x_ref[src].astype(jnp.float32)
        inverse = lax.rsqrt(jnp.mean(value * value, axis=-1, keepdims=True) + norm_eps)
        scaled = value * inverse
        d_scaled = d_normed * gain_ref[...]
        mean = jnp.mean(d_scaled * scaled, axis=-1, keepdims=True)
        out = dr_ref[src].astype(jnp.float32) + inverse * (d_scaled - scaled * mean)
        buf[at] = out.astype(jnp.bfloat16)
        prod = d_normed * scaled
        g_src[pl.ds(0, 8)] = g_src[pl.ds(0, 8)] + prod[:8] + prod[8:]
        return carry

    def row_send(b, wait):
        src = buf.at[pl.ds(b * quarter, quarter)]
        dst = ig.at[z % 2]
        zz = 2 * c + b
        here = (cz == c) & (zz == z)
        copy = remote(src, dst, i_s.at[b], i_r.at[z % 2], (2 * pair + cz, zz))
        keep = pltpu.make_async_copy(src, dst, loc.at[2])
        pl.when(jnp.logical_not(here))(copy.wait_send if wait else copy.start)
        pl.when(here)(keep.wait if wait else keep.start)

    per = quarter // 16
    lax.fori_loop(0, per, rows_of, 0)
    lax.fori_loop(per, per + per // 2, rows_of, 0)
    row_send(0, False)
    lax.fori_loop(per + per // 2, 2 * per, rows_of, 0)
    q_load.wait()
    o_load.wait()
    row_send(1, False)

    each = width // total

    def gain_tile(o):
        return g_src.at[:, pl.ds(pl.multiple_of(o * each // 128 * 128, 128), 128)]

    own_gain = pltpu.make_async_copy(gain_tile(me), g_all.at[me], loc.at[3])
    own_gain.start()

    def send_gain(o, carry):
        other = lax.rem(me + o, total)
        remote(gain_tile(other), g_all.at[me], g_s, g_r, (other // n_z, lax.rem(other, n_z))).start()
        return carry

    lax.fori_loop(1, total, send_gain, 0)

    def second(b, rows, own_ref, got_ref, put_ref, cut):
        for core in range(2):

            def add(r, carry):
                at = pl.ds(pl.multiple_of(r * 16, 16), 16)
                src, lanes = cut(core, b, r)
                value = own_ref[src, lanes].astype(jnp.float32)
                for k in range(n_d - 1):
                    value = value + got_ref[k, src, lanes].astype(jnp.float32)
                put_ref[core, b, at] = value.astype(jnp.bfloat16)
                return carry

            lax.fori_loop(0, rows // 16, add, 0)

    def second_send(b, put_ref, fin_ref, f_s, f_r, spare, wait):
        for core in range(2):
            here = (core == c) & (2 * c + b == z)
            src = put_ref.at[core, b]
            copy = remote(src, fin_ref.at[z], f_s.at[core, b], f_r.at[z], (2 * pair + core, 2 * c + b))
            keep = pltpu.make_async_copy(src, fin_ref.at[z], loc.at[spare])
            pl.when(jnp.logical_not(here))(copy.wait_send if wait else copy.start)
            pl.when(here)(keep.wait if wait else keep.start)

    def q_cut(core, b, r):
        return pl.ds(pl.multiple_of(core * q_rows + r * 16, 16), 16), pl.ds(b * q_cols, q_cols)

    def o_cut(core, b, r):
        return pl.ds(pl.multiple_of(core * o_rows + r * 16, 16), 16), pl.ds(b * o_cols, o_cols)

    def last(rows, fin_ref, out_ref):
        def add(r, carry):
            at = pl.ds(pl.multiple_of(r * 16, 16), 16)
            value = fin_ref[0, at].astype(jnp.float32)
            for zs in range(1, n_z):
                value = value + fin_ref[zs, at].astype(jnp.float32)
            out_ref[at] = value
            return carry

        lax.fori_loop(0, rows // 16, add, 0)

    o_args = (o_put, o_fin, of_s, of_r, 4)
    q_args = (q_put, q_fin, qf_s, qf_r, 5)
    for b in range(2):
        for k in range(1, n_d):
            o_send(k, b).wait_recv()
        second(b, o_rows, o_own, o_got, o_put, o_cut)
        if b:
            second_send(0, *o_args, False)
    for b in range(2):
        for k in range(1, n_d):
            q_send(k, b).wait_recv()
        second(b, q_rows, q_own, q_got, q_put, q_cut)
        if b:
            second_send(0, *q_args, False)
        else:
            second_send(1, *o_args, False)

    def arrived(fin_ref, f_s, f_r):
        for zs in range(n_z):
            at = fin_ref.at[zs]
            from_here = (cz == c) & (zs == z)
            pl.when(jnp.logical_not(from_here))(remote(at, at, f_s.at[0, 0], f_r.at[zs], (d, z)).wait_recv)

    def own_done(args):
        for b in range(2):
            second_send(b, *args, True)

    own_done(o_args)
    arrived(o_fin, of_s, of_r)
    value = o_fin[0].astype(jnp.float32)
    for zs in range(1, n_z):
        value = value + o_fin[zs].astype(jnp.float32)
    go[...] = value.T
    second_send(1, *q_args, False)
    own_done(q_args)
    arrived(q_fin, qf_s, qf_r)
    last(q_rows, q_fin, gq)

    many = g_all.at[pl.ds(0, total - 1)]
    gain_copy = remote(many, many, g_s, g_r, (d, z))
    gain_copy.wait_send()
    gain_copy.wait_recv()
    own_gain.wait()
    gains[...] = jnp.zeros_like(gains)

    def add_gain(o, carry):
        gains[...] = gains[...] + g_all[o]
        return carry

    lax.fori_loop(0, total, add_gain, 0)

    swap.wait_send()
    for b in range(2):
        row_send(b, True)
        for k in range(1, n_d):
            o_send(k, b).wait_send()
            q_send(k, b).wait_send()
    for i in range(2):
        from_here = (cz == c) & (2 * c + i == z)
        at = ig.at[i]
        pl.when(jnp.logical_not(from_here))(remote(at, at, i_s.at[0], i_r.at[i], (d, z)).wait_recv)


def hand_out(dn, x, dr, gain, gain2, qt, ot, n_dp, n_z):
    full, width = x.shape
    n_d = n_dp // 2
    total = n_dp * n_z
    q_rows, q_cols = qt.shape[0] // n_dp, qt.shape[1] // 2
    o_rows, o_cols = ot.shape[0] // n_dp, ot.shape[1] // 2
    b16 = jnp.bfloat16
    return pl.pallas_call(
        functools.partial(hand_out_kernel, n_dp, n_z),
        in_specs=[VMEM_SPEC] * 5 + [ANY_SPEC] * 2,
        out_specs=[ANY_SPEC] + [VMEM_SPEC] * 3,
        out_shape=[
            jax.ShapeDtypeStruct((2, full // 4, width), b16),
            jax.ShapeDtypeStruct((q_rows, q_cols), jnp.float32),
            jax.ShapeDtypeStruct((o_cols, o_rows), jnp.float32),
            jax.ShapeDtypeStruct((16, 128), jnp.float32),
        ],
        scratch_shapes=[
            pltpu.VMEM((full // 2, width), b16), pltpu.VMEM((full // 2, width), b16),
            pltpu.VMEM((n_d - 1, 2 * q_rows, 2 * q_cols), b16), pltpu.VMEM((2 * q_rows, 2 * q_cols), b16),
            pltpu.VMEM((2, 2, q_rows, q_cols), b16), pltpu.VMEM((n_z, q_rows, q_cols), b16),
            pltpu.VMEM((n_d - 1, 2 * o_rows, 2 * o_cols), b16), pltpu.VMEM((2 * o_rows, 2 * o_cols), b16),
            pltpu.VMEM((2, 2, o_rows, o_cols), b16), pltpu.VMEM((n_z, o_rows, o_cols), b16),
            pltpu.VMEM((16, width), jnp.float32), pltpu.VMEM((total, 16, 128), jnp.float32),
            DMA, DMA, DMA((2,)), DMA((2,)), DMA((n_d - 1, 2)), DMA((n_d - 1, 2)), DMA((2, 2)), DMA((n_z,)),
            DMA((n_d - 1, 2)), DMA((n_d - 1, 2)), DMA((2, 2)), DMA((n_z,)), DMA, DMA, DMA((6,)),
        ],
        compiler_params=pltpu.CompilerParams(collective_id=5, has_side_effects=True, vmem_limit_bytes=56 * 1024 * 1024),
        cost_estimate=pl.CostEstimate(flops=0, bytes_accessed=300_000_000, transcendentals=0),
        name="hand_out",
    )(dn, x, dr, gain, gain2, qt, ot)


def rms_forward(values, gain_wide):
    inverse = lax.rsqrt(jnp.mean(values * values, axis=-1, keepdims=True) + norm_eps)
    scaled = values * inverse
    return (scaled, inverse, (scaled * gain_wide).astype(jnp.bfloat16))


def rms_backward(d_normed, scaled, inverse, gain_wide):
    d_scaled = d_normed * gain_wide
    d_values = inverse * (d_scaled - scaled * jnp.mean(d_scaled * scaled, axis=-1, keepdims=True))
    return (d_values, jnp.sum(d_normed * scaled, axis=0))


def adam_update(weight, grad, first, second):
    new_first = beta_one * first + (1.0 - beta_one) * grad
    new_second = beta_two * second + (1.0 - beta_two) * grad * grad
    first_hat = new_first / (1.0 - beta_one**step_count)
    second_hat = new_second / (1.0 - beta_two**step_count)
    new_weight = weight - learn_rate * (
        first_hat / (jnp.sqrt(second_hat) + adam_eps) + weight_decay * weight
    )
    return (new_weight, new_first, new_second)


def contract_rows(left, right):
    return lax.dot_general(
        left, right, (((0,), (0,)), ((), ())), preferred_element_type=jnp.float32
    )


def times_transpose(left, right):
    return lax.dot_general(
        left, right, (((1,), (1,)), ((), ())), preferred_element_type=jnp.float32
    )


def per_device(
    block_input,
    segment_ids,
    cotangent,
    attn_gain,
    qkv_weight,
    out_weight,
    mlp_gain,
    gate_up_weight,
    down_weight,
    first_attn_gain,
    first_qkv,
    first_out,
    first_mlp_gain,
    first_gate_up,
    first_down,
    second_attn_gain,
    second_qkv,
    second_out,
    second_mlp_gain,
    second_gate_up,
    second_down,
):
    seqs_here, local_len, width = block_input.shape
    full_len = segment_ids.shape[1]
    n_dp = lax.axis_size("dp")
    n_z = lax.axis_size("seq")
    groups = HEADS // KV_HEADS
    unit_count = down_weight.shape[0]
    z_here = lax.axis_index("seq")
    owned = attn_gain.shape[0]
    gain_line = jnp.concatenate([attn_gain, mlp_gain]).astype(jnp.bfloat16).astype(jnp.float32)
    gain_tile = jnp.pad(gain_line[None], ((0, 7), (0, LANES - 2 * owned)))
    seg_tile = jnp.pad(segment_ids, ((0, 8 - seqs_here), (0, 0)))
    gate_up_cols = lax.all_gather(
        gate_up_weight.astype(jnp.bfloat16).reshape(-1, 2 * unit_count), "dp", axis=0, tiled=True
    )
    down_rows = lax.all_gather(down_weight.astype(jnp.bfloat16), "dp", axis=1, tiled=True)
    cot_all = lax.all_gather(cotangent, "seq", axis=1, tiled=True)
    rows_in, qkv_cols, gain_all, seg_all = gather_in(
        block_input, qkv_weight.astype(jnp.bfloat16), gain_tile, seg_tile, n_dp, n_z
    )
    gain_one = gain_all[:, 0, :owned].reshape(1, width)
    gain_two = gain_all[:, 0, owned : 2 * owned].reshape(1, width)
    seg_here = lax.dynamic_slice(seg_all, (z_here // 2, z_here % 2, 0), (1, 1, full_len))[0]
    tables = attn_tables(seg_here)
    scaled_one, inverse_one, normed_one = rms_forward(rows_in.astype(jnp.float32), gain_one)
    qkv = jnp.dot(normed_one, qkv_cols, preferred_element_type=jnp.float32)
    turned, lse, attended16 = attn_forward(qkv, *tables, full_len, groups)
    out_rows = gather_out(out_weight.astype(jnp.bfloat16).T, n_dp, n_z)
    attn_part = times_transpose(attended16, out_rows)
    resid_all = share_resid(attn_part.astype(jnp.bfloat16), rows_in, n_z)
    total_rows = seqs_here * full_len
    resid = resid_all.reshape(total_rows, width).astype(jnp.float32)
    scaled_two, inverse_two, normed_two = rms_forward(resid, gain_two)
    gate_up = jnp.dot(normed_two, gate_up_cols, preferred_element_type=jnp.float32)
    gate_part = gate_up[:, :unit_count]
    up_part = gate_up[:, unit_count:]
    sigmoid_gate = jax.nn.sigmoid(gate_part)
    active = gate_part * sigmoid_gate
    hidden16 = (active * up_part).astype(jnp.bfloat16)
    cot_rows = cot_all.reshape(total_rows, width)
    d_hidden = times_transpose(cot_rows, down_rows)
    d_gate = d_hidden * up_part * sigmoid_gate * (1.0 + gate_part * (1.0 - sigmoid_gate))
    d_up = d_hidden * active
    d_gate_up16 = jnp.concatenate([d_gate, d_up], 1).astype(jnp.bfloat16)
    down_term = contract_rows(cot_rows, hidden16)
    down_sum = lax.psum_scatter(
        down_term.astype(jnp.bfloat16), "dp", scatter_dimension=0, tiled=True
    ).astype(jnp.float32)
    grad_down = down_sum.T
    d_normed_two = times_transpose(d_gate_up16, gate_up_cols).astype(jnp.bfloat16)
    d_resid16, gain_two_part = sum_line(
        d_normed_two.reshape(resid_all.shape), resid_all, cot_all, gain_two, n_z
    )
    gate_up_term = contract_rows(normed_two, d_gate_up16)
    grad_gate_up = (
        lax.psum_scatter(gate_up_term.astype(jnp.bfloat16), "dp", scatter_dimension=0, tiled=True)
        .reshape(gate_up_weight.shape)
        .astype(jnp.float32)
    )
    down_part = jnp.dot(hidden16, down_rows, preferred_element_type=jnp.float32)
    down_here = lax.psum_scatter(
        down_part.astype(jnp.bfloat16).reshape(resid_all.shape), "seq", scatter_dimension=1, tiled=True
    ).astype(jnp.float32)
    resid_here = lax.dynamic_slice_in_dim(resid_all, z_here * local_len, local_len, 1)
    output = (resid_here.astype(jnp.float32) + down_here).astype(jnp.bfloat16)
    d_attended = jnp.dot(d_resid16, out_rows, preferred_element_type=jnp.float32).astype(jnp.bfloat16)
    d_qkv16 = attn_backward(turned, d_attended, lse, *tables, full_len, groups)
    d_normed_one = times_transpose(d_qkv16, qkv_cols).astype(jnp.bfloat16)
    qkv_term = contract_rows(normed_one, d_qkv16).astype(jnp.bfloat16)
    out_term = contract_rows(d_resid16, attended16).astype(jnp.bfloat16)
    input_grad, grad_qkv, grad_out, gain_sums = hand_out(
        d_normed_one, rows_in, d_resid16, gain_one, gain_two_part, qkv_term, out_term, n_dp, n_z
    )
    flat = lax.axis_index("dp") * n_z + z_here
    gain_sums = lax.dynamic_slice(
        jnp.sum(gain_sums.reshape(2, 8, LANES), axis=1), (0, flat * owned % LANES), (2, owned)
    )
    grad_gain_one = gain_sums[0]
    grad_gain_two = gain_sums[1]
    w_one, m_one, v_one = adam_update(attn_gain, grad_gain_one, first_attn_gain, second_attn_gain)
    w_qkv, m_qkv, v_qkv = adam_update(qkv_weight, grad_qkv, first_qkv, second_qkv)
    w_out, m_out, v_out = adam_update(out_weight, grad_out, first_out, second_out)
    w_two, m_two, v_two = adam_update(mlp_gain, grad_gain_two, first_mlp_gain, second_mlp_gain)
    w_gu, m_gu, v_gu = adam_update(gate_up_weight, grad_gate_up, first_gate_up, second_gate_up)
    w_down, m_down, v_down = adam_update(down_weight, grad_down, first_down, second_down)
    return (
        output,
        input_grad,
        grad_gain_one,
        grad_qkv,
        grad_out,
        grad_gain_two,
        grad_gate_up,
        grad_down,
        w_one,
        w_qkv,
        w_out,
        w_two,
        w_gu,
        w_down,
        m_one,
        m_qkv,
        m_out,
        m_two,
        m_gu,
        m_down,
        v_one,
        v_qkv,
        v_out,
        v_two,
        v_gu,
        v_down,
    )


def solution(mesh):
    in_specs = (
        P("dp", "seq", None),
        P("dp", None),
        P("dp", "seq", None),
        P(("dp", "seq")),
        P("dp", "seq"),
        P("seq", "dp"),
        P(("dp", "seq")),
        P("dp", None, "seq"),
        P("seq", "dp"),
        P(("dp", "seq")),
        P("dp", "seq"),
        P("seq", "dp"),
        P(("dp", "seq")),
        P("dp", None, "seq"),
        P("seq", "dp"),
        P(("dp", "seq")),
        P("dp", "seq"),
        P("seq", "dp"),
        P(("dp", "seq")),
        P("dp", None, "seq"),
        P("seq", "dp"),
    )
    out_specs = (
        P("dp", "seq", None),
        P("dp", "seq", None),
        P(("dp", "seq")),
        P("dp", "seq"),
        P("seq", "dp"),
        P(("dp", "seq")),
        P("dp", None, "seq"),
        P("seq", "dp"),
        P(("dp", "seq")),
        P("dp", "seq"),
        P("seq", "dp"),
        P(("dp", "seq")),
        P("dp", None, "seq"),
        P("seq", "dp"),
        P(("dp", "seq")),
        P("dp", "seq"),
        P("seq", "dp"),
        P(("dp", "seq")),
        P("dp", None, "seq"),
        P("seq", "dp"),
        P(("dp", "seq")),
        P("dp", "seq"),
        P("seq", "dp"),
        P(("dp", "seq")),
        P("dp", None, "seq"),
        P("seq", "dp"),
    )
    return jax.shard_map(
        per_device, mesh=mesh, in_specs=in_specs, out_specs=out_specs, check_vma=False
    )
```

```python
import functools

import jax
import jax.numpy as jnp
from jax import lax
from jax.experimental import pallas as pl
from jax.experimental.pallas import tpu as pltpu
from jax.sharding import PartitionSpec as P


HEADS = 32
KV_HEADS = 8
norm_eps = 1e-05
beta_one = 0.9
beta_two = 0.95
learn_rate = 0.01
weight_decay = 0.1
adam_eps = 1e-08
step_count = 10.0
masked_score = -1e30


HEAD_DIM = 64
LANES = 128


def dot_t(a, b):
    return lax.dot_general(a, b, (((1,), (1,)), ((), ())), preferred_element_type=jnp.float32)


def dot_n(a, b):
    return lax.dot_general(a, b, (((1,), (0,)), ((), ())), preferred_element_type=jnp.float32)


def dot_c(a, b):
    return lax.dot_general(a, b, (((0,), (0,)), ((), ())), preferred_element_type=jnp.float32)


def swap_halves(u):
    lane = lax.broadcasted_iota(jnp.int32, u.shape, 1)
    return jnp.where(lane % 64 < 32, pltpu.roll(u, 96, 1), pltpu.roll(u, 32, 1))


def turn(u, cos_wide, sin_wide):
    return u * cos_wide + swap_halves(u) * sin_wide


def key_start(block, q_rows, reach):
    return max(0, (block * q_rows - reach + 1) // q_rows * q_rows)


def attn_forward_kernel(pairs, q_rows, reach, qkv_ref, cos_ref, sin_ref, seg_col_ref, seg_row_ref,
                        turned_ref, lse_ref, out_ref):
    full_len = qkv_ref.shape[0]
    lane = lax.broadcasted_iota(jnp.int32, (full_len, LANES), 1)
    low = lane < HEAD_DIM
    cos_q = cos_ref[...]
    sin_q = sin_ref[...]
    kv = qkv_ref[:, pairs * LANES:].astype(jnp.float32)
    kv16 = turn(kv, jnp.where(low, cos_q, 1.0), jnp.where(low, sin_q, 0.0)).astype(jnp.bfloat16)
    turned_ref[:, pairs * LANES:] = kv16
    kv32 = kv16.astype(jnp.float32)
    rolled = pltpu.roll(kv32, HEAD_DIM, 1)
    zero = jnp.zeros_like(kv32)
    keys = (jnp.where(low, kv32, zero).astype(jnp.bfloat16), jnp.where(low, zero, rolled).astype(jnp.bfloat16))
    vals = (jnp.where(low, rolled, zero).astype(jnp.bfloat16), jnp.where(low, zero, kv32).astype(jnp.bfloat16))
    for pair in range(pairs):
        cols = slice(pair * LANES, (pair + 1) * LANES)
        query = turn(qkv_ref[:, cols].astype(jnp.float32), cos_q, sin_q) .astype(jnp.bfloat16)
        turned_ref[:, cols] = query
    for block in range(full_len // q_rows):
        first = key_start(block, q_rows, reach)
        last = (block + 1) * q_rows
        rows = slice(block * q_rows, last)
        span = slice(first, last)
        i = lax.broadcasted_iota(jnp.int32, (q_rows, last - first), 0) + block * q_rows
        j = lax.broadcasted_iota(jnp.int32, (q_rows, last - first), 1) + first
        allowed = (j <= i) & (seg_col_ref[rows, :1] == seg_row_ref[:1, span])
        for pair in range(pairs):
            cols = slice(pair * LANES, (pair + 1) * LANES)
            query = turned_ref[rows, cols]
            total = None
            for half in range(2):
                scores = dot_t(query, keys[half][span]) * (HEAD_DIM ** -0.5)
                scores = jnp.where(allowed, scores, masked_score)
                top = jnp.max(scores, axis=1, keepdims=True)
                lse = top + jnp.log(jnp.sum(jnp.exp(scores - top), axis=1, keepdims=True))
                probs = jnp.exp(scores - lse).astype(jnp.bfloat16)
                part = dot_n(probs, vals[half][span])
                total = part if total is None else total + part
                head = 2 * pair + half
                lse_ref[rows, head:head + 1] = lse
            out_ref[rows, cols] = total.astype(jnp.bfloat16)


def attn_backward_kernel(pairs, q_rows, reach, turned_ref, d_out_ref, lse_ref, cos_ref, sin_ref, seg_col_ref,
                         seg_row_ref, grad_ref, dk_ref, dv_ref):
    full_len = turned_ref.shape[0]
    lane = lax.broadcasted_iota(jnp.int32, (full_len, LANES), 1)
    low = lane < HEAD_DIM
    kv32 = turned_ref[:, pairs * LANES:].astype(jnp.float32)
    rolled = pltpu.roll(kv32, HEAD_DIM, 1)
    zero = jnp.zeros_like(kv32)
    keys = (jnp.where(low, kv32, zero).astype(jnp.bfloat16), jnp.where(low, zero, rolled).astype(jnp.bfloat16))
    vals = (jnp.where(low, rolled, zero).astype(jnp.bfloat16), jnp.where(low, zero, kv32).astype(jnp.bfloat16))
    dk_ref[...] = jnp.zeros_like(dk_ref)
    dv_ref[...] = jnp.zeros_like(dv_ref)
    low_rows = low[:q_rows]
    scale = HEAD_DIM ** -0.5
    for block in range(full_len // q_rows):
        first = key_start(block, q_rows, reach)
        last = (block + 1) * q_rows
        rows = slice(block * q_rows, last)
        span = slice(first, last)
        i = lax.broadcasted_iota(jnp.int32, (q_rows, last - first), 0) + block * q_rows
        j = lax.broadcasted_iota(jnp.int32, (q_rows, last - first), 1) + first
        allowed = (j <= i) & (seg_col_ref[rows, :1] == seg_row_ref[:1, span])
        cos_q = cos_ref[rows]
        sin_q = sin_ref[rows]
        for pair in range(pairs):
            cols = slice(pair * LANES, (pair + 1) * LANES)
            query = turned_ref[rows, cols]
            d_out = d_out_ref[rows, cols]
            q32 = query.astype(jnp.float32)
            o32 = d_out.astype(jnp.float32)
            d_query = None
            d_key = None
            d_val = None
            for half in range(2):
                keep = low_rows if half == 0 else ~low_rows
                q_only = jnp.where(keep, q32, 0.0).astype(jnp.bfloat16)
                o_only = jnp.where(keep, o32, 0.0).astype(jnp.bfloat16)
                head = 2 * pair + half
                scores = dot_t(query, keys[half][span]) * scale
                scores = jnp.where(allowed, scores, masked_score)
                probs = jnp.exp(scores - lse_ref[rows, head:head + 1])
                d_probs = dot_t(d_out, vals[half][span])
                delta = jnp.sum(probs * d_probs, axis=1, keepdims=True)
                d_scores = (probs * (d_probs - delta) * scale).astype(jnp.bfloat16)
                probs16 = probs.astype(jnp.bfloat16)
                dq = dot_n(d_scores, keys[half][span])
                dk = dot_c(d_scores, q_only)
                dv = dot_c(probs16, o_only)
                d_query = dq if d_query is None else d_query + dq
                d_key = dk if d_key is None else d_key + dk
                d_val = dv if d_val is None else d_val + dv
            dk_ref[span] = dk_ref[span] + d_key
            dv_ref[span] = dv_ref[span] + d_val
            grad_ref[rows, cols] = turn(d_query, cos_q, -sin_q).astype(jnp.bfloat16)
    d_key = dk_ref[...]
    d_val = dv_ref[...]
    d_key = d_key + pltpu.roll(d_key, HEAD_DIM, 1)
    d_val = d_val + pltpu.roll(d_val, HEAD_DIM, 1)
    d_key = turn(d_key, cos_ref[...], -sin_ref[...])
    grad_ref[:, pairs * LANES:] = jnp.where(low, d_key, d_val).astype(jnp.bfloat16)


def attn_specs(full_len, width):
    line = pl.BlockSpec((full_len, width), lambda s, g: (s, g))
    table = pl.BlockSpec((full_len, LANES), lambda s, g: (s, 0))
    row = pl.BlockSpec((8, full_len), lambda s, g: (s, 0))
    return line, table, row


Q_ROWS = 128
REACH = 256


def attn_gather_kernel(n_dp, pairs, q_rows, reach, qkv_ref, cos_ref, sin_ref, seg_col_ref, seg_row_ref, vo_ref,
                       turned_ref, lse_ref, out_ref, wo, d_s, d_r, loc):
    _, z, pair, c = place()
    n_d = n_dp // 2
    step = pl.program_id(1)
    steps = pl.num_programs(1)
    rows = vo_ref.shape[0]
    parts = 2
    part = rows // parts // 2

    def spot(owner, t, h):
        return wo.at[pl.ds(pl.multiple_of(owner * rows + (2 * t + h) * part, part), part)]

    spread = Spread(n_d, pair, c, z, parts, spot, d_s, d_r)
    keep = pltpu.make_async_copy(vo_ref, wo.at[pl.ds(pl.multiple_of(pair * rows, rows), rows)], loc)

    @pl.when(step == 0)
    def _():
        keep.start()
        barrier = pltpu.get_barrier_semaphore()
        for k in range(1, n_d):
            pl.semaphore_signal(barrier, inc=1, device_id=(2 * (pair ^ k) + c, z), device_id_type=MESH)
        pl.semaphore_wait(barrier, n_d - 1)
        keep.wait()
        for t in range(parts):
            spread.own(t)

    attn_forward_kernel(pairs, q_rows, reach, qkv_ref, cos_ref, sin_ref, seg_col_ref, seg_row_ref, turned_ref, lse_ref, out_ref)

    @pl.when(step == steps - 2)
    def _():
        spread.pass_on(0)

    @pl.when(step == steps - 1)
    def _():
        spread.pass_on(1)
        spread.finish()


def attn_forward(qkv, cos, sin, seg_col, seg_row, vo, full_len, groups, n_dp):
    pairs = groups // 2
    width = (groups + 2) * HEAD_DIM
    seqs = qkv.shape[0] // full_len
    kv = qkv.shape[1] // width
    n_d = n_dp // 2
    line, table, row = attn_specs(full_len, width)
    outw = pl.BlockSpec((full_len, groups * HEAD_DIM), lambda s, g: (s, g))
    rows = seqs * full_len
    return pl.pallas_call(
        functools.partial(attn_gather_kernel, n_dp, pairs, Q_ROWS, REACH),
        grid=(seqs, kv),
        in_specs=[line, table, table, table, row, VMEM_SPEC],
        out_specs=[line, pl.BlockSpec((full_len, LANES), lambda s, g: (s, g)), outw, ANY_SPEC],
        out_shape=[
            jax.ShapeDtypeStruct((rows, kv * width), jnp.bfloat16),
            jax.ShapeDtypeStruct((rows, kv * LANES), jnp.float32),
            jax.ShapeDtypeStruct((rows, kv * groups * HEAD_DIM), jnp.bfloat16),
            jax.ShapeDtypeStruct((n_d * vo.shape[0], vo.shape[1]), jnp.bfloat16),
        ],
        scratch_shapes=[DMA((n_d - 1, 2, 2)), DMA((n_d - 1, 2, 2)), DMA],
        compiler_params=pltpu.CompilerParams(collective_id=4, has_side_effects=True),
        cost_estimate=pl.CostEstimate(flops=4 * rows * full_len * kv * LANES * groups, bytes_accessed=150_000_000, transcendentals=0),
        name="attn_forward",
    )(qkv, cos, sin, seg_col, seg_row, vo)


def attn_backward(turned, d_out, lse, cos, sin, seg_col, seg_row, full_len, groups):
    pairs = groups // 2
    width = (groups + 2) * HEAD_DIM
    seqs = turned.shape[0] // full_len
    kv = turned.shape[1] // width
    line, table, row = attn_specs(full_len, width)
    outw = pl.BlockSpec((full_len, groups * HEAD_DIM), lambda s, g: (s, g))
    rows = seqs * full_len
    return pl.pallas_call(
        functools.partial(attn_backward_kernel, pairs, Q_ROWS, REACH),
        grid=(seqs, kv),
        in_specs=[line, outw, pl.BlockSpec((full_len, LANES), lambda s, g: (s, g)), table, table, table, row],
        out_specs=line,
        out_shape=jax.ShapeDtypeStruct((rows, kv * width), jnp.bfloat16),
        scratch_shapes=[pltpu.VMEM((full_len, LANES), jnp.float32)] * 2,
        cost_estimate=pl.CostEstimate(flops=10 * rows * full_len * kv * LANES * groups, bytes_accessed=rows * kv * width * 6, transcendentals=0),
        name="attn_backward",
    )(turned, d_out, lse, cos, sin, seg_col, seg_row)


def attn_tables(segment_ids):
    seqs, full_len = segment_ids.shape
    earlier = (segment_ids[..., None, :] < segment_ids[..., :, None]).astype(jnp.int32)
    positions = jnp.arange(full_len, dtype=jnp.int32) - jnp.sum(earlier, axis=-1, dtype=jnp.int32)
    inverse = 500000.0 ** (-2.0 * jnp.arange(HEAD_DIM // 2, dtype=jnp.float32) / HEAD_DIM)
    angles = positions.astype(jnp.float32)[..., None] * inverse
    cos = jnp.cos(angles)
    sin = jnp.sin(angles)
    cos = jnp.concatenate([cos] * 4, -1).reshape(seqs * full_len, LANES)
    sin = jnp.concatenate([-sin, sin] * 2, -1).reshape(seqs * full_len, LANES)
    seg_col = jnp.broadcast_to(segment_ids[:, :, None], (seqs, full_len, LANES)).reshape(seqs * full_len, LANES)
    seg_row = jnp.broadcast_to(segment_ids[:, None, :], (seqs, 8, full_len)).reshape(seqs * 8, full_len)
    return cos, sin, seg_col, seg_row


MESH = pl.DeviceIdType.MESH
VMEM_SPEC = pl.BlockSpec(memory_space=pltpu.VMEM)
ANY_SPEC = pl.BlockSpec(memory_space=pl.ANY)
DMA = pltpu.SemaphoreType.DMA


def place():
    d = lax.axis_index("dp")
    z = lax.axis_index("seq")
    return d, z, d // 2, d % 2


def remote(src, dst, send, recv, dev):
    return pltpu.make_async_remote_copy(
        src_ref=src, dst_ref=dst, send_sem=send, recv_sem=recv, device_id=dev, device_id_type=MESH
    )


def greet_all(n_dp, n_z, d, z):
    barrier = pltpu.get_barrier_semaphore()
    me = d * n_z + z

    def one(o, carry):
        other = lax.rem(me + o, n_dp * n_z)
        pl.semaphore_signal(barrier, inc=1, device_id=(other // n_z, lax.rem(other, n_z)), device_id_type=MESH)
        return carry

    lax.fori_loop(1, n_dp * n_z, one, 0)
    pl.semaphore_wait(barrier, n_dp * n_z - 1)


def greet_line(n_z, d, z, extra=()):
    barrier = pltpu.get_barrier_semaphore()
    c = d % 2
    for o in range(n_z):
        zz = lax.rem(z + o, n_z)
        for core in range(2):
            if o == 0 and core == 0:
                continue
            pl.semaphore_signal(barrier, inc=1, device_id=(d - c + lax.rem(c + core, 2), zz), device_id_type=MESH)
    for dev in extra:
        pl.semaphore_signal(barrier, inc=1, device_id=dev, device_id_type=MESH)
    pl.semaphore_wait(barrier, 2 * n_z - 1 + len(extra))


def block_at(ref, shape, row, col):
    return ref.at[pl.ds(pl.multiple_of(row * shape[0], shape[0]), shape[0]),
                  pl.ds(pl.multiple_of(col * shape[1], shape[1]), shape[1])]


class Spread:
    def __init__(self, n_d, pair, c, z, parts, spot, send, recv):
        self.n_d, self.pair, self.parts, self.spot = n_d, pair, parts, spot
        self.send, self.recv = send, recv
        self.dev = lambda k: (2 * (pair ^ k) + c, z)

    def copy(self, slot, owner, t, h, to):
        at = self.spot(owner, t, h)
        return remote(at, at, self.send.at[slot, t, h], self.recv.at[slot, t, h], self.dev(to))

    def own(self, t):
        if self.n_d == 4:
            for h in range(2):
                self.copy(0, self.pair, t, h, 1).start()
                self.copy(1, self.pair, t, 1 - h, 2).start()
        else:
            for k in range(1, self.n_d):
                for h in range(2):
                    self.copy(k - 1, self.pair, t, h, k).start()

    def pass_on(self, t):
        if self.n_d == 4:
            self.copy(0, self.pair ^ 1, t, 0, 1).wait_recv()
            self.copy(2, self.pair ^ 1, t, 0, 2).start()
            self.copy(1, self.pair ^ 2, t, 1, 2).wait_recv()
            self.copy(2, self.pair ^ 2, t, 1, 1).start()

    def finish(self):
        for t in range(self.parts):
            if self.n_d == 4:
                self.copy(0, self.pair ^ 1, t, 1, 1).wait_recv()
                self.copy(1, self.pair ^ 2, t, 0, 2).wait_recv()
                for h in range(2):
                    self.copy(2, self.pair ^ 3, t, h, 1).wait_recv()
                    for slot in range(3):
                        self.copy(slot, self.pair, t, h, 1).wait_send()
            else:
                for k in range(1, self.n_d):
                    for h in range(2):
                        self.copy(k - 1, self.pair ^ k, t, h, k).wait_recv()
                        self.copy(k - 1, self.pair, t, h, k).wait_send()


def gather_in_kernel(n_dp, n_z, x_ref, w_ref, v_ref, g_ref, s_ref, xs, wq, vo, ga, sg,
                     x_s, x_r, f_s, f_r, w_s, w_r, v_s, v_r, d_s, d_r, g_s, g_r, s_s, s_r, loc):
    d, z, pair, c = place()
    n_d = n_dp // 2
    me = d * n_z + z
    total = n_dp * n_z
    rows = x_ref.shape[1]
    half = rows // 2
    shape = w_ref.shape
    cz = z // 2
    greet_all(n_dp, n_z, d, z)

    def line_stage(src, dst, send, recv, spare, wait):
        for o in range(n_z):
            copy = remote(src, dst, send.at[o], recv.at[c, z % 2], (2 * pair + cz, lax.rem(z + o, n_z)))
            act = copy.wait_send if wait else copy.start
            if o == 0:
                pl.when(c != cz)(act)
                if not wait:
                    pl.when(c == cz)(pltpu.make_async_copy(src, dst, loc.at[spare]).start)
            else:
                act()

    my_block = block_at(wq, shape, d, z % 2)
    line_stage(w_ref, my_block, w_s, w_r, 0, False)

    for i in range(2):
        for h in range(2):
            src = x_ref.at[i, pl.ds(h * half, half)]
            dst = xs.at[pl.ds(pl.multiple_of(z * rows + h * half, half), half)]
            zz = 2 * c + i
            mine = (h == c) & (zz == z)
            copy = remote(src, dst, x_s.at[i, h], x_r.at[z], (2 * pair + h, zz))
            pl.when(jnp.logical_not(mine))(copy.start)
            pl.when(mine)(lambda src=src, dst=dst: pltpu.make_async_copy(src, dst, loc.at[1]).start())

    seg_copy = remote(s_ref, sg.at[c], s_s, s_r, (2 * pair + 1 - c, z))
    seg_copy.start()
    own_seg = pltpu.make_async_copy(s_ref, sg.at[c], loc.at[2])
    own_seg.start()
    own_gain = pltpu.make_async_copy(g_ref, ga.at[me], loc.at[3])
    own_gain.start()

    def send_gain(o, carry):
        other = lax.rem(me + o, total)
        remote(g_ref, ga.at[me], g_s, g_r, (other // n_z, lax.rem(other, n_z))).start()
        return carry

    lax.fori_loop(1, total, send_gain, 0)

    first = jnp.where(c == cz, z % 2, 1 - c)

    def turn_of(t):
        return t % 2, (first if t < 2 else 1 - first)

    def spot(owner, t, h):
        core, b = turn_of(t)
        part = shape[0] // 2
        return wq.at[pl.ds(pl.multiple_of((2 * owner + core) * shape[0] + h * part, part), part),
                     pl.ds(pl.multiple_of(b * shape[1], shape[1]), shape[1])]

    spread = Spread(n_d, pair, c, z, 4, spot, d_s, d_r)
    for t in range(4):
        core, b = turn_of(t)
        blk = block_at(wq, shape, 2 * pair + core, b)
        mine = (core == c) & (2 * c + b == z)
        arrive = remote(w_ref, blk, w_s.at[0], w_r.at[core, b], (d, z))
        pl.when(jnp.logical_not(mine))(arrive.wait_recv)
        pl.when(mine)(lambda blk=blk: pltpu.make_async_copy(w_ref, blk, loc.at[0]).wait())
        spread.own(t)
        if t == 1:
            line_stage(v_ref, block_at(vo, v_ref.shape, c, z % 2), v_s, v_r, 4, False)
        if t > 0:
            spread.pass_on(t - 1)

    for o in range(n_z):
        zs = lax.rem(z + o, n_z)
        src = xs.at[pl.ds(pl.multiple_of(zs * rows + c * half, half), half)]
        mine = (cz == c) & (zs == z)
        arrive = remote(src, src, x_s.at[0, 0], x_r.at[zs], (d, z))
        pl.when(jnp.logical_not(mine))(arrive.wait_recv)
        pl.when(mine)(lambda src=src: pltpu.make_async_copy(src, src, loc.at[1]).wait())
        remote(src, src, f_s.at[zs], f_r.at[zs], (2 * pair + 1 - c, z)).start()
    spread.pass_on(3)

    line_stage(w_ref, my_block, w_s, w_r, 0, True)
    line_stage(v_ref, block_at(vo, v_ref.shape, c, z % 2), v_s, v_r, 4, True)
    for i in range(2):
        for h in range(2):
            src = x_ref.at[i, pl.ds(h * half, half)]
            mine = (h == c) & (2 * c + i == z)
            copy = remote(src, src, x_s.at[i, h], x_r.at[0], (d, z))
            pl.when(jnp.logical_not(mine))(copy.wait_send)
    for zs in range(n_z):
        src = xs.at[pl.ds(zs * rows, half)]
        copy = remote(src, src, f_s.at[zs], f_r.at[zs], (d, z))
        copy.wait_send()
        copy.wait_recv()
    for core in range(2):
        for b in range(2):
            blk = block_at(vo, v_ref.shape, core, b)
            mine = (core == c) & (2 * c + b == z)
            pl.when(jnp.logical_not(mine))(remote(blk, blk, v_s.at[0], v_r.at[core, b], (d, z)).wait_recv)
            pl.when(mine)(pltpu.make_async_copy(v_ref, blk, loc.at[4]).wait)
    seg_copy.wait_send()
    remote(s_ref, sg.at[1 - c], s_s, s_r, (d, z)).wait_recv()
    own_seg.wait()
    own_gain.wait()
    many = ga.at[pl.ds(0, total - 1)]
    gains = remote(many, many, g_s, g_r, (d, z))
    gains.wait_send()
    gains.wait_recv()
    spread.finish()


def gather_in(x_loc, w, v, gain_tile, seg_tile, n_dp, n_z):
    _, rows, width = x_loc.shape
    n_d = n_dp // 2
    total = n_dp * n_z
    return pl.pallas_call(
        functools.partial(gather_in_kernel, n_dp, n_z),
        in_specs=[VMEM_SPEC] * 5,
        out_specs=[ANY_SPEC] * 5,
        out_shape=[
            jax.ShapeDtypeStruct((rows * n_z, width), x_loc.dtype),
            jax.ShapeDtypeStruct((w.shape[0] * n_dp, 2 * w.shape[1]), w.dtype),
            jax.ShapeDtypeStruct((v.shape[0] * 2, 2 * v.shape[1]), v.dtype),
            jax.ShapeDtypeStruct((total,) + gain_tile.shape, gain_tile.dtype),
            jax.ShapeDtypeStruct((2,) + seg_tile.shape, seg_tile.dtype),
        ],
        scratch_shapes=[
            DMA((2, 2)), DMA((n_z,)), DMA((n_z,)), DMA((n_z,)), DMA((n_z,)), DMA((2, 2)), DMA((n_z,)), DMA((2, 2)),
            DMA((n_d - 1, 4, 2)), DMA((n_d - 1, 4, 2)), DMA, DMA, DMA, DMA, DMA((5,)),
        ],
        compiler_params=pltpu.CompilerParams(collective_id=1, has_side_effects=True),
        cost_estimate=pl.CostEstimate(flops=0, bytes_accessed=200_000_000, transcendentals=0),
        name="gather_in",
    )(x_loc, w, v, gain_tile, seg_tile)


def share_resid_kernel(n_z, part_ref, x_ref, out, got, buf, p_s, p_r, u_s, u_r, loc):
    d, z, pair, c = place()
    cz = z // 2
    full = x_ref.shape[0]
    half = full // 2
    unit = half // 2
    greet_line(n_z, d, z)
    mine = pl.ds(pl.multiple_of(c * half, half), half)
    theirs = pl.ds(pl.multiple_of((1 - c) * half, half), half)
    swap = remote(part_ref.at[theirs], got, p_s, p_r, (2 * pair + 1 - c, z))
    swap.start()
    swap.wait_recv()

    def add(r, carry):
        at = pl.ds(pl.multiple_of(r * 16, 16), 16)
        src = pl.ds(pl.multiple_of(c * half + r * 16, 16), 16)
        total = x_ref[src].astype(jnp.float32) + part_ref[src].astype(jnp.float32) + got[at].astype(jnp.float32)
        buf[at] = total.astype(jnp.bfloat16)
        return carry

    def spot(jl, h, k):
        return out.at[jl, pl.ds(pl.multiple_of(h * half + k * unit, unit), unit)]

    def sends(k, wait):
        src = buf.at[pl.ds(k * unit, unit)]
        dst = spot(z % 2, c, k)
        for o, zz in ((0, z), (1, z - 1), (2, z + 1)):
            copy = remote(src, dst, u_s.at[o, k], u_r.at[z % 2, c, k], (2 * pair + cz, zz))
            act = copy.wait_send if wait else copy.start
            if o == 0:
                keep = pltpu.make_async_copy(src, dst, loc.at[k])
                pl.when(c != cz)(act)
                pl.when(c == cz)(keep.wait if wait else keep.start)
            elif o == 1:
                pl.when(z > 0)(act)
            else:
                pl.when(z < n_z - 1)(act)

    per = unit // 16
    lax.fori_loop(0, per, add, 0)
    lax.fori_loop(per, per + per // 2, add, 0)
    sends(0, False)
    lax.fori_loop(per + per // 2, 2 * per, add, 0)
    swap.wait_send()
    sends(1, False)

    def relay(dist, sign, jl_wait):
        j = z + sign * dist
        ok = (j >= 2 * c) & (j <= 2 * c + 1)
        to = z - sign
        more = (to >= 0) & (to <= n_z - 1)
        jl = lax.rem(j + n_z, 2)

        @pl.when(ok)
        def _():
            for k in range(2):
                for h in range(2):
                    at = spot(jl, h, k)
                    copy = remote(at, at, u_s.at[3 + (0 if sign < 0 else 1), 4 * jl + 2 * h + k], u_r.at[jl, h, k], (2 * pair + c, to))
                    if jl_wait:
                        copy.wait_recv()
                        pl.when(more)(copy.start)
                    else:
                        pl.when(more)(copy.wait_send)

    order = [(dist, sign) for dist in range(1, n_z) for sign in (-1, 1)]
    for dist, sign in order:
        relay(dist, sign, True)

    @pl.when(c == cz)
    def _():
        for k in range(2):
            at = spot(z % 2, 1 - c, k)
            remote(at, at, u_s.at[0, 0], u_r.at[z % 2, 1 - c, k], (d, z)).wait_recv()

    for dist, sign in order:
        relay(dist, sign, False)
    sends(0, True)
    sends(1, True)


def share_resid(part, x, n_z):
    full, width = x.shape
    return pl.pallas_call(
        functools.partial(share_resid_kernel, n_z),
        in_specs=[VMEM_SPEC] * 2,
        out_specs=ANY_SPEC,
        out_shape=jax.ShapeDtypeStruct((2, full, width), jnp.bfloat16),
        scratch_shapes=[
            pltpu.VMEM((full // 2, width), jnp.bfloat16), pltpu.VMEM((full // 2, width), jnp.bfloat16),
            DMA, DMA, DMA((5, 8)), DMA((2, 2, 2)), DMA((2,)),
        ],
        compiler_params=pltpu.CompilerParams(collective_id=2, has_side_effects=True),
        cost_estimate=pl.CostEstimate(flops=0, bytes_accessed=200_000_000, transcendentals=0),
        name="share_resid",
    )(part, x)


CHUNKS = 8


def sum_line_kernel(n_z, part_ref, resid_all, cot_all, gain_ref, d_out, gain_out, got, buf, resid_ref, cot_ref,
                    s_s, s_r, p_s, p_r, loc, rows_sem):
    d, z, pair, c = place()
    cz = z // 2
    full, _ = buf.shape
    rows = full // CHUNKS
    fetch = (
        pltpu.make_async_copy(resid_all.at[z % 2], resid_ref, rows_sem.at[0]),
        pltpu.make_async_copy(cot_all.at[z % 2], cot_ref, rows_sem.at[1]),
    )
    for one in fetch:
        one.start()
    greet_line(n_z, d, z)
    gain_out[...] = jnp.zeros_like(gain_out)
    own = c == cz
    steps = [(k, t) for k in range(CHUNKS) for t in range(2)]

    def where_is(k, t):
        jl = jnp.bitwise_xor(c, t)
        return jl, 2 * c + jl, pl.ds(k * rows, rows)

    def copy_on(k, t, side, src):
        jl, _, at = where_is(k, t)
        to = z + 1 if side == 0 else z - 1
        return remote(src, got.at[side, jl, at], s_s.at[t, k], s_r.at[side, jl, k], (2 * pair + c, to))

    def arrived(side, jl, k):
        at = got.at[side, jl, pl.ds(k * rows, rows)]
        return remote(at, at, s_s.at[0, 0], s_r.at[side, jl, k], (d, z))

    def add_in(side, jl, k):
        def one(r, carry):
            at = pl.ds(pl.multiple_of(k * rows + r * 16, 16), 16)
            got[side, jl, at] = (got[side, jl, at].astype(jnp.float32) + part_ref[jl, at].astype(jnp.float32)).astype(jnp.bfloat16)
            return carry

        lax.fori_loop(0, rows // 16, one, 0)

    def finish(jl, k):
        def one(r, carry):
            at = pl.ds(pl.multiple_of(k * rows + r * 16, 16), 16)
            total = part_ref[jl, at].astype(jnp.float32)
            left = got[0, jl, at].astype(jnp.float32)
            right = got[1, jl, at].astype(jnp.float32)
            total = total + jnp.where(z > 0, left, 0.0) + jnp.where(z < n_z - 1, right, 0.0)
            value = resid_ref[at].astype(jnp.float32)
            inverse = lax.rsqrt(jnp.mean(value * value, axis=-1, keepdims=True) + norm_eps)
            scaled = value * inverse
            d_scaled = total * gain_ref[...]
            mean = jnp.mean(d_scaled * scaled, axis=-1, keepdims=True)
            d_resid = cot_ref[at].astype(jnp.float32) + inverse * (d_scaled - scaled * mean)
            buf[at] = d_resid.astype(jnp.bfloat16)
            prod = total * scaled
            gain_out[...] = gain_out[...] + prod[:8] + prod[8:]
            return carry

        lax.fori_loop(0, rows // 16, one, 0)

    def to_partner(k):
        at = pl.ds(k * rows, rows)
        return remote(buf.at[at], d_out.at[at], p_s.at[k], p_r.at[k], (2 * pair + 1 - c, z))

    def keep(k):
        at = pl.ds(k * rows, rows)
        return pltpu.make_async_copy(buf.at[at], d_out.at[at], loc.at[k])

    def send_step(k, t, wait):
        jl, j, at = where_is(k, t)
        for side in range(2):
            going = (z < j) if side == 0 else (z > j)
            edge = (z == 0) if side == 0 else (z == n_z - 1)
            edge_copy = copy_on(k, t, side, part_ref.at[jl, at])
            inner_copy = copy_on(k, t, side, got.at[side, jl, at])
            pl.when(going & edge)(edge_copy.wait_send if wait else edge_copy.start)
            pl.when(going & jnp.logical_not(edge))(inner_copy.wait_send if wait else inner_copy.start)

    def publish(k, wait):
        @pl.when(own)
        def _():
            if wait:
                to_partner(k).wait_send()
                keep(k).wait()
            else:
                to_partner(k).start()
                keep(k).start()

    def own_chunk(k):
        @pl.when(own)
        def _():
            if k == 0:
                for one in fetch:
                    one.wait()
            jl = z % 2
            pl.when(z > 0)(arrived(0, jl, k).wait_recv)
            pl.when(z < n_z - 1)(arrived(1, jl, k).wait_recv)
            finish(jl, k)
            if k > 0:
                to_partner(k - 1).start()
                keep(k - 1).start()

    for n, (k, t) in enumerate(steps):
        jl, j, at = where_is(k, t)
        for side in range(2):
            going = (z < j) if side == 0 else (z > j)
            inner = (z > 0) if side == 0 else (z < n_z - 1)

            @pl.when(going & inner)
            def _():
                arrived(side, jl, k).wait_recv()
                add_in(side, jl, k)

        if n > 0:
            send_step(*steps[n - 1], False)
        if t == 1 and k > 0:
            own_chunk(k - 1)
    send_step(*steps[-1], False)
    own_chunk(CHUNKS - 1)

    @pl.when(jnp.logical_not(own))
    def _():
        for one in fetch:
            one.wait()

    @pl.when(own)
    def _():
        to_partner(CHUNKS - 1).start()
        keep(CHUNKS - 1).start()

    for k, t in steps:
        send_step(k, t, True)
    for k in range(CHUNKS):
        publish(k, True)
        at = d_out.at[pl.ds(k * rows, rows)]
        pl.when(jnp.logical_not(own))(remote(at, at, p_s.at[k], p_r.at[k], (d, z)).wait_recv)


def sum_line(part, resid, cot, gain, n_z):
    _, full, width = part.shape
    return pl.pallas_call(
        functools.partial(sum_line_kernel, n_z),
        in_specs=[VMEM_SPEC, ANY_SPEC, ANY_SPEC, VMEM_SPEC],
        out_specs=[ANY_SPEC, VMEM_SPEC],
        out_shape=[jax.ShapeDtypeStruct((full, width), jnp.bfloat16), jax.ShapeDtypeStruct((8, width), jnp.float32)],
        scratch_shapes=[
            pltpu.VMEM((2, 2, full, width), jnp.bfloat16), pltpu.VMEM((full, width), jnp.bfloat16),
            pltpu.VMEM((full, width), jnp.bfloat16), pltpu.VMEM((full, width), jnp.bfloat16),
            DMA((2, CHUNKS)), DMA((2, 2, CHUNKS)), DMA((CHUNKS,)), DMA((CHUNKS,)), DMA((CHUNKS,)), DMA((2,)),
        ],
        compiler_params=pltpu.CompilerParams(collective_id=3, has_side_effects=True, vmem_limit_bytes=56 * 1024 * 1024),
        cost_estimate=pl.CostEstimate(flops=0, bytes_accessed=200_000_000, transcendentals=0),
        name="sum_line",
    )(part, resid, cot, gain)


def hand_out_kernel(n_dp, n_z, dn_ref, x_ref, dr_ref, gain_ref, gain2_ref, qt_ref, ot_ref,
                    ig, gq, go, gains, got, buf, q_got, q_own, q_mid, q_put, q_fin, o_got, o_own, o_mid, o_put, o_fin, g_src, g_all,
                    p_s, p_r, i_s, i_r, q_s, q_r, qf_s, qf_r, o_s, o_r, of_s, of_r, g_s, g_r, loc):
    d, z, pair, c = place()
    n_d = n_dp // 2
    total = n_dp * n_z
    me = d * n_z + z
    cz = z // 2
    full, width = x_ref.shape
    half = full // 2
    quarter = half // 2
    q_rows, q_cols = q_fin.shape[1:]
    o_rows, o_cols = o_fin.shape[1:]
    relay = n_d == 4

    def region(ref, rows, cols, owner, b):
        return ref.at[pl.ds(pl.multiple_of(owner * 2 * rows, 2 * rows), 2 * rows), pl.ds(b * cols, cols)]

    class First:
        def __init__(self, src, rows, cols, got_ref, own_ref, mid_ref, put_ref, send, recv, spare):
            self.src, self.rows, self.cols, self.got, self.own, self.mid = src, rows, cols, got_ref, own_ref, mid_ref
            self.put, self.send, self.recv, self.spare = put_ref, send, recv, spare

        def slot(self, n, b):
            return self.got.at[n, :, pl.ds(b * self.cols, self.cols)]

        def copy(self, n, b, owner, to):
            src = region(self.src, self.rows, self.cols, owner, b)
            return remote(src, self.slot(n, b), self.send.at[n, b], self.recv.at[n, b], (2 * (pair ^ to) + c, z))

        def load(self, b):
            yield pltpu.make_async_copy(region(self.src, self.rows, self.cols, pair, b), self.own.at[:, pl.ds(b * self.cols, self.cols)], loc.at[self.spare + b])
            if relay:
                yield pltpu.make_async_copy(region(self.src, self.rows, self.cols, pair ^ (2 >> b), b), self.mid.at[:, pl.ds(b * self.cols, self.cols)], loc.at[self.spare + 2 + b])

        def begin(self, b):
            if relay:
                near = 1 + b
                self.copy(1, b, pair ^ 3, near).start()
                self.copy(0, b, pair ^ near, near).start()
            else:
                for k in range(1, n_d):
                    self.copy(k - 1, b, pair ^ k, k).start()

        def arrived(self, n, b):
            remote(self.slot(n, b), self.slot(n, b), self.send.at[n, b], self.recv.at[n, b], (d, z)).wait_recv()

        def middle(self, b):
            if not relay:
                return
            self.arrived(1, b)
            lanes = pl.ds(b * self.cols, self.cols)

            def add(r, carry):
                at = pl.ds(pl.multiple_of(r * 16, 16), 16)
                self.mid[at, lanes] = (self.mid[at, lanes].astype(jnp.float32) + self.got[1, at, lanes].astype(jnp.float32)).astype(jnp.bfloat16)
                return carry

            lax.fori_loop(0, 2 * self.rows // 16, add, 0)

        def middle_copy(self, b):
            src = self.mid.at[:, pl.ds(b * self.cols, self.cols)]
            return remote(src, self.slot(2, b), self.send.at[2, b], self.recv.at[2, b], (2 * (pair ^ (2 >> b)) + c, z))

        def total(self, b):
            slots = (0, 2) if relay else range(n_d - 1)
            for n in slots:
                self.arrived(n, b)
            lanes = pl.ds(b * self.cols, self.cols)
            for core in range(2):

                def add(r, carry):
                    at = pl.ds(pl.multiple_of(r * 16, 16), 16)
                    src = pl.ds(pl.multiple_of(core * self.rows + r * 16, 16), 16)
                    value = self.own[src, lanes].astype(jnp.float32)
                    for n in slots:
                        value = value + self.got[n, src, lanes].astype(jnp.float32)
                    self.put[core, b, at] = value.astype(jnp.bfloat16)
                    return carry

                lax.fori_loop(0, self.rows // 16, add, 0)

        def sent(self, b):
            for n in range(n_d - 1):
                remote(self.slot(n, b), self.slot(n, b), self.send.at[n, b], self.recv.at[n, b], (d, z)).wait_send()

    o_first = First(ot_ref, o_rows, o_cols, o_got, o_own, o_mid, o_put, o_s, o_r, 6)
    q_first = First(qt_ref, q_rows, q_cols, q_got, q_own, q_mid, q_put, q_s, q_r, 10)
    firsts = [(o_first, 0), (o_first, 1), (q_first, 0), (q_first, 1)]
    for one, b in firsts:
        for copy in one.load(b):
            copy.start()
    greet_all(n_dp, n_z, d, z)

    mine = pl.ds(pl.multiple_of(c * half, half), half)
    theirs = pl.ds(pl.multiple_of((1 - c) * half, half), half)
    swap = remote(dn_ref.at[theirs], got, p_s, p_r, (2 * pair + 1 - c, z))
    swap.start()
    for one, b in firsts:
        one.begin(b)

    g_src[pl.ds(0, 8)] = jnp.zeros((8, width), jnp.float32)
    g_src[pl.ds(8, 8)] = gain2_ref[...]
    swap.wait_recv()

    def rows_of(r, carry):
        at = pl.ds(pl.multiple_of(r * 16, 16), 16)
        src = pl.ds(pl.multiple_of(c * half + r * 16, 16), 16)
        d_normed = dn_ref[src].astype(jnp.float32) + got[at].astype(jnp.float32)
        value = x_ref[src].astype(jnp.float32)
        inverse = lax.rsqrt(jnp.mean(value * value, axis=-1, keepdims=True) + norm_eps)
        scaled = value * inverse
        d_scaled = d_normed * gain_ref[...]
        mean = jnp.mean(d_scaled * scaled, axis=-1, keepdims=True)
        out = dr_ref[src].astype(jnp.float32) + inverse * (d_scaled - scaled * mean)
        buf[at] = out.astype(jnp.bfloat16)
        prod = d_normed * scaled
        g_src[pl.ds(0, 8)] = g_src[pl.ds(0, 8)] + prod[:8] + prod[8:]
        return carry

    def row_send(b, wait):
        src = buf.at[pl.ds(b * quarter, quarter)]
        dst = ig.at[z % 2]
        zz = 2 * c + b
        here = (cz == c) & (zz == z)
        copy = remote(src, dst, i_s.at[b], i_r.at[z % 2], (2 * pair + cz, zz))
        keep = pltpu.make_async_copy(src, dst, loc.at[2])
        pl.when(jnp.logical_not(here))(copy.wait_send if wait else copy.start)
        pl.when(here)(keep.wait if wait else keep.start)

    per = quarter // 16
    lax.fori_loop(0, per, rows_of, 0)
    lax.fori_loop(per, per + per // 2, rows_of, 0)
    row_send(0, False)
    lax.fori_loop(per + per // 2, 2 * per, rows_of, 0)
    for one, b in firsts:
        for copy in one.load(b):
            copy.wait()
    row_send(1, False)

    each = width // total

    def gain_tile(o):
        return g_src.at[:, pl.ds(pl.multiple_of(o * each // 128 * 128, 128), 128)]

    own_gain = pltpu.make_async_copy(gain_tile(me), g_all.at[me], loc.at[3])
    own_gain.start()

    def send_gain(o, carry):
        other = lax.rem(me + o, total)
        remote(gain_tile(other), g_all.at[me], g_s, g_r, (other // n_z, lax.rem(other, n_z))).start()
        return carry

    lax.fori_loop(1, total, send_gain, 0)

    def second_send(b, put_ref, fin_ref, f_s, f_r, spare, wait):
        for core in range(2):
            here = (core == c) & (2 * c + b == z)
            src = put_ref.at[core, b]
            copy = remote(src, fin_ref.at[z], f_s.at[core, b], f_r.at[z], (2 * pair + core, 2 * c + b))
            keep = pltpu.make_async_copy(src, fin_ref.at[z], loc.at[spare])
            pl.when(jnp.logical_not(here))(copy.wait_send if wait else copy.start)
            pl.when(here)(keep.wait if wait else keep.start)

    def last(rows, fin_ref, out_ref):
        def add(r, carry):
            at = pl.ds(pl.multiple_of(r * 16, 16), 16)
            value = fin_ref[0, at].astype(jnp.float32)
            for zs in range(1, n_z):
                value = value + fin_ref[zs, at].astype(jnp.float32)
            out_ref[at] = value
            return carry

        lax.fori_loop(0, rows // 16, add, 0)

    o_args = (o_put, o_fin, of_s, of_r, 4)
    q_args = (q_put, q_fin, qf_s, qf_r, 5)
    if relay:
        for n, (one, b) in enumerate(firsts):
            one.middle(b)
            if n:
                last_one, last_b = firsts[n - 1]
                last_one.middle_copy(last_b).start()
    o_first.total(0)
    if relay:
        q_first.middle_copy(1).start()
    o_first.total(1)
    second_send(0, *o_args, False)
    q_first.total(0)
    second_send(1, *o_args, False)
    q_first.total(1)
    second_send(0, *q_args, False)

    def arrived(fin_ref, f_s, f_r):
        for zs in range(n_z):
            at = fin_ref.at[zs]
            from_here = (cz == c) & (zs == z)
            pl.when(jnp.logical_not(from_here))(remote(at, at, f_s.at[0, 0], f_r.at[zs], (d, z)).wait_recv)

    def own_done(args):
        for b in range(2):
            second_send(b, *args, True)

    own_done(o_args)
    arrived(o_fin, of_s, of_r)
    value = o_fin[0].astype(jnp.float32)
    for zs in range(1, n_z):
        value = value + o_fin[zs].astype(jnp.float32)
    go[...] = value.T
    second_send(1, *q_args, False)
    own_done(q_args)
    arrived(q_fin, qf_s, qf_r)
    last(q_rows, q_fin, gq)

    many = g_all.at[pl.ds(0, total - 1)]
    gain_copy = remote(many, many, g_s, g_r, (d, z))
    gain_copy.wait_send()
    gain_copy.wait_recv()
    own_gain.wait()
    gains[...] = jnp.zeros_like(gains)

    def add_gain(o, carry):
        gains[...] = gains[...] + g_all[o]
        return carry

    lax.fori_loop(0, total, add_gain, 0)

    swap.wait_send()
    for b in range(2):
        row_send(b, True)
        o_first.sent(b)
        q_first.sent(b)
    for i in range(2):
        from_here = (cz == c) & (2 * c + i == z)
        at = ig.at[i]
        pl.when(jnp.logical_not(from_here))(remote(at, at, i_s.at[0], i_r.at[i], (d, z)).wait_recv)


def hand_out(dn, x, dr, gain, gain2, qt, ot, n_dp, n_z):
    full, width = x.shape
    n_d = n_dp // 2
    total = n_dp * n_z
    q_rows, q_cols = qt.shape[0] // n_dp, qt.shape[1] // 2
    o_rows, o_cols = ot.shape[0] // n_dp, ot.shape[1] // 2
    b16 = jnp.bfloat16
    return pl.pallas_call(
        functools.partial(hand_out_kernel, n_dp, n_z),
        in_specs=[VMEM_SPEC] * 5 + [ANY_SPEC] * 2,
        out_specs=[ANY_SPEC] + [VMEM_SPEC] * 3,
        out_shape=[
            jax.ShapeDtypeStruct((2, full // 4, width), b16),
            jax.ShapeDtypeStruct((q_rows, q_cols), jnp.float32),
            jax.ShapeDtypeStruct((o_cols, o_rows), jnp.float32),
            jax.ShapeDtypeStruct((16, 128), jnp.float32),
        ],
        scratch_shapes=[
            pltpu.VMEM((full // 2, width), b16), pltpu.VMEM((full // 2, width), b16),
            pltpu.VMEM((n_d - 1, 2 * q_rows, 2 * q_cols), b16), pltpu.VMEM((2 * q_rows, 2 * q_cols), b16),
            pltpu.VMEM((2 * q_rows, 2 * q_cols), b16),
            pltpu.VMEM((2, 2, q_rows, q_cols), b16), pltpu.VMEM((n_z, q_rows, q_cols), b16),
            pltpu.VMEM((n_d - 1, 2 * o_rows, 2 * o_cols), b16), pltpu.VMEM((2 * o_rows, 2 * o_cols), b16),
            pltpu.VMEM((2 * o_rows, 2 * o_cols), b16),
            pltpu.VMEM((2, 2, o_rows, o_cols), b16), pltpu.VMEM((n_z, o_rows, o_cols), b16),
            pltpu.VMEM((16, width), jnp.float32), pltpu.VMEM((total, 16, 128), jnp.float32),
            DMA, DMA, DMA((2,)), DMA((2,)), DMA((n_d - 1, 2)), DMA((n_d - 1, 2)), DMA((2, 2)), DMA((n_z,)),
            DMA((n_d - 1, 2)), DMA((n_d - 1, 2)), DMA((2, 2)), DMA((n_z,)), DMA, DMA, DMA((14,)),
        ],
        compiler_params=pltpu.CompilerParams(collective_id=5, has_side_effects=True, vmem_limit_bytes=56 * 1024 * 1024),
        cost_estimate=pl.CostEstimate(flops=0, bytes_accessed=300_000_000, transcendentals=0),
        name="hand_out",
    )(dn, x, dr, gain, gain2, qt, ot)


def rms_forward(values, gain_wide):
    inverse = lax.rsqrt(jnp.mean(values * values, axis=-1, keepdims=True) + norm_eps)
    scaled = values * inverse
    return (scaled, inverse, (scaled * gain_wide).astype(jnp.bfloat16))


def adam_update(weight, grad, first, second):
    new_first = beta_one * first + (1.0 - beta_one) * grad
    new_second = beta_two * second + (1.0 - beta_two) * grad * grad
    first_hat = new_first / (1.0 - beta_one**step_count)
    second_hat = new_second / (1.0 - beta_two**step_count)
    new_weight = weight - learn_rate * (
        first_hat / (jnp.sqrt(second_hat) + adam_eps) + weight_decay * weight
    )
    return (new_weight, new_first, new_second)


def contract_rows(left, right):
    return lax.dot_general(
        left, right, (((0,), (0,)), ((), ())), preferred_element_type=jnp.float32
    )


def times_transpose(left, right):
    return lax.dot_general(
        left, right, (((1,), (1,)), ((), ())), preferred_element_type=jnp.float32
    )


def layer_step(
    block_input,
    segment_ids,
    cotangent,
    attn_gain,
    qkv_weight,
    out_weight,
    mlp_gain,
    gate_up_weight,
    down_weight,
    first_attn_gain,
    first_qkv,
    first_out,
    first_mlp_gain,
    first_gate_up,
    first_down,
    second_attn_gain,
    second_qkv,
    second_out,
    second_mlp_gain,
    second_gate_up,
    second_down,
):
    seqs_here, local_len, width = block_input.shape
    full_len = segment_ids.shape[1]
    n_dp = lax.axis_size("dp")
    n_z = lax.axis_size("seq")
    groups = HEADS // KV_HEADS
    unit_count = down_weight.shape[0]
    z_here = lax.axis_index("seq")
    owned = attn_gain.shape[0]
    gain_line = jnp.concatenate([attn_gain, mlp_gain]).astype(jnp.bfloat16).astype(jnp.float32)
    gain_tile = jnp.pad(gain_line[None], ((0, 7), (0, LANES - 2 * owned)))
    seg_tile = jnp.pad(segment_ids, ((0, 8 - seqs_here), (0, 0)))
    gate_up_cols = lax.all_gather(
        gate_up_weight.astype(jnp.bfloat16).reshape(-1, 2 * unit_count), "dp", axis=0, tiled=True
    )
    rows_in, qkv_cols, out_line, gain_all, seg_all = gather_in(
        block_input,
        qkv_weight.astype(jnp.bfloat16),
        out_weight.astype(jnp.bfloat16).T,
        gain_tile,
        seg_tile,
        n_dp,
        n_z,
    )
    cot_late, down_late, _ = lax.optimization_barrier(
        (cotangent, down_weight.astype(jnp.bfloat16), gain_all)
    )
    cot_all = lax.all_gather(cot_late, "seq", axis=1, tiled=True)
    down_rows = lax.all_gather(down_late, "dp", axis=1, tiled=True)
    gain_one = gain_all[:, 0, :owned].reshape(1, width)
    gain_two = gain_all[:, 0, owned : 2 * owned].reshape(1, width)
    seg_here = lax.dynamic_slice(seg_all, (z_here // 2, z_here % 2, 0), (1, 1, full_len))[0]
    tables = attn_tables(seg_here)
    _, _, normed_one = rms_forward(rows_in.astype(jnp.float32), gain_one)
    qkv = jnp.dot(normed_one, qkv_cols, preferred_element_type=jnp.float32)
    turned, lse, attended16, out_rows = attn_forward(qkv, *tables, out_line, full_len, groups, n_dp)
    attn_part = times_transpose(attended16, out_rows)
    resid_all = share_resid(attn_part.astype(jnp.bfloat16), rows_in, n_z)
    total_rows = seqs_here * full_len
    resid = resid_all.reshape(total_rows, width).astype(jnp.float32)
    _, _, normed_two = rms_forward(resid, gain_two)
    gate_up = jnp.dot(normed_two, gate_up_cols, preferred_element_type=jnp.float32)
    gate_part = gate_up[:, :unit_count]
    up_part = gate_up[:, unit_count:]
    sigmoid_gate = jax.nn.sigmoid(gate_part)
    active = gate_part * sigmoid_gate
    hidden16 = (active * up_part).astype(jnp.bfloat16)
    cot_rows = cot_all.reshape(total_rows, width)
    d_hidden = times_transpose(cot_rows, down_rows)
    d_gate = d_hidden * up_part * sigmoid_gate * (1.0 + gate_part * (1.0 - sigmoid_gate))
    d_up = d_hidden * active
    d_gate_up16 = jnp.concatenate([d_gate, d_up], 1).astype(jnp.bfloat16)
    down_term = contract_rows(cot_rows, hidden16).astype(jnp.bfloat16)
    d_gate_up_next, down_term = lax.optimization_barrier((d_gate_up16, down_term))
    down_sum = lax.psum_scatter(down_term, "dp", scatter_dimension=0, tiled=True)
    grad_down = down_sum.astype(jnp.float32).T
    gate_up_term = contract_rows(normed_two, d_gate_up_next).astype(jnp.bfloat16)
    d_gate_up_next, gate_up_term = lax.optimization_barrier((d_gate_up16, gate_up_term))
    gate_up_sum = lax.psum_scatter(gate_up_term, "dp", scatter_dimension=0, tiled=True)
    grad_gate_up = gate_up_sum.reshape(gate_up_weight.shape).astype(jnp.float32)
    d_normed_two = times_transpose(d_gate_up_next, gate_up_cols).astype(jnp.bfloat16)
    d_resid16, gain_two_part = sum_line(
        d_normed_two.reshape(resid_all.shape), resid_all, cot_all, gain_two, n_z
    )
    hidden_late, _ = lax.optimization_barrier((hidden16, d_resid16))
    down_part = jnp.dot(hidden_late, down_rows, preferred_element_type=jnp.float32)
    down_here = lax.psum_scatter(
        down_part.astype(jnp.bfloat16).reshape(resid_all.shape), "seq", scatter_dimension=1, tiled=True
    )
    down_here = down_here.astype(jnp.float32)
    resid_here = lax.dynamic_slice_in_dim(resid_all, z_here * local_len, local_len, 1)
    output = (resid_here.astype(jnp.float32) + down_here).astype(jnp.bfloat16)
    d_attended = jnp.dot(d_resid16, out_rows, preferred_element_type=jnp.float32).astype(jnp.bfloat16)
    d_qkv16 = attn_backward(turned, d_attended, lse, *tables, full_len, groups)
    d_normed_one = times_transpose(d_qkv16, qkv_cols).astype(jnp.bfloat16)
    qkv_term = contract_rows(normed_one, d_qkv16).astype(jnp.bfloat16)
    out_term = contract_rows(d_resid16, attended16).astype(jnp.bfloat16)
    input_grad, grad_qkv, grad_out, gain_sums = hand_out(
        d_normed_one, rows_in, d_resid16, gain_one, gain_two_part, qkv_term, out_term, n_dp, n_z
    )
    flat = lax.axis_index("dp") * n_z + z_here
    gain_sums = lax.dynamic_slice(
        jnp.sum(gain_sums.reshape(2, 8, LANES), axis=1), (0, flat * owned % LANES), (2, owned)
    )
    grad_gain_one = gain_sums[0]
    grad_gain_two = gain_sums[1]
    w_one, m_one, v_one = adam_update(attn_gain, grad_gain_one, first_attn_gain, second_attn_gain)
    w_qkv, m_qkv, v_qkv = adam_update(qkv_weight, grad_qkv, first_qkv, second_qkv)
    w_out, m_out, v_out = adam_update(out_weight, grad_out, first_out, second_out)
    w_two, m_two, v_two = adam_update(mlp_gain, grad_gain_two, first_mlp_gain, second_mlp_gain)
    w_gu, m_gu, v_gu = adam_update(gate_up_weight, grad_gate_up, first_gate_up, second_gate_up)
    w_down, m_down, v_down = adam_update(down_weight, grad_down, first_down, second_down)
    return (
        output,
        input_grad,
        grad_gain_one,
        grad_qkv,
        grad_out,
        grad_gain_two,
        grad_gate_up,
        grad_down,
        w_one,
        w_qkv,
        w_out,
        w_two,
        w_gu,
        w_down,
        m_one,
        m_qkv,
        m_out,
        m_two,
        m_gu,
        m_down,
        v_one,
        v_qkv,
        v_out,
        v_two,
        v_gu,
        v_down,
    )


def solution(mesh):
    in_specs = (
        P("dp", "seq", None),
        P("dp", None),
        P("dp", "seq", None),
        P(("dp", "seq")),
        P("dp", "seq"),
        P("seq", "dp"),
        P(("dp", "seq")),
        P("dp", None, "seq"),
        P("seq", "dp"),
        P(("dp", "seq")),
        P("dp", "seq"),
        P("seq", "dp"),
        P(("dp", "seq")),
        P("dp", None, "seq"),
        P("seq", "dp"),
        P(("dp", "seq")),
        P("dp", "seq"),
        P("seq", "dp"),
        P(("dp", "seq")),
        P("dp", None, "seq"),
        P("seq", "dp"),
    )
    out_specs = (
        P("dp", "seq", None),
        P("dp", "seq", None),
        P(("dp", "seq")),
        P("dp", "seq"),
        P("seq", "dp"),
        P(("dp", "seq")),
        P("dp", None, "seq"),
        P("seq", "dp"),
        P(("dp", "seq")),
        P("dp", "seq"),
        P("seq", "dp"),
        P(("dp", "seq")),
        P("dp", None, "seq"),
        P("seq", "dp"),
        P(("dp", "seq")),
        P("dp", "seq"),
        P("seq", "dp"),
        P(("dp", "seq")),
        P("dp", None, "seq"),
        P("seq", "dp"),
        P(("dp", "seq")),
        P("dp", "seq"),
        P("seq", "dp"),
        P(("dp", "seq")),
        P("dp", None, "seq"),
        P("seq", "dp"),
    )
    return jax.shard_map(layer_step, mesh=mesh, in_specs=in_specs, out_specs=out_specs, check_vma=False)
```

```python
import functools

import jax
import jax.numpy as jnp
from jax import lax
from jax.experimental import pallas as pl
from jax.experimental.pallas import tpu as pltpu
from jax.sharding import PartitionSpec as P


HEADS = 32
KV_HEADS = 8
norm_eps = 1e-05
beta_one = 0.9
beta_two = 0.95
learn_rate = 0.01
weight_decay = 0.1
adam_eps = 1e-08
step_count = 10.0
masked_score = -1e30


HEAD_DIM = 64
LANES = 128


def dot_t(a, b):
    return lax.dot_general(a, b, (((1,), (1,)), ((), ())), preferred_element_type=jnp.float32)


def dot_n(a, b):
    return lax.dot_general(a, b, (((1,), (0,)), ((), ())), preferred_element_type=jnp.float32)


def dot_c(a, b):
    return lax.dot_general(a, b, (((0,), (0,)), ((), ())), preferred_element_type=jnp.float32)


def swap_halves(u):
    lane = lax.broadcasted_iota(jnp.int32, u.shape, 1)
    return jnp.where(lane % 64 < 32, pltpu.roll(u, 96, 1), pltpu.roll(u, 32, 1))


def turn(u, cos_wide, sin_wide):
    return u * cos_wide + swap_halves(u) * sin_wide


def key_start(block, q_rows, reach):
    return max(0, (block * q_rows - reach + 1) // q_rows * q_rows)


def attn_forward_kernel(pairs, q_rows, reach, qkv_ref, cos_ref, sin_ref, seg_col_ref, seg_row_ref,
                        turned_ref, lse_ref, out_ref):
    full_len = qkv_ref.shape[0]
    lane = lax.broadcasted_iota(jnp.int32, (full_len, LANES), 1)
    low = lane < HEAD_DIM
    cos_q = cos_ref[...]
    sin_q = sin_ref[...]
    kv = qkv_ref[:, pairs * LANES:].astype(jnp.float32)
    kv16 = turn(kv, jnp.where(low, cos_q, 1.0), jnp.where(low, sin_q, 0.0)).astype(jnp.bfloat16)
    turned_ref[:, pairs * LANES:] = kv16
    kv32 = kv16.astype(jnp.float32)
    rolled = pltpu.roll(kv32, HEAD_DIM, 1)
    zero = jnp.zeros_like(kv32)
    keys = (jnp.where(low, kv32, zero).astype(jnp.bfloat16), jnp.where(low, zero, rolled).astype(jnp.bfloat16))
    vals = (jnp.where(low, rolled, zero).astype(jnp.bfloat16), jnp.where(low, zero, kv32).astype(jnp.bfloat16))
    for pair in range(pairs):
        cols = slice(pair * LANES, (pair + 1) * LANES)
        query = turn(qkv_ref[:, cols].astype(jnp.float32), cos_q, sin_q) .astype(jnp.bfloat16)
        turned_ref[:, cols] = query
    for block in range(full_len // q_rows):
        first = key_start(block, q_rows, reach)
        last = (block + 1) * q_rows
        rows = slice(block * q_rows, last)
        span = slice(first, last)
        i = lax.broadcasted_iota(jnp.int32, (q_rows, last - first), 0) + block * q_rows
        j = lax.broadcasted_iota(jnp.int32, (q_rows, last - first), 1) + first
        allowed = (j <= i) & (seg_col_ref[rows, :1] == seg_row_ref[:1, span])
        for pair in range(pairs):
            cols = slice(pair * LANES, (pair + 1) * LANES)
            query = turned_ref[rows, cols]
            total = None
            for half in range(2):
                scores = dot_t(query, keys[half][span]) * (HEAD_DIM ** -0.5)
                scores = jnp.where(allowed, scores, masked_score)
                top = jnp.max(scores, axis=1, keepdims=True)
                lse = top + jnp.log(jnp.sum(jnp.exp(scores - top), axis=1, keepdims=True))
                probs = jnp.exp(scores - lse).astype(jnp.bfloat16)
                part = dot_n(probs, vals[half][span])
                total = part if total is None else total + part
                head = 2 * pair + half
                lse_ref[rows, head:head + 1] = lse
            out_ref[rows, cols] = total.astype(jnp.bfloat16)


def attn_backward_kernel(pairs, q_rows, reach, turned_ref, d_out_ref, lse_ref, cos_ref, sin_ref, seg_col_ref,
                         seg_row_ref, grad_ref, dk_ref, dv_ref):
    full_len = turned_ref.shape[0]
    lane = lax.broadcasted_iota(jnp.int32, (full_len, LANES), 1)
    low = lane < HEAD_DIM
    kv32 = turned_ref[:, pairs * LANES:].astype(jnp.float32)
    rolled = pltpu.roll(kv32, HEAD_DIM, 1)
    zero = jnp.zeros_like(kv32)
    keys = (jnp.where(low, kv32, zero).astype(jnp.bfloat16), jnp.where(low, zero, rolled).astype(jnp.bfloat16))
    vals = (jnp.where(low, rolled, zero).astype(jnp.bfloat16), jnp.where(low, zero, kv32).astype(jnp.bfloat16))
    dk_ref[...] = jnp.zeros_like(dk_ref)
    dv_ref[...] = jnp.zeros_like(dv_ref)
    low_rows = low[:q_rows]
    scale = HEAD_DIM ** -0.5
    for block in range(full_len // q_rows):
        first = key_start(block, q_rows, reach)
        last = (block + 1) * q_rows
        rows = slice(block * q_rows, last)
        span = slice(first, last)
        i = lax.broadcasted_iota(jnp.int32, (q_rows, last - first), 0) + block * q_rows
        j = lax.broadcasted_iota(jnp.int32, (q_rows, last - first), 1) + first
        allowed = (j <= i) & (seg_col_ref[rows, :1] == seg_row_ref[:1, span])
        cos_q = cos_ref[rows]
        sin_q = sin_ref[rows]
        for pair in range(pairs):
            cols = slice(pair * LANES, (pair + 1) * LANES)
            query = turned_ref[rows, cols]
            d_out = d_out_ref[rows, cols]
            q32 = query.astype(jnp.float32)
            o32 = d_out.astype(jnp.float32)
            d_query = None
            d_key = None
            d_val = None
            for half in range(2):
                keep = low_rows if half == 0 else ~low_rows
                q_only = jnp.where(keep, q32, 0.0).astype(jnp.bfloat16)
                o_only = jnp.where(keep, o32, 0.0).astype(jnp.bfloat16)
                head = 2 * pair + half
                scores = dot_t(query, keys[half][span]) * scale
                scores = jnp.where(allowed, scores, masked_score)
                probs = jnp.exp(scores - lse_ref[rows, head:head + 1])
                d_probs = dot_t(d_out, vals[half][span])
                delta = jnp.sum(probs * d_probs, axis=1, keepdims=True)
                d_scores = (probs * (d_probs - delta) * scale).astype(jnp.bfloat16)
                probs16 = probs.astype(jnp.bfloat16)
                dq = dot_n(d_scores, keys[half][span])
                dk = dot_c(d_scores, q_only)
                dv = dot_c(probs16, o_only)
                d_query = dq if d_query is None else d_query + dq
                d_key = dk if d_key is None else d_key + dk
                d_val = dv if d_val is None else d_val + dv
            dk_ref[span] = dk_ref[span] + d_key
            dv_ref[span] = dv_ref[span] + d_val
            grad_ref[rows, cols] = turn(d_query, cos_q, -sin_q).astype(jnp.bfloat16)
    d_key = dk_ref[...]
    d_val = dv_ref[...]
    d_key = d_key + pltpu.roll(d_key, HEAD_DIM, 1)
    d_val = d_val + pltpu.roll(d_val, HEAD_DIM, 1)
    d_key = turn(d_key, cos_ref[...], -sin_ref[...])
    grad_ref[:, pairs * LANES:] = jnp.where(low, d_key, d_val).astype(jnp.bfloat16)


def attn_specs(full_len, width):
    line = pl.BlockSpec((full_len, width), lambda s, g: (s, g))
    table = pl.BlockSpec((full_len, LANES), lambda s, g: (s, 0))
    row = pl.BlockSpec((8, full_len), lambda s, g: (s, 0))
    return line, table, row


Q_ROWS = 128
REACH = 256


def attn_gather_kernel(n_dp, pairs, q_rows, reach, qkv_ref, cos_ref, sin_ref, seg_col_ref, seg_row_ref, vo_ref,
                       turned_ref, lse_ref, out_ref, wo, d_s, d_r, loc):
    _, z, pair, c = place()
    n_d = n_dp // 2
    step = pl.program_id(1)
    steps = pl.num_programs(1)
    rows = vo_ref.shape[0]
    parts = 2
    part = rows // parts // 2

    def spot(owner, t, h):
        return wo.at[pl.ds(pl.multiple_of(owner * rows + (2 * t + h) * part, part), part)]

    spread = Spread(n_d, pair, c, z, parts, spot, d_s, d_r)
    keep = pltpu.make_async_copy(vo_ref, wo.at[pl.ds(pl.multiple_of(pair * rows, rows), rows)], loc)

    @pl.when(step == 0)
    def _():
        keep.start()
        barrier = pltpu.get_barrier_semaphore()
        for k in range(1, n_d):
            pl.semaphore_signal(barrier, inc=1, device_id=(2 * (pair ^ k) + c, z), device_id_type=MESH)
        pl.semaphore_wait(barrier, n_d - 1)
        keep.wait()
        for t in range(parts):
            spread.own(t)

    attn_forward_kernel(pairs, q_rows, reach, qkv_ref, cos_ref, sin_ref, seg_col_ref, seg_row_ref, turned_ref, lse_ref, out_ref)

    @pl.when(step == steps - 2)
    def _():
        spread.pass_on(0)

    @pl.when(step == steps - 1)
    def _():
        spread.pass_on(1)
        spread.finish()


def attn_forward(qkv, cos, sin, seg_col, seg_row, vo, full_len, groups, n_dp):
    pairs = groups // 2
    width = (groups + 2) * HEAD_DIM
    seqs = qkv.shape[0] // full_len
    kv = qkv.shape[1] // width
    n_d = n_dp // 2
    line, table, row = attn_specs(full_len, width)
    outw = pl.BlockSpec((full_len, groups * HEAD_DIM), lambda s, g: (s, g))
    rows = seqs * full_len
    return pl.pallas_call(
        functools.partial(attn_gather_kernel, n_dp, pairs, Q_ROWS, REACH),
        grid=(seqs, kv),
        in_specs=[line, table, table, table, row, VMEM_SPEC],
        out_specs=[line, pl.BlockSpec((full_len, LANES), lambda s, g: (s, g)), outw, ANY_SPEC],
        out_shape=[
            jax.ShapeDtypeStruct((rows, kv * width), jnp.bfloat16),
            jax.ShapeDtypeStruct((rows, kv * LANES), jnp.float32),
            jax.ShapeDtypeStruct((rows, kv * groups * HEAD_DIM), jnp.bfloat16),
            jax.ShapeDtypeStruct((n_d * vo.shape[0], vo.shape[1]), jnp.bfloat16),
        ],
        scratch_shapes=[DMA((n_d - 1, 2, 2)), DMA((n_d - 1, 2, 2)), DMA],
        compiler_params=pltpu.CompilerParams(collective_id=4, has_side_effects=True),
        cost_estimate=pl.CostEstimate(flops=4 * rows * full_len * kv * LANES * groups, bytes_accessed=150_000_000, transcendentals=0),
        name="attn_forward",
    )(qkv, cos, sin, seg_col, seg_row, vo)


def attn_backward(turned, d_out, lse, cos, sin, seg_col, seg_row, full_len, groups):
    pairs = groups // 2
    width = (groups + 2) * HEAD_DIM
    seqs = turned.shape[0] // full_len
    kv = turned.shape[1] // width
    line, table, row = attn_specs(full_len, width)
    outw = pl.BlockSpec((full_len, groups * HEAD_DIM), lambda s, g: (s, g))
    rows = seqs * full_len
    return pl.pallas_call(
        functools.partial(attn_backward_kernel, pairs, Q_ROWS, REACH),
        grid=(seqs, kv),
        in_specs=[line, outw, pl.BlockSpec((full_len, LANES), lambda s, g: (s, g)), table, table, table, row],
        out_specs=line,
        out_shape=jax.ShapeDtypeStruct((rows, kv * width), jnp.bfloat16),
        scratch_shapes=[pltpu.VMEM((full_len, LANES), jnp.float32)] * 2,
        cost_estimate=pl.CostEstimate(flops=10 * rows * full_len * kv * LANES * groups, bytes_accessed=rows * kv * width * 6, transcendentals=0),
        name="attn_backward",
    )(turned, d_out, lse, cos, sin, seg_col, seg_row)


def attn_tables(segment_ids):
    seqs, full_len = segment_ids.shape
    earlier = (segment_ids[..., None, :] < segment_ids[..., :, None]).astype(jnp.int32)
    positions = jnp.arange(full_len, dtype=jnp.int32) - jnp.sum(earlier, axis=-1, dtype=jnp.int32)
    inverse = 500000.0 ** (-2.0 * jnp.arange(HEAD_DIM // 2, dtype=jnp.float32) / HEAD_DIM)
    angles = positions.astype(jnp.float32)[..., None] * inverse
    cos = jnp.cos(angles)
    sin = jnp.sin(angles)
    cos = jnp.concatenate([cos] * 4, -1).reshape(seqs * full_len, LANES)
    sin = jnp.concatenate([-sin, sin] * 2, -1).reshape(seqs * full_len, LANES)
    seg_col = jnp.broadcast_to(segment_ids[:, :, None], (seqs, full_len, LANES)).reshape(seqs * full_len, LANES)
    seg_row = jnp.broadcast_to(segment_ids[:, None, :], (seqs, 8, full_len)).reshape(seqs * 8, full_len)
    return cos, sin, seg_col, seg_row


MESH = pl.DeviceIdType.MESH
VMEM_SPEC = pl.BlockSpec(memory_space=pltpu.VMEM)
ANY_SPEC = pl.BlockSpec(memory_space=pl.ANY)
DMA = pltpu.SemaphoreType.DMA


def place():
    d = lax.axis_index("dp")
    z = lax.axis_index("seq")
    return d, z, d // 2, d % 2


def remote(src, dst, send, recv, dev):
    return pltpu.make_async_remote_copy(
        src_ref=src, dst_ref=dst, send_sem=send, recv_sem=recv, device_id=dev, device_id_type=MESH
    )


def greet_all(n_dp, n_z, d, z):
    barrier = pltpu.get_barrier_semaphore()
    me = d * n_z + z

    def one(o, carry):
        other = lax.rem(me + o, n_dp * n_z)
        pl.semaphore_signal(barrier, inc=1, device_id=(other // n_z, lax.rem(other, n_z)), device_id_type=MESH)
        return carry

    lax.fori_loop(1, n_dp * n_z, one, 0)
    pl.semaphore_wait(barrier, n_dp * n_z - 1)


def greet_line(n_z, d, z, extra=()):
    barrier = pltpu.get_barrier_semaphore()
    c = d % 2
    for o in range(n_z):
        zz = lax.rem(z + o, n_z)
        for core in range(2):
            if o == 0 and core == 0:
                continue
            pl.semaphore_signal(barrier, inc=1, device_id=(d - c + lax.rem(c + core, 2), zz), device_id_type=MESH)
    for dev in extra:
        pl.semaphore_signal(barrier, inc=1, device_id=dev, device_id_type=MESH)
    pl.semaphore_wait(barrier, 2 * n_z - 1 + len(extra))


def block_at(ref, shape, row, col):
    return ref.at[pl.ds(pl.multiple_of(row * shape[0], shape[0]), shape[0]),
                  pl.ds(pl.multiple_of(col * shape[1], shape[1]), shape[1])]


class Spread:
    def __init__(self, n_d, pair, c, z, parts, spot, send, recv):
        self.n_d, self.pair, self.parts, self.spot = n_d, pair, parts, spot
        self.send, self.recv = send, recv
        self.dev = lambda k: (2 * (pair ^ k) + c, z)

    def copy(self, slot, owner, t, h, to):
        at = self.spot(owner, t, h)
        return remote(at, at, self.send.at[slot, t, h], self.recv.at[slot, t, h], self.dev(to))

    def own(self, t):
        if self.n_d == 4:
            for h in range(2):
                self.copy(0, self.pair, t, h, 1).start()
                self.copy(1, self.pair, t, 1 - h, 2).start()
        else:
            for k in range(1, self.n_d):
                for h in range(2):
                    self.copy(k - 1, self.pair, t, h, k).start()

    def pass_on(self, t):
        if self.n_d == 4:
            self.copy(0, self.pair ^ 1, t, 0, 1).wait_recv()
            self.copy(2, self.pair ^ 1, t, 0, 2).start()
            self.copy(1, self.pair ^ 2, t, 1, 2).wait_recv()
            self.copy(2, self.pair ^ 2, t, 1, 1).start()

    def rest(self, t):
        if self.n_d == 4:
            self.copy(0, self.pair ^ 1, t, 1, 1).wait_recv()
            self.copy(1, self.pair ^ 2, t, 0, 2).wait_recv()
        else:
            for k in range(1, self.n_d):
                for h in range(2):
                    self.copy(k - 1, self.pair ^ k, t, h, k).wait_recv()

    def far(self, t):
        if self.n_d == 4:
            for h in range(2):
                self.copy(2, self.pair ^ 3, t, h, 1).wait_recv()

    def sent(self):
        for t in range(self.parts):
            for h in range(2):
                for slot in range(self.n_d - 1):
                    self.copy(slot, self.pair, t, h, 1).wait_send()

    def finish(self):
        for t in range(self.parts):
            if self.n_d == 4:
                self.copy(0, self.pair ^ 1, t, 1, 1).wait_recv()
                self.copy(1, self.pair ^ 2, t, 0, 2).wait_recv()
                for h in range(2):
                    self.copy(2, self.pair ^ 3, t, h, 1).wait_recv()
                    for slot in range(3):
                        self.copy(slot, self.pair, t, h, 1).wait_send()
            else:
                for k in range(1, self.n_d):
                    for h in range(2):
                        self.copy(k - 1, self.pair ^ k, t, h, k).wait_recv()
                        self.copy(k - 1, self.pair, t, h, k).wait_send()


def gather_in_kernel(n_dp, n_z, x_ref, w_ref, v_ref, g_ref, s_ref, xs, wq, vo, ga, sg,
                     x_s, x_r, f_s, f_r, w_s, w_r, v_s, v_r, d_s, d_r, g_s, g_r, s_s, s_r, loc):
    d, z, pair, c = place()
    n_d = n_dp // 2
    me = d * n_z + z
    total = n_dp * n_z
    rows = x_ref.shape[1]
    half = rows // 2
    shape = w_ref.shape
    cz = z // 2
    greet_all(n_dp, n_z, d, z)

    def line_stage(src, dst, send, recv, spare, wait):
        for o in range(n_z):
            copy = remote(src, dst, send.at[o], recv.at[c, z % 2], (2 * pair + cz, lax.rem(z + o, n_z)))
            act = copy.wait_send if wait else copy.start
            if o == 0:
                pl.when(c != cz)(act)
                if not wait:
                    pl.when(c == cz)(pltpu.make_async_copy(src, dst, loc.at[spare]).start)
            else:
                act()

    my_block = block_at(wq, shape, d, z % 2)
    line_stage(w_ref, my_block, w_s, w_r, 0, False)

    for i in range(2):
        for h in range(2):
            src = x_ref.at[i, pl.ds(h * half, half)]
            dst = xs.at[pl.ds(pl.multiple_of(z * rows + h * half, half), half)]
            zz = 2 * c + i
            mine = (h == c) & (zz == z)
            copy = remote(src, dst, x_s.at[i, h], x_r.at[z], (2 * pair + h, zz))
            pl.when(jnp.logical_not(mine))(copy.start)
            pl.when(mine)(lambda src=src, dst=dst: pltpu.make_async_copy(src, dst, loc.at[1]).start())

    seg_copy = remote(s_ref, sg.at[c], s_s, s_r, (2 * pair + 1 - c, z))
    seg_copy.start()
    own_seg = pltpu.make_async_copy(s_ref, sg.at[c], loc.at[2])
    own_seg.start()
    own_gain = pltpu.make_async_copy(g_ref, ga.at[me], loc.at[3])
    own_gain.start()

    def send_gain(o, carry):
        other = lax.rem(me + o, total)
        remote(g_ref, ga.at[me], g_s, g_r, (other // n_z, lax.rem(other, n_z))).start()
        return carry

    lax.fori_loop(1, total, send_gain, 0)

    first = jnp.where(c == cz, z % 2, 1 - c)

    def turn_of(t):
        return t % 2, (first if t < 2 else 1 - first)

    def spot(owner, t, h):
        core, b = turn_of(t)
        part = shape[0] // 2
        return wq.at[pl.ds(pl.multiple_of((2 * owner + core) * shape[0] + h * part, part), part),
                     pl.ds(pl.multiple_of(b * shape[1], shape[1]), shape[1])]

    spread = Spread(n_d, pair, c, z, 4, spot, d_s, d_r)
    for t in range(4):
        core, b = turn_of(t)
        blk = block_at(wq, shape, 2 * pair + core, b)
        mine = (core == c) & (2 * c + b == z)
        arrive = remote(w_ref, blk, w_s.at[0], w_r.at[core, b], (d, z))
        pl.when(jnp.logical_not(mine))(arrive.wait_recv)
        pl.when(mine)(lambda blk=blk: pltpu.make_async_copy(w_ref, blk, loc.at[0]).wait())
        spread.own(t)
        if t == 1:
            line_stage(v_ref, block_at(vo, v_ref.shape, c, z % 2), v_s, v_r, 4, False)
        if t > 0:
            spread.pass_on(t - 1)

    for o in range(n_z):
        zs = lax.rem(z + o, n_z)
        src = xs.at[pl.ds(pl.multiple_of(zs * rows + c * half, half), half)]
        mine = (cz == c) & (zs == z)
        arrive = remote(src, src, x_s.at[0, 0], x_r.at[zs], (d, z))
        pl.when(jnp.logical_not(mine))(arrive.wait_recv)
        pl.when(mine)(lambda src=src: pltpu.make_async_copy(src, src, loc.at[1]).wait())
        remote(src, src, f_s.at[zs], f_r.at[zs], (2 * pair + 1 - c, z)).start()
    spread.pass_on(3)

    line_stage(w_ref, my_block, w_s, w_r, 0, True)
    line_stage(v_ref, block_at(vo, v_ref.shape, c, z % 2), v_s, v_r, 4, True)
    for i in range(2):
        for h in range(2):
            src = x_ref.at[i, pl.ds(h * half, half)]
            mine = (h == c) & (2 * c + i == z)
            copy = remote(src, src, x_s.at[i, h], x_r.at[0], (d, z))
            pl.when(jnp.logical_not(mine))(copy.wait_send)
    for zs in range(n_z):
        src = xs.at[pl.ds(zs * rows, half)]
        copy = remote(src, src, f_s.at[zs], f_r.at[zs], (d, z))
        copy.wait_send()
        copy.wait_recv()
    for core in range(2):
        for b in range(2):
            blk = block_at(vo, v_ref.shape, core, b)
            mine = (core == c) & (2 * c + b == z)
            pl.when(jnp.logical_not(mine))(remote(blk, blk, v_s.at[0], v_r.at[core, b], (d, z)).wait_recv)
            pl.when(mine)(pltpu.make_async_copy(v_ref, blk, loc.at[4]).wait)
    seg_copy.wait_send()
    remote(s_ref, sg.at[1 - c], s_s, s_r, (d, z)).wait_recv()
    own_seg.wait()
    own_gain.wait()
    many = ga.at[pl.ds(0, total - 1)]
    gains = remote(many, many, g_s, g_r, (d, z))
    gains.wait_send()
    gains.wait_recv()
    spread.finish()


def gather_in(x_loc, w, v, gain_tile, seg_tile, n_dp, n_z):
    _, rows, width = x_loc.shape
    n_d = n_dp // 2
    total = n_dp * n_z
    return pl.pallas_call(
        functools.partial(gather_in_kernel, n_dp, n_z),
        in_specs=[VMEM_SPEC] * 5,
        out_specs=[ANY_SPEC] * 5,
        out_shape=[
            jax.ShapeDtypeStruct((rows * n_z, width), x_loc.dtype),
            jax.ShapeDtypeStruct((w.shape[0] * n_dp, 2 * w.shape[1]), w.dtype),
            jax.ShapeDtypeStruct((v.shape[0] * 2, 2 * v.shape[1]), v.dtype),
            jax.ShapeDtypeStruct((total,) + gain_tile.shape, gain_tile.dtype),
            jax.ShapeDtypeStruct((2,) + seg_tile.shape, seg_tile.dtype),
        ],
        scratch_shapes=[
            DMA((2, 2)), DMA((n_z,)), DMA((n_z,)), DMA((n_z,)), DMA((n_z,)), DMA((2, 2)), DMA((n_z,)), DMA((2, 2)),
            DMA((n_d - 1, 4, 2)), DMA((n_d - 1, 4, 2)), DMA, DMA, DMA, DMA, DMA((5,)),
        ],
        compiler_params=pltpu.CompilerParams(collective_id=1, has_side_effects=True),
        cost_estimate=pl.CostEstimate(flops=0, bytes_accessed=200_000_000, transcendentals=0),
        name="gather_in",
    )(x_loc, w, v, gain_tile, seg_tile)


def share_resid_kernel(n_dp, n_z, part_ref, x_ref, w_ref, out, wall, got, buf, p_s, p_r, u_s, u_r, d_s, d_r, c_s, c_r, loc):
    d, z, pair, c = place()
    n_d = n_dp // 2
    cz = z // 2
    full = x_ref.shape[0]
    half = full // 2
    unit = half // 2
    w_rows = w_ref.shape[0]
    parts = 4
    piece = w_rows // parts
    own_copy = pltpu.make_async_copy(w_ref, wall.at[pl.ds(pl.multiple_of(d * w_rows, w_rows), w_rows)], loc.at[2])
    own_copy.start()
    greet_line(n_z, d, z, [(2 * (pair ^ k) + c, z) for k in range(1, n_d)])
    mine = pl.ds(pl.multiple_of(c * half, half), half)
    theirs = pl.ds(pl.multiple_of((1 - c) * half, half), half)
    swap = remote(part_ref.at[theirs], got, p_s, p_r, (2 * pair + 1 - c, z))
    swap.start()

    def spot_w(owner, t, h):
        sub = piece // 2
        return wall.at[pl.ds(pl.multiple_of((2 * owner + c) * w_rows + (2 * t + h) * sub, sub), sub)]

    def across(k, t, core):
        at = wall.at[pl.ds(pl.multiple_of((2 * (pair ^ k) + core) * w_rows + t * piece, piece), piece)]
        return remote(at, at, c_s.at[k, t], c_r.at[k, t], (2 * pair + 1 - c, z))

    spread = Spread(n_d, pair, c, z, parts, spot_w, d_s, d_r)
    own_copy.wait()
    for t in range(parts):
        spread.own(t)
        across(0, t, c).start()

    swap.wait_recv()

    def add(r, carry):
        at = pl.ds(pl.multiple_of(r * 16, 16), 16)
        src = pl.ds(pl.multiple_of(c * half + r * 16, 16), 16)
        total = x_ref[src].astype(jnp.float32) + part_ref[src].astype(jnp.float32) + got[at].astype(jnp.float32)
        buf[at] = total.astype(jnp.bfloat16)
        return carry

    def spot(jl, h, k):
        return out.at[jl, pl.ds(pl.multiple_of(h * half + k * unit, unit), unit)]

    def sends(k, wait):
        src = buf.at[pl.ds(k * unit, unit)]
        dst = spot(z % 2, c, k)
        for o, zz in ((1, z - 1), (2, z + 1), (0, z)):
            copy = remote(src, dst, u_s.at[o, k], u_r.at[z % 2, c, k], (2 * pair + cz, zz))
            act = copy.wait_send if wait else copy.start
            if o == 0:
                keep = pltpu.make_async_copy(src, dst, loc.at[k])
                pl.when(c != cz)(act)
                pl.when(c == cz)(keep.wait if wait else keep.start)
            elif o == 1:
                pl.when(z > 0)(act)
            else:
                pl.when(z < n_z - 1)(act)

    per = unit // 16
    lax.fori_loop(0, per, add, 0)
    lax.fori_loop(per, per + per // 2, add, 0)
    sends(0, False)
    lax.fori_loop(per + per // 2, 2 * per, add, 0)
    swap.wait_send()
    sends(1, False)

    def relay(dist, sign, k, h, begin):
        j = z + sign * dist
        ok = (j >= 2 * c) & (j <= 2 * c + 1)
        to = z - sign
        more = (to >= 0) & (to <= n_z - 1)
        jl = lax.rem(j + n_z, 2)
        at = spot(jl, h, k)
        copy = remote(at, at, u_s.at[3 + (0 if sign < 0 else 1), 4 * jl + 2 * h + k], u_r.at[jl, h, k], (2 * pair + c, to))
        if begin:

            @pl.when(ok)
            def _():
                copy.wait_recv()
                pl.when(more)(copy.start)
        else:
            pl.when(ok & more)(copy.wait_send)

    def take(t):
        spread.pass_on(t)

    def rest(t):
        spread.rest(t)
        for k in range(1, n_d):
            if n_d != 4 or k != 3:
                across(k, t, c).start()

    def far(t):
        if n_d == 4:
            spread.far(t)
            across(3, t, c).start()

    links = []
    for t in range(parts):
        links += [(take, t), (rest, t)]
    links += [(far, t) for t in range(parts)]
    line = [(dist, k, h) for dist in range(1, n_z) for k in range(2) for h in range(2)]
    for n in range(max(len(links), len(line))):
        if n < len(line):
            dist, k, h = line[n]
            for sign in (-1, 1):
                relay(dist, sign, k, h, True)
        if n < len(links):
            links[n][0](links[n][1])

    @pl.when(c == cz)
    def _():
        for k in range(2):
            at = spot(z % 2, 1 - c, k)
            remote(at, at, u_s.at[0, 0], u_r.at[z % 2, 1 - c, k], (d, z)).wait_recv()

    for dist, k, h in line:
        for sign in (-1, 1):
            relay(dist, sign, k, h, False)
    sends(0, True)
    sends(1, True)
    spread.sent()
    for k in range(n_d):
        for t in range(parts):
            across(k, t, c).wait_send()
            across(k, t, 1 - c).wait_recv()


def share_resid(part, x, w, n_dp, n_z):
    full, width = x.shape
    n_d = n_dp // 2
    return pl.pallas_call(
        functools.partial(share_resid_kernel, n_dp, n_z),
        in_specs=[VMEM_SPEC] * 3,
        out_specs=[ANY_SPEC] * 2,
        out_shape=[
            jax.ShapeDtypeStruct((2, full, width), jnp.bfloat16),
            jax.ShapeDtypeStruct((n_dp * w.shape[0], w.shape[1]), jnp.bfloat16),
        ],
        scratch_shapes=[
            pltpu.VMEM((full // 2, width), jnp.bfloat16), pltpu.VMEM((full // 2, width), jnp.bfloat16),
            DMA, DMA, DMA((5, 8)), DMA((2, 2, 2)), DMA((n_d - 1, 4, 2)), DMA((n_d - 1, 4, 2)), DMA((n_d, 4)), DMA((n_d, 4)),
            DMA((3,)),
        ],
        compiler_params=pltpu.CompilerParams(collective_id=2, has_side_effects=True),
        cost_estimate=pl.CostEstimate(flops=0, bytes_accessed=200_000_000, transcendentals=0),
        name="share_resid",
    )(part, x, w)


CHUNKS = 8


def sum_line_kernel(n_z, part_ref, resid_all, cot_all, gain_ref, d_out, gain_out, got, buf, resid_ref, cot_ref,
                    s_s, s_r, p_s, p_r, loc, rows_sem):
    d, z, pair, c = place()
    cz = z // 2
    full, _ = buf.shape
    rows = full // CHUNKS
    fetch = (
        pltpu.make_async_copy(resid_all.at[z % 2], resid_ref, rows_sem.at[0]),
        pltpu.make_async_copy(cot_all.at[z % 2], cot_ref, rows_sem.at[1]),
    )
    for one in fetch:
        one.start()
    greet_line(n_z, d, z)
    gain_out[...] = jnp.zeros_like(gain_out)
    own = c == cz
    steps = [(k, t) for k in range(CHUNKS) for t in range(2)]

    def where_is(k, t):
        jl = jnp.bitwise_xor(c, t)
        return jl, 2 * c + jl, pl.ds(k * rows, rows)

    def copy_on(k, t, side, src):
        jl, _, at = where_is(k, t)
        to = z + 1 if side == 0 else z - 1
        return remote(src, got.at[side, jl, at], s_s.at[t, k], s_r.at[side, jl, k], (2 * pair + c, to))

    def arrived(side, jl, k):
        at = got.at[side, jl, pl.ds(k * rows, rows)]
        return remote(at, at, s_s.at[0, 0], s_r.at[side, jl, k], (d, z))

    def add_in(side, jl, k):
        def one(r, carry):
            at = pl.ds(pl.multiple_of(k * rows + r * 16, 16), 16)
            got[side, jl, at] = (got[side, jl, at].astype(jnp.float32) + part_ref[jl, at].astype(jnp.float32)).astype(jnp.bfloat16)
            return carry

        lax.fori_loop(0, rows // 16, one, 0)

    def finish(jl, k):
        def one(r, carry):
            at = pl.ds(pl.multiple_of(k * rows + r * 16, 16), 16)
            total = part_ref[jl, at].astype(jnp.float32)
            left = got[0, jl, at].astype(jnp.float32)
            right = got[1, jl, at].astype(jnp.float32)
            total = total + jnp.where(z > 0, left, 0.0) + jnp.where(z < n_z - 1, right, 0.0)
            value = resid_ref[at].astype(jnp.float32)
            inverse = lax.rsqrt(jnp.mean(value * value, axis=-1, keepdims=True) + norm_eps)
            scaled = value * inverse
            d_scaled = total * gain_ref[...]
            mean = jnp.mean(d_scaled * scaled, axis=-1, keepdims=True)
            d_resid = cot_ref[at].astype(jnp.float32) + inverse * (d_scaled - scaled * mean)
            buf[at] = d_resid.astype(jnp.bfloat16)
            prod = total * scaled
            gain_out[...] = gain_out[...] + prod[:8] + prod[8:]
            return carry

        lax.fori_loop(0, rows // 16, one, 0)

    def to_partner(k):
        at = pl.ds(k * rows, rows)
        return remote(buf.at[at], d_out.at[at], p_s.at[k], p_r.at[k], (2 * pair + 1 - c, z))

    def keep(k):
        at = pl.ds(k * rows, rows)
        return pltpu.make_async_copy(buf.at[at], d_out.at[at], loc.at[k])

    def send_step(k, t, wait):
        jl, j, at = where_is(k, t)
        for side in range(2):
            going = (z < j) if side == 0 else (z > j)
            edge = (z == 0) if side == 0 else (z == n_z - 1)
            edge_copy = copy_on(k, t, side, part_ref.at[jl, at])
            inner_copy = copy_on(k, t, side, got.at[side, jl, at])
            pl.when(going & edge)(edge_copy.wait_send if wait else edge_copy.start)
            pl.when(going & jnp.logical_not(edge))(inner_copy.wait_send if wait else inner_copy.start)

    def publish(k, wait):
        @pl.when(own)
        def _():
            if wait:
                to_partner(k).wait_send()
                keep(k).wait()
            else:
                to_partner(k).start()
                keep(k).start()

    def own_chunk(k):
        @pl.when(own)
        def _():
            if k == 0:
                for one in fetch:
                    one.wait()
            jl = z % 2
            pl.when(z > 0)(arrived(0, jl, k).wait_recv)
            pl.when(z < n_z - 1)(arrived(1, jl, k).wait_recv)
            finish(jl, k)
            if k > 0:
                to_partner(k - 1).start()
                keep(k - 1).start()

    for n, (k, t) in enumerate(steps):
        jl, j, at = where_is(k, t)
        for side in range(2):
            going = (z < j) if side == 0 else (z > j)
            inner = (z > 0) if side == 0 else (z < n_z - 1)

            @pl.when(going & inner)
            def _():
                arrived(side, jl, k).wait_recv()
                add_in(side, jl, k)

        if n > 0:
            send_step(*steps[n - 1], False)
        if t == 1 and k > 0:
            own_chunk(k - 1)
    send_step(*steps[-1], False)
    own_chunk(CHUNKS - 1)

    @pl.when(jnp.logical_not(own))
    def _():
        for one in fetch:
            one.wait()

    @pl.when(own)
    def _():
        to_partner(CHUNKS - 1).start()
        keep(CHUNKS - 1).start()

    for k, t in steps:
        send_step(k, t, True)
    for k in range(CHUNKS):
        publish(k, True)
        at = d_out.at[pl.ds(k * rows, rows)]
        pl.when(jnp.logical_not(own))(remote(at, at, p_s.at[k], p_r.at[k], (d, z)).wait_recv)


def sum_line(part, resid, cot, gain, n_z):
    _, full, width = part.shape
    return pl.pallas_call(
        functools.partial(sum_line_kernel, n_z),
        in_specs=[VMEM_SPEC, ANY_SPEC, ANY_SPEC, VMEM_SPEC],
        out_specs=[ANY_SPEC, VMEM_SPEC],
        out_shape=[jax.ShapeDtypeStruct((full, width), jnp.bfloat16), jax.ShapeDtypeStruct((8, width), jnp.float32)],
        scratch_shapes=[
            pltpu.VMEM((2, 2, full, width), jnp.bfloat16), pltpu.VMEM((full, width), jnp.bfloat16),
            pltpu.VMEM((full, width), jnp.bfloat16), pltpu.VMEM((full, width), jnp.bfloat16),
            DMA((2, CHUNKS)), DMA((2, 2, CHUNKS)), DMA((CHUNKS,)), DMA((CHUNKS,)), DMA((CHUNKS,)), DMA((2,)),
        ],
        compiler_params=pltpu.CompilerParams(collective_id=3, has_side_effects=True, vmem_limit_bytes=56 * 1024 * 1024),
        cost_estimate=pl.CostEstimate(flops=0, bytes_accessed=200_000_000, transcendentals=0),
        name="sum_line",
    )(part, resid, cot, gain)


def hand_out_kernel(n_dp, n_z, dn_ref, x_ref, dr_ref, gain_ref, gain2_ref, qt_ref, ot_ref,
                    ig, gq, go, gains, got, buf, q_got, q_own, q_mid, q_put, q_fin, o_got, o_own, o_mid, o_put, o_fin, g_src, g_all,
                    p_s, p_r, i_s, i_r, q_s, q_r, qf_s, qf_r, o_s, o_r, of_s, of_r, g_s, g_r, loc):
    d, z, pair, c = place()
    n_d = n_dp // 2
    total = n_dp * n_z
    me = d * n_z + z
    cz = z // 2
    full, width = x_ref.shape
    half = full // 2
    quarter = half // 2
    q_rows, q_cols = q_fin.shape[1:]
    o_rows, o_cols = o_fin.shape[1:]
    relay = n_d == 4

    def region(ref, rows, cols, owner, b):
        return ref.at[pl.ds(pl.multiple_of(owner * 2 * rows, 2 * rows), 2 * rows), pl.ds(b * cols, cols)]

    class First:
        def __init__(self, src, rows, cols, got_ref, own_ref, mid_ref, put_ref, send, recv, spare):
            self.src, self.rows, self.cols, self.got, self.own, self.mid = src, rows, cols, got_ref, own_ref, mid_ref
            self.put, self.send, self.recv, self.spare = put_ref, send, recv, spare

        def slot(self, n, b):
            return self.got.at[n, :, pl.ds(b * self.cols, self.cols)]

        def copy(self, n, b, owner, to):
            src = region(self.src, self.rows, self.cols, owner, b)
            return remote(src, self.slot(n, b), self.send.at[n, b], self.recv.at[n, b], (2 * (pair ^ to) + c, z))

        def load(self, b):
            yield pltpu.make_async_copy(region(self.src, self.rows, self.cols, pair, b), self.own.at[:, pl.ds(b * self.cols, self.cols)], loc.at[self.spare + b])
            if relay:
                yield pltpu.make_async_copy(region(self.src, self.rows, self.cols, pair ^ (2 >> b), b), self.mid.at[:, pl.ds(b * self.cols, self.cols)], loc.at[self.spare + 2 + b])

        def begin(self, b):
            if relay:
                near = 1 + b
                self.copy(1, b, pair ^ 3, near).start()
                self.copy(0, b, pair ^ near, near).start()
            else:
                for k in range(1, n_d):
                    self.copy(k - 1, b, pair ^ k, k).start()

        def arrived(self, n, b):
            remote(self.slot(n, b), self.slot(n, b), self.send.at[n, b], self.recv.at[n, b], (d, z)).wait_recv()

        def middle(self, b):
            if not relay:
                return
            self.arrived(1, b)
            lanes = pl.ds(b * self.cols, self.cols)

            def add(r, carry):
                at = pl.ds(pl.multiple_of(r * 16, 16), 16)
                self.mid[at, lanes] = (self.mid[at, lanes].astype(jnp.float32) + self.got[1, at, lanes].astype(jnp.float32)).astype(jnp.bfloat16)
                return carry

            lax.fori_loop(0, 2 * self.rows // 16, add, 0)

        def middle_copy(self, b):
            src = self.mid.at[:, pl.ds(b * self.cols, self.cols)]
            return remote(src, self.slot(2, b), self.send.at[2, b], self.recv.at[2, b], (2 * (pair ^ (2 >> b)) + c, z))

        def total(self, b):
            slots = (0, 2) if relay else range(n_d - 1)
            for n in slots:
                self.arrived(n, b)
            lanes = pl.ds(b * self.cols, self.cols)
            for core in range(2):

                def add(r, carry):
                    at = pl.ds(pl.multiple_of(r * 16, 16), 16)
                    src = pl.ds(pl.multiple_of(core * self.rows + r * 16, 16), 16)
                    value = self.own[src, lanes].astype(jnp.float32)
                    for n in slots:
                        value = value + self.got[n, src, lanes].astype(jnp.float32)
                    self.put[core, b, at] = value.astype(jnp.bfloat16)
                    return carry

                lax.fori_loop(0, self.rows // 16, add, 0)

        def sent(self, b):
            for n in range(n_d - 1):
                remote(self.slot(n, b), self.slot(n, b), self.send.at[n, b], self.recv.at[n, b], (d, z)).wait_send()

    o_first = First(ot_ref, o_rows, o_cols, o_got, o_own, o_mid, o_put, o_s, o_r, 6)
    q_first = First(qt_ref, q_rows, q_cols, q_got, q_own, q_mid, q_put, q_s, q_r, 10)
    firsts = [(o_first, 0), (o_first, 1), (q_first, 0), (q_first, 1)]
    for one, b in firsts:
        for copy in one.load(b):
            copy.start()
    greet_all(n_dp, n_z, d, z)

    mine = pl.ds(pl.multiple_of(c * half, half), half)
    theirs = pl.ds(pl.multiple_of((1 - c) * half, half), half)
    swap = remote(dn_ref.at[theirs], got, p_s, p_r, (2 * pair + 1 - c, z))
    swap.start()
    for one, b in firsts:
        one.begin(b)

    g_src[pl.ds(0, 8)] = jnp.zeros((8, width), jnp.float32)
    g_src[pl.ds(8, 8)] = gain2_ref[...]
    swap.wait_recv()

    def rows_of(r, carry):
        at = pl.ds(pl.multiple_of(r * 16, 16), 16)
        src = pl.ds(pl.multiple_of(c * half + r * 16, 16), 16)
        d_normed = dn_ref[src].astype(jnp.float32) + got[at].astype(jnp.float32)
        value = x_ref[src].astype(jnp.float32)
        inverse = lax.rsqrt(jnp.mean(value * value, axis=-1, keepdims=True) + norm_eps)
        scaled = value * inverse
        d_scaled = d_normed * gain_ref[...]
        mean = jnp.mean(d_scaled * scaled, axis=-1, keepdims=True)
        out = dr_ref[src].astype(jnp.float32) + inverse * (d_scaled - scaled * mean)
        buf[at] = out.astype(jnp.bfloat16)
        prod = d_normed * scaled
        g_src[pl.ds(0, 8)] = g_src[pl.ds(0, 8)] + prod[:8] + prod[8:]
        return carry

    def row_send(b, wait):
        src = buf.at[pl.ds(b * quarter, quarter)]
        dst = ig.at[z % 2]
        zz = 2 * c + b
        here = (cz == c) & (zz == z)
        copy = remote(src, dst, i_s.at[b], i_r.at[z % 2], (2 * pair + cz, zz))
        keep = pltpu.make_async_copy(src, dst, loc.at[2])
        pl.when(jnp.logical_not(here))(copy.wait_send if wait else copy.start)
        pl.when(here)(keep.wait if wait else keep.start)

    per = quarter // 16
    lax.fori_loop(0, per, rows_of, 0)
    lax.fori_loop(per, per + per // 2, rows_of, 0)
    row_send(0, False)
    lax.fori_loop(per + per // 2, 2 * per, rows_of, 0)
    for one, b in firsts:
        for copy in one.load(b):
            copy.wait()
    row_send(1, False)

    each = width // total

    def gain_tile(o):
        return g_src.at[:, pl.ds(pl.multiple_of(o * each // 128 * 128, 128), 128)]

    own_gain = pltpu.make_async_copy(gain_tile(me), g_all.at[me], loc.at[3])
    own_gain.start()

    def send_gain(o, carry):
        other = lax.rem(me + o, total)
        remote(gain_tile(other), g_all.at[me], g_s, g_r, (other // n_z, lax.rem(other, n_z))).start()
        return carry

    lax.fori_loop(1, total, send_gain, 0)

    def second_send(b, put_ref, fin_ref, f_s, f_r, spare, wait):
        for core in range(2):
            here = (core == c) & (2 * c + b == z)
            src = put_ref.at[core, b]
            copy = remote(src, fin_ref.at[z], f_s.at[core, b], f_r.at[z], (2 * pair + core, 2 * c + b))
            keep = pltpu.make_async_copy(src, fin_ref.at[z], loc.at[spare])
            pl.when(jnp.logical_not(here))(copy.wait_send if wait else copy.start)
            pl.when(here)(keep.wait if wait else keep.start)

    def last(rows, fin_ref, out_ref):
        def add(r, carry):
            at = pl.ds(pl.multiple_of(r * 16, 16), 16)
            value = fin_ref[0, at].astype(jnp.float32)
            for zs in range(1, n_z):
                value = value + fin_ref[zs, at].astype(jnp.float32)
            out_ref[at] = value
            return carry

        lax.fori_loop(0, rows // 16, add, 0)

    o_args = (o_put, o_fin, of_s, of_r, 4)
    q_args = (q_put, q_fin, qf_s, qf_r, 5)
    if relay:
        for n, (one, b) in enumerate(firsts):
            one.middle(b)
            if n:
                last_one, last_b = firsts[n - 1]
                last_one.middle_copy(last_b).start()
    o_first.total(0)
    if relay:
        q_first.middle_copy(1).start()
    o_first.total(1)
    second_send(0, *o_args, False)
    q_first.total(0)
    second_send(1, *o_args, False)
    q_first.total(1)
    second_send(0, *q_args, False)

    def arrived(fin_ref, f_s, f_r):
        for zs in range(n_z):
            at = fin_ref.at[zs]
            from_here = (cz == c) & (zs == z)
            pl.when(jnp.logical_not(from_here))(remote(at, at, f_s.at[0, 0], f_r.at[zs], (d, z)).wait_recv)

    def own_done(args):
        for b in range(2):
            second_send(b, *args, True)

    own_done(o_args)
    arrived(o_fin, of_s, of_r)
    value = o_fin[0].astype(jnp.float32)
    for zs in range(1, n_z):
        value = value + o_fin[zs].astype(jnp.float32)
    go[...] = value.T
    second_send(1, *q_args, False)
    own_done(q_args)
    arrived(q_fin, qf_s, qf_r)
    last(q_rows, q_fin, gq)

    many = g_all.at[pl.ds(0, total - 1)]
    gain_copy = remote(many, many, g_s, g_r, (d, z))
    gain_copy.wait_send()
    gain_copy.wait_recv()
    own_gain.wait()
    gains[...] = jnp.zeros_like(gains)

    def add_gain(o, carry):
        gains[...] = gains[...] + g_all[o]
        return carry

    lax.fori_loop(0, total, add_gain, 0)

    swap.wait_send()
    for b in range(2):
        row_send(b, True)
        o_first.sent(b)
        q_first.sent(b)
    for i in range(2):
        from_here = (cz == c) & (2 * c + i == z)
        at = ig.at[i]
        pl.when(jnp.logical_not(from_here))(remote(at, at, i_s.at[0], i_r.at[i], (d, z)).wait_recv)


def hand_out(dn, x, dr, gain, gain2, qt, ot, n_dp, n_z):
    full, width = x.shape
    n_d = n_dp // 2
    total = n_dp * n_z
    q_rows, q_cols = qt.shape[0] // n_dp, qt.shape[1] // 2
    o_rows, o_cols = ot.shape[0] // n_dp, ot.shape[1] // 2
    b16 = jnp.bfloat16
    return pl.pallas_call(
        functools.partial(hand_out_kernel, n_dp, n_z),
        in_specs=[VMEM_SPEC] * 5 + [ANY_SPEC] * 2,
        out_specs=[ANY_SPEC] + [VMEM_SPEC] * 3,
        out_shape=[
            jax.ShapeDtypeStruct((2, full // 4, width), b16),
            jax.ShapeDtypeStruct((q_rows, q_cols), jnp.float32),
            jax.ShapeDtypeStruct((o_cols, o_rows), jnp.float32),
            jax.ShapeDtypeStruct((16, 128), jnp.float32),
        ],
        scratch_shapes=[
            pltpu.VMEM((full // 2, width), b16), pltpu.VMEM((full // 2, width), b16),
            pltpu.VMEM((n_d - 1, 2 * q_rows, 2 * q_cols), b16), pltpu.VMEM((2 * q_rows, 2 * q_cols), b16),
            pltpu.VMEM((2 * q_rows, 2 * q_cols), b16),
            pltpu.VMEM((2, 2, q_rows, q_cols), b16), pltpu.VMEM((n_z, q_rows, q_cols), b16),
            pltpu.VMEM((n_d - 1, 2 * o_rows, 2 * o_cols), b16), pltpu.VMEM((2 * o_rows, 2 * o_cols), b16),
            pltpu.VMEM((2 * o_rows, 2 * o_cols), b16),
            pltpu.VMEM((2, 2, o_rows, o_cols), b16), pltpu.VMEM((n_z, o_rows, o_cols), b16),
            pltpu.VMEM((16, width), jnp.float32), pltpu.VMEM((total, 16, 128), jnp.float32),
            DMA, DMA, DMA((2,)), DMA((2,)), DMA((n_d - 1, 2)), DMA((n_d - 1, 2)), DMA((2, 2)), DMA((n_z,)),
            DMA((n_d - 1, 2)), DMA((n_d - 1, 2)), DMA((2, 2)), DMA((n_z,)), DMA, DMA, DMA((14,)),
        ],
        compiler_params=pltpu.CompilerParams(collective_id=5, has_side_effects=True, vmem_limit_bytes=56 * 1024 * 1024),
        cost_estimate=pl.CostEstimate(flops=0, bytes_accessed=300_000_000, transcendentals=0),
        name="hand_out",
    )(dn, x, dr, gain, gain2, qt, ot)


def rms_forward(values, gain_wide):
    inverse = lax.rsqrt(jnp.mean(values * values, axis=-1, keepdims=True) + norm_eps)
    scaled = values * inverse
    return (scaled, inverse, (scaled * gain_wide).astype(jnp.bfloat16))


def adam_update(weight, grad, first, second):
    new_first = beta_one * first + (1.0 - beta_one) * grad
    new_second = beta_two * second + (1.0 - beta_two) * grad * grad
    first_hat = new_first / (1.0 - beta_one**step_count)
    second_hat = new_second / (1.0 - beta_two**step_count)
    new_weight = weight - learn_rate * (
        first_hat / (jnp.sqrt(second_hat) + adam_eps) + weight_decay * weight
    )
    return (new_weight, new_first, new_second)


def contract_rows(left, right):
    return lax.dot_general(
        left, right, (((0,), (0,)), ((), ())), preferred_element_type=jnp.float32
    )


def times_transpose(left, right):
    return lax.dot_general(
        left, right, (((1,), (1,)), ((), ())), preferred_element_type=jnp.float32
    )


def layer_step(
    block_input,
    segment_ids,
    cotangent,
    attn_gain,
    qkv_weight,
    out_weight,
    mlp_gain,
    gate_up_weight,
    down_weight,
    first_attn_gain,
    first_qkv,
    first_out,
    first_mlp_gain,
    first_gate_up,
    first_down,
    second_attn_gain,
    second_qkv,
    second_out,
    second_mlp_gain,
    second_gate_up,
    second_down,
):
    seqs_here, local_len, width = block_input.shape
    full_len = segment_ids.shape[1]
    n_dp = lax.axis_size("dp")
    n_z = lax.axis_size("seq")
    groups = HEADS // KV_HEADS
    unit_count = down_weight.shape[0]
    z_here = lax.axis_index("seq")
    owned = attn_gain.shape[0]
    gain_line = jnp.concatenate([attn_gain, mlp_gain]).astype(jnp.bfloat16).astype(jnp.float32)
    gain_tile = jnp.pad(gain_line[None], ((0, 7), (0, LANES - 2 * owned)))
    seg_tile = jnp.pad(segment_ids, ((0, 8 - seqs_here), (0, 0)))
    gate_up_here = gate_up_weight.astype(jnp.bfloat16).reshape(-1, 2 * unit_count)
    down_rows = lax.all_gather(down_weight.astype(jnp.bfloat16), "dp", axis=1, tiled=True)
    rows_in, qkv_cols, out_line, gain_all, seg_all = gather_in(
        block_input,
        qkv_weight.astype(jnp.bfloat16),
        out_weight.astype(jnp.bfloat16).T,
        gain_tile,
        seg_tile,
        n_dp,
        n_z,
    )
    cot_late, _ = lax.optimization_barrier((cotangent, gain_all))
    cot_all = lax.all_gather(cot_late, "seq", axis=1, tiled=True)
    gain_one = gain_all[:, 0, :owned].reshape(1, width)
    gain_two = gain_all[:, 0, owned : 2 * owned].reshape(1, width)
    seg_here = lax.dynamic_slice(seg_all, (z_here // 2, z_here % 2, 0), (1, 1, full_len))[0]
    tables = attn_tables(seg_here)
    _, _, normed_one = rms_forward(rows_in.astype(jnp.float32), gain_one)
    qkv = jnp.dot(normed_one, qkv_cols, preferred_element_type=jnp.float32)
    turned, lse, attended16, out_rows = attn_forward(qkv, *tables, out_line, full_len, groups, n_dp)
    attn_part = times_transpose(attended16, out_rows)
    resid_all, gate_up_cols = share_resid(
        attn_part.astype(jnp.bfloat16), rows_in, gate_up_here, n_dp, n_z
    )
    total_rows = seqs_here * full_len
    resid = resid_all.reshape(total_rows, width).astype(jnp.float32)
    _, _, normed_two = rms_forward(resid, gain_two)
    gate_up = jnp.dot(normed_two, gate_up_cols, preferred_element_type=jnp.float32)
    gate_part = gate_up[:, :unit_count]
    up_part = gate_up[:, unit_count:]
    sigmoid_gate = jax.nn.sigmoid(gate_part)
    active = gate_part * sigmoid_gate
    hidden16 = (active * up_part).astype(jnp.bfloat16)
    cot_rows = cot_all.reshape(total_rows, width)
    d_hidden = times_transpose(cot_rows, down_rows)
    d_gate = d_hidden * up_part * sigmoid_gate * (1.0 + gate_part * (1.0 - sigmoid_gate))
    d_up = d_hidden * active
    d_gate_up16 = jnp.concatenate([d_gate, d_up], 1).astype(jnp.bfloat16)
    down_part = jnp.dot(hidden16, down_rows, preferred_element_type=jnp.float32)
    down_here = lax.psum_scatter(
        down_part.astype(jnp.bfloat16).reshape(resid_all.shape), "seq", scatter_dimension=1, tiled=True
    )
    gate_up_term = contract_rows(normed_two, d_gate_up16).astype(jnp.bfloat16)
    gate_up_sum = lax.psum_scatter(gate_up_term, "dp", scatter_dimension=0, tiled=True)
    grad_gate_up = gate_up_sum.reshape(gate_up_weight.shape).astype(jnp.float32)
    down_term = contract_rows(cot_rows, hidden16).astype(jnp.bfloat16)
    down_sum = lax.psum_scatter(down_term, "dp", scatter_dimension=0, tiled=True)
    grad_down = down_sum.astype(jnp.float32).T
    d_normed_two = times_transpose(d_gate_up16, gate_up_cols).astype(jnp.bfloat16)
    d_resid16, gain_two_part = sum_line(
        d_normed_two.reshape(resid_all.shape), resid_all, cot_all, gain_two, n_z
    )
    down_here = down_here.astype(jnp.float32)
    resid_here = lax.dynamic_slice_in_dim(resid_all, z_here * local_len, local_len, 1)
    output = (resid_here.astype(jnp.float32) + down_here).astype(jnp.bfloat16)
    d_attended = jnp.dot(d_resid16, out_rows, preferred_element_type=jnp.float32).astype(jnp.bfloat16)
    d_qkv16 = attn_backward(turned, d_attended, lse, *tables, full_len, groups)
    d_normed_one = times_transpose(d_qkv16, qkv_cols).astype(jnp.bfloat16)
    qkv_term = contract_rows(normed_one, d_qkv16).astype(jnp.bfloat16)
    out_term = contract_rows(d_resid16, attended16).astype(jnp.bfloat16)
    input_grad, grad_qkv, grad_out, gain_sums = hand_out(
        d_normed_one, rows_in, d_resid16, gain_one, gain_two_part, qkv_term, out_term, n_dp, n_z
    )
    flat = lax.axis_index("dp") * n_z + z_here
    gain_sums = lax.dynamic_slice(
        jnp.sum(gain_sums.reshape(2, 8, LANES), axis=1), (0, flat * owned % LANES), (2, owned)
    )
    grad_gain_one = gain_sums[0]
    grad_gain_two = gain_sums[1]
    w_one, m_one, v_one = adam_update(attn_gain, grad_gain_one, first_attn_gain, second_attn_gain)
    w_qkv, m_qkv, v_qkv = adam_update(qkv_weight, grad_qkv, first_qkv, second_qkv)
    w_out, m_out, v_out = adam_update(out_weight, grad_out, first_out, second_out)
    w_two, m_two, v_two = adam_update(mlp_gain, grad_gain_two, first_mlp_gain, second_mlp_gain)
    w_gu, m_gu, v_gu = adam_update(gate_up_weight, grad_gate_up, first_gate_up, second_gate_up)
    w_down, m_down, v_down = adam_update(down_weight, grad_down, first_down, second_down)
    return (
        output,
        input_grad,
        grad_gain_one,
        grad_qkv,
        grad_out,
        grad_gain_two,
        grad_gate_up,
        grad_down,
        w_one,
        w_qkv,
        w_out,
        w_two,
        w_gu,
        w_down,
        m_one,
        m_qkv,
        m_out,
        m_two,
        m_gu,
        m_down,
        v_one,
        v_qkv,
        v_out,
        v_two,
        v_gu,
        v_down,
    )


def solution(mesh):
    in_specs = (
        P("dp", "seq", None),
        P("dp", None),
        P("dp", "seq", None),
        P(("dp", "seq")),
        P("dp", "seq"),
        P("seq", "dp"),
        P(("dp", "seq")),
        P("dp", None, "seq"),
        P("seq", "dp"),
        P(("dp", "seq")),
        P("dp", "seq"),
        P("seq", "dp"),
        P(("dp", "seq")),
        P("dp", None, "seq"),
        P("seq", "dp"),
        P(("dp", "seq")),
        P("dp", "seq"),
        P("seq", "dp"),
        P(("dp", "seq")),
        P("dp", None, "seq"),
        P("seq", "dp"),
    )
    out_specs = (
        P("dp", "seq", None),
        P("dp", "seq", None),
        P(("dp", "seq")),
        P("dp", "seq"),
        P("seq", "dp"),
        P(("dp", "seq")),
        P("dp", None, "seq"),
        P("seq", "dp"),
        P(("dp", "seq")),
        P("dp", "seq"),
        P("seq", "dp"),
        P(("dp", "seq")),
        P("dp", None, "seq"),
        P("seq", "dp"),
        P(("dp", "seq")),
        P("dp", "seq"),
        P("seq", "dp"),
        P(("dp", "seq")),
        P("dp", None, "seq"),
        P("seq", "dp"),
        P(("dp", "seq")),
        P("dp", "seq"),
        P("seq", "dp"),
        P(("dp", "seq")),
        P("dp", None, "seq"),
        P("seq", "dp"),
    )
    return jax.shard_map(layer_step, mesh=mesh, in_specs=in_specs, out_specs=out_specs, check_vma=False)
```

```python
import functools

import jax
import jax.numpy as jnp
from jax import lax
from jax.experimental import pallas as pl
from jax.experimental.pallas import tpu as pltpu
from jax.sharding import PartitionSpec as P


HEADS = 32
KV_HEADS = 8
norm_eps = 1e-05
beta_one = 0.9
beta_two = 0.95
learn_rate = 0.01
weight_decay = 0.1
adam_eps = 1e-08
step_count = 10.0
masked_score = -1e30


HEAD_DIM = 64
LANES = 128


def dot_t(a, b):
    return lax.dot_general(a, b, (((1,), (1,)), ((), ())), preferred_element_type=jnp.float32)


def dot_n(a, b):
    return lax.dot_general(a, b, (((1,), (0,)), ((), ())), preferred_element_type=jnp.float32)


def dot_c(a, b):
    return lax.dot_general(a, b, (((0,), (0,)), ((), ())), preferred_element_type=jnp.float32)


def swap_halves(u):
    lane = lax.broadcasted_iota(jnp.int32, u.shape, 1)
    return jnp.where(lane % 64 < 32, pltpu.roll(u, 96, 1), pltpu.roll(u, 32, 1))


def turn(u, cos_wide, sin_wide):
    return u * cos_wide + swap_halves(u) * sin_wide


def key_start(block, q_rows, reach):
    return max(0, (block * q_rows - reach + 1) // q_rows * q_rows)


def attn_forward_kernel(pairs, q_rows, reach, qkv_ref, cos_ref, sin_ref, seg_col_ref, seg_row_ref,
                        turned_ref, lse_ref, out_ref):
    full_len = qkv_ref.shape[0]
    lane = lax.broadcasted_iota(jnp.int32, (full_len, LANES), 1)
    low = lane < HEAD_DIM
    cos_q = cos_ref[...]
    sin_q = sin_ref[...]
    kv = qkv_ref[:, pairs * LANES:].astype(jnp.float32)
    kv16 = turn(kv, jnp.where(low, cos_q, 1.0), jnp.where(low, sin_q, 0.0)).astype(jnp.bfloat16)
    turned_ref[:, pairs * LANES:] = kv16
    kv32 = kv16.astype(jnp.float32)
    rolled = pltpu.roll(kv32, HEAD_DIM, 1)
    zero = jnp.zeros_like(kv32)
    keys = (jnp.where(low, kv32, zero).astype(jnp.bfloat16), jnp.where(low, zero, rolled).astype(jnp.bfloat16))
    vals = (jnp.where(low, rolled, zero).astype(jnp.bfloat16), jnp.where(low, zero, kv32).astype(jnp.bfloat16))
    for pair in range(pairs):
        cols = slice(pair * LANES, (pair + 1) * LANES)
        query = turn(qkv_ref[:, cols].astype(jnp.float32), cos_q, sin_q) .astype(jnp.bfloat16)
        turned_ref[:, cols] = query
    for block in range(full_len // q_rows):
        first = key_start(block, q_rows, reach)
        last = (block + 1) * q_rows
        rows = slice(block * q_rows, last)
        span = slice(first, last)
        i = lax.broadcasted_iota(jnp.int32, (q_rows, last - first), 0) + block * q_rows
        j = lax.broadcasted_iota(jnp.int32, (q_rows, last - first), 1) + first
        allowed = (j <= i) & (seg_col_ref[rows, :1] == seg_row_ref[:1, span])
        for pair in range(pairs):
            cols = slice(pair * LANES, (pair + 1) * LANES)
            query = turned_ref[rows, cols]
            total = None
            for half in range(2):
                scores = dot_t(query, keys[half][span]) * (HEAD_DIM ** -0.5)
                scores = jnp.where(allowed, scores, masked_score)
                top = jnp.max(scores, axis=1, keepdims=True)
                lse = top + jnp.log(jnp.sum(jnp.exp(scores - top), axis=1, keepdims=True))
                probs = jnp.exp(scores - lse).astype(jnp.bfloat16)
                part = dot_n(probs, vals[half][span])
                total = part if total is None else total + part
                head = 2 * pair + half
                lse_ref[rows, head:head + 1] = lse
            out_ref[rows, cols] = total.astype(jnp.bfloat16)


def attn_backward_kernel(pairs, q_rows, reach, turned_ref, d_out_ref, lse_ref, cos_ref, sin_ref, seg_col_ref,
                         seg_row_ref, grad_ref, dk_ref, dv_ref):
    full_len = turned_ref.shape[0]
    lane = lax.broadcasted_iota(jnp.int32, (full_len, LANES), 1)
    low = lane < HEAD_DIM
    kv32 = turned_ref[:, pairs * LANES:].astype(jnp.float32)
    rolled = pltpu.roll(kv32, HEAD_DIM, 1)
    zero = jnp.zeros_like(kv32)
    keys = (jnp.where(low, kv32, zero).astype(jnp.bfloat16), jnp.where(low, zero, rolled).astype(jnp.bfloat16))
    vals = (jnp.where(low, rolled, zero).astype(jnp.bfloat16), jnp.where(low, zero, kv32).astype(jnp.bfloat16))
    dk_ref[...] = jnp.zeros_like(dk_ref)
    dv_ref[...] = jnp.zeros_like(dv_ref)
    low_rows = low[:q_rows]
    scale = HEAD_DIM ** -0.5
    for block in range(full_len // q_rows):
        first = key_start(block, q_rows, reach)
        last = (block + 1) * q_rows
        rows = slice(block * q_rows, last)
        span = slice(first, last)
        i = lax.broadcasted_iota(jnp.int32, (q_rows, last - first), 0) + block * q_rows
        j = lax.broadcasted_iota(jnp.int32, (q_rows, last - first), 1) + first
        allowed = (j <= i) & (seg_col_ref[rows, :1] == seg_row_ref[:1, span])
        cos_q = cos_ref[rows]
        sin_q = sin_ref[rows]
        for pair in range(pairs):
            cols = slice(pair * LANES, (pair + 1) * LANES)
            query = turned_ref[rows, cols]
            d_out = d_out_ref[rows, cols]
            q32 = query.astype(jnp.float32)
            o32 = d_out.astype(jnp.float32)
            d_query = None
            d_key = None
            d_val = None
            for half in range(2):
                keep = low_rows if half == 0 else ~low_rows
                q_only = jnp.where(keep, q32, 0.0).astype(jnp.bfloat16)
                o_only = jnp.where(keep, o32, 0.0).astype(jnp.bfloat16)
                head = 2 * pair + half
                scores = dot_t(query, keys[half][span]) * scale
                scores = jnp.where(allowed, scores, masked_score)
                probs = jnp.exp(scores - lse_ref[rows, head:head + 1])
                d_probs = dot_t(d_out, vals[half][span])
                delta = jnp.sum(probs * d_probs, axis=1, keepdims=True)
                d_scores = (probs * (d_probs - delta) * scale).astype(jnp.bfloat16)
                probs16 = probs.astype(jnp.bfloat16)
                dq = dot_n(d_scores, keys[half][span])
                dk = dot_c(d_scores, q_only)
                dv = dot_c(probs16, o_only)
                d_query = dq if d_query is None else d_query + dq
                d_key = dk if d_key is None else d_key + dk
                d_val = dv if d_val is None else d_val + dv
            dk_ref[span] = dk_ref[span] + d_key
            dv_ref[span] = dv_ref[span] + d_val
            grad_ref[rows, cols] = turn(d_query, cos_q, -sin_q).astype(jnp.bfloat16)
    d_key = dk_ref[...]
    d_val = dv_ref[...]
    d_key = d_key + pltpu.roll(d_key, HEAD_DIM, 1)
    d_val = d_val + pltpu.roll(d_val, HEAD_DIM, 1)
    d_key = turn(d_key, cos_ref[...], -sin_ref[...])
    grad_ref[:, pairs * LANES:] = jnp.where(low, d_key, d_val).astype(jnp.bfloat16)


def attn_specs(full_len, width):
    line = pl.BlockSpec((full_len, width), lambda s, g: (s, g))
    table = pl.BlockSpec((full_len, LANES), lambda s, g: (s, 0))
    row = pl.BlockSpec((8, full_len), lambda s, g: (s, 0))
    return line, table, row


Q_ROWS = 128
REACH = 256


def attn_gather_kernel(n_dp, pairs, q_rows, reach, qkv_ref, cos_ref, sin_ref, seg_col_ref, seg_row_ref, vo_ref,
                       turned_ref, lse_ref, out_ref, wo, d_s, d_r, loc):
    _, z, pair, c = place()
    n_d = n_dp // 2
    step = pl.program_id(1)
    steps = pl.num_programs(1)
    rows = vo_ref.shape[0]
    parts = 2
    part = rows // parts // 2

    def spot(owner, t, h):
        return wo.at[pl.ds(pl.multiple_of(owner * rows + (2 * t + h) * part, part), part)]

    spread = Spread(n_d, pair, c, z, parts, spot, d_s, d_r)
    keep = pltpu.make_async_copy(vo_ref, wo.at[pl.ds(pl.multiple_of(pair * rows, rows), rows)], loc)

    @pl.when(step == 0)
    def _():
        keep.start()
        barrier = pltpu.get_barrier_semaphore()
        for k in range(1, n_d):
            pl.semaphore_signal(barrier, inc=1, device_id=(2 * (pair ^ k) + c, z), device_id_type=MESH)
        pl.semaphore_wait(barrier, n_d - 1)
        keep.wait()
        for t in range(parts):
            spread.own(t)

    attn_forward_kernel(pairs, q_rows, reach, qkv_ref, cos_ref, sin_ref, seg_col_ref, seg_row_ref, turned_ref, lse_ref, out_ref)

    @pl.when(step == steps - 2)
    def _():
        spread.pass_on(0)

    @pl.when(step == steps - 1)
    def _():
        spread.pass_on(1)
        spread.finish()


def attn_forward(qkv, cos, sin, seg_col, seg_row, vo, full_len, groups, n_dp):
    pairs = groups // 2
    width = (groups + 2) * HEAD_DIM
    seqs = qkv.shape[0] // full_len
    kv = qkv.shape[1] // width
    n_d = n_dp // 2
    line, table, row = attn_specs(full_len, width)
    outw = pl.BlockSpec((full_len, groups * HEAD_DIM), lambda s, g: (s, g))
    rows = seqs * full_len
    return pl.pallas_call(
        functools.partial(attn_gather_kernel, n_dp, pairs, Q_ROWS, REACH),
        grid=(seqs, kv),
        in_specs=[line, table, table, table, row, VMEM_SPEC],
        out_specs=[line, pl.BlockSpec((full_len, LANES), lambda s, g: (s, g)), outw, ANY_SPEC],
        out_shape=[
            jax.ShapeDtypeStruct((rows, kv * width), jnp.bfloat16),
            jax.ShapeDtypeStruct((rows, kv * LANES), jnp.float32),
            jax.ShapeDtypeStruct((rows, kv * groups * HEAD_DIM), jnp.bfloat16),
            jax.ShapeDtypeStruct((n_d * vo.shape[0], vo.shape[1]), jnp.bfloat16),
        ],
        scratch_shapes=[DMA((n_d - 1, 2, 2)), DMA((n_d - 1, 2, 2)), DMA],
        compiler_params=pltpu.CompilerParams(collective_id=4, has_side_effects=True),
        cost_estimate=pl.CostEstimate(flops=4 * rows * full_len * kv * LANES * groups, bytes_accessed=150_000_000, transcendentals=0),
        name="attn_forward",
    )(qkv, cos, sin, seg_col, seg_row, vo)


def attn_backward(turned, d_out, lse, cos, sin, seg_col, seg_row, full_len, groups):
    pairs = groups // 2
    width = (groups + 2) * HEAD_DIM
    seqs = turned.shape[0] // full_len
    kv = turned.shape[1] // width
    line, table, row = attn_specs(full_len, width)
    outw = pl.BlockSpec((full_len, groups * HEAD_DIM), lambda s, g: (s, g))
    rows = seqs * full_len
    return pl.pallas_call(
        functools.partial(attn_backward_kernel, pairs, Q_ROWS, REACH),
        grid=(seqs, kv),
        in_specs=[line, outw, pl.BlockSpec((full_len, LANES), lambda s, g: (s, g)), table, table, table, row],
        out_specs=line,
        out_shape=jax.ShapeDtypeStruct((rows, kv * width), jnp.bfloat16),
        scratch_shapes=[pltpu.VMEM((full_len, LANES), jnp.float32)] * 2,
        cost_estimate=pl.CostEstimate(flops=10 * rows * full_len * kv * LANES * groups, bytes_accessed=rows * kv * width * 6, transcendentals=0),
        name="attn_backward",
    )(turned, d_out, lse, cos, sin, seg_col, seg_row)


def attn_tables(segment_ids):
    seqs, full_len = segment_ids.shape
    earlier = (segment_ids[..., None, :] < segment_ids[..., :, None]).astype(jnp.int32)
    positions = jnp.arange(full_len, dtype=jnp.int32) - jnp.sum(earlier, axis=-1, dtype=jnp.int32)
    inverse = 500000.0 ** (-2.0 * jnp.arange(HEAD_DIM // 2, dtype=jnp.float32) / HEAD_DIM)
    angles = positions.astype(jnp.float32)[..., None] * inverse
    cos = jnp.cos(angles)
    sin = jnp.sin(angles)
    cos = jnp.concatenate([cos] * 4, -1).reshape(seqs * full_len, LANES)
    sin = jnp.concatenate([-sin, sin] * 2, -1).reshape(seqs * full_len, LANES)
    seg_col = jnp.broadcast_to(segment_ids[:, :, None], (seqs, full_len, LANES)).reshape(seqs * full_len, LANES)
    seg_row = jnp.broadcast_to(segment_ids[:, None, :], (seqs, 8, full_len)).reshape(seqs * 8, full_len)
    return cos, sin, seg_col, seg_row


MESH = pl.DeviceIdType.MESH
VMEM_SPEC = pl.BlockSpec(memory_space=pltpu.VMEM)
ANY_SPEC = pl.BlockSpec(memory_space=pl.ANY)
DMA = pltpu.SemaphoreType.DMA


def place():
    d = lax.axis_index("dp")
    z = lax.axis_index("seq")
    return d, z, d // 2, d % 2


def remote(src, dst, send, recv, dev):
    return pltpu.make_async_remote_copy(
        src_ref=src, dst_ref=dst, send_sem=send, recv_sem=recv, device_id=dev, device_id_type=MESH
    )


def greet_all(n_dp, n_z, d, z):
    barrier = pltpu.get_barrier_semaphore()
    me = d * n_z + z

    def one(o, carry):
        other = lax.rem(me + o, n_dp * n_z)
        pl.semaphore_signal(barrier, inc=1, device_id=(other // n_z, lax.rem(other, n_z)), device_id_type=MESH)
        return carry

    lax.fori_loop(1, n_dp * n_z, one, 0)
    pl.semaphore_wait(barrier, n_dp * n_z - 1)


def greet_line(n_z, d, z, extra=()):
    barrier = pltpu.get_barrier_semaphore()
    c = d % 2
    for o in range(n_z):
        zz = lax.rem(z + o, n_z)
        for core in range(2):
            if o == 0 and core == 0:
                continue
            pl.semaphore_signal(barrier, inc=1, device_id=(d - c + lax.rem(c + core, 2), zz), device_id_type=MESH)
    for dev in extra:
        pl.semaphore_signal(barrier, inc=1, device_id=dev, device_id_type=MESH)
    pl.semaphore_wait(barrier, 2 * n_z - 1 + len(extra))


def block_at(ref, shape, row, col):
    return ref.at[pl.ds(pl.multiple_of(row * shape[0], shape[0]), shape[0]),
                  pl.ds(pl.multiple_of(col * shape[1], shape[1]), shape[1])]


class Spread:
    def __init__(self, n_d, pair, c, z, parts, spot, send, recv):
        self.n_d, self.pair, self.parts, self.spot = n_d, pair, parts, spot
        self.send, self.recv = send, recv
        self.dev = lambda k: (2 * (pair ^ k) + c, z)

    def copy(self, slot, owner, t, h, to):
        at = self.spot(owner, t, h)
        return remote(at, at, self.send.at[slot, t, h], self.recv.at[slot, t, h], self.dev(to))

    def own(self, t):
        if self.n_d == 4:
            for h in range(2):
                self.copy(0, self.pair, t, h, 1).start()
                self.copy(1, self.pair, t, 1 - h, 2).start()
        else:
            for k in range(1, self.n_d):
                for h in range(2):
                    self.copy(k - 1, self.pair, t, h, k).start()

    def pass_on(self, t):
        if self.n_d == 4:
            self.copy(0, self.pair ^ 1, t, 0, 1).wait_recv()
            self.copy(2, self.pair ^ 1, t, 0, 2).start()
            self.copy(1, self.pair ^ 2, t, 1, 2).wait_recv()
            self.copy(2, self.pair ^ 2, t, 1, 1).start()

    def rest(self, t):
        if self.n_d == 4:
            self.copy(0, self.pair ^ 1, t, 1, 1).wait_recv()
            self.copy(1, self.pair ^ 2, t, 0, 2).wait_recv()
        else:
            for k in range(1, self.n_d):
                for h in range(2):
                    self.copy(k - 1, self.pair ^ k, t, h, k).wait_recv()

    def far(self, t):
        if self.n_d == 4:
            for h in range(2):
                self.copy(2, self.pair ^ 3, t, h, 1).wait_recv()

    def sent(self):
        for t in range(self.parts):
            for h in range(2):
                for slot in range(self.n_d - 1):
                    self.copy(slot, self.pair, t, h, 1).wait_send()

    def finish(self):
        for t in range(self.parts):
            if self.n_d == 4:
                self.copy(0, self.pair ^ 1, t, 1, 1).wait_recv()
                self.copy(1, self.pair ^ 2, t, 0, 2).wait_recv()
                for h in range(2):
                    self.copy(2, self.pair ^ 3, t, h, 1).wait_recv()
                    for slot in range(3):
                        self.copy(slot, self.pair, t, h, 1).wait_send()
            else:
                for k in range(1, self.n_d):
                    for h in range(2):
                        self.copy(k - 1, self.pair ^ k, t, h, k).wait_recv()
                        self.copy(k - 1, self.pair, t, h, k).wait_send()


def gather_in_kernel(n_dp, n_z, x_ref, w_ref, v_ref, g_ref, s_ref, xs, wq, vo, ga, sg,
                     x_s, x_r, f_s, f_r, w_s, w_r, v_s, v_r, d_s, d_r, g_s, g_r, s_s, s_r, loc):
    d, z, pair, c = place()
    n_d = n_dp // 2
    me = d * n_z + z
    total = n_dp * n_z
    rows = x_ref.shape[1]
    half = rows // 2
    shape = w_ref.shape
    cz = z // 2
    greet_all(n_dp, n_z, d, z)

    def line_stage(src, dst, send, recv, spare, wait):
        for o in range(n_z):
            copy = remote(src, dst, send.at[o], recv.at[c, z % 2], (2 * pair + cz, lax.rem(z + o, n_z)))
            act = copy.wait_send if wait else copy.start
            if o == 0:
                pl.when(c != cz)(act)
                if not wait:
                    pl.when(c == cz)(pltpu.make_async_copy(src, dst, loc.at[spare]).start)
            else:
                act()

    my_block = block_at(wq, shape, d, z % 2)
    line_stage(w_ref, my_block, w_s, w_r, 0, False)

    for i in range(2):
        for h in range(2):
            src = x_ref.at[i, pl.ds(h * half, half)]
            dst = xs.at[pl.ds(pl.multiple_of(z * rows + h * half, half), half)]
            zz = 2 * c + i
            mine = (h == c) & (zz == z)
            copy = remote(src, dst, x_s.at[i, h], x_r.at[z], (2 * pair + h, zz))
            pl.when(jnp.logical_not(mine))(copy.start)
            pl.when(mine)(lambda src=src, dst=dst: pltpu.make_async_copy(src, dst, loc.at[1]).start())

    seg_copy = remote(s_ref, sg.at[c], s_s, s_r, (2 * pair + 1 - c, z))
    seg_copy.start()
    own_seg = pltpu.make_async_copy(s_ref, sg.at[c], loc.at[2])
    own_seg.start()
    own_gain = pltpu.make_async_copy(g_ref, ga.at[me], loc.at[3])
    own_gain.start()

    def send_gain(o, carry):
        other = lax.rem(me + o, total)
        remote(g_ref, ga.at[me], g_s, g_r, (other // n_z, lax.rem(other, n_z))).start()
        return carry

    lax.fori_loop(1, total, send_gain, 0)

    first = jnp.where(c == cz, z % 2, 1 - c)

    def turn_of(t):
        return t % 2, (first if t < 2 else 1 - first)

    def spot(owner, t, h):
        core, b = turn_of(t)
        part = shape[0] // 2
        return wq.at[pl.ds(pl.multiple_of((2 * owner + core) * shape[0] + h * part, part), part),
                     pl.ds(pl.multiple_of(b * shape[1], shape[1]), shape[1])]

    spread = Spread(n_d, pair, c, z, 4, spot, d_s, d_r)
    for t in range(4):
        core, b = turn_of(t)
        blk = block_at(wq, shape, 2 * pair + core, b)
        mine = (core == c) & (2 * c + b == z)
        arrive = remote(w_ref, blk, w_s.at[0], w_r.at[core, b], (d, z))
        pl.when(jnp.logical_not(mine))(arrive.wait_recv)
        pl.when(mine)(lambda blk=blk: pltpu.make_async_copy(w_ref, blk, loc.at[0]).wait())
        spread.own(t)
        if t == 1:
            line_stage(v_ref, block_at(vo, v_ref.shape, c, z % 2), v_s, v_r, 4, False)
        if t > 0:
            spread.pass_on(t - 1)

    for o in range(n_z):
        zs = lax.rem(z + o, n_z)
        src = xs.at[pl.ds(pl.multiple_of(zs * rows + c * half, half), half)]
        mine = (cz == c) & (zs == z)
        arrive = remote(src, src, x_s.at[0, 0], x_r.at[zs], (d, z))
        pl.when(jnp.logical_not(mine))(arrive.wait_recv)
        pl.when(mine)(lambda src=src: pltpu.make_async_copy(src, src, loc.at[1]).wait())
        remote(src, src, f_s.at[zs], f_r.at[zs], (2 * pair + 1 - c, z)).start()
    spread.pass_on(3)

    line_stage(w_ref, my_block, w_s, w_r, 0, True)
    line_stage(v_ref, block_at(vo, v_ref.shape, c, z % 2), v_s, v_r, 4, True)
    for i in range(2):
        for h in range(2):
            src = x_ref.at[i, pl.ds(h * half, half)]
            mine = (h == c) & (2 * c + i == z)
            copy = remote(src, src, x_s.at[i, h], x_r.at[0], (d, z))
            pl.when(jnp.logical_not(mine))(copy.wait_send)
    for zs in range(n_z):
        src = xs.at[pl.ds(zs * rows, half)]
        copy = remote(src, src, f_s.at[zs], f_r.at[zs], (d, z))
        copy.wait_send()
        copy.wait_recv()
    for core in range(2):
        for b in range(2):
            blk = block_at(vo, v_ref.shape, core, b)
            mine = (core == c) & (2 * c + b == z)
            pl.when(jnp.logical_not(mine))(remote(blk, blk, v_s.at[0], v_r.at[core, b], (d, z)).wait_recv)
            pl.when(mine)(pltpu.make_async_copy(v_ref, blk, loc.at[4]).wait)
    seg_copy.wait_send()
    remote(s_ref, sg.at[1 - c], s_s, s_r, (d, z)).wait_recv()
    own_seg.wait()
    own_gain.wait()
    many = ga.at[pl.ds(0, total - 1)]
    gains = remote(many, many, g_s, g_r, (d, z))
    gains.wait_send()
    gains.wait_recv()
    spread.finish()


def gather_in(x_loc, w, v, gain_tile, seg_tile, n_dp, n_z):
    _, rows, width = x_loc.shape
    n_d = n_dp // 2
    total = n_dp * n_z
    return pl.pallas_call(
        functools.partial(gather_in_kernel, n_dp, n_z),
        in_specs=[VMEM_SPEC] * 5,
        out_specs=[ANY_SPEC] * 5,
        out_shape=[
            jax.ShapeDtypeStruct((rows * n_z, width), x_loc.dtype),
            jax.ShapeDtypeStruct((w.shape[0] * n_dp, 2 * w.shape[1]), w.dtype),
            jax.ShapeDtypeStruct((v.shape[0] * 2, 2 * v.shape[1]), v.dtype),
            jax.ShapeDtypeStruct((total,) + gain_tile.shape, gain_tile.dtype),
            jax.ShapeDtypeStruct((2,) + seg_tile.shape, seg_tile.dtype),
        ],
        scratch_shapes=[
            DMA((2, 2)), DMA((n_z,)), DMA((n_z,)), DMA((n_z,)), DMA((n_z,)), DMA((2, 2)), DMA((n_z,)), DMA((2, 2)),
            DMA((n_d - 1, 4, 2)), DMA((n_d - 1, 4, 2)), DMA, DMA, DMA, DMA, DMA((5,)),
        ],
        compiler_params=pltpu.CompilerParams(collective_id=1, has_side_effects=True),
        cost_estimate=pl.CostEstimate(flops=0, bytes_accessed=200_000_000, transcendentals=0),
        name="gather_in",
    )(x_loc, w, v, gain_tile, seg_tile)


def share_resid_kernel(n_dp, n_z, part_ref, x_ref, w_ref, out, wall, got, buf, p_s, p_r, u_s, u_r, d_s, d_r, c_s, c_r, loc):
    d, z, pair, c = place()
    n_d = n_dp // 2
    cz = z // 2
    full = x_ref.shape[0]
    half = full // 2
    unit = half // 2
    w_rows = w_ref.shape[0]
    parts = 4
    piece = w_rows // parts
    own_copy = pltpu.make_async_copy(w_ref, wall.at[pl.ds(pl.multiple_of(d * w_rows, w_rows), w_rows)], loc.at[2])
    own_copy.start()
    greet_line(n_z, d, z, [(2 * (pair ^ k) + c, z) for k in range(1, n_d)])
    mine = pl.ds(pl.multiple_of(c * half, half), half)
    theirs = pl.ds(pl.multiple_of((1 - c) * half, half), half)
    swap = remote(part_ref.at[theirs], got, p_s, p_r, (2 * pair + 1 - c, z))
    swap.start()

    def spot_w(owner, t, h):
        sub = piece // 2
        return wall.at[pl.ds(pl.multiple_of((2 * owner + c) * w_rows + (2 * t + h) * sub, sub), sub)]

    def across(k, t, core):
        at = wall.at[pl.ds(pl.multiple_of((2 * (pair ^ k) + core) * w_rows + t * piece, piece), piece)]
        return remote(at, at, c_s.at[k, t], c_r.at[k, t], (2 * pair + 1 - c, z))

    spread = Spread(n_d, pair, c, z, parts, spot_w, d_s, d_r)
    own_copy.wait()
    for t in range(parts):
        spread.own(t)
        across(0, t, c).start()

    swap.wait_recv()

    def add(r, carry):
        at = pl.ds(pl.multiple_of(r * 16, 16), 16)
        src = pl.ds(pl.multiple_of(c * half + r * 16, 16), 16)
        total = x_ref[src].astype(jnp.float32) + part_ref[src].astype(jnp.float32) + got[at].astype(jnp.float32)
        buf[at] = total.astype(jnp.bfloat16)
        return carry

    def spot(jl, h, k):
        return out.at[jl, pl.ds(pl.multiple_of(h * half + k * unit, unit), unit)]

    def sends(k, wait):
        src = buf.at[pl.ds(k * unit, unit)]
        dst = spot(z % 2, c, k)
        for o, zz in ((1, z - 1), (2, z + 1), (0, z)):
            copy = remote(src, dst, u_s.at[o, k], u_r.at[z % 2, c, k], (2 * pair + cz, zz))
            act = copy.wait_send if wait else copy.start
            if o == 0:
                keep = pltpu.make_async_copy(src, dst, loc.at[k])
                pl.when(c != cz)(act)
                pl.when(c == cz)(keep.wait if wait else keep.start)
            elif o == 1:
                pl.when(z > 0)(act)
            else:
                pl.when(z < n_z - 1)(act)

    per = unit // 16
    lax.fori_loop(0, per, add, 0)
    lax.fori_loop(per, per + per // 2, add, 0)
    sends(0, False)
    lax.fori_loop(per + per // 2, 2 * per, add, 0)
    swap.wait_send()
    sends(1, False)

    def relay(dist, sign, k, h, begin):
        j = z + sign * dist
        ok = (j >= 2 * c) & (j <= 2 * c + 1)
        to = z - sign
        more = (to >= 0) & (to <= n_z - 1)
        jl = lax.rem(j + n_z, 2)
        at = spot(jl, h, k)
        copy = remote(at, at, u_s.at[3 + (0 if sign < 0 else 1), 4 * jl + 2 * h + k], u_r.at[jl, h, k], (2 * pair + c, to))
        if begin:

            @pl.when(ok)
            def _():
                copy.wait_recv()
                pl.when(more)(copy.start)
        else:
            pl.when(ok & more)(copy.wait_send)

    def take(t):
        spread.pass_on(t)

    def rest(t):
        spread.rest(t)
        for k in range(1, n_d):
            if n_d != 4 or k != 3:
                across(k, t, c).start()

    def far(t):
        if n_d == 4:
            spread.far(t)
            across(3, t, c).start()

    links = []
    for t in range(parts):
        links += [(take, t), (rest, t)]
    links += [(far, t) for t in range(parts)]
    line = [(dist, k, h) for dist in range(1, n_z) for k in range(2) for h in range(2)]
    for n in range(max(len(links), len(line))):
        if n < len(line):
            dist, k, h = line[n]
            for sign in (-1, 1):
                relay(dist, sign, k, h, True)
        if n < len(links):
            links[n][0](links[n][1])

    @pl.when(c == cz)
    def _():
        for k in range(2):
            at = spot(z % 2, 1 - c, k)
            remote(at, at, u_s.at[0, 0], u_r.at[z % 2, 1 - c, k], (d, z)).wait_recv()

    for dist, k, h in line:
        for sign in (-1, 1):
            relay(dist, sign, k, h, False)
    sends(0, True)
    sends(1, True)
    spread.sent()
    for k in range(n_d):
        for t in range(parts):
            across(k, t, c).wait_send()
            across(k, t, 1 - c).wait_recv()


def share_resid(part, x, w, n_dp, n_z):
    full, width = x.shape
    n_d = n_dp // 2
    return pl.pallas_call(
        functools.partial(share_resid_kernel, n_dp, n_z),
        in_specs=[VMEM_SPEC] * 3,
        out_specs=[ANY_SPEC] * 2,
        out_shape=[
            jax.ShapeDtypeStruct((2, full, width), jnp.bfloat16),
            jax.ShapeDtypeStruct((n_dp * w.shape[0], w.shape[1]), jnp.bfloat16),
        ],
        scratch_shapes=[
            pltpu.VMEM((full // 2, width), jnp.bfloat16), pltpu.VMEM((full // 2, width), jnp.bfloat16),
            DMA, DMA, DMA((5, 8)), DMA((2, 2, 2)), DMA((n_d - 1, 4, 2)), DMA((n_d - 1, 4, 2)), DMA((n_d, 4)), DMA((n_d, 4)),
            DMA((3,)),
        ],
        compiler_params=pltpu.CompilerParams(collective_id=2, has_side_effects=True),
        cost_estimate=pl.CostEstimate(flops=0, bytes_accessed=200_000_000, transcendentals=0),
        name="share_resid",
    )(part, x, w)


CHUNKS = 8


def sum_line_kernel(n_z, part_ref, resid_all, cot_all, gain_ref, d_out, gain_out, got, buf, resid_ref, cot_ref,
                    s_s, s_r, p_s, p_r, loc, rows_sem):
    d, z, pair, c = place()
    cz = z // 2
    full, _ = buf.shape
    rows = full // CHUNKS
    fetch = (
        pltpu.make_async_copy(resid_all.at[z % 2], resid_ref, rows_sem.at[0]),
        pltpu.make_async_copy(cot_all.at[z % 2], cot_ref, rows_sem.at[1]),
    )
    for one in fetch:
        one.start()
    greet_line(n_z, d, z)
    gain_out[...] = jnp.zeros_like(gain_out)
    own = c == cz
    steps = [(k, t) for k in range(CHUNKS) for t in range(2)]

    def where_is(k, t):
        jl = jnp.bitwise_xor(c, t)
        return jl, 2 * c + jl, pl.ds(k * rows, rows)

    def copy_on(k, t, side, src):
        jl, _, at = where_is(k, t)
        to = z + 1 if side == 0 else z - 1
        return remote(src, got.at[side, jl, at], s_s.at[t, k], s_r.at[side, jl, k], (2 * pair + c, to))

    def arrived(side, jl, k):
        at = got.at[side, jl, pl.ds(k * rows, rows)]
        return remote(at, at, s_s.at[0, 0], s_r.at[side, jl, k], (d, z))

    def add_in(side, jl, k):
        def one(r, carry):
            at = pl.ds(pl.multiple_of(k * rows + r * 16, 16), 16)
            got[side, jl, at] = (got[side, jl, at].astype(jnp.float32) + part_ref[jl, at].astype(jnp.float32)).astype(jnp.bfloat16)
            return carry

        lax.fori_loop(0, rows // 16, one, 0)

    def finish(jl, k):
        def one(r, carry):
            at = pl.ds(pl.multiple_of(k * rows + r * 16, 16), 16)
            total = part_ref[jl, at].astype(jnp.float32)
            left = got[0, jl, at].astype(jnp.float32)
            right = got[1, jl, at].astype(jnp.float32)
            total = total + jnp.where(z > 0, left, 0.0) + jnp.where(z < n_z - 1, right, 0.0)
            value = resid_ref[at].astype(jnp.float32)
            inverse = lax.rsqrt(jnp.mean(value * value, axis=-1, keepdims=True) + norm_eps)
            scaled = value * inverse
            d_scaled = total * gain_ref[...]
            mean = jnp.mean(d_scaled * scaled, axis=-1, keepdims=True)
            d_resid = cot_ref[at].astype(jnp.float32) + inverse * (d_scaled - scaled * mean)
            buf[at] = d_resid.astype(jnp.bfloat16)
            prod = total * scaled
            gain_out[...] = gain_out[...] + prod[:8] + prod[8:]
            return carry

        lax.fori_loop(0, rows // 16, one, 0)

    def to_partner(k):
        at = pl.ds(k * rows, rows)
        return remote(buf.at[at], d_out.at[at], p_s.at[k], p_r.at[k], (2 * pair + 1 - c, z))

    def keep(k):
        at = pl.ds(k * rows, rows)
        return pltpu.make_async_copy(buf.at[at], d_out.at[at], loc.at[k])

    def send_step(k, t, wait):
        jl, j, at = where_is(k, t)
        for side in range(2):
            going = (z < j) if side == 0 else (z > j)
            edge = (z == 0) if side == 0 else (z == n_z - 1)
            edge_copy = copy_on(k, t, side, part_ref.at[jl, at])
            inner_copy = copy_on(k, t, side, got.at[side, jl, at])
            pl.when(going & edge)(edge_copy.wait_send if wait else edge_copy.start)
            pl.when(going & jnp.logical_not(edge))(inner_copy.wait_send if wait else inner_copy.start)

    def publish(k, wait):
        @pl.when(own)
        def _():
            if wait:
                to_partner(k).wait_send()
                keep(k).wait()
            else:
                to_partner(k).start()
                keep(k).start()

    def own_chunk(k):
        @pl.when(own)
        def _():
            if k == 0:
                for one in fetch:
                    one.wait()
            jl = z % 2
            pl.when(z > 0)(arrived(0, jl, k).wait_recv)
            pl.when(z < n_z - 1)(arrived(1, jl, k).wait_recv)
            finish(jl, k)
            if k > 0:
                to_partner(k - 1).start()
                keep(k - 1).start()

    for n, (k, t) in enumerate(steps):
        jl, j, at = where_is(k, t)
        for side in range(2):
            going = (z < j) if side == 0 else (z > j)
            inner = (z > 0) if side == 0 else (z < n_z - 1)

            @pl.when(going & inner)
            def _():
                arrived(side, jl, k).wait_recv()
                add_in(side, jl, k)

        if n > 0:
            send_step(*steps[n - 1], False)
        if t == 1 and k > 0:
            own_chunk(k - 1)
    send_step(*steps[-1], False)
    own_chunk(CHUNKS - 1)

    @pl.when(jnp.logical_not(own))
    def _():
        for one in fetch:
            one.wait()

    @pl.when(own)
    def _():
        to_partner(CHUNKS - 1).start()
        keep(CHUNKS - 1).start()

    for k, t in steps:
        send_step(k, t, True)
    for k in range(CHUNKS):
        publish(k, True)
        at = d_out.at[pl.ds(k * rows, rows)]
        pl.when(jnp.logical_not(own))(remote(at, at, p_s.at[k], p_r.at[k], (d, z)).wait_recv)


def sum_line(part, resid, cot, gain, n_z):
    _, full, width = part.shape
    return pl.pallas_call(
        functools.partial(sum_line_kernel, n_z),
        in_specs=[VMEM_SPEC, ANY_SPEC, ANY_SPEC, VMEM_SPEC],
        out_specs=[ANY_SPEC, VMEM_SPEC],
        out_shape=[jax.ShapeDtypeStruct((full, width), jnp.bfloat16), jax.ShapeDtypeStruct((8, width), jnp.float32)],
        scratch_shapes=[
            pltpu.VMEM((2, 2, full, width), jnp.bfloat16), pltpu.VMEM((full, width), jnp.bfloat16),
            pltpu.VMEM((full, width), jnp.bfloat16), pltpu.VMEM((full, width), jnp.bfloat16),
            DMA((2, CHUNKS)), DMA((2, 2, CHUNKS)), DMA((CHUNKS,)), DMA((CHUNKS,)), DMA((CHUNKS,)), DMA((2,)),
        ],
        compiler_params=pltpu.CompilerParams(collective_id=3, has_side_effects=True, vmem_limit_bytes=56 * 1024 * 1024),
        cost_estimate=pl.CostEstimate(flops=0, bytes_accessed=200_000_000, transcendentals=0),
        name="sum_line",
    )(part, resid, cot, gain)


class Adam:
    def __init__(self, count, sources, targets, views, bufs, sems, compute):
        self.count, self.sources, self.targets, self.views = count, sources, targets, views
        self.ins, self.outs = bufs[:4], bufs[4:]
        self.in_sem, self.out_sem = sems
        self.compute = compute

    def each(self, i, slot, inward):
        view_grad, view = self.views
        for n in range(4):
            if inward:
                cut = view_grad if n == 0 else view
                yield pltpu.make_async_copy(cut(self.sources[n], i), self.ins[n].at[slot], self.in_sem.at[slot, n])
            else:
                yield pltpu.make_async_copy(self.outs[n].at[slot], view(self.targets[n], i), self.out_sem.at[slot, n])

    def start(self):
        for copy in self.each(0, 0, True):
            copy.start()

    def run(self, low, high):
        def one(i, carry):
            slot = lax.rem(i, 2)

            @pl.when(i + 1 < self.count)
            def _():
                for copy in self.each(i + 1, 1 - slot, True):
                    copy.start()

            for copy in self.each(i, slot, True):
                copy.wait()

            @pl.when(i >= 2)
            def _():
                for copy in self.each(i - 2, slot, False):
                    copy.wait()

            self.compute(slot)
            for copy in self.each(i, slot, False):
                copy.start()
            return carry

        lax.fori_loop(low, high, one, 0)

    def end(self):
        for i in range(max(0, self.count - 2), self.count):
            for copy in self.each(i, i % 2, False):
                copy.wait()


def wide_compute(ins, outs):
    width = ins[1].shape[-1]

    def compute(slot):
        for n in range(2):
            grad = ins[0][slot, :, n * width : (n + 1) * width].astype(jnp.float32)
            value = adam_update(ins[1][slot, :, n], grad, ins[2][slot, :, n], ins[3][slot, :, n])
            outs[0][slot, :, n] = grad
            for k in range(3):
                outs[1 + k][slot, :, n] = value[k]

    return compute


def turned_compute(ins, outs):
    def compute(slot):
        grad = ins[0][slot].astype(jnp.float32).T
        value = adam_update(ins[1][slot], grad, ins[2][slot], ins[3][slot])
        outs[0][slot] = grad
        for k in range(3):
            outs[1 + k][slot] = value[k]

    return compute


WIDE_ROWS = 16
TURNED_ROWS = 128


def hand_out_kernel(n_dp, n_z, dn_ref, x_ref, dr_ref, gain_ref, gain2_ref, qt_ref, ot_ref, *refs):
    wide_in, turned_in = refs[0:4], refs[4:8]
    ig, gq, go, gains = refs[8:12]
    wide_out, turned_out = refs[12:16], refs[16:20]
    (got, buf, q_got, q_own, q_mid, q_put, q_fin, o_got, o_own, o_mid, o_put, o_fin, g_src, g_all) = refs[20:34]
    wide_bufs, turned_bufs = refs[34:42], refs[42:50]
    (p_s, p_r, i_s, i_r, q_s, q_r, qf_s, qf_r, o_s, o_r, of_s, of_r, g_s, g_r, q_loc, o_loc, loc,
     a_in, a_out, b_in, b_out) = refs[50:]
    d, z, pair, c = place()
    n_d = n_dp // 2
    total = n_dp * n_z
    me = d * n_z + z
    cz = z // 2
    full, width = x_ref.shape
    half = full // 2
    quarter = half // 2
    q_rows, q_cols = q_fin.shape[1:]
    o_rows, o_cols = o_fin.shape[1:]
    relay = n_d == 4

    wide = Adam(
        wide_in[1].shape[0] // WIDE_ROWS, wide_in, wide_out,
        (lambda ref, i: ref.at[pl.ds(pl.multiple_of(i * WIDE_ROWS, WIDE_ROWS), WIDE_ROWS)],) * 2,
        wide_bufs, (a_in, a_out), wide_compute(wide_bufs[:4], wide_bufs[4:]),
    )
    turned = Adam(
        turned_in[1].shape[0] // TURNED_ROWS, turned_in, turned_out,
        (lambda ref, i: ref.at[:, pl.ds(pl.multiple_of(i * TURNED_ROWS, TURNED_ROWS), TURNED_ROWS)],
         lambda ref, i: ref.at[pl.ds(pl.multiple_of(i * TURNED_ROWS, TURNED_ROWS), TURNED_ROWS)]),
        turned_bufs, (b_in, b_out), turned_compute(turned_bufs[:4], turned_bufs[4:]),
    )

    class First:
        def __init__(self, src, rows, cols, bufs, sems, spare):
            self.src, self.rows, self.cols, self.spare = src, rows, cols, spare
            self.got, self.own, self.mid, self.put, self.fin = bufs
            self.send, self.recv, self.f_send, self.f_recv, self.loc = sems

        def block(self, ref, b, core):
            return ref.at[pl.ds(core * self.rows, self.rows), pl.ds(b * self.cols, self.cols)]

        def source(self, owner, b, core):
            return self.src.at[pl.ds(pl.multiple_of((2 * owner + core) * self.rows, self.rows), self.rows), pl.ds(b * self.cols, self.cols)]

        def copy(self, n, b, core, owner, to):
            return remote(self.source(owner, b, core), self.block(self.got.at[n], b, core), self.send.at[n, b, core],
                          self.recv.at[n, b, core], (2 * (pair ^ to) + c, z))

        def loads(self, b, core):
            yield pltpu.make_async_copy(self.source(pair, b, core), self.block(self.own, b, core), self.loc.at[0, b, core])
            if relay:
                yield pltpu.make_async_copy(self.source(pair ^ (2 >> b), b, core), self.block(self.mid, b, core), self.loc.at[1, b, core])

        def begin(self, core):
            for b in range(2):
                if relay:
                    self.copy(1, b, core, pair ^ 3, 1 + b).start()
            for b in range(2):
                if relay:
                    self.copy(0, b, core, pair ^ (1 + b), 1 + b).start()
                else:
                    for k in range(1, n_d):
                        self.copy(k - 1, b, core, pair ^ k, k).start()

        def arrived(self, n, b, core):
            at = self.block(self.got.at[n], b, core)
            remote(at, at, self.send.at[n, b, core], self.recv.at[n, b, core], (d, z)).wait_recv()

        def cut(self, b, core, r):
            return pl.ds(pl.multiple_of(core * self.rows + r * 16, 16), 16), pl.ds(b * self.cols, self.cols)

        def middle_copy(self, b, core):
            return remote(self.block(self.mid, b, core), self.block(self.got.at[2], b, core), self.send.at[2, b, core],
                          self.recv.at[2, b, core], (2 * (pair ^ (2 >> b)) + c, z))

        def middle(self, core, between):
            if not relay:
                return
            for b in range(2):
                self.arrived(1, b, core)

                def add(r, carry):
                    at = self.cut(b, core, r)
                    self.mid[at] = (self.mid[at].astype(jnp.float32) + self.got[(1,) + at].astype(jnp.float32)).astype(jnp.bfloat16)
                    return carry

                lax.fori_loop(0, self.rows // 16, add, 0)
            self.middle_copy(0, core).start()
            between()
            self.middle_copy(1, core).start()

        def total(self, core, between):
            slots = (0, 2) if relay else range(n_d - 1)
            for b in range(2):
                for n in slots:
                    self.arrived(n, b, core)

                def add(r, carry):
                    at = self.cut(b, core, r)
                    value = self.own[at].astype(jnp.float32)
                    for n in slots:
                        value = value + self.got[(n,) + at].astype(jnp.float32)
                    self.put[core, b, pl.ds(pl.multiple_of(r * 16, 16), 16)] = value.astype(jnp.bfloat16)
                    return carry

                lax.fori_loop(0, self.rows // 16, add, 0)
            self.second(0, core, False)
            between()
            self.second(1, core, False)

        def second(self, b, core, wait):
            here = (core == c) & (2 * c + b == z)
            src = self.put.at[core, b]
            copy = remote(src, self.fin.at[z], self.f_send.at[core, b], self.f_recv.at[z], (2 * pair + core, 2 * c + b))
            keep = pltpu.make_async_copy(src, self.fin.at[z], loc.at[self.spare])
            pl.when(jnp.logical_not(here))(copy.wait_send if wait else copy.start)
            pl.when(here)(keep.wait if wait else keep.start)

        def final(self):
            for core in range(2):
                for b in range(2):
                    self.second(b, core, True)
            for zs in range(n_z):
                at = self.fin.at[zs]
                from_here = (cz == c) & (zs == z)
                pl.when(jnp.logical_not(from_here))(remote(at, at, self.f_send.at[0, 0], self.f_recv.at[zs], (d, z)).wait_recv)

        def sent(self):
            for b in range(2):
                for core in range(2):
                    for n in range(n_d - 1):
                        at = self.block(self.got.at[n], b, core)
                        remote(at, at, self.send.at[n, b, core], self.recv.at[n, b, core], (d, z)).wait_send()

    o_first = First(ot_ref, o_rows, o_cols, (o_got, o_own, o_mid, o_put, o_fin), (o_s, o_r, of_s, of_r, o_loc), 2)
    q_first = First(qt_ref, q_rows, q_cols, (q_got, q_own, q_mid, q_put, q_fin), (q_s, q_r, qf_s, qf_r, q_loc), 3)
    for one in (o_first, q_first):
        for core in range(2):
            for b in range(2):
                for copy in one.loads(b, core):
                    copy.start()
    turned.start()
    wide.start()
    greet_all(n_dp, n_z, d, z)

    mine = pl.ds(pl.multiple_of(c * half, half), half)
    theirs = pl.ds(pl.multiple_of((1 - c) * half, half), half)
    swap = remote(dn_ref.at[theirs], got, p_s, p_r, (2 * pair + 1 - c, z))
    swap.start()
    o_first.begin(0)
    o_first.begin(1)

    g_src[pl.ds(0, 8)] = jnp.zeros((8, width), jnp.float32)
    g_src[pl.ds(8, 8)] = gain2_ref[...]
    swap.wait_recv()

    def rows_of(r, carry):
        at = pl.ds(pl.multiple_of(r * 16, 16), 16)
        src = pl.ds(pl.multiple_of(c * half + r * 16, 16), 16)
        d_normed = dn_ref[src].astype(jnp.float32) + got[at].astype(jnp.float32)
        value = x_ref[src].astype(jnp.float32)
        inverse = lax.rsqrt(jnp.mean(value * value, axis=-1, keepdims=True) + norm_eps)
        scaled = value * inverse
        d_scaled = d_normed * gain_ref[...]
        mean = jnp.mean(d_scaled * scaled, axis=-1, keepdims=True)
        out = dr_ref[src].astype(jnp.float32) + inverse * (d_scaled - scaled * mean)
        buf[at] = out.astype(jnp.bfloat16)
        prod = d_normed * scaled
        g_src[pl.ds(0, 8)] = g_src[pl.ds(0, 8)] + prod[:8] + prod[8:]
        return carry

    def row_send(b, wait):
        src = buf.at[pl.ds(b * quarter, quarter)]
        dst = ig.at[z % 2]
        zz = 2 * c + b
        here = (cz == c) & (zz == z)
        copy = remote(src, dst, i_s.at[b], i_r.at[z % 2], (2 * pair + cz, zz))
        keep = pltpu.make_async_copy(src, dst, loc.at[0])
        pl.when(jnp.logical_not(here))(copy.wait_send if wait else copy.start)
        pl.when(here)(keep.wait if wait else keep.start)

    for one in (o_first, q_first):
        for core in range(2):
            for b in range(2):
                for copy in one.loads(b, core):
                    copy.wait()
    per = quarter // 16
    lax.fori_loop(0, per, rows_of, 0)
    o_first.middle(0, lambda: row_send(0, False))
    q_first.begin(0)
    lax.fori_loop(per, 2 * per, rows_of, 0)
    o_first.middle(1, lambda: row_send(1, False))
    q_first.begin(1)

    each = width // total

    def gain_tile(o):
        return g_src.at[:, pl.ds(pl.multiple_of(o * each // 128 * 128, 128), 128)]

    own_gain = pltpu.make_async_copy(gain_tile(me), g_all.at[me], loc.at[1])
    own_gain.start()

    def send_gain(o, carry):
        other = lax.rem(me + o, total)
        remote(gain_tile(other), g_all.at[me], g_s, g_r, (other // n_z, lax.rem(other, n_z))).start()
        return carry

    lax.fori_loop(1, total, send_gain, 0)

    def share(adam, n, parts):
        return lambda: adam.run(n * adam.count // parts, (n + 1) * adam.count // parts)

    share(turned, 0, 2)()
    o_first.total(0, share(wide, 0, 8))
    q_first.middle(0, share(wide, 1, 8))
    share(turned, 1, 2)()
    o_first.total(1, share(wide, 2, 8))
    share(wide, 3, 8)()
    q_first.middle(1, share(wide, 4, 8))
    share(wide, 5, 8)()
    q_first.total(0, share(wide, 6, 8))
    q_first.total(1, share(wide, 7, 8))

    o_first.final()
    value = o_fin[0].astype(jnp.float32)
    for zs in range(1, n_z):
        value = value + o_fin[zs].astype(jnp.float32)
    go[...] = value.T
    turned.end()
    wide.end()

    many = g_all.at[pl.ds(0, total - 1)]
    gain_copy = remote(many, many, g_s, g_r, (d, z))
    gain_copy.wait_send()
    gain_copy.wait_recv()
    own_gain.wait()
    gains[...] = jnp.zeros_like(gains)

    def add_gain(o, carry):
        gains[...] = gains[...] + g_all[o]
        return carry

    lax.fori_loop(0, total, add_gain, 0)

    swap.wait_send()
    for b in range(2):
        row_send(b, True)
    for i in range(2):
        from_here = (cz == c) & (2 * c + i == z)
        at = ig.at[i]
        pl.when(jnp.logical_not(from_here))(remote(at, at, i_s.at[0], i_r.at[i], (d, z)).wait_recv)
    o_first.sent()
    q_first.sent()
    q_first.final()

    def last(r, carry):
        at = pl.ds(pl.multiple_of(r * 16, 16), 16)
        value = q_fin[0, at].astype(jnp.float32)
        for zs in range(1, n_z):
            value = value + q_fin[zs, at].astype(jnp.float32)
        gq[at] = value
        return carry

    lax.fori_loop(0, q_rows // 16, last, 0)


def hand_out(dn, x, dr, gain, gain2, qt, ot, wide, turned, n_dp, n_z):
    full, width = x.shape
    n_d = n_dp // 2
    total = n_dp * n_z
    q_rows, q_cols = qt.shape[0] // n_dp, qt.shape[1] // 2
    o_rows, o_cols = ot.shape[0] // n_dp, ot.shape[1] // 2
    b16 = jnp.bfloat16
    f32 = jnp.float32

    def weight_bufs(rows, cols):
        return [
            pltpu.VMEM((n_d - 1, 2 * rows, 2 * cols), b16), pltpu.VMEM((2 * rows, 2 * cols), b16),
            pltpu.VMEM((2 * rows, 2 * cols), b16), pltpu.VMEM((2, 2, rows, cols), b16), pltpu.VMEM((n_z, rows, cols), b16),
        ]

    wide_shape = (2, WIDE_ROWS) + wide[1].shape[1:]
    turned_shape = (2, TURNED_ROWS, turned[1].shape[1])
    weight_sems = [DMA((n_d - 1, 2, 2)), DMA((n_d - 1, 2, 2)), DMA((2, 2)), DMA((n_z,))]
    return pl.pallas_call(
        functools.partial(hand_out_kernel, n_dp, n_z),
        in_specs=[VMEM_SPEC] * 5 + [ANY_SPEC] * 10,
        out_specs=[ANY_SPEC] + [VMEM_SPEC] * 3 + [ANY_SPEC] * 8,
        out_shape=[
            jax.ShapeDtypeStruct((2, full // 4, width), b16),
            jax.ShapeDtypeStruct((q_rows, q_cols), f32),
            jax.ShapeDtypeStruct((o_cols, o_rows), f32),
            jax.ShapeDtypeStruct((16, 128), f32),
        ]
        + [jax.ShapeDtypeStruct(wide[1].shape, f32)] * 4
        + [jax.ShapeDtypeStruct(turned[1].shape, f32)] * 4,
        scratch_shapes=[
            pltpu.VMEM((full // 2, width), b16), pltpu.VMEM((full // 2, width), b16),
            *weight_bufs(q_rows, q_cols), *weight_bufs(o_rows, o_cols),
            pltpu.VMEM((16, width), f32), pltpu.VMEM((total, 16, 128), f32),
            pltpu.VMEM((2, WIDE_ROWS, wide[0].shape[1]), b16), *[pltpu.VMEM(wide_shape, f32)] * 7,
            pltpu.VMEM((2, turned[0].shape[0], TURNED_ROWS), b16), *[pltpu.VMEM(turned_shape, f32)] * 7,
            DMA, DMA, DMA((2,)), DMA((2,)), *weight_sems, *weight_sems, DMA, DMA,
            DMA((2, 2, 2)), DMA((2, 2, 2)), DMA((4,)), DMA((2, 4)), DMA((2, 4)), DMA((2, 4)), DMA((2, 4)),
        ],
        compiler_params=pltpu.CompilerParams(collective_id=5, has_side_effects=True, vmem_limit_bytes=58 * 1024 * 1024),
        cost_estimate=pl.CostEstimate(flops=0, bytes_accessed=300_000_000, transcendentals=0),
        name="hand_out",
    )(dn, x, dr, gain, gain2, qt, ot, *wide, *turned)


def rms_forward(values, gain_wide):
    inverse = lax.rsqrt(jnp.mean(values * values, axis=-1, keepdims=True) + norm_eps)
    scaled = values * inverse
    return (scaled, inverse, (scaled * gain_wide).astype(jnp.bfloat16))


def adam_update(weight, grad, first, second):
    new_first = beta_one * first + (1.0 - beta_one) * grad
    new_second = beta_two * second + (1.0 - beta_two) * grad * grad
    first_hat = new_first / (1.0 - beta_one**step_count)
    second_hat = new_second / (1.0 - beta_two**step_count)
    new_weight = weight - learn_rate * (
        first_hat / (jnp.sqrt(second_hat) + adam_eps) + weight_decay * weight
    )
    return (new_weight, new_first, new_second)


def contract_rows(left, right):
    return lax.dot_general(
        left, right, (((0,), (0,)), ((), ())), preferred_element_type=jnp.float32
    )


def times_transpose(left, right):
    return lax.dot_general(
        left, right, (((1,), (1,)), ((), ())), preferred_element_type=jnp.float32
    )


def layer_step(
    block_input,
    segment_ids,
    cotangent,
    attn_gain,
    qkv_weight,
    out_weight,
    mlp_gain,
    gate_up_weight,
    down_weight,
    first_attn_gain,
    first_qkv,
    first_out,
    first_mlp_gain,
    first_gate_up,
    first_down,
    second_attn_gain,
    second_qkv,
    second_out,
    second_mlp_gain,
    second_gate_up,
    second_down,
):
    seqs_here, local_len, width = block_input.shape
    full_len = segment_ids.shape[1]
    n_dp = lax.axis_size("dp")
    n_z = lax.axis_size("seq")
    groups = HEADS // KV_HEADS
    unit_count = down_weight.shape[0]
    z_here = lax.axis_index("seq")
    owned = attn_gain.shape[0]
    gain_line = jnp.concatenate([attn_gain, mlp_gain]).astype(jnp.bfloat16).astype(jnp.float32)
    gain_tile = jnp.pad(gain_line[None], ((0, 7), (0, LANES - 2 * owned)))
    seg_tile = jnp.pad(segment_ids, ((0, 8 - seqs_here), (0, 0)))
    gate_up_here = gate_up_weight.astype(jnp.bfloat16).reshape(-1, 2 * unit_count)
    down_rows = lax.all_gather(down_weight.astype(jnp.bfloat16), "dp", axis=1, tiled=True)
    rows_in, qkv_cols, out_line, gain_all, seg_all = gather_in(
        block_input,
        qkv_weight.astype(jnp.bfloat16),
        out_weight.astype(jnp.bfloat16).T,
        gain_tile,
        seg_tile,
        n_dp,
        n_z,
    )
    cot_late, _ = lax.optimization_barrier((cotangent, gain_all))
    cot_all = lax.all_gather(cot_late, "seq", axis=1, tiled=True)
    gain_one = gain_all[:, 0, :owned].reshape(1, width)
    gain_two = gain_all[:, 0, owned : 2 * owned].reshape(1, width)
    seg_here = lax.dynamic_slice(seg_all, (z_here // 2, z_here % 2, 0), (1, 1, full_len))[0]
    tables = attn_tables(seg_here)
    _, _, normed_one = rms_forward(rows_in.astype(jnp.float32), gain_one)
    qkv = jnp.dot(normed_one, qkv_cols, preferred_element_type=jnp.float32)
    turned, lse, attended16, out_rows = attn_forward(qkv, *tables, out_line, full_len, groups, n_dp)
    attn_part = times_transpose(attended16, out_rows)
    resid_all, gate_up_cols = share_resid(
        attn_part.astype(jnp.bfloat16), rows_in, gate_up_here, n_dp, n_z
    )
    total_rows = seqs_here * full_len
    resid = resid_all.reshape(total_rows, width).astype(jnp.float32)
    _, _, normed_two = rms_forward(resid, gain_two)
    gate_up = jnp.dot(normed_two, gate_up_cols, preferred_element_type=jnp.float32)
    gate_part = gate_up[:, :unit_count]
    up_part = gate_up[:, unit_count:]
    sigmoid_gate = jax.nn.sigmoid(gate_part)
    active = gate_part * sigmoid_gate
    hidden16 = (active * up_part).astype(jnp.bfloat16)
    cot_rows = cot_all.reshape(total_rows, width)
    d_hidden = times_transpose(cot_rows, down_rows)
    d_gate = d_hidden * up_part * sigmoid_gate * (1.0 + gate_part * (1.0 - sigmoid_gate))
    d_up = d_hidden * active
    d_gate_up16 = jnp.concatenate([d_gate, d_up], 1).astype(jnp.bfloat16)
    down_part = jnp.dot(hidden16, down_rows, preferred_element_type=jnp.float32)
    down_here = lax.psum_scatter(
        down_part.astype(jnp.bfloat16).reshape(resid_all.shape), "seq", scatter_dimension=1, tiled=True
    )
    gate_up_term = contract_rows(normed_two, d_gate_up16).astype(jnp.bfloat16)
    gate_up_sum = lax.psum_scatter(gate_up_term, "dp", scatter_dimension=0, tiled=True)
    down_term = contract_rows(cot_rows, hidden16).astype(jnp.bfloat16)
    down_sum = lax.psum_scatter(down_term, "dp", scatter_dimension=0, tiled=True)
    d_normed_two = times_transpose(d_gate_up16, gate_up_cols).astype(jnp.bfloat16)
    d_resid16, gain_two_part = sum_line(
        d_normed_two.reshape(resid_all.shape), resid_all, cot_all, gain_two, n_z
    )
    down_here = down_here.astype(jnp.float32)
    resid_here = lax.dynamic_slice_in_dim(resid_all, z_here * local_len, local_len, 1)
    output = (resid_here.astype(jnp.float32) + down_here).astype(jnp.bfloat16)
    d_attended = jnp.dot(d_resid16, out_rows, preferred_element_type=jnp.float32).astype(jnp.bfloat16)
    d_qkv16 = attn_backward(turned, d_attended, lse, *tables, full_len, groups)
    d_normed_one = times_transpose(d_qkv16, qkv_cols).astype(jnp.bfloat16)
    qkv_term = contract_rows(normed_one, d_qkv16).astype(jnp.bfloat16)
    out_term = contract_rows(d_resid16, attended16).astype(jnp.bfloat16)
    input_grad, grad_qkv, grad_out, gain_sums, *updated = hand_out(
        d_normed_one,
        rows_in,
        d_resid16,
        gain_one,
        gain_two_part,
        qkv_term,
        out_term,
        (gate_up_sum, gate_up_weight, first_gate_up, second_gate_up),
        (down_sum, down_weight, first_down, second_down),
        n_dp,
        n_z,
    )
    grad_gate_up, w_gu, m_gu, v_gu, grad_down, w_down, m_down, v_down = updated
    flat = lax.axis_index("dp") * n_z + z_here
    gain_sums = lax.dynamic_slice(
        jnp.sum(gain_sums.reshape(2, 8, LANES), axis=1), (0, flat * owned % LANES), (2, owned)
    )
    grad_gain_one = gain_sums[0]
    grad_gain_two = gain_sums[1]
    w_one, m_one, v_one = adam_update(attn_gain, grad_gain_one, first_attn_gain, second_attn_gain)
    w_qkv, m_qkv, v_qkv = adam_update(qkv_weight, grad_qkv, first_qkv, second_qkv)
    w_out, m_out, v_out = adam_update(out_weight, grad_out, first_out, second_out)
    w_two, m_two, v_two = adam_update(mlp_gain, grad_gain_two, first_mlp_gain, second_mlp_gain)
    return (
        output,
        input_grad,
        grad_gain_one,
        grad_qkv,
        grad_out,
        grad_gain_two,
        grad_gate_up,
        grad_down,
        w_one,
        w_qkv,
        w_out,
        w_two,
        w_gu,
        w_down,
        m_one,
        m_qkv,
        m_out,
        m_two,
        m_gu,
        m_down,
        v_one,
        v_qkv,
        v_out,
        v_two,
        v_gu,
        v_down,
    )


def solution(mesh):
    in_specs = (
        P("dp", "seq", None),
        P("dp", None),
        P("dp", "seq", None),
        P(("dp", "seq")),
        P("dp", "seq"),
        P("seq", "dp"),
        P(("dp", "seq")),
        P("dp", None, "seq"),
        P("seq", "dp"),
        P(("dp", "seq")),
        P("dp", "seq"),
        P("seq", "dp"),
        P(("dp", "seq")),
        P("dp", None, "seq"),
        P("seq", "dp"),
        P(("dp", "seq")),
        P("dp", "seq"),
        P("seq", "dp"),
        P(("dp", "seq")),
        P("dp", None, "seq"),
        P("seq", "dp"),
    )
    out_specs = (
        P("dp", "seq", None),
        P("dp", "seq", None),
        P(("dp", "seq")),
        P("dp", "seq"),
        P("seq", "dp"),
        P(("dp", "seq")),
        P("dp", None, "seq"),
        P("seq", "dp"),
        P(("dp", "seq")),
        P("dp", "seq"),
        P("seq", "dp"),
        P(("dp", "seq")),
        P("dp", None, "seq"),
        P("seq", "dp"),
        P(("dp", "seq")),
        P("dp", "seq"),
        P("seq", "dp"),
        P(("dp", "seq")),
        P("dp", None, "seq"),
        P("seq", "dp"),
        P(("dp", "seq")),
        P("dp", "seq"),
        P("seq", "dp"),
        P(("dp", "seq")),
        P("dp", None, "seq"),
        P("seq", "dp"),
    )
    return jax.shard_map(layer_step, mesh=mesh, in_specs=in_specs, out_specs=out_specs, check_vma=False)
```

```python
import functools

import jax
import jax.numpy as jnp
from jax import lax
from jax.experimental import pallas as pl
from jax.experimental.pallas import tpu as pltpu
from jax.sharding import PartitionSpec as P


HEADS = 32
KV_HEADS = 8
norm_eps = 1e-05
beta_one = 0.9
beta_two = 0.95
learn_rate = 0.01
weight_decay = 0.1
adam_eps = 1e-08
step_count = 10.0
masked_score = -1e30


HEAD_DIM = 64
LANES = 128


def dot_t(a, b):
    return lax.dot_general(a, b, (((1,), (1,)), ((), ())), preferred_element_type=jnp.float32)


def dot_n(a, b):
    return lax.dot_general(a, b, (((1,), (0,)), ((), ())), preferred_element_type=jnp.float32)


def dot_c(a, b):
    return lax.dot_general(a, b, (((0,), (0,)), ((), ())), preferred_element_type=jnp.float32)


def swap_halves(u):
    lane = lax.broadcasted_iota(jnp.int32, u.shape, 1)
    return jnp.where(lane % 64 < 32, pltpu.roll(u, 96, 1), pltpu.roll(u, 32, 1))


def turn(u, cos_wide, sin_wide):
    return u * cos_wide + swap_halves(u) * sin_wide


def key_start(block, q_rows, reach):
    return max(0, (block * q_rows - reach + 1) // q_rows * q_rows)


def attn_forward_kernel(pairs, q_rows, reach, qkv_ref, cos_ref, sin_ref, seg_col_ref, seg_row_ref,
                        turned_ref, lse_ref, out_ref):
    full_len = qkv_ref.shape[0]
    lane = lax.broadcasted_iota(jnp.int32, (full_len, LANES), 1)
    low = lane < HEAD_DIM
    cos_q = cos_ref[...]
    sin_q = sin_ref[...]
    kv = qkv_ref[:, pairs * LANES:].astype(jnp.float32)
    kv16 = turn(kv, jnp.where(low, cos_q, 1.0), jnp.where(low, sin_q, 0.0)).astype(jnp.bfloat16)
    turned_ref[:, pairs * LANES:] = kv16
    kv32 = kv16.astype(jnp.float32)
    rolled = pltpu.roll(kv32, HEAD_DIM, 1)
    zero = jnp.zeros_like(kv32)
    keys = (jnp.where(low, kv32, zero).astype(jnp.bfloat16), jnp.where(low, zero, rolled).astype(jnp.bfloat16))
    vals = (jnp.where(low, rolled, zero).astype(jnp.bfloat16), jnp.where(low, zero, kv32).astype(jnp.bfloat16))
    for pair in range(pairs):
        cols = slice(pair * LANES, (pair + 1) * LANES)
        query = turn(qkv_ref[:, cols].astype(jnp.float32), cos_q, sin_q) .astype(jnp.bfloat16)
        turned_ref[:, cols] = query
    for block in range(full_len // q_rows):
        first = key_start(block, q_rows, reach)
        last = (block + 1) * q_rows
        rows = slice(block * q_rows, last)
        span = slice(first, last)
        i = lax.broadcasted_iota(jnp.int32, (q_rows, last - first), 0) + block * q_rows
        j = lax.broadcasted_iota(jnp.int32, (q_rows, last - first), 1) + first
        allowed = (j <= i) & (seg_col_ref[rows, :1] == seg_row_ref[:1, span])
        for pair in range(pairs):
            cols = slice(pair * LANES, (pair + 1) * LANES)
            query = turned_ref[rows, cols]
            total = None
            for half in range(2):
                scores = dot_t(query, keys[half][span]) * (HEAD_DIM ** -0.5)
                scores = jnp.where(allowed, scores, masked_score)
                top = jnp.max(scores, axis=1, keepdims=True)
                lse = top + jnp.log(jnp.sum(jnp.exp(scores - top), axis=1, keepdims=True))
                probs = jnp.exp(scores - lse).astype(jnp.bfloat16)
                part = dot_n(probs, vals[half][span])
                total = part if total is None else total + part
                head = 2 * pair + half
                lse_ref[rows, head:head + 1] = lse
            out_ref[rows, cols] = total.astype(jnp.bfloat16)


def attn_backward_kernel(pairs, q_rows, reach, turned_ref, d_out_ref, lse_ref, cos_ref, sin_ref, seg_col_ref,
                         seg_row_ref, grad_ref, dk_ref, dv_ref):
    full_len = turned_ref.shape[0]
    lane = lax.broadcasted_iota(jnp.int32, (full_len, LANES), 1)
    low = lane < HEAD_DIM
    kv32 = turned_ref[:, pairs * LANES:].astype(jnp.float32)
    rolled = pltpu.roll(kv32, HEAD_DIM, 1)
    zero = jnp.zeros_like(kv32)
    keys = (jnp.where(low, kv32, zero).astype(jnp.bfloat16), jnp.where(low, zero, rolled).astype(jnp.bfloat16))
    vals = (jnp.where(low, rolled, zero).astype(jnp.bfloat16), jnp.where(low, zero, kv32).astype(jnp.bfloat16))
    dk_ref[...] = jnp.zeros_like(dk_ref)
    dv_ref[...] = jnp.zeros_like(dv_ref)
    low_rows = low[:q_rows]
    scale = HEAD_DIM ** -0.5
    for block in range(full_len // q_rows):
        first = key_start(block, q_rows, reach)
        last = (block + 1) * q_rows
        rows = slice(block * q_rows, last)
        span = slice(first, last)
        i = lax.broadcasted_iota(jnp.int32, (q_rows, last - first), 0) + block * q_rows
        j = lax.broadcasted_iota(jnp.int32, (q_rows, last - first), 1) + first
        allowed = (j <= i) & (seg_col_ref[rows, :1] == seg_row_ref[:1, span])
        cos_q = cos_ref[rows]
        sin_q = sin_ref[rows]
        for pair in range(pairs):
            cols = slice(pair * LANES, (pair + 1) * LANES)
            query = turned_ref[rows, cols]
            d_out = d_out_ref[rows, cols]
            q32 = query.astype(jnp.float32)
            o32 = d_out.astype(jnp.float32)
            d_query = None
            d_key = None
            d_val = None
            for half in range(2):
                keep = low_rows if half == 0 else ~low_rows
                q_only = jnp.where(keep, q32, 0.0).astype(jnp.bfloat16)
                o_only = jnp.where(keep, o32, 0.0).astype(jnp.bfloat16)
                head = 2 * pair + half
                scores = dot_t(query, keys[half][span]) * scale
                scores = jnp.where(allowed, scores, masked_score)
                probs = jnp.exp(scores - lse_ref[rows, head:head + 1])
                d_probs = dot_t(d_out, vals[half][span])
                delta = jnp.sum(probs * d_probs, axis=1, keepdims=True)
                d_scores = (probs * (d_probs - delta) * scale).astype(jnp.bfloat16)
                probs16 = probs.astype(jnp.bfloat16)
                dq = dot_n(d_scores, keys[half][span])
                dk = dot_c(d_scores, q_only)
                dv = dot_c(probs16, o_only)
                d_query = dq if d_query is None else d_query + dq
                d_key = dk if d_key is None else d_key + dk
                d_val = dv if d_val is None else d_val + dv
            dk_ref[span] = dk_ref[span] + d_key
            dv_ref[span] = dv_ref[span] + d_val
            grad_ref[rows, cols] = turn(d_query, cos_q, -sin_q).astype(jnp.bfloat16)
    d_key = dk_ref[...]
    d_val = dv_ref[...]
    d_key = d_key + pltpu.roll(d_key, HEAD_DIM, 1)
    d_val = d_val + pltpu.roll(d_val, HEAD_DIM, 1)
    d_key = turn(d_key, cos_ref[...], -sin_ref[...])
    grad_ref[:, pairs * LANES:] = jnp.where(low, d_key, d_val).astype(jnp.bfloat16)


def attn_specs(full_len, width):
    line = pl.BlockSpec((full_len, width), lambda s, g: (s, g))
    table = pl.BlockSpec((full_len, LANES), lambda s, g: (s, 0))
    row = pl.BlockSpec((8, full_len), lambda s, g: (s, 0))
    return line, table, row


Q_ROWS = 128
REACH = 256


def attn_gather_kernel(n_dp, pairs, q_rows, reach, qkv_ref, cos_ref, sin_ref, seg_col_ref, seg_row_ref, vo_ref,
                       turned_ref, lse_ref, out_ref, wo, d_s, d_r, loc):
    _, z, pair, c = place()
    n_d = n_dp // 2
    step = pl.program_id(1)
    steps = pl.num_programs(1)
    rows = vo_ref.shape[0]
    parts = 2
    part = rows // parts // 2

    def spot(owner, t, h):
        return wo.at[pl.ds(pl.multiple_of(owner * rows + (2 * t + h) * part, part), part)]

    spread = Spread(n_d, pair, c, z, parts, spot, d_s, d_r)
    keep = pltpu.make_async_copy(vo_ref, wo.at[pl.ds(pl.multiple_of(pair * rows, rows), rows)], loc)

    @pl.when(step == 0)
    def _():
        keep.start()
        barrier = pltpu.get_barrier_semaphore()
        for k in range(1, n_d):
            pl.semaphore_signal(barrier, inc=1, device_id=(2 * (pair ^ k) + c, z), device_id_type=MESH)
        pl.semaphore_wait(barrier, n_d - 1)
        keep.wait()
        for t in range(parts):
            spread.own(t)

    attn_forward_kernel(pairs, q_rows, reach, qkv_ref, cos_ref, sin_ref, seg_col_ref, seg_row_ref, turned_ref, lse_ref, out_ref)

    @pl.when(step == steps - 2)
    def _():
        spread.pass_on(0)

    @pl.when(step == steps - 1)
    def _():
        spread.pass_on(1)
        spread.finish()


def attn_forward(qkv, cos, sin, seg_col, seg_row, vo, full_len, groups, n_dp):
    pairs = groups // 2
    width = (groups + 2) * HEAD_DIM
    seqs = qkv.shape[0] // full_len
    kv = qkv.shape[1] // width
    n_d = n_dp // 2
    line, table, row = attn_specs(full_len, width)
    outw = pl.BlockSpec((full_len, groups * HEAD_DIM), lambda s, g: (s, g))
    rows = seqs * full_len
    return pl.pallas_call(
        functools.partial(attn_gather_kernel, n_dp, pairs, Q_ROWS, REACH),
        grid=(seqs, kv),
        in_specs=[line, table, table, table, row, VMEM_SPEC],
        out_specs=[line, pl.BlockSpec((full_len, LANES), lambda s, g: (s, g)), outw, ANY_SPEC],
        out_shape=[
            jax.ShapeDtypeStruct((rows, kv * width), jnp.bfloat16),
            jax.ShapeDtypeStruct((rows, kv * LANES), jnp.float32),
            jax.ShapeDtypeStruct((rows, kv * groups * HEAD_DIM), jnp.bfloat16),
            jax.ShapeDtypeStruct((n_d * vo.shape[0], vo.shape[1]), jnp.bfloat16),
        ],
        scratch_shapes=[DMA((n_d - 1, 2, 2)), DMA((n_d - 1, 2, 2)), DMA],
        compiler_params=pltpu.CompilerParams(collective_id=4, has_side_effects=True),
        cost_estimate=pl.CostEstimate(flops=4 * rows * full_len * kv * LANES * groups, bytes_accessed=150_000_000, transcendentals=0),
        name="attn_forward",
    )(qkv, cos, sin, seg_col, seg_row, vo)


def attn_backward(turned, d_out, lse, cos, sin, seg_col, seg_row, full_len, groups):
    pairs = groups // 2
    width = (groups + 2) * HEAD_DIM
    seqs = turned.shape[0] // full_len
    kv = turned.shape[1] // width
    line, table, row = attn_specs(full_len, width)
    outw = pl.BlockSpec((full_len, groups * HEAD_DIM), lambda s, g: (s, g))
    rows = seqs * full_len
    return pl.pallas_call(
        functools.partial(attn_backward_kernel, pairs, Q_ROWS, REACH),
        grid=(seqs, kv),
        in_specs=[line, outw, pl.BlockSpec((full_len, LANES), lambda s, g: (s, g)), table, table, table, row],
        out_specs=line,
        out_shape=jax.ShapeDtypeStruct((rows, kv * width), jnp.bfloat16),
        scratch_shapes=[pltpu.VMEM((full_len, LANES), jnp.float32)] * 2,
        cost_estimate=pl.CostEstimate(flops=10 * rows * full_len * kv * LANES * groups, bytes_accessed=rows * kv * width * 6, transcendentals=0),
        name="attn_backward",
    )(turned, d_out, lse, cos, sin, seg_col, seg_row)


def attn_tables(segment_ids):
    seqs, full_len = segment_ids.shape
    earlier = (segment_ids[..., None, :] < segment_ids[..., :, None]).astype(jnp.int32)
    positions = jnp.arange(full_len, dtype=jnp.int32) - jnp.sum(earlier, axis=-1, dtype=jnp.int32)
    inverse = 500000.0 ** (-2.0 * jnp.arange(HEAD_DIM // 2, dtype=jnp.float32) / HEAD_DIM)
    angles = positions.astype(jnp.float32)[..., None] * inverse
    cos = jnp.cos(angles)
    sin = jnp.sin(angles)
    cos = jnp.concatenate([cos] * 4, -1).reshape(seqs * full_len, LANES)
    sin = jnp.concatenate([-sin, sin] * 2, -1).reshape(seqs * full_len, LANES)
    seg_col = jnp.broadcast_to(segment_ids[:, :, None], (seqs, full_len, LANES)).reshape(seqs * full_len, LANES)
    seg_row = jnp.broadcast_to(segment_ids[:, None, :], (seqs, 8, full_len)).reshape(seqs * 8, full_len)
    return cos, sin, seg_col, seg_row


MESH = pl.DeviceIdType.MESH
VMEM_SPEC = pl.BlockSpec(memory_space=pltpu.VMEM)
ANY_SPEC = pl.BlockSpec(memory_space=pl.ANY)
DMA = pltpu.SemaphoreType.DMA


def place():
    d = lax.axis_index("dp")
    z = lax.axis_index("seq")
    return d, z, d // 2, d % 2


def remote(src, dst, send, recv, dev):
    return pltpu.make_async_remote_copy(
        src_ref=src, dst_ref=dst, send_sem=send, recv_sem=recv, device_id=dev, device_id_type=MESH
    )


def greet_all(n_dp, n_z, d, z):
    barrier = pltpu.get_barrier_semaphore()
    me = d * n_z + z

    def one(o, carry):
        other = lax.rem(me + o, n_dp * n_z)
        pl.semaphore_signal(barrier, inc=1, device_id=(other // n_z, lax.rem(other, n_z)), device_id_type=MESH)
        return carry

    lax.fori_loop(1, n_dp * n_z, one, 0)
    pl.semaphore_wait(barrier, n_dp * n_z - 1)


def greet_line(n_z, d, z, extra=()):
    barrier = pltpu.get_barrier_semaphore()
    c = d % 2
    for o in range(n_z):
        zz = lax.rem(z + o, n_z)
        for core in range(2):
            if o == 0 and core == 0:
                continue
            pl.semaphore_signal(barrier, inc=1, device_id=(d - c + lax.rem(c + core, 2), zz), device_id_type=MESH)
    for dev in extra:
        pl.semaphore_signal(barrier, inc=1, device_id=dev, device_id_type=MESH)
    pl.semaphore_wait(barrier, 2 * n_z - 1 + len(extra))


def block_at(ref, shape, row, col):
    return ref.at[pl.ds(pl.multiple_of(row * shape[0], shape[0]), shape[0]),
                  pl.ds(pl.multiple_of(col * shape[1], shape[1]), shape[1])]


class Spread:
    def __init__(self, n_d, pair, c, z, parts, spot, send, recv):
        self.n_d, self.pair, self.parts, self.spot = n_d, pair, parts, spot
        self.send, self.recv = send, recv
        self.dev = lambda k: (2 * (pair ^ k) + c, z)

    def copy(self, slot, owner, t, h, to):
        at = self.spot(owner, t, h)
        return remote(at, at, self.send.at[slot, t, h], self.recv.at[slot, t, h], self.dev(to))

    def own(self, t):
        if self.n_d == 4:
            for h in range(2):
                self.copy(0, self.pair, t, h, 1).start()
                self.copy(1, self.pair, t, 1 - h, 2).start()
        else:
            for k in range(1, self.n_d):
                for h in range(2):
                    self.copy(k - 1, self.pair, t, h, k).start()

    def pass_on(self, t):
        if self.n_d == 4:
            self.copy(0, self.pair ^ 1, t, 0, 1).wait_recv()
            self.copy(2, self.pair ^ 1, t, 0, 2).start()
            self.copy(1, self.pair ^ 2, t, 1, 2).wait_recv()
            self.copy(2, self.pair ^ 2, t, 1, 1).start()

    def rest(self, t):
        if self.n_d == 4:
            self.copy(0, self.pair ^ 1, t, 1, 1).wait_recv()
            self.copy(1, self.pair ^ 2, t, 0, 2).wait_recv()
        else:
            for k in range(1, self.n_d):
                for h in range(2):
                    self.copy(k - 1, self.pair ^ k, t, h, k).wait_recv()

    def far(self, t):
        if self.n_d == 4:
            for h in range(2):
                self.copy(2, self.pair ^ 3, t, h, 1).wait_recv()

    def sent(self):
        for t in range(self.parts):
            for h in range(2):
                for slot in range(self.n_d - 1):
                    self.copy(slot, self.pair, t, h, 1).wait_send()

    def finish(self):
        for t in range(self.parts):
            if self.n_d == 4:
                self.copy(0, self.pair ^ 1, t, 1, 1).wait_recv()
                self.copy(1, self.pair ^ 2, t, 0, 2).wait_recv()
                for h in range(2):
                    self.copy(2, self.pair ^ 3, t, h, 1).wait_recv()
                    for slot in range(3):
                        self.copy(slot, self.pair, t, h, 1).wait_send()
            else:
                for k in range(1, self.n_d):
                    for h in range(2):
                        self.copy(k - 1, self.pair ^ k, t, h, k).wait_recv()
                        self.copy(k - 1, self.pair, t, h, k).wait_send()


def gather_in_kernel(n_dp, n_z, x_ref, w_ref, v_ref, g_ref, s_ref, gu_ref, xs, wq, vo, ga, sg, gu16, gu_in, gu_out,
                     x_s, x_r, f_s, f_r, w_s, w_r, v_s, v_r, d_s, d_r, g_s, g_r, s_s, s_r, loc, gu_is, gu_os):
    d, z, pair, c = place()
    n_d = n_dp // 2
    me = d * n_z + z
    total = n_dp * n_z
    rows = x_ref.shape[1]
    half = rows // 2
    shape = w_ref.shape
    cz = z // 2
    chunks = gu_ref.shape[0] // WIDE_ROWS
    gu_width = gu_ref.shape[2]

    def chunk_in(i, slot):
        return pltpu.make_async_copy(gu_ref.at[pl.ds(pl.multiple_of(i * WIDE_ROWS, WIDE_ROWS), WIDE_ROWS)], gu_in.at[slot], gu_is.at[slot])

    def chunk_out(i, slot):
        return pltpu.make_async_copy(gu_out.at[slot], gu16.at[pl.ds(pl.multiple_of(i * WIDE_ROWS, WIDE_ROWS), WIDE_ROWS)], gu_os.at[slot])

    def round_chunks(low, high):
        def one(i, carry):
            slot = lax.rem(i, 2)
            pl.when(i + 1 < chunks)(chunk_in(i + 1, 1 - slot).start)
            chunk_in(i, slot).wait()
            pl.when(i >= 2)(chunk_out(i - 2, slot).wait)
            for n in range(2):
                gu_out[slot, :, n * gu_width : (n + 1) * gu_width] = gu_in[slot, :, n].astype(jnp.bfloat16)
            chunk_out(i, slot).start()
            return carry

        lax.fori_loop(low, high, one, 0)

    chunk_in(0, 0).start()
    greet_all(n_dp, n_z, d, z)

    def line_stage(src, dst, send, recv, spare, wait):
        for o in range(n_z):
            copy = remote(src, dst, send.at[o], recv.at[c, z % 2], (2 * pair + cz, lax.rem(z + o, n_z)))
            act = copy.wait_send if wait else copy.start
            if o == 0:
                pl.when(c != cz)(act)
                if not wait:
                    pl.when(c == cz)(pltpu.make_async_copy(src, dst, loc.at[spare]).start)
            else:
                act()

    my_block = block_at(wq, shape, d, z % 2)
    line_stage(w_ref, my_block, w_s, w_r, 0, False)

    for i in range(2):
        for h in range(2):
            src = x_ref.at[i, pl.ds(h * half, half)]
            dst = xs.at[pl.ds(pl.multiple_of(z * rows + h * half, half), half)]
            zz = 2 * c + i
            mine = (h == c) & (zz == z)
            copy = remote(src, dst, x_s.at[i, h], x_r.at[z], (2 * pair + h, zz))
            pl.when(jnp.logical_not(mine))(copy.start)
            pl.when(mine)(lambda src=src, dst=dst: pltpu.make_async_copy(src, dst, loc.at[1]).start())

    seg_copy = remote(s_ref, sg.at[c], s_s, s_r, (2 * pair + 1 - c, z))
    seg_copy.start()
    own_seg = pltpu.make_async_copy(s_ref, sg.at[c], loc.at[2])
    own_seg.start()
    own_gain = pltpu.make_async_copy(g_ref, ga.at[me], loc.at[3])
    own_gain.start()

    def send_gain(o, carry):
        other = lax.rem(me + o, total)
        remote(g_ref, ga.at[me], g_s, g_r, (other // n_z, lax.rem(other, n_z))).start()
        return carry

    lax.fori_loop(1, total, send_gain, 0)

    first = jnp.where(c == cz, z % 2, 1 - c)

    def turn_of(t):
        return t % 2, (first if t < 2 else 1 - first)

    def spot(owner, t, h):
        core, b = turn_of(t)
        part = shape[0] // 2
        return wq.at[pl.ds(pl.multiple_of((2 * owner + core) * shape[0] + h * part, part), part),
                     pl.ds(pl.multiple_of(b * shape[1], shape[1]), shape[1])]

    spread = Spread(n_d, pair, c, z, 4, spot, d_s, d_r)
    for t in range(4):
        core, b = turn_of(t)
        blk = block_at(wq, shape, 2 * pair + core, b)
        mine = (core == c) & (2 * c + b == z)
        arrive = remote(w_ref, blk, w_s.at[0], w_r.at[core, b], (d, z))
        pl.when(jnp.logical_not(mine))(arrive.wait_recv)
        pl.when(mine)(lambda blk=blk: pltpu.make_async_copy(w_ref, blk, loc.at[0]).wait())
        spread.own(t)
        if t == 1:
            line_stage(v_ref, block_at(vo, v_ref.shape, c, z % 2), v_s, v_r, 4, False)
        if t > 0:
            spread.pass_on(t - 1)
        round_chunks(t * chunks // 4, (t + 1) * chunks // 4)

    for o in range(n_z):
        zs = lax.rem(z + o, n_z)
        src = xs.at[pl.ds(pl.multiple_of(zs * rows + c * half, half), half)]
        mine = (cz == c) & (zs == z)
        arrive = remote(src, src, x_s.at[0, 0], x_r.at[zs], (d, z))
        pl.when(jnp.logical_not(mine))(arrive.wait_recv)
        pl.when(mine)(lambda src=src: pltpu.make_async_copy(src, src, loc.at[1]).wait())
        remote(src, src, f_s.at[zs], f_r.at[zs], (2 * pair + 1 - c, z)).start()
    spread.pass_on(3)

    line_stage(w_ref, my_block, w_s, w_r, 0, True)
    line_stage(v_ref, block_at(vo, v_ref.shape, c, z % 2), v_s, v_r, 4, True)
    for i in range(2):
        for h in range(2):
            src = x_ref.at[i, pl.ds(h * half, half)]
            mine = (h == c) & (2 * c + i == z)
            copy = remote(src, src, x_s.at[i, h], x_r.at[0], (d, z))
            pl.when(jnp.logical_not(mine))(copy.wait_send)
    for zs in range(n_z):
        src = xs.at[pl.ds(zs * rows, half)]
        copy = remote(src, src, f_s.at[zs], f_r.at[zs], (d, z))
        copy.wait_send()
        copy.wait_recv()
    for core in range(2):
        for b in range(2):
            blk = block_at(vo, v_ref.shape, core, b)
            mine = (core == c) & (2 * c + b == z)
            pl.when(jnp.logical_not(mine))(remote(blk, blk, v_s.at[0], v_r.at[core, b], (d, z)).wait_recv)
            pl.when(mine)(pltpu.make_async_copy(v_ref, blk, loc.at[4]).wait)
    for i in range(max(0, chunks - 2), chunks):
        chunk_out(i, i % 2).wait()
    seg_copy.wait_send()
    remote(s_ref, sg.at[1 - c], s_s, s_r, (d, z)).wait_recv()
    own_seg.wait()
    own_gain.wait()
    many = ga.at[pl.ds(0, total - 1)]
    gains = remote(many, many, g_s, g_r, (d, z))
    gains.wait_send()
    gains.wait_recv()
    spread.finish()


def gather_in(x_loc, w, v, gain_tile, seg_tile, wide, n_dp, n_z):
    _, rows, width = x_loc.shape
    n_d = n_dp // 2
    total = n_dp * n_z
    return pl.pallas_call(
        functools.partial(gather_in_kernel, n_dp, n_z),
        in_specs=[VMEM_SPEC] * 5 + [ANY_SPEC],
        out_specs=[ANY_SPEC] * 6,
        out_shape=[
            jax.ShapeDtypeStruct((rows * n_z, width), x_loc.dtype),
            jax.ShapeDtypeStruct((w.shape[0] * n_dp, 2 * w.shape[1]), w.dtype),
            jax.ShapeDtypeStruct((v.shape[0] * 2, 2 * v.shape[1]), v.dtype),
            jax.ShapeDtypeStruct((total,) + gain_tile.shape, gain_tile.dtype),
            jax.ShapeDtypeStruct((2,) + seg_tile.shape, seg_tile.dtype),
            jax.ShapeDtypeStruct((wide.shape[0], wide.shape[1] * wide.shape[2]), jnp.bfloat16),
        ],
        scratch_shapes=[
            pltpu.VMEM((2, WIDE_ROWS) + wide.shape[1:], jnp.float32),
            pltpu.VMEM((2, WIDE_ROWS, wide.shape[1] * wide.shape[2]), jnp.bfloat16),
            DMA((2, 2)), DMA((n_z,)), DMA((n_z,)), DMA((n_z,)), DMA((n_z,)), DMA((2, 2)), DMA((n_z,)), DMA((2, 2)),
            DMA((n_d - 1, 4, 2)), DMA((n_d - 1, 4, 2)), DMA, DMA, DMA, DMA, DMA((5,)), DMA((2,)), DMA((2,)),
        ],
        compiler_params=pltpu.CompilerParams(collective_id=1, has_side_effects=True),
        cost_estimate=pl.CostEstimate(flops=0, bytes_accessed=200_000_000, transcendentals=0),
        name="gather_in",
    )(x_loc, w, v, gain_tile, seg_tile, wide)


def share_resid_kernel(n_dp, n_z, part_ref, x_ref, w_ref, out, wall, got, buf, p_s, p_r, u_s, u_r, d_s, d_r, c_s, c_r, loc):
    d, z, pair, c = place()
    n_d = n_dp // 2
    cz = z // 2
    full = x_ref.shape[0]
    half = full // 2
    unit = half // 2
    w_rows = w_ref.shape[0]
    parts = 4
    piece = w_rows // parts
    own_copy = pltpu.make_async_copy(w_ref, wall.at[pl.ds(pl.multiple_of(d * w_rows, w_rows), w_rows)], loc.at[2])
    own_copy.start()
    greet_line(n_z, d, z, [(2 * (pair ^ k) + c, z) for k in range(1, n_d)])
    mine = pl.ds(pl.multiple_of(c * half, half), half)
    theirs = pl.ds(pl.multiple_of((1 - c) * half, half), half)
    swap = remote(part_ref.at[theirs], got, p_s, p_r, (2 * pair + 1 - c, z))
    swap.start()

    def spot_w(owner, t, h):
        sub = piece // 2
        return wall.at[pl.ds(pl.multiple_of((2 * owner + c) * w_rows + (2 * t + h) * sub, sub), sub)]

    def across(k, t, core):
        at = wall.at[pl.ds(pl.multiple_of((2 * (pair ^ k) + core) * w_rows + t * piece, piece), piece)]
        return remote(at, at, c_s.at[k, t], c_r.at[k, t], (2 * pair + 1 - c, z))

    spread = Spread(n_d, pair, c, z, parts, spot_w, d_s, d_r)
    own_copy.wait()
    for t in range(parts):
        spread.own(t)
        across(0, t, c).start()

    swap.wait_recv()

    def add(r, carry):
        at = pl.ds(pl.multiple_of(r * 16, 16), 16)
        src = pl.ds(pl.multiple_of(c * half + r * 16, 16), 16)
        total = x_ref[src].astype(jnp.float32) + part_ref[src].astype(jnp.float32) + got[at].astype(jnp.float32)
        buf[at] = total.astype(jnp.bfloat16)
        return carry

    def spot(jl, h, k):
        return out.at[jl, pl.ds(pl.multiple_of(h * half + k * unit, unit), unit)]

    def sends(k, wait):
        src = buf.at[pl.ds(k * unit, unit)]
        dst = spot(z % 2, c, k)
        for o, zz in ((1, z - 1), (2, z + 1), (0, z)):
            copy = remote(src, dst, u_s.at[o, k], u_r.at[z % 2, c, k], (2 * pair + cz, zz))
            act = copy.wait_send if wait else copy.start
            if o == 0:
                keep = pltpu.make_async_copy(src, dst, loc.at[k])
                pl.when(c != cz)(act)
                pl.when(c == cz)(keep.wait if wait else keep.start)
            elif o == 1:
                pl.when(z > 0)(act)
            else:
                pl.when(z < n_z - 1)(act)

    per = unit // 16
    lax.fori_loop(0, per, add, 0)
    lax.fori_loop(per, per + per // 2, add, 0)
    sends(0, False)
    lax.fori_loop(per + per // 2, 2 * per, add, 0)
    swap.wait_send()
    sends(1, False)

    def relay(dist, sign, k, h, begin):
        j = z + sign * dist
        ok = (j >= 2 * c) & (j <= 2 * c + 1)
        to = z - sign
        more = (to >= 0) & (to <= n_z - 1)
        jl = lax.rem(j + n_z, 2)
        at = spot(jl, h, k)
        copy = remote(at, at, u_s.at[3 + (0 if sign < 0 else 1), 4 * jl + 2 * h + k], u_r.at[jl, h, k], (2 * pair + c, to))
        if begin:

            @pl.when(ok)
            def _():
                copy.wait_recv()
                pl.when(more)(copy.start)
        else:
            pl.when(ok & more)(copy.wait_send)

    def take(t):
        spread.pass_on(t)

    def rest(t):
        spread.rest(t)
        for k in range(1, n_d):
            if n_d != 4 or k != 3:
                across(k, t, c).start()

    def far(t):
        if n_d == 4:
            spread.far(t)
            across(3, t, c).start()

    links = []
    for t in range(parts):
        links += [(take, t), (rest, t)]
    links += [(far, t) for t in range(parts)]
    line = [(dist, k, h) for dist in range(1, n_z) for k in range(2) for h in range(2)]
    for n in range(max(len(links), len(line))):
        if n < len(line):
            dist, k, h = line[n]
            for sign in (-1, 1):
                relay(dist, sign, k, h, True)
        if n < len(links):
            links[n][0](links[n][1])

    @pl.when(c == cz)
    def _():
        for k in range(2):
            at = spot(z % 2, 1 - c, k)
            remote(at, at, u_s.at[0, 0], u_r.at[z % 2, 1 - c, k], (d, z)).wait_recv()

    for dist, k, h in line:
        for sign in (-1, 1):
            relay(dist, sign, k, h, False)
    sends(0, True)
    sends(1, True)
    spread.sent()
    for k in range(n_d):
        for t in range(parts):
            across(k, t, c).wait_send()
            across(k, t, 1 - c).wait_recv()


def share_resid(part, x, w, n_dp, n_z):
    full, width = x.shape
    n_d = n_dp // 2
    return pl.pallas_call(
        functools.partial(share_resid_kernel, n_dp, n_z),
        in_specs=[VMEM_SPEC] * 3,
        out_specs=[ANY_SPEC] * 2,
        out_shape=[
            jax.ShapeDtypeStruct((2, full, width), jnp.bfloat16),
            jax.ShapeDtypeStruct((n_dp * w.shape[0], w.shape[1]), jnp.bfloat16),
        ],
        scratch_shapes=[
            pltpu.VMEM((full // 2, width), jnp.bfloat16), pltpu.VMEM((full // 2, width), jnp.bfloat16),
            DMA, DMA, DMA((5, 8)), DMA((2, 2, 2)), DMA((n_d - 1, 4, 2)), DMA((n_d - 1, 4, 2)), DMA((n_d, 4)), DMA((n_d, 4)),
            DMA((3,)),
        ],
        compiler_params=pltpu.CompilerParams(collective_id=2, has_side_effects=True),
        cost_estimate=pl.CostEstimate(flops=0, bytes_accessed=200_000_000, transcendentals=0),
        name="share_resid",
    )(part, x, w)


CHUNKS = 8


def sum_line_kernel(n_z, part_ref, resid_all, cot_all, gain_ref, d_out, gain_out, got, buf, resid_ref, cot_ref,
                    s_s, s_r, p_s, p_r, loc, rows_sem):
    d, z, pair, c = place()
    cz = z // 2
    full, _ = buf.shape
    rows = full // CHUNKS
    fetch = (
        pltpu.make_async_copy(resid_all.at[z % 2], resid_ref, rows_sem.at[0]),
        pltpu.make_async_copy(cot_all.at[z % 2], cot_ref, rows_sem.at[1]),
    )
    for one in fetch:
        one.start()
    greet_line(n_z, d, z)
    gain_out[...] = jnp.zeros_like(gain_out)
    own = c == cz
    steps = [(k, t) for k in range(CHUNKS) for t in range(2)]

    def where_is(k, t):
        jl = jnp.bitwise_xor(c, t)
        return jl, 2 * c + jl, pl.ds(k * rows, rows)

    def copy_on(k, t, side, src):
        jl, _, at = where_is(k, t)
        to = z + 1 if side == 0 else z - 1
        return remote(src, got.at[side, jl, at], s_s.at[t, k], s_r.at[side, jl, k], (2 * pair + c, to))

    def arrived(side, jl, k):
        at = got.at[side, jl, pl.ds(k * rows, rows)]
        return remote(at, at, s_s.at[0, 0], s_r.at[side, jl, k], (d, z))

    def add_in(side, jl, k):
        def one(r, carry):
            at = pl.ds(pl.multiple_of(k * rows + r * 16, 16), 16)
            got[side, jl, at] = (got[side, jl, at].astype(jnp.float32) + part_ref[jl, at].astype(jnp.float32)).astype(jnp.bfloat16)
            return carry

        lax.fori_loop(0, rows // 16, one, 0)

    def finish(jl, k):
        def one(r, carry):
            at = pl.ds(pl.multiple_of(k * rows + r * 16, 16), 16)
            total = part_ref[jl, at].astype(jnp.float32)
            left = got[0, jl, at].astype(jnp.float32)
            right = got[1, jl, at].astype(jnp.float32)
            total = total + jnp.where(z > 0, left, 0.0) + jnp.where(z < n_z - 1, right, 0.0)
            value = resid_ref[at].astype(jnp.float32)
            inverse = lax.rsqrt(jnp.mean(value * value, axis=-1, keepdims=True) + norm_eps)
            scaled = value * inverse
            d_scaled = total * gain_ref[...]
            mean = jnp.mean(d_scaled * scaled, axis=-1, keepdims=True)
            d_resid = cot_ref[at].astype(jnp.float32) + inverse * (d_scaled - scaled * mean)
            buf[at] = d_resid.astype(jnp.bfloat16)
            prod = total * scaled
            gain_out[...] = gain_out[...] + prod[:8] + prod[8:]
            return carry

        lax.fori_loop(0, rows // 16, one, 0)

    def to_partner(k):
        at = pl.ds(k * rows, rows)
        return remote(buf.at[at], d_out.at[at], p_s.at[k], p_r.at[k], (2 * pair + 1 - c, z))

    def keep(k):
        at = pl.ds(k * rows, rows)
        return pltpu.make_async_copy(buf.at[at], d_out.at[at], loc.at[k])

    def send_step(k, t, wait):
        jl, j, at = where_is(k, t)
        for side in range(2):
            going = (z < j) if side == 0 else (z > j)
            edge = (z == 0) if side == 0 else (z == n_z - 1)
            edge_copy = copy_on(k, t, side, part_ref.at[jl, at])
            inner_copy = copy_on(k, t, side, got.at[side, jl, at])
            pl.when(going & edge)(edge_copy.wait_send if wait else edge_copy.start)
            pl.when(going & jnp.logical_not(edge))(inner_copy.wait_send if wait else inner_copy.start)

    def publish(k, wait):
        @pl.when(own)
        def _():
            if wait:
                to_partner(k).wait_send()
                keep(k).wait()
            else:
                to_partner(k).start()
                keep(k).start()

    def own_chunk(k):
        @pl.when(own)
        def _():
            if k == 0:
                for one in fetch:
                    one.wait()
            jl = z % 2
            pl.when(z > 0)(arrived(0, jl, k).wait_recv)
            pl.when(z < n_z - 1)(arrived(1, jl, k).wait_recv)
            finish(jl, k)
            if k > 0:
                to_partner(k - 1).start()
                keep(k - 1).start()

    for n, (k, t) in enumerate(steps):
        jl, j, at = where_is(k, t)
        for side in range(2):
            going = (z < j) if side == 0 else (z > j)
            inner = (z > 0) if side == 0 else (z < n_z - 1)

            @pl.when(going & inner)
            def _():
                arrived(side, jl, k).wait_recv()
                add_in(side, jl, k)

        if n > 0:
            send_step(*steps[n - 1], False)
        if t == 1 and k > 0:
            own_chunk(k - 1)
    send_step(*steps[-1], False)
    own_chunk(CHUNKS - 1)

    @pl.when(jnp.logical_not(own))
    def _():
        for one in fetch:
            one.wait()

    @pl.when(own)
    def _():
        to_partner(CHUNKS - 1).start()
        keep(CHUNKS - 1).start()

    for k, t in steps:
        send_step(k, t, True)
    for k in range(CHUNKS):
        publish(k, True)
        at = d_out.at[pl.ds(k * rows, rows)]
        pl.when(jnp.logical_not(own))(remote(at, at, p_s.at[k], p_r.at[k], (d, z)).wait_recv)


def sum_line(part, resid, cot, gain, n_z):
    _, full, width = part.shape
    return pl.pallas_call(
        functools.partial(sum_line_kernel, n_z),
        in_specs=[VMEM_SPEC, ANY_SPEC, ANY_SPEC, VMEM_SPEC],
        out_specs=[ANY_SPEC, VMEM_SPEC],
        out_shape=[jax.ShapeDtypeStruct((full, width), jnp.bfloat16), jax.ShapeDtypeStruct((8, width), jnp.float32)],
        scratch_shapes=[
            pltpu.VMEM((2, 2, full, width), jnp.bfloat16), pltpu.VMEM((full, width), jnp.bfloat16),
            pltpu.VMEM((full, width), jnp.bfloat16), pltpu.VMEM((full, width), jnp.bfloat16),
            DMA((2, CHUNKS)), DMA((2, 2, CHUNKS)), DMA((CHUNKS,)), DMA((CHUNKS,)), DMA((CHUNKS,)), DMA((2,)),
        ],
        compiler_params=pltpu.CompilerParams(collective_id=3, has_side_effects=True, vmem_limit_bytes=56 * 1024 * 1024),
        cost_estimate=pl.CostEstimate(flops=0, bytes_accessed=200_000_000, transcendentals=0),
        name="sum_line",
    )(part, resid, cot, gain)


WIDE_ROWS = 16
TURNED_ROWS = 256


def adam_wide_kernel(grad_ref, w_ref, m_ref, v_ref, g_out, w_out, m_out, v_out):
    width = w_ref.shape[-1]
    for n in range(2):
        grad = grad_ref[:, n * width : (n + 1) * width].astype(jnp.float32)
        weight, first, second = adam_update(w_ref[:, n], grad, m_ref[:, n], v_ref[:, n])
        g_out[:, n] = grad
        w_out[:, n] = weight
        m_out[:, n] = first
        v_out[:, n] = second


def adam_turned_kernel(grad_ref, w_ref, m_ref, v_ref, g_out, w_out, m_out, v_out):
    grad = grad_ref[...].astype(jnp.float32).T
    weight, first, second = adam_update(w_ref[...], grad, m_ref[...], v_ref[...])
    g_out[...] = grad
    w_out[...] = weight
    m_out[...] = first
    v_out[...] = second


def adam_call(kernel, grid, grad_spec, spec, arrays):
    shape = jax.ShapeDtypeStruct(arrays[1].shape, jnp.float32)
    return pl.pallas_call(
        kernel,
        grid=(grid,),
        in_specs=[grad_spec] + [spec] * 3,
        out_specs=[spec] * 4,
        out_shape=[shape] * 4,
        cost_estimate=pl.CostEstimate(flops=20 * shape.size, bytes_accessed=30 * shape.size, transcendentals=0),
    )(*arrays)


def adam_wide(*arrays):
    rows, _, width = arrays[1].shape
    return adam_call(
        adam_wide_kernel, rows // WIDE_ROWS,
        pl.BlockSpec((WIDE_ROWS, 2 * width), lambda i: (i, 0)),
        pl.BlockSpec((WIDE_ROWS, 2, width), lambda i: (i, 0, 0)),
        arrays,
    )


def adam_turned(*arrays):
    rows, cols = arrays[1].shape
    return adam_call(
        adam_turned_kernel, rows // TURNED_ROWS,
        pl.BlockSpec((cols, TURNED_ROWS), lambda i: (0, i)),
        pl.BlockSpec((TURNED_ROWS, cols), lambda i: (i, 0)),
        arrays,
    )


def hand_out_kernel(n_dp, n_z, dn_ref, x_ref, dr_ref, gain_ref, gain2_ref, qt_ref, ot_ref, ig, gq, go, gains,
                    got, buf, q_got, q_own, q_mid, q_put, q_fin, o_got, o_own, o_mid, o_put, o_fin, g_src, g_all,
                    p_s, p_r, i_s, i_r, q_s, q_r, qf_s, qf_r, o_s, o_r, of_s, of_r, g_s, g_r, q_loc, o_loc, loc):
    d, z, pair, c = place()
    n_d = n_dp // 2
    total = n_dp * n_z
    me = d * n_z + z
    cz = z // 2
    full, width = x_ref.shape
    half = full // 2
    quarter = half // 2
    q_rows, q_cols = q_fin.shape[1:]
    o_rows, o_cols = o_fin.shape[1:]
    relay = n_d == 4

    class First:
        def __init__(self, src, rows, cols, bufs, sems, spare):
            self.src, self.rows, self.cols, self.spare = src, rows, cols, spare
            self.got, self.own, self.mid, self.put, self.fin = bufs
            self.send, self.recv, self.f_send, self.f_recv, self.loc = sems

        def block(self, ref, b, core):
            return ref.at[pl.ds(core * self.rows, self.rows), pl.ds(b * self.cols, self.cols)]

        def source(self, owner, b, core):
            return self.src.at[pl.ds(pl.multiple_of((2 * owner + core) * self.rows, self.rows), self.rows), pl.ds(b * self.cols, self.cols)]

        def copy(self, n, b, core, owner, to):
            return remote(self.source(owner, b, core), self.block(self.got.at[n], b, core), self.send.at[n, b, core],
                          self.recv.at[n, b, core], (2 * (pair ^ to) + c, z))

        def loads(self, b, core):
            yield pltpu.make_async_copy(self.source(pair, b, core), self.block(self.own, b, core), self.loc.at[0, b, core])
            if relay:
                yield pltpu.make_async_copy(self.source(pair ^ (2 >> b), b, core), self.block(self.mid, b, core), self.loc.at[1, b, core])

        def begin(self, core):
            for b in range(2):
                if relay:
                    self.copy(1, b, core, pair ^ 3, 1 + b).start()
            for b in range(2):
                if relay:
                    self.copy(0, b, core, pair ^ (1 + b), 1 + b).start()
                else:
                    for k in range(1, n_d):
                        self.copy(k - 1, b, core, pair ^ k, k).start()

        def arrived(self, n, b, core):
            at = self.block(self.got.at[n], b, core)
            remote(at, at, self.send.at[n, b, core], self.recv.at[n, b, core], (d, z)).wait_recv()

        def cut(self, b, core, r):
            return pl.ds(pl.multiple_of(core * self.rows + r * 16, 16), 16), pl.ds(b * self.cols, self.cols)

        def middle_copy(self, b, core):
            return remote(self.block(self.mid, b, core), self.block(self.got.at[2], b, core), self.send.at[2, b, core],
                          self.recv.at[2, b, core], (2 * (pair ^ (2 >> b)) + c, z))

        def middle(self, core, between):
            if not relay:
                return
            for b in range(2):
                self.arrived(1, b, core)

                def add(r, carry):
                    at = self.cut(b, core, r)
                    self.mid[at] = (self.mid[at].astype(jnp.float32) + self.got[(1,) + at].astype(jnp.float32)).astype(jnp.bfloat16)
                    return carry

                lax.fori_loop(0, self.rows // 16, add, 0)
            self.middle_copy(0, core).start()
            between()
            self.middle_copy(1, core).start()

        def total(self, core, between):
            slots = (0, 2) if relay else range(n_d - 1)
            for b in range(2):
                for n in slots:
                    self.arrived(n, b, core)

                def add(r, carry):
                    at = self.cut(b, core, r)
                    value = self.own[at].astype(jnp.float32)
                    for n in slots:
                        value = value + self.got[(n,) + at].astype(jnp.float32)
                    self.put[core, b, pl.ds(pl.multiple_of(r * 16, 16), 16)] = value.astype(jnp.bfloat16)
                    return carry

                lax.fori_loop(0, self.rows // 16, add, 0)
            self.second(0, core, False)
            between()
            self.second(1, core, False)

        def second(self, b, core, wait):
            here = (core == c) & (2 * c + b == z)
            src = self.put.at[core, b]
            copy = remote(src, self.fin.at[z], self.f_send.at[core, b], self.f_recv.at[z], (2 * pair + core, 2 * c + b))
            keep = pltpu.make_async_copy(src, self.fin.at[z], loc.at[self.spare])
            pl.when(jnp.logical_not(here))(copy.wait_send if wait else copy.start)
            pl.when(here)(keep.wait if wait else keep.start)

        def final(self):
            for core in range(2):
                for b in range(2):
                    self.second(b, core, True)
            for zs in range(n_z):
                at = self.fin.at[zs]
                from_here = (cz == c) & (zs == z)
                pl.when(jnp.logical_not(from_here))(remote(at, at, self.f_send.at[0, 0], self.f_recv.at[zs], (d, z)).wait_recv)

        def sent(self):
            for b in range(2):
                for core in range(2):
                    for n in range(n_d - 1):
                        at = self.block(self.got.at[n], b, core)
                        remote(at, at, self.send.at[n, b, core], self.recv.at[n, b, core], (d, z)).wait_send()

    o_first = First(ot_ref, o_rows, o_cols, (o_got, o_own, o_mid, o_put, o_fin), (o_s, o_r, of_s, of_r, o_loc), 2)
    q_first = First(qt_ref, q_rows, q_cols, (q_got, q_own, q_mid, q_put, q_fin), (q_s, q_r, qf_s, qf_r, q_loc), 3)
    for one in (o_first, q_first):
        for core in range(2):
            for b in range(2):
                for copy in one.loads(b, core):
                    copy.start()
    greet_all(n_dp, n_z, d, z)

    mine = pl.ds(pl.multiple_of(c * half, half), half)
    theirs = pl.ds(pl.multiple_of((1 - c) * half, half), half)
    swap = remote(dn_ref.at[theirs], got, p_s, p_r, (2 * pair + 1 - c, z))
    swap.start()
    o_first.begin(0)
    o_first.begin(1)

    g_src[pl.ds(0, 8)] = jnp.zeros((8, width), jnp.float32)
    g_src[pl.ds(8, 8)] = gain2_ref[...]
    swap.wait_recv()

    def rows_of(r, carry):
        at = pl.ds(pl.multiple_of(r * 16, 16), 16)
        src = pl.ds(pl.multiple_of(c * half + r * 16, 16), 16)
        d_normed = dn_ref[src].astype(jnp.float32) + got[at].astype(jnp.float32)
        value = x_ref[src].astype(jnp.float32)
        inverse = lax.rsqrt(jnp.mean(value * value, axis=-1, keepdims=True) + norm_eps)
        scaled = value * inverse
        d_scaled = d_normed * gain_ref[...]
        mean = jnp.mean(d_scaled * scaled, axis=-1, keepdims=True)
        out = dr_ref[src].astype(jnp.float32) + inverse * (d_scaled - scaled * mean)
        buf[at] = out.astype(jnp.bfloat16)
        prod = d_normed * scaled
        g_src[pl.ds(0, 8)] = g_src[pl.ds(0, 8)] + prod[:8] + prod[8:]
        return carry

    def row_send(b, wait):
        src = buf.at[pl.ds(b * quarter, quarter)]
        dst = ig.at[z % 2]
        zz = 2 * c + b
        here = (cz == c) & (zz == z)
        copy = remote(src, dst, i_s.at[b], i_r.at[z % 2], (2 * pair + cz, zz))
        keep = pltpu.make_async_copy(src, dst, loc.at[0])
        pl.when(jnp.logical_not(here))(copy.wait_send if wait else copy.start)
        pl.when(here)(keep.wait if wait else keep.start)

    for one in (o_first, q_first):
        for core in range(2):
            for b in range(2):
                for copy in one.loads(b, core):
                    copy.wait()
    nothing = lambda: None
    per = quarter // 16
    lax.fori_loop(0, per, rows_of, 0)
    o_first.middle(0, lambda: row_send(0, False))
    q_first.begin(0)
    lax.fori_loop(per, 2 * per, rows_of, 0)
    o_first.middle(1, lambda: row_send(1, False))
    q_first.begin(1)

    each = width // total

    def gain_tile(o):
        return g_src.at[:, pl.ds(pl.multiple_of(o * each // 128 * 128, 128), 128)]

    own_gain = pltpu.make_async_copy(gain_tile(me), g_all.at[me], loc.at[1])
    own_gain.start()

    def send_gain(o, carry):
        other = lax.rem(me + o, total)
        remote(gain_tile(other), g_all.at[me], g_s, g_r, (other // n_z, lax.rem(other, n_z))).start()
        return carry

    lax.fori_loop(1, total, send_gain, 0)

    o_first.total(0, nothing)
    q_first.middle(0, nothing)
    o_first.total(1, nothing)
    q_first.middle(1, nothing)
    q_first.total(0, nothing)
    q_first.total(1, nothing)

    o_first.final()
    value = o_fin[0].astype(jnp.float32)
    for zs in range(1, n_z):
        value = value + o_fin[zs].astype(jnp.float32)
    go[...] = value.T

    many = g_all.at[pl.ds(0, total - 1)]
    gain_copy = remote(many, many, g_s, g_r, (d, z))
    gain_copy.wait_send()
    gain_copy.wait_recv()
    own_gain.wait()
    gains[...] = jnp.zeros_like(gains)

    def add_gain(o, carry):
        gains[...] = gains[...] + g_all[o]
        return carry

    lax.fori_loop(0, total, add_gain, 0)

    swap.wait_send()
    for b in range(2):
        row_send(b, True)
    for i in range(2):
        from_here = (cz == c) & (2 * c + i == z)
        at = ig.at[i]
        pl.when(jnp.logical_not(from_here))(remote(at, at, i_s.at[0], i_r.at[i], (d, z)).wait_recv)
    o_first.sent()
    q_first.sent()
    q_first.final()

    def last(r, carry):
        at = pl.ds(pl.multiple_of(r * 16, 16), 16)
        value = q_fin[0, at].astype(jnp.float32)
        for zs in range(1, n_z):
            value = value + q_fin[zs, at].astype(jnp.float32)
        gq[at] = value
        return carry

    lax.fori_loop(0, q_rows // 16, last, 0)


def hand_out(dn, x, dr, gain, gain2, qt, ot, n_dp, n_z):
    full, width = x.shape
    n_d = n_dp // 2
    total = n_dp * n_z
    q_rows, q_cols = qt.shape[0] // n_dp, qt.shape[1] // 2
    o_rows, o_cols = ot.shape[0] // n_dp, ot.shape[1] // 2
    b16 = jnp.bfloat16
    f32 = jnp.float32

    def weight_bufs(rows, cols):
        return [
            pltpu.VMEM((n_d - 1, 2 * rows, 2 * cols), b16), pltpu.VMEM((2 * rows, 2 * cols), b16),
            pltpu.VMEM((2 * rows, 2 * cols), b16), pltpu.VMEM((2, 2, rows, cols), b16), pltpu.VMEM((n_z, rows, cols), b16),
        ]

    weight_sems = [DMA((n_d - 1, 2, 2)), DMA((n_d - 1, 2, 2)), DMA((2, 2)), DMA((n_z,))]
    return pl.pallas_call(
        functools.partial(hand_out_kernel, n_dp, n_z),
        in_specs=[VMEM_SPEC] * 5 + [ANY_SPEC] * 2,
        out_specs=[ANY_SPEC] + [VMEM_SPEC] * 3,
        out_shape=[
            jax.ShapeDtypeStruct((2, full // 4, width), b16),
            jax.ShapeDtypeStruct((q_rows, q_cols), f32),
            jax.ShapeDtypeStruct((o_cols, o_rows), f32),
            jax.ShapeDtypeStruct((16, 128), f32),
        ],
        scratch_shapes=[
            pltpu.VMEM((full // 2, width), b16), pltpu.VMEM((full // 2, width), b16),
            *weight_bufs(q_rows, q_cols), *weight_bufs(o_rows, o_cols),
            pltpu.VMEM((16, width), f32), pltpu.VMEM((total, 16, 128), f32),
            DMA, DMA, DMA((2,)), DMA((2,)), *weight_sems, *weight_sems, DMA, DMA,
            DMA((2, 2, 2)), DMA((2, 2, 2)), DMA((4,)),
        ],
        compiler_params=pltpu.CompilerParams(collective_id=5, has_side_effects=True, vmem_limit_bytes=58 * 1024 * 1024),
        cost_estimate=pl.CostEstimate(flops=0, bytes_accessed=300_000_000, transcendentals=0),
        name="hand_out",
    )(dn, x, dr, gain, gain2, qt, ot)


def rms_forward(values, gain_wide):
    inverse = lax.rsqrt(jnp.mean(values * values, axis=-1, keepdims=True) + norm_eps)
    scaled = values * inverse
    return (scaled, inverse, (scaled * gain_wide).astype(jnp.bfloat16))


def adam_update(weight, grad, first, second):
    new_first = beta_one * first + (1.0 - beta_one) * grad
    new_second = beta_two * second + (1.0 - beta_two) * grad * grad
    first_hat = new_first / (1.0 - beta_one**step_count)
    second_hat = new_second / (1.0 - beta_two**step_count)
    new_weight = weight - learn_rate * (
        first_hat / (jnp.sqrt(second_hat) + adam_eps) + weight_decay * weight
    )
    return (new_weight, new_first, new_second)


def contract_rows(left, right):
    return lax.dot_general(
        left, right, (((0,), (0,)), ((), ())), preferred_element_type=jnp.float32
    )


def times_transpose(left, right):
    return lax.dot_general(
        left, right, (((1,), (1,)), ((), ())), preferred_element_type=jnp.float32
    )


def layer_step(
    block_input,
    segment_ids,
    cotangent,
    attn_gain,
    qkv_weight,
    out_weight,
    mlp_gain,
    gate_up_weight,
    down_weight,
    first_attn_gain,
    first_qkv,
    first_out,
    first_mlp_gain,
    first_gate_up,
    first_down,
    second_attn_gain,
    second_qkv,
    second_out,
    second_mlp_gain,
    second_gate_up,
    second_down,
):
    seqs_here, local_len, width = block_input.shape
    full_len = segment_ids.shape[1]
    n_dp = lax.axis_size("dp")
    n_z = lax.axis_size("seq")
    groups = HEADS // KV_HEADS
    unit_count = down_weight.shape[0]
    z_here = lax.axis_index("seq")
    owned = attn_gain.shape[0]
    gain_line = jnp.concatenate([attn_gain, mlp_gain]).astype(jnp.bfloat16).astype(jnp.float32)
    gain_tile = jnp.pad(gain_line[None], ((0, 7), (0, LANES - 2 * owned)))
    seg_tile = jnp.pad(segment_ids, ((0, 8 - seqs_here), (0, 0)))
    down_rows = lax.all_gather(down_weight.astype(jnp.bfloat16), "dp", axis=1, tiled=True)
    rows_in, qkv_cols, out_line, gain_all, seg_all, gate_up_here = gather_in(
        block_input,
        qkv_weight.astype(jnp.bfloat16),
        out_weight.astype(jnp.bfloat16).T,
        gain_tile,
        seg_tile,
        gate_up_weight,
        n_dp,
        n_z,
    )
    cot_late, _ = lax.optimization_barrier((cotangent, gain_all))
    cot_all = lax.all_gather(cot_late, "seq", axis=1, tiled=True)
    gain_one = gain_all[:, 0, :owned].reshape(1, width)
    gain_two = gain_all[:, 0, owned : 2 * owned].reshape(1, width)
    seg_here = lax.dynamic_slice(seg_all, (z_here // 2, z_here % 2, 0), (1, 1, full_len))[0]
    tables = attn_tables(seg_here)
    _, _, normed_one = rms_forward(rows_in.astype(jnp.float32), gain_one)
    qkv = jnp.dot(normed_one, qkv_cols, preferred_element_type=jnp.float32)
    turned, lse, attended16, out_rows = attn_forward(qkv, *tables, out_line, full_len, groups, n_dp)
    attn_part = times_transpose(attended16, out_rows)
    resid_all, gate_up_cols = share_resid(
        attn_part.astype(jnp.bfloat16), rows_in, gate_up_here, n_dp, n_z
    )
    total_rows = seqs_here * full_len
    resid = resid_all.reshape(total_rows, width).astype(jnp.float32)
    _, _, normed_two = rms_forward(resid, gain_two)
    gate_up = jnp.dot(normed_two, gate_up_cols, preferred_element_type=jnp.float32)
    gate_part = gate_up[:, :unit_count]
    up_part = gate_up[:, unit_count:]
    sigmoid_gate = jax.nn.sigmoid(gate_part)
    active = gate_part * sigmoid_gate
    hidden16 = (active * up_part).astype(jnp.bfloat16)
    cot_rows = cot_all.reshape(total_rows, width)
    d_hidden = times_transpose(cot_rows, down_rows)
    d_gate = d_hidden * up_part * sigmoid_gate * (1.0 + gate_part * (1.0 - sigmoid_gate))
    d_up = d_hidden * active
    d_gate_up16 = jnp.concatenate([d_gate, d_up], 1).astype(jnp.bfloat16)
    down_part = jnp.dot(hidden16, down_rows, preferred_element_type=jnp.float32)
    down16 = down_part.astype(jnp.bfloat16).reshape(resid_all.shape)
    gate_up_term = contract_rows(normed_two, d_gate_up16).astype(jnp.bfloat16)
    gate_up_sum = lax.psum_scatter(gate_up_term, "dp", scatter_dimension=0, tiled=True)
    down_term = contract_rows(cot_rows, hidden16).astype(jnp.bfloat16)
    down_sum = lax.psum_scatter(down_term, "dp", scatter_dimension=0, tiled=True)
    d_normed_two = times_transpose(d_gate_up16, gate_up_cols).astype(jnp.bfloat16)
    d_resid16, gain_two_part = sum_line(
        d_normed_two.reshape(resid_all.shape), resid_all, cot_all, gain_two, n_z
    )
    down16, _ = lax.optimization_barrier((down16, d_resid16))
    pieces = [
        lax.dynamic_slice_in_dim(down16, (z_here + o) % n_z * local_len, local_len, 1)
        for o in range(n_z)
    ]
    for o in range(1, n_z):
        pieces[o] = lax.ppermute(pieces[o], "seq", [(i, (i + o) % n_z) for i in range(n_z)])
    down_here = sum(piece.astype(jnp.float32) for piece in pieces)
    resid_here = lax.dynamic_slice_in_dim(resid_all, z_here * local_len, local_len, 1)
    output = (resid_here.astype(jnp.float32) + down_here).astype(jnp.bfloat16)
    d_attended = jnp.dot(d_resid16, out_rows, preferred_element_type=jnp.float32).astype(jnp.bfloat16)
    d_qkv16 = attn_backward(turned, d_attended, lse, *tables, full_len, groups)
    d_normed_one = times_transpose(d_qkv16, qkv_cols).astype(jnp.bfloat16)
    qkv_term = contract_rows(normed_one, d_qkv16).astype(jnp.bfloat16)
    out_term = contract_rows(d_resid16, attended16).astype(jnp.bfloat16)
    input_grad, grad_qkv, grad_out, gain_sums = hand_out(
        d_normed_one,
        rows_in,
        d_resid16,
        gain_one,
        gain_two_part,
        qkv_term,
        out_term,
        n_dp,
        n_z,
    )
    grad_gate_up, w_gu, m_gu, v_gu = adam_wide(
        gate_up_sum, gate_up_weight, first_gate_up, second_gate_up
    )
    grad_down, w_down, m_down, v_down = adam_turned(
        down_sum, down_weight, first_down, second_down
    )
    flat = lax.axis_index("dp") * n_z + z_here
    gain_sums = lax.dynamic_slice(
        jnp.sum(gain_sums.reshape(2, 8, LANES), axis=1), (0, flat * owned % LANES), (2, owned)
    )
    grad_gain_one = gain_sums[0]
    grad_gain_two = gain_sums[1]
    w_one, m_one, v_one = adam_update(attn_gain, grad_gain_one, first_attn_gain, second_attn_gain)
    w_qkv, m_qkv, v_qkv = adam_update(qkv_weight, grad_qkv, first_qkv, second_qkv)
    w_out, m_out, v_out = adam_update(out_weight, grad_out, first_out, second_out)
    w_two, m_two, v_two = adam_update(mlp_gain, grad_gain_two, first_mlp_gain, second_mlp_gain)
    return (
        output,
        input_grad,
        grad_gain_one,
        grad_qkv,
        grad_out,
        grad_gain_two,
        grad_gate_up,
        grad_down,
        w_one,
        w_qkv,
        w_out,
        w_two,
        w_gu,
        w_down,
        m_one,
        m_qkv,
        m_out,
        m_two,
        m_gu,
        m_down,
        v_one,
        v_qkv,
        v_out,
        v_two,
        v_gu,
        v_down,
    )


def solution(mesh):
    in_specs = (
        P("dp", "seq", None),
        P("dp", None),
        P("dp", "seq", None),
        P(("dp", "seq")),
        P("dp", "seq"),
        P("seq", "dp"),
        P(("dp", "seq")),
        P("dp", None, "seq"),
        P("seq", "dp"),
        P(("dp", "seq")),
        P("dp", "seq"),
        P("seq", "dp"),
        P(("dp", "seq")),
        P("dp", None, "seq"),
        P("seq", "dp"),
        P(("dp", "seq")),
        P("dp", "seq"),
        P("seq", "dp"),
        P(("dp", "seq")),
        P("dp", None, "seq"),
        P("seq", "dp"),
    )
    out_specs = (
        P("dp", "seq", None),
        P("dp", "seq", None),
        P(("dp", "seq")),
        P("dp", "seq"),
        P("seq", "dp"),
        P(("dp", "seq")),
        P("dp", None, "seq"),
        P("seq", "dp"),
        P(("dp", "seq")),
        P("dp", "seq"),
        P("seq", "dp"),
        P(("dp", "seq")),
        P("dp", None, "seq"),
        P("seq", "dp"),
        P(("dp", "seq")),
        P("dp", "seq"),
        P("seq", "dp"),
        P(("dp", "seq")),
        P("dp", None, "seq"),
        P("seq", "dp"),
        P(("dp", "seq")),
        P("dp", "seq"),
        P("seq", "dp"),
        P(("dp", "seq")),
        P("dp", None, "seq"),
        P("seq", "dp"),
    )
    return jax.shard_map(layer_step, mesh=mesh, in_specs=in_specs, out_specs=out_specs, check_vma=False)
```

```python
import functools

import jax
import jax.numpy as jnp
from jax import lax
from jax.experimental import pallas as pl
from jax.experimental.pallas import tpu as pltpu
from jax.sharding import PartitionSpec as P


HEADS = 32
KV_HEADS = 8
norm_eps = 1e-05
beta_one = 0.9
beta_two = 0.95
learn_rate = 0.01
weight_decay = 0.1
adam_eps = 1e-08
step_count = 10.0
masked_score = -1e30


HEAD_DIM = 64
LANES = 128


def dot_t(a, b):
    return lax.dot_general(a, b, (((1,), (1,)), ((), ())), preferred_element_type=jnp.float32)


def dot_n(a, b):
    return lax.dot_general(a, b, (((1,), (0,)), ((), ())), preferred_element_type=jnp.float32)


def dot_c(a, b):
    return lax.dot_general(a, b, (((0,), (0,)), ((), ())), preferred_element_type=jnp.float32)


def swap_halves(u):
    lane = lax.broadcasted_iota(jnp.int32, u.shape, 1)
    return jnp.where(lane % 64 < 32, pltpu.roll(u, 96, 1), pltpu.roll(u, 32, 1))


def turn(u, cos_wide, sin_wide):
    return u * cos_wide + swap_halves(u) * sin_wide


def key_start(block, q_rows, reach):
    return max(0, (block * q_rows - reach + 1) // q_rows * q_rows)


def attn_forward_kernel(pairs, q_rows, reach, qkv_ref, cos_ref, sin_ref, seg_col_ref, seg_row_ref,
                        turned_ref, lse_ref, out_ref):
    full_len = qkv_ref.shape[0]
    lane = lax.broadcasted_iota(jnp.int32, (full_len, LANES), 1)
    low = lane < HEAD_DIM
    cos_q = cos_ref[...]
    sin_q = sin_ref[...]
    kv = qkv_ref[:, pairs * LANES:].astype(jnp.float32)
    kv16 = turn(kv, jnp.where(low, cos_q, 1.0), jnp.where(low, sin_q, 0.0)).astype(jnp.bfloat16)
    turned_ref[:, pairs * LANES:] = kv16
    kv32 = kv16.astype(jnp.float32)
    rolled = pltpu.roll(kv32, HEAD_DIM, 1)
    zero = jnp.zeros_like(kv32)
    keys = (jnp.where(low, kv32, zero).astype(jnp.bfloat16), jnp.where(low, zero, rolled).astype(jnp.bfloat16))
    vals = (jnp.where(low, rolled, zero).astype(jnp.bfloat16), jnp.where(low, zero, kv32).astype(jnp.bfloat16))
    for pair in range(pairs):
        cols = slice(pair * LANES, (pair + 1) * LANES)
        query = turn(qkv_ref[:, cols].astype(jnp.float32), cos_q, sin_q) .astype(jnp.bfloat16)
        turned_ref[:, cols] = query
    for block in range(full_len // q_rows):
        first = key_start(block, q_rows, reach)
        last = (block + 1) * q_rows
        rows = slice(block * q_rows, last)
        span = slice(first, last)
        i = lax.broadcasted_iota(jnp.int32, (q_rows, last - first), 0) + block * q_rows
        j = lax.broadcasted_iota(jnp.int32, (q_rows, last - first), 1) + first
        allowed = (j <= i) & (seg_col_ref[rows, :1] == seg_row_ref[:1, span])
        for pair in range(pairs):
            cols = slice(pair * LANES, (pair + 1) * LANES)
            query = turned_ref[rows, cols]
            total = None
            for half in range(2):
                scores = dot_t(query, keys[half][span]) * (HEAD_DIM ** -0.5)
                scores = jnp.where(allowed, scores, masked_score)
                top = jnp.max(scores, axis=1, keepdims=True)
                lse = top + jnp.log(jnp.sum(jnp.exp(scores - top), axis=1, keepdims=True))
                probs = jnp.exp(scores - lse).astype(jnp.bfloat16)
                part = dot_n(probs, vals[half][span])
                total = part if total is None else total + part
                head = 2 * pair + half
                lse_ref[rows, head:head + 1] = lse
            out_ref[rows, cols] = total.astype(jnp.bfloat16)


def attn_backward_kernel(pairs, q_rows, reach, turned_ref, d_out_ref, lse_ref, cos_ref, sin_ref, seg_col_ref,
                         seg_row_ref, grad_ref, dk_ref, dv_ref):
    full_len = turned_ref.shape[0]
    lane = lax.broadcasted_iota(jnp.int32, (full_len, LANES), 1)
    low = lane < HEAD_DIM
    kv32 = turned_ref[:, pairs * LANES:].astype(jnp.float32)
    rolled = pltpu.roll(kv32, HEAD_DIM, 1)
    zero = jnp.zeros_like(kv32)
    keys = (jnp.where(low, kv32, zero).astype(jnp.bfloat16), jnp.where(low, zero, rolled).astype(jnp.bfloat16))
    vals = (jnp.where(low, rolled, zero).astype(jnp.bfloat16), jnp.where(low, zero, kv32).astype(jnp.bfloat16))
    dk_ref[...] = jnp.zeros_like(dk_ref)
    dv_ref[...] = jnp.zeros_like(dv_ref)
    low_rows = low[:q_rows]
    scale = HEAD_DIM ** -0.5
    for block in range(full_len // q_rows):
        first = key_start(block, q_rows, reach)
        last = (block + 1) * q_rows
        rows = slice(block * q_rows, last)
        span = slice(first, last)
        i = lax.broadcasted_iota(jnp.int32, (q_rows, last - first), 0) + block * q_rows
        j = lax.broadcasted_iota(jnp.int32, (q_rows, last - first), 1) + first
        allowed = (j <= i) & (seg_col_ref[rows, :1] == seg_row_ref[:1, span])
        cos_q = cos_ref[rows]
        sin_q = sin_ref[rows]
        for pair in range(pairs):
            cols = slice(pair * LANES, (pair + 1) * LANES)
            query = turned_ref[rows, cols]
            d_out = d_out_ref[rows, cols]
            q32 = query.astype(jnp.float32)
            o32 = d_out.astype(jnp.float32)
            d_query = None
            d_key = None
            d_val = None
            for half in range(2):
                keep = low_rows if half == 0 else ~low_rows
                q_only = jnp.where(keep, q32, 0.0).astype(jnp.bfloat16)
                o_only = jnp.where(keep, o32, 0.0).astype(jnp.bfloat16)
                head = 2 * pair + half
                scores = dot_t(query, keys[half][span]) * scale
                scores = jnp.where(allowed, scores, masked_score)
                probs = jnp.exp(scores - lse_ref[rows, head:head + 1])
                d_probs = dot_t(d_out, vals[half][span])
                delta = jnp.sum(probs * d_probs, axis=1, keepdims=True)
                d_scores = (probs * (d_probs - delta) * scale).astype(jnp.bfloat16)
                probs16 = probs.astype(jnp.bfloat16)
                dq = dot_n(d_scores, keys[half][span])
                dk = dot_c(d_scores, q_only)
                dv = dot_c(probs16, o_only)
                d_query = dq if d_query is None else d_query + dq
                d_key = dk if d_key is None else d_key + dk
                d_val = dv if d_val is None else d_val + dv
            dk_ref[span] = dk_ref[span] + d_key
            dv_ref[span] = dv_ref[span] + d_val
            grad_ref[rows, cols] = turn(d_query, cos_q, -sin_q).astype(jnp.bfloat16)
    d_key = dk_ref[...]
    d_val = dv_ref[...]
    d_key = d_key + pltpu.roll(d_key, HEAD_DIM, 1)
    d_val = d_val + pltpu.roll(d_val, HEAD_DIM, 1)
    d_key = turn(d_key, cos_ref[...], -sin_ref[...])
    grad_ref[:, pairs * LANES:] = jnp.where(low, d_key, d_val).astype(jnp.bfloat16)


def attn_specs(full_len, width):
    line = pl.BlockSpec((full_len, width), lambda s, g: (s, g))
    table = pl.BlockSpec((full_len, LANES), lambda s, g: (s, 0))
    row = pl.BlockSpec((8, full_len), lambda s, g: (s, 0))
    return line, table, row


Q_ROWS = 128
REACH = 256


def attn_gather_kernel(n_dp, pairs, q_rows, reach, qkv_ref, cos_ref, sin_ref, seg_col_ref, seg_row_ref, vo_ref,
                       turned_ref, lse_ref, out_ref, wo, d_s, d_r, loc):
    _, z, pair, c = place()
    n_d = n_dp // 2
    step = pl.program_id(1)
    steps = pl.num_programs(1)
    rows = vo_ref.shape[0]
    parts = 2
    part = rows // parts // 2

    def spot(owner, t, h):
        return wo.at[pl.ds(pl.multiple_of(owner * rows + (2 * t + h) * part, part), part)]

    spread = Spread(n_d, pair, c, z, parts, spot, d_s, d_r)
    keep = pltpu.make_async_copy(vo_ref, wo.at[pl.ds(pl.multiple_of(pair * rows, rows), rows)], loc)

    @pl.when(step == 0)
    def _():
        keep.start()
        barrier = pltpu.get_barrier_semaphore()
        for k in range(1, n_d):
            pl.semaphore_signal(barrier, inc=1, device_id=(2 * (pair ^ k) + c, z), device_id_type=MESH)
        pl.semaphore_wait(barrier, n_d - 1)
        keep.wait()
        for t in range(parts):
            spread.own(t)

    attn_forward_kernel(pairs, q_rows, reach, qkv_ref, cos_ref, sin_ref, seg_col_ref, seg_row_ref, turned_ref, lse_ref, out_ref)

    @pl.when(step == steps - 2)
    def _():
        spread.pass_on(0)

    @pl.when(step == steps - 1)
    def _():
        spread.pass_on(1)
        spread.finish()


def attn_forward(qkv, cos, sin, seg_col, seg_row, vo, full_len, groups, n_dp):
    pairs = groups // 2
    width = (groups + 2) * HEAD_DIM
    seqs = qkv.shape[0] // full_len
    kv = qkv.shape[1] // width
    n_d = n_dp // 2
    line, table, row = attn_specs(full_len, width)
    outw = pl.BlockSpec((full_len, groups * HEAD_DIM), lambda s, g: (s, g))
    rows = seqs * full_len
    return pl.pallas_call(
        functools.partial(attn_gather_kernel, n_dp, pairs, Q_ROWS, REACH),
        grid=(seqs, kv),
        in_specs=[line, table, table, table, row, VMEM_SPEC],
        out_specs=[line, pl.BlockSpec((full_len, LANES), lambda s, g: (s, g)), outw, ANY_SPEC],
        out_shape=[
            jax.ShapeDtypeStruct((rows, kv * width), jnp.bfloat16),
            jax.ShapeDtypeStruct((rows, kv * LANES), jnp.float32),
            jax.ShapeDtypeStruct((rows, kv * groups * HEAD_DIM), jnp.bfloat16),
            jax.ShapeDtypeStruct((n_d * vo.shape[0], vo.shape[1]), jnp.bfloat16),
        ],
        scratch_shapes=[DMA((n_d - 1, 2, 2)), DMA((n_d - 1, 2, 2)), DMA],
        compiler_params=pltpu.CompilerParams(collective_id=4, has_side_effects=True),
        cost_estimate=pl.CostEstimate(flops=4 * rows * full_len * kv * LANES * groups, bytes_accessed=150_000_000, transcendentals=0),
        name="attn_forward",
    )(qkv, cos, sin, seg_col, seg_row, vo)


def attn_backward(turned, d_out, lse, cos, sin, seg_col, seg_row, full_len, groups):
    pairs = groups // 2
    width = (groups + 2) * HEAD_DIM
    seqs = turned.shape[0] // full_len
    kv = turned.shape[1] // width
    line, table, row = attn_specs(full_len, width)
    outw = pl.BlockSpec((full_len, groups * HEAD_DIM), lambda s, g: (s, g))
    rows = seqs * full_len
    return pl.pallas_call(
        functools.partial(attn_backward_kernel, pairs, Q_ROWS, REACH),
        grid=(seqs, kv),
        in_specs=[line, outw, pl.BlockSpec((full_len, LANES), lambda s, g: (s, g)), table, table, table, row],
        out_specs=line,
        out_shape=jax.ShapeDtypeStruct((rows, kv * width), jnp.bfloat16),
        scratch_shapes=[pltpu.VMEM((full_len, LANES), jnp.float32)] * 2,
        cost_estimate=pl.CostEstimate(flops=10 * rows * full_len * kv * LANES * groups, bytes_accessed=rows * kv * width * 6, transcendentals=0),
        name="attn_backward",
    )(turned, d_out, lse, cos, sin, seg_col, seg_row)


def attn_tables(segment_ids):
    seqs, full_len = segment_ids.shape
    earlier = (segment_ids[..., None, :] < segment_ids[..., :, None]).astype(jnp.int32)
    positions = jnp.arange(full_len, dtype=jnp.int32) - jnp.sum(earlier, axis=-1, dtype=jnp.int32)
    inverse = 500000.0 ** (-2.0 * jnp.arange(HEAD_DIM // 2, dtype=jnp.float32) / HEAD_DIM)
    angles = positions.astype(jnp.float32)[..., None] * inverse
    cos = jnp.cos(angles)
    sin = jnp.sin(angles)
    cos = jnp.concatenate([cos] * 4, -1).reshape(seqs * full_len, LANES)
    sin = jnp.concatenate([-sin, sin] * 2, -1).reshape(seqs * full_len, LANES)
    seg_col = jnp.broadcast_to(segment_ids[:, :, None], (seqs, full_len, LANES)).reshape(seqs * full_len, LANES)
    seg_row = jnp.broadcast_to(segment_ids[:, None, :], (seqs, 8, full_len)).reshape(seqs * 8, full_len)
    return cos, sin, seg_col, seg_row


MESH = pl.DeviceIdType.MESH
VMEM_SPEC = pl.BlockSpec(memory_space=pltpu.VMEM)
ANY_SPEC = pl.BlockSpec(memory_space=pl.ANY)
DMA = pltpu.SemaphoreType.DMA


def place():
    d = lax.axis_index("dp")
    z = lax.axis_index("seq")
    return d, z, d // 2, d % 2


def remote(src, dst, send, recv, dev):
    return pltpu.make_async_remote_copy(
        src_ref=src, dst_ref=dst, send_sem=send, recv_sem=recv, device_id=dev, device_id_type=MESH
    )


def greet_all(n_dp, n_z, d, z):
    barrier = pltpu.get_barrier_semaphore()
    me = d * n_z + z

    def one(o, carry):
        other = lax.rem(me + o, n_dp * n_z)
        pl.semaphore_signal(barrier, inc=1, device_id=(other // n_z, lax.rem(other, n_z)), device_id_type=MESH)
        return carry

    lax.fori_loop(1, n_dp * n_z, one, 0)
    pl.semaphore_wait(barrier, n_dp * n_z - 1)


def greet_line(n_z, d, z, extra=()):
    barrier = pltpu.get_barrier_semaphore()
    c = d % 2
    for o in range(n_z):
        zz = lax.rem(z + o, n_z)
        for core in range(2):
            if o == 0 and core == 0:
                continue
            pl.semaphore_signal(barrier, inc=1, device_id=(d - c + lax.rem(c + core, 2), zz), device_id_type=MESH)
    for dev in extra:
        pl.semaphore_signal(barrier, inc=1, device_id=dev, device_id_type=MESH)
    pl.semaphore_wait(barrier, 2 * n_z - 1 + len(extra))


def block_at(ref, shape, row, col):
    return ref.at[pl.ds(pl.multiple_of(row * shape[0], shape[0]), shape[0]),
                  pl.ds(pl.multiple_of(col * shape[1], shape[1]), shape[1])]


class Spread:
    def __init__(self, n_d, pair, c, z, parts, spot, send, recv):
        self.n_d, self.pair, self.parts, self.spot = n_d, pair, parts, spot
        self.send, self.recv = send, recv
        self.dev = lambda k: (2 * (pair ^ k) + c, z)

    def copy(self, slot, owner, t, h, to):
        at = self.spot(owner, t, h)
        return remote(at, at, self.send.at[slot, t, h], self.recv.at[slot, t, h], self.dev(to))

    def own(self, t):
        if self.n_d == 4:
            for h in range(2):
                self.copy(0, self.pair, t, h, 1).start()
                self.copy(1, self.pair, t, 1 - h, 2).start()
        else:
            for k in range(1, self.n_d):
                for h in range(2):
                    self.copy(k - 1, self.pair, t, h, k).start()

    def pass_on(self, t):
        if self.n_d == 4:
            self.copy(0, self.pair ^ 1, t, 0, 1).wait_recv()
            self.copy(2, self.pair ^ 1, t, 0, 2).start()
            self.copy(1, self.pair ^ 2, t, 1, 2).wait_recv()
            self.copy(2, self.pair ^ 2, t, 1, 1).start()

    def rest(self, t):
        if self.n_d == 4:
            self.copy(0, self.pair ^ 1, t, 1, 1).wait_recv()
            self.copy(1, self.pair ^ 2, t, 0, 2).wait_recv()
        else:
            for k in range(1, self.n_d):
                for h in range(2):
                    self.copy(k - 1, self.pair ^ k, t, h, k).wait_recv()

    def far(self, t):
        if self.n_d == 4:
            for h in range(2):
                self.copy(2, self.pair ^ 3, t, h, 1).wait_recv()

    def sent(self):
        for t in range(self.parts):
            for h in range(2):
                for slot in range(self.n_d - 1):
                    self.copy(slot, self.pair, t, h, 1).wait_send()

    def finish(self):
        for t in range(self.parts):
            if self.n_d == 4:
                self.copy(0, self.pair ^ 1, t, 1, 1).wait_recv()
                self.copy(1, self.pair ^ 2, t, 0, 2).wait_recv()
                for h in range(2):
                    self.copy(2, self.pair ^ 3, t, h, 1).wait_recv()
                    for slot in range(3):
                        self.copy(slot, self.pair, t, h, 1).wait_send()
            else:
                for k in range(1, self.n_d):
                    for h in range(2):
                        self.copy(k - 1, self.pair ^ k, t, h, k).wait_recv()
                        self.copy(k - 1, self.pair, t, h, k).wait_send()


def gather_in_kernel(n_dp, n_z, x_ref, w_ref, v_ref, g_ref, s_ref, gu_ref, xs, wq, vo, ga, sg, gu16, gu_in, gu_out,
                     x_s, x_r, f_s, f_r, w_s, w_r, v_s, v_r, d_s, d_r, g_s, g_r, s_s, s_r, loc, gu_is, gu_os):
    d, z, pair, c = place()
    n_d = n_dp // 2
    me = d * n_z + z
    total = n_dp * n_z
    rows = x_ref.shape[1]
    half = rows // 2
    shape = w_ref.shape
    cz = z // 2
    chunks = gu_ref.shape[0] // WIDE_ROWS
    gu_width = gu_ref.shape[2]

    def chunk_in(i, slot):
        return pltpu.make_async_copy(gu_ref.at[pl.ds(pl.multiple_of(i * WIDE_ROWS, WIDE_ROWS), WIDE_ROWS)], gu_in.at[slot], gu_is.at[slot])

    def chunk_out(i, slot):
        return pltpu.make_async_copy(gu_out.at[slot], gu16.at[pl.ds(pl.multiple_of(i * WIDE_ROWS, WIDE_ROWS), WIDE_ROWS)], gu_os.at[slot])

    def round_chunks(low, high):
        def one(i, carry):
            slot = lax.rem(i, 2)
            pl.when(i + 1 < chunks)(chunk_in(i + 1, 1 - slot).start)
            chunk_in(i, slot).wait()
            pl.when(i >= 2)(chunk_out(i - 2, slot).wait)
            for n in range(2):
                gu_out[slot, :, n * gu_width : (n + 1) * gu_width] = gu_in[slot, :, n].astype(jnp.bfloat16)
            chunk_out(i, slot).start()
            return carry

        lax.fori_loop(low, high, one, 0)

    chunk_in(0, 0).start()
    greet_all(n_dp, n_z, d, z)

    def line_stage(src, dst, send, recv, spare, wait):
        for o in range(n_z):
            copy = remote(src, dst, send.at[o], recv.at[c, z % 2], (2 * pair + cz, lax.rem(z + o, n_z)))
            act = copy.wait_send if wait else copy.start
            if o == 0:
                pl.when(c != cz)(act)
                if not wait:
                    pl.when(c == cz)(pltpu.make_async_copy(src, dst, loc.at[spare]).start)
            else:
                act()

    my_block = block_at(wq, shape, d, z % 2)
    line_stage(w_ref, my_block, w_s, w_r, 0, False)

    for i in range(2):
        for h in range(2):
            src = x_ref.at[i, pl.ds(h * half, half)]
            dst = xs.at[pl.ds(pl.multiple_of(z * rows + h * half, half), half)]
            zz = 2 * c + i
            mine = (h == c) & (zz == z)
            copy = remote(src, dst, x_s.at[i, h], x_r.at[z], (2 * pair + h, zz))
            pl.when(jnp.logical_not(mine))(copy.start)
            pl.when(mine)(lambda src=src, dst=dst: pltpu.make_async_copy(src, dst, loc.at[1]).start())

    seg_copy = remote(s_ref, sg.at[c], s_s, s_r, (2 * pair + 1 - c, z))
    seg_copy.start()
    own_seg = pltpu.make_async_copy(s_ref, sg.at[c], loc.at[2])
    own_seg.start()
    own_gain = pltpu.make_async_copy(g_ref, ga.at[me], loc.at[3])
    own_gain.start()

    def send_gain(o, carry):
        other = lax.rem(me + o, total)
        remote(g_ref, ga.at[me], g_s, g_r, (other // n_z, lax.rem(other, n_z))).start()
        return carry

    lax.fori_loop(1, total, send_gain, 0)

    first = jnp.where(c == cz, z % 2, 1 - c)

    def turn_of(t):
        return t % 2, (first if t < 2 else 1 - first)

    def spot(owner, t, h):
        core, b = turn_of(t)
        part = shape[0] // 2
        return wq.at[pl.ds(pl.multiple_of((2 * owner + core) * shape[0] + h * part, part), part),
                     pl.ds(pl.multiple_of(b * shape[1], shape[1]), shape[1])]

    spread = Spread(n_d, pair, c, z, 4, spot, d_s, d_r)
    for t in range(4):
        core, b = turn_of(t)
        blk = block_at(wq, shape, 2 * pair + core, b)
        mine = (core == c) & (2 * c + b == z)
        arrive = remote(w_ref, blk, w_s.at[0], w_r.at[core, b], (d, z))
        pl.when(jnp.logical_not(mine))(arrive.wait_recv)
        pl.when(mine)(lambda blk=blk: pltpu.make_async_copy(w_ref, blk, loc.at[0]).wait())
        spread.own(t)
        if t == 1:
            line_stage(v_ref, block_at(vo, v_ref.shape, c, z % 2), v_s, v_r, 4, False)
        if t > 0:
            spread.pass_on(t - 1)
        round_chunks(t * chunks // 4, (t + 1) * chunks // 4)

    for o in range(n_z):
        zs = lax.rem(z + o, n_z)
        src = xs.at[pl.ds(pl.multiple_of(zs * rows + c * half, half), half)]
        mine = (cz == c) & (zs == z)
        arrive = remote(src, src, x_s.at[0, 0], x_r.at[zs], (d, z))
        pl.when(jnp.logical_not(mine))(arrive.wait_recv)
        pl.when(mine)(lambda src=src: pltpu.make_async_copy(src, src, loc.at[1]).wait())
        remote(src, src, f_s.at[zs], f_r.at[zs], (2 * pair + 1 - c, z)).start()
    spread.pass_on(3)

    line_stage(w_ref, my_block, w_s, w_r, 0, True)
    line_stage(v_ref, block_at(vo, v_ref.shape, c, z % 2), v_s, v_r, 4, True)
    for i in range(2):
        for h in range(2):
            src = x_ref.at[i, pl.ds(h * half, half)]
            mine = (h == c) & (2 * c + i == z)
            copy = remote(src, src, x_s.at[i, h], x_r.at[0], (d, z))
            pl.when(jnp.logical_not(mine))(copy.wait_send)
    for zs in range(n_z):
        src = xs.at[pl.ds(zs * rows, half)]
        copy = remote(src, src, f_s.at[zs], f_r.at[zs], (d, z))
        copy.wait_send()
        copy.wait_recv()
    for core in range(2):
        for b in range(2):
            blk = block_at(vo, v_ref.shape, core, b)
            mine = (core == c) & (2 * c + b == z)
            pl.when(jnp.logical_not(mine))(remote(blk, blk, v_s.at[0], v_r.at[core, b], (d, z)).wait_recv)
            pl.when(mine)(pltpu.make_async_copy(v_ref, blk, loc.at[4]).wait)
    for i in range(max(0, chunks - 2), chunks):
        chunk_out(i, i % 2).wait()
    seg_copy.wait_send()
    remote(s_ref, sg.at[1 - c], s_s, s_r, (d, z)).wait_recv()
    own_seg.wait()
    own_gain.wait()
    many = ga.at[pl.ds(0, total - 1)]
    gains = remote(many, many, g_s, g_r, (d, z))
    gains.wait_send()
    gains.wait_recv()
    spread.finish()


def gather_in(x_loc, w, v, gain_tile, seg_tile, wide, n_dp, n_z):
    _, rows, width = x_loc.shape
    n_d = n_dp // 2
    total = n_dp * n_z
    return pl.pallas_call(
        functools.partial(gather_in_kernel, n_dp, n_z),
        in_specs=[VMEM_SPEC] * 5 + [ANY_SPEC],
        out_specs=[ANY_SPEC] * 6,
        out_shape=[
            jax.ShapeDtypeStruct((rows * n_z, width), x_loc.dtype),
            jax.ShapeDtypeStruct((w.shape[0] * n_dp, 2 * w.shape[1]), w.dtype),
            jax.ShapeDtypeStruct((v.shape[0] * 2, 2 * v.shape[1]), v.dtype),
            jax.ShapeDtypeStruct((total,) + gain_tile.shape, gain_tile.dtype),
            jax.ShapeDtypeStruct((2,) + seg_tile.shape, seg_tile.dtype),
            jax.ShapeDtypeStruct((wide.shape[0], wide.shape[1] * wide.shape[2]), jnp.bfloat16),
        ],
        scratch_shapes=[
            pltpu.VMEM((2, WIDE_ROWS) + wide.shape[1:], jnp.float32),
            pltpu.VMEM((2, WIDE_ROWS, wide.shape[1] * wide.shape[2]), jnp.bfloat16),
            DMA((2, 2)), DMA((n_z,)), DMA((n_z,)), DMA((n_z,)), DMA((n_z,)), DMA((2, 2)), DMA((n_z,)), DMA((2, 2)),
            DMA((n_d - 1, 4, 2)), DMA((n_d - 1, 4, 2)), DMA, DMA, DMA, DMA, DMA((5,)), DMA((2,)), DMA((2,)),
        ],
        compiler_params=pltpu.CompilerParams(collective_id=1, has_side_effects=True),
        cost_estimate=pl.CostEstimate(flops=0, bytes_accessed=200_000_000, transcendentals=0),
        name="gather_in",
    )(x_loc, w, v, gain_tile, seg_tile, wide)


def share_resid_kernel(n_dp, n_z, part_ref, x_ref, w_ref, out, wall, got, buf, p_s, p_r, u_s, u_r, d_s, d_r, c_s, c_r, loc):
    d, z, pair, c = place()
    n_d = n_dp // 2
    cz = z // 2
    full = x_ref.shape[0]
    half = full // 2
    unit = half // 2
    w_rows = w_ref.shape[0]
    parts = 4
    piece = w_rows // parts
    own_copy = pltpu.make_async_copy(w_ref, wall.at[pl.ds(pl.multiple_of(d * w_rows, w_rows), w_rows)], loc.at[2])
    own_copy.start()
    greet_line(n_z, d, z, [(2 * (pair ^ k) + c, z) for k in range(1, n_d)])
    mine = pl.ds(pl.multiple_of(c * half, half), half)
    theirs = pl.ds(pl.multiple_of((1 - c) * half, half), half)
    swap = remote(part_ref.at[theirs], got, p_s, p_r, (2 * pair + 1 - c, z))
    swap.start()

    def spot_w(owner, t, h):
        sub = piece // 2
        return wall.at[pl.ds(pl.multiple_of((2 * owner + c) * w_rows + (2 * t + h) * sub, sub), sub)]

    def across(k, t, core):
        at = wall.at[pl.ds(pl.multiple_of((2 * (pair ^ k) + core) * w_rows + t * piece, piece), piece)]
        return remote(at, at, c_s.at[k, t], c_r.at[k, t], (2 * pair + 1 - c, z))

    spread = Spread(n_d, pair, c, z, parts, spot_w, d_s, d_r)
    own_copy.wait()
    for t in range(parts):
        spread.own(t)
        across(0, t, c).start()

    swap.wait_recv()

    def add(r, carry):
        at = pl.ds(pl.multiple_of(r * 16, 16), 16)
        src = pl.ds(pl.multiple_of(c * half + r * 16, 16), 16)
        total = x_ref[src].astype(jnp.float32) + part_ref[src].astype(jnp.float32) + got[at].astype(jnp.float32)
        buf[at] = total.astype(jnp.bfloat16)
        return carry

    def spot(jl, h, k):
        return out.at[jl, pl.ds(pl.multiple_of(h * half + k * unit, unit), unit)]

    def sends(k, wait):
        src = buf.at[pl.ds(k * unit, unit)]
        dst = spot(z % 2, c, k)
        for o, zz in ((1, z - 1), (2, z + 1), (0, z)):
            copy = remote(src, dst, u_s.at[o, k], u_r.at[z % 2, c, k], (2 * pair + cz, zz))
            act = copy.wait_send if wait else copy.start
            if o == 0:
                keep = pltpu.make_async_copy(src, dst, loc.at[k])
                pl.when(c != cz)(act)
                pl.when(c == cz)(keep.wait if wait else keep.start)
            elif o == 1:
                pl.when(z > 0)(act)
            else:
                pl.when(z < n_z - 1)(act)

    per = unit // 16
    lax.fori_loop(0, per, add, 0)
    lax.fori_loop(per, per + per // 2, add, 0)
    sends(0, False)
    lax.fori_loop(per + per // 2, 2 * per, add, 0)
    swap.wait_send()
    sends(1, False)

    def relay(dist, sign, k, h, begin):
        j = z + sign * dist
        ok = (j >= 2 * c) & (j <= 2 * c + 1)
        to = z - sign
        more = (to >= 0) & (to <= n_z - 1)
        jl = lax.rem(j + n_z, 2)
        at = spot(jl, h, k)
        copy = remote(at, at, u_s.at[3 + (0 if sign < 0 else 1), 4 * jl + 2 * h + k], u_r.at[jl, h, k], (2 * pair + c, to))
        if begin:

            @pl.when(ok)
            def _():
                copy.wait_recv()
                pl.when(more)(copy.start)
        else:
            pl.when(ok & more)(copy.wait_send)

    def take(t):
        spread.pass_on(t)

    def rest(t):
        spread.rest(t)
        for k in range(1, n_d):
            if n_d != 4 or k != 3:
                across(k, t, c).start()

    def far(t):
        if n_d == 4:
            spread.far(t)
            across(3, t, c).start()

    links = []
    for t in range(parts):
        links += [(take, t), (rest, t)]
    links += [(far, t) for t in range(parts)]
    line = [(dist, k, h) for dist in range(1, n_z) for k in range(2) for h in range(2)]
    for n in range(max(len(links), len(line))):
        if n < len(line):
            dist, k, h = line[n]
            for sign in (-1, 1):
                relay(dist, sign, k, h, True)
        if n < len(links):
            links[n][0](links[n][1])

    @pl.when(c == cz)
    def _():
        for k in range(2):
            at = spot(z % 2, 1 - c, k)
            remote(at, at, u_s.at[0, 0], u_r.at[z % 2, 1 - c, k], (d, z)).wait_recv()

    for dist, k, h in line:
        for sign in (-1, 1):
            relay(dist, sign, k, h, False)
    sends(0, True)
    sends(1, True)
    spread.sent()
    for k in range(n_d):
        for t in range(parts):
            across(k, t, c).wait_send()
            across(k, t, 1 - c).wait_recv()


def share_resid(part, x, w, n_dp, n_z):
    full, width = x.shape
    n_d = n_dp // 2
    return pl.pallas_call(
        functools.partial(share_resid_kernel, n_dp, n_z),
        in_specs=[VMEM_SPEC] * 3,
        out_specs=[ANY_SPEC] * 2,
        out_shape=[
            jax.ShapeDtypeStruct((2, full, width), jnp.bfloat16),
            jax.ShapeDtypeStruct((n_dp * w.shape[0], w.shape[1]), jnp.bfloat16),
        ],
        scratch_shapes=[
            pltpu.VMEM((full // 2, width), jnp.bfloat16), pltpu.VMEM((full // 2, width), jnp.bfloat16),
            DMA, DMA, DMA((5, 8)), DMA((2, 2, 2)), DMA((n_d - 1, 4, 2)), DMA((n_d - 1, 4, 2)), DMA((n_d, 4)), DMA((n_d, 4)),
            DMA((3,)),
        ],
        compiler_params=pltpu.CompilerParams(collective_id=2, has_side_effects=True),
        cost_estimate=pl.CostEstimate(flops=0, bytes_accessed=200_000_000, transcendentals=0),
        name="share_resid",
    )(part, x, w)


CHUNKS = 8


def sum_line_kernel(n_z, part_ref, resid_all, cot_all, gain_ref, hid_ref, down_ref, d_out, gain_out, rows_out, got, buf,
                    resid_ref, cot_ref, hid, down, rows_buf, s_s, s_r, p_s, p_r, loc, rows_sem, mul_sem, out_sem):
    d, z, pair, c = place()
    cz = z // 2
    full, width = buf.shape
    rows = full // CHUNKS
    fetch = (
        pltpu.make_async_copy(resid_all.at[z % 2], resid_ref, rows_sem.at[0]),
        pltpu.make_async_copy(cot_all.at[z % 2], cot_ref, rows_sem.at[1]),
    )
    factors = (pltpu.make_async_copy(hid_ref, hid, mul_sem.at[0]), pltpu.make_async_copy(down_ref, down, mul_sem.at[1]))
    for one in fetch + factors:
        one.start()
    tile = rows_buf.shape[2]
    tiles = width // tile

    def tile_out(j):
        return pltpu.make_async_copy(rows_buf.at[j % 2], rows_out.at[:, pl.ds(j * tile, tile)], out_sem.at[j % 2])

    def multiply(j):
        if j >= tiles:
            return
        if j == 0:
            for one in factors:
                one.wait()
        if j >= 2:
            tile_out(j - 2).wait()
        rows_buf[j % 2] = dot_n(hid[...], down[:, j * tile : (j + 1) * tile]).astype(jnp.bfloat16)
        tile_out(j).start()

    greet_line(n_z, d, z)
    gain_out[...] = jnp.zeros_like(gain_out)
    own = c == cz
    steps = [(k, t) for k in range(CHUNKS) for t in range(2)]

    def where_is(k, t):
        jl = jnp.bitwise_xor(c, t)
        return jl, 2 * c + jl, pl.ds(k * rows, rows)

    def copy_on(k, t, side, src):
        jl, _, at = where_is(k, t)
        to = z + 1 if side == 0 else z - 1
        return remote(src, got.at[side, jl, at], s_s.at[t, k], s_r.at[side, jl, k], (2 * pair + c, to))

    def arrived(side, jl, k):
        at = got.at[side, jl, pl.ds(k * rows, rows)]
        return remote(at, at, s_s.at[0, 0], s_r.at[side, jl, k], (d, z))

    def add_in(side, jl, k):
        def one(r, carry):
            at = pl.ds(pl.multiple_of(k * rows + r * 16, 16), 16)
            got[side, jl, at] = (got[side, jl, at].astype(jnp.float32) + part_ref[jl, at].astype(jnp.float32)).astype(jnp.bfloat16)
            return carry

        lax.fori_loop(0, rows // 16, one, 0)

    def finish(jl, k):
        def one(r, carry):
            at = pl.ds(pl.multiple_of(k * rows + r * 16, 16), 16)
            total = part_ref[jl, at].astype(jnp.float32)
            left = got[0, jl, at].astype(jnp.float32)
            right = got[1, jl, at].astype(jnp.float32)
            total = total + jnp.where(z > 0, left, 0.0) + jnp.where(z < n_z - 1, right, 0.0)
            value = resid_ref[at].astype(jnp.float32)
            inverse = lax.rsqrt(jnp.mean(value * value, axis=-1, keepdims=True) + norm_eps)
            scaled = value * inverse
            d_scaled = total * gain_ref[...]
            mean = jnp.mean(d_scaled * scaled, axis=-1, keepdims=True)
            d_resid = cot_ref[at].astype(jnp.float32) + inverse * (d_scaled - scaled * mean)
            buf[at] = d_resid.astype(jnp.bfloat16)
            prod = total * scaled
            gain_out[...] = gain_out[...] + prod[:8] + prod[8:]
            return carry

        lax.fori_loop(0, rows // 16, one, 0)

    def to_partner(k):
        at = pl.ds(k * rows, rows)
        return remote(buf.at[at], d_out.at[at], p_s.at[k], p_r.at[k], (2 * pair + 1 - c, z))

    def keep(k):
        at = pl.ds(k * rows, rows)
        return pltpu.make_async_copy(buf.at[at], d_out.at[at], loc.at[k])

    def send_step(k, t, wait):
        jl, j, at = where_is(k, t)
        for side in range(2):
            going = (z < j) if side == 0 else (z > j)
            edge = (z == 0) if side == 0 else (z == n_z - 1)
            edge_copy = copy_on(k, t, side, part_ref.at[jl, at])
            inner_copy = copy_on(k, t, side, got.at[side, jl, at])
            pl.when(going & edge)(edge_copy.wait_send if wait else edge_copy.start)
            pl.when(going & jnp.logical_not(edge))(inner_copy.wait_send if wait else inner_copy.start)

    def publish(k, wait):
        @pl.when(own)
        def _():
            if wait:
                to_partner(k).wait_send()
                keep(k).wait()
            else:
                to_partner(k).start()
                keep(k).start()

    def own_chunk(k):
        @pl.when(own)
        def _():
            if k == 0:
                for one in fetch:
                    one.wait()
            jl = z % 2
            pl.when(z > 0)(arrived(0, jl, k).wait_recv)
            pl.when(z < n_z - 1)(arrived(1, jl, k).wait_recv)
            finish(jl, k)
            if k > 0:
                to_partner(k - 1).start()
                keep(k - 1).start()

    for n, (k, t) in enumerate(steps):
        jl, j, at = where_is(k, t)
        for side in range(2):
            going = (z < j) if side == 0 else (z > j)
            inner = (z > 0) if side == 0 else (z < n_z - 1)

            @pl.when(going & inner)
            def _():
                arrived(side, jl, k).wait_recv()
                add_in(side, jl, k)

        if n > 0:
            send_step(*steps[n - 1], False)
        if t == 0:
            multiply(k)
        if t == 1 and k > 0:
            own_chunk(k - 1)
    send_step(*steps[-1], False)
    own_chunk(CHUNKS - 1)
    for j in range(CHUNKS, tiles):
        multiply(j)

    @pl.when(jnp.logical_not(own))
    def _():
        for one in fetch:
            one.wait()

    @pl.when(own)
    def _():
        to_partner(CHUNKS - 1).start()
        keep(CHUNKS - 1).start()

    for j in range(max(0, tiles - 2), tiles):
        tile_out(j).wait()
    for k, t in steps:
        send_step(k, t, True)
    for k in range(CHUNKS):
        publish(k, True)
        at = d_out.at[pl.ds(k * rows, rows)]
        pl.when(jnp.logical_not(own))(remote(at, at, p_s.at[k], p_r.at[k], (d, z)).wait_recv)


def sum_line(part, resid, cot, gain, hidden, down, n_z):
    _, full, width = part.shape
    return pl.pallas_call(
        functools.partial(sum_line_kernel, n_z),
        in_specs=[VMEM_SPEC, ANY_SPEC, ANY_SPEC, VMEM_SPEC, ANY_SPEC, ANY_SPEC],
        out_specs=[ANY_SPEC, VMEM_SPEC, ANY_SPEC],
        out_shape=[
            jax.ShapeDtypeStruct((full, width), jnp.bfloat16),
            jax.ShapeDtypeStruct((8, width), jnp.float32),
            jax.ShapeDtypeStruct((hidden.shape[0], width), jnp.bfloat16),
        ],
        scratch_shapes=[
            pltpu.VMEM((2, 2, full, width), jnp.bfloat16), pltpu.VMEM((full, width), jnp.bfloat16),
            pltpu.VMEM((full, width), jnp.bfloat16), pltpu.VMEM((full, width), jnp.bfloat16),
            pltpu.VMEM(hidden.shape, jnp.bfloat16), pltpu.VMEM(down.shape, jnp.bfloat16),
            pltpu.VMEM((2, hidden.shape[0], 256), jnp.bfloat16),
            DMA((2, CHUNKS)), DMA((2, 2, CHUNKS)), DMA((CHUNKS,)), DMA((CHUNKS,)), DMA((CHUNKS,)), DMA((2,)), DMA((2,)), DMA((2,)),
        ],
        compiler_params=pltpu.CompilerParams(collective_id=3, has_side_effects=True, vmem_limit_bytes=56 * 1024 * 1024),
        cost_estimate=pl.CostEstimate(flops=0, bytes_accessed=200_000_000, transcendentals=0),
        name="sum_line",
    )(part, resid, cot, gain, hidden, down)


WIDE_ROWS = 32
TURNED_ROWS = 512


def adam_wide_kernel(grad_ref, w_ref, m_ref, v_ref, g_out, w_out, m_out, v_out):
    width = w_ref.shape[-1]
    for n in range(2):
        grad = grad_ref[:, n * width : (n + 1) * width].astype(jnp.float32)
        weight, first, second = adam_update(w_ref[:, n], grad, m_ref[:, n], v_ref[:, n])
        g_out[:, n] = grad
        w_out[:, n] = weight
        m_out[:, n] = first
        v_out[:, n] = second


def adam_turned_kernel(grad_ref, w_ref, m_ref, v_ref, g_out, w_out, m_out, v_out):
    grad = grad_ref[...].astype(jnp.float32).T
    weight, first, second = adam_update(w_ref[...], grad, m_ref[...], v_ref[...])
    g_out[...] = grad
    w_out[...] = weight
    m_out[...] = first
    v_out[...] = second


def adam_call(kernel, grid, grad_spec, spec, arrays):
    shape = jax.ShapeDtypeStruct(arrays[1].shape, jnp.float32)
    return pl.pallas_call(
        kernel,
        grid=(grid,),
        in_specs=[grad_spec] + [spec] * 3,
        out_specs=[spec] * 4,
        out_shape=[shape] * 4,
        cost_estimate=pl.CostEstimate(flops=20 * shape.size, bytes_accessed=30 * shape.size, transcendentals=0),
    )(*arrays)


def adam_wide(*arrays):
    rows, _, width = arrays[1].shape
    return adam_call(
        adam_wide_kernel, rows // WIDE_ROWS,
        pl.BlockSpec((WIDE_ROWS, 2 * width), lambda i: (i, 0)),
        pl.BlockSpec((WIDE_ROWS, 2, width), lambda i: (i, 0, 0)),
        arrays,
    )


def adam_turned(*arrays):
    rows, cols = arrays[1].shape
    return adam_call(
        adam_turned_kernel, rows // TURNED_ROWS,
        pl.BlockSpec((cols, TURNED_ROWS), lambda i: (0, i)),
        pl.BlockSpec((TURNED_ROWS, cols), lambda i: (i, 0)),
        arrays,
    )


def hand_out_kernel(n_dp, n_z, dq_ref, n_ref, x_ref, dr_ref, gain_ref, gain2_ref, wq_ref, ot_ref, ig, gq, go, gains,
                    dn_ref, wq, got, buf, q_base, q_got, q_put, q_fin, o_base, o_got, o_put, o_fin, g_src, g_all,
                    p_s, p_r, i_s, i_r, q_s, q_r, qf_s, qf_r, o_s, o_r, of_s, of_r, g_s, g_r, loc):
    d, z, pair, c = place()
    n_d = n_dp // 2
    total = n_dp * n_z
    me = d * n_z + z
    cz = z // 2
    full, width = x_ref.shape
    half = full // 2
    quarter = half // 2
    q_rows, q_cols = q_fin.shape[1:]
    o_rows, o_cols = o_fin.shape[1:]
    relay = n_d == 4

    class First:
        def __init__(self, rows, cols, bufs, sems, spare):
            self.rows, self.cols, self.spare = rows, cols, spare
            self.base, self.got, self.put, self.fin = bufs
            self.send, self.recv, self.f_send, self.f_recv = sems

        def block(self, ref, b, core):
            return ref.at[pl.ds(core * self.rows, self.rows), pl.ds(b * self.cols, self.cols)]

        def source(self, owner, b, core):
            return self.base.at[pl.ds(pl.multiple_of((2 * owner + core) * self.rows, self.rows), self.rows), pl.ds(b * self.cols, self.cols)]

        def cut_of(self, owner, b, core, r):
            start = (2 * owner + core) * self.rows + r * 16
            return pl.ds(pl.multiple_of(start, 16), 16), pl.ds(b * self.cols, self.cols)

        def copy(self, n, b, core, owner, to):
            return remote(self.source(owner, b, core), self.block(self.got.at[n], b, core), self.send.at[n, b, core],
                          self.recv.at[n, b, core], (2 * (pair ^ to) + c, z))

        def begin(self, core):
            for b in range(2):
                if relay:
                    self.copy(1, b, core, pair ^ 3, 1 + b).start()
            for b in range(2):
                if relay:
                    self.copy(0, b, core, pair ^ (1 + b), 1 + b).start()
                else:
                    for k in range(1, n_d):
                        self.copy(k - 1, b, core, pair ^ k, k).start()

        def arrived(self, n, b, core):
            at = self.block(self.got.at[n], b, core)
            remote(at, at, self.send.at[n, b, core], self.recv.at[n, b, core], (d, z)).wait_recv()

        def cut(self, b, core, r):
            return pl.ds(pl.multiple_of(core * self.rows + r * 16, 16), 16), pl.ds(b * self.cols, self.cols)

        def middle_copy(self, b, core):
            return remote(self.source(pair ^ (2 >> b), b, core), self.block(self.got.at[2], b, core), self.send.at[2, b, core],
                          self.recv.at[2, b, core], (2 * (pair ^ (2 >> b)) + c, z))

        def middle(self, core, between):
            if not relay:
                return
            for b in range(2):
                self.arrived(1, b, core)

                def add(r, carry):
                    at = self.cut(b, core, r)
                    mid = self.cut_of(pair ^ (2 >> b), b, core, r)
                    self.base[mid] = (self.base[mid].astype(jnp.float32) + self.got[(1,) + at].astype(jnp.float32)).astype(jnp.bfloat16)
                    return carry

                lax.fori_loop(0, self.rows // 16, add, 0)
            self.middle_copy(0, core).start()
            between()
            self.middle_copy(1, core).start()

        def total(self, core, between):
            slots = (0, 2) if relay else range(n_d - 1)
            for b in range(2):
                for n in slots:
                    self.arrived(n, b, core)

                def add(r, carry):
                    at = self.cut(b, core, r)
                    value = self.base[self.cut_of(pair, b, core, r)].astype(jnp.float32)
                    for n in slots:
                        value = value + self.got[(n,) + at].astype(jnp.float32)
                    self.put[core, b, pl.ds(pl.multiple_of(r * 16, 16), 16)] = value.astype(jnp.bfloat16)
                    return carry

                lax.fori_loop(0, self.rows // 16, add, 0)
            self.second(0, core, False)
            between()
            self.second(1, core, False)

        def second(self, b, core, wait):
            here = (core == c) & (2 * c + b == z)
            src = self.put.at[core, b]
            copy = remote(src, self.fin.at[z], self.f_send.at[core, b], self.f_recv.at[z], (2 * pair + core, 2 * c + b))
            keep = pltpu.make_async_copy(src, self.fin.at[z], loc.at[self.spare])
            pl.when(jnp.logical_not(here))(copy.wait_send if wait else copy.start)
            pl.when(here)(keep.wait if wait else keep.start)

        def final(self):
            for core in range(2):
                for b in range(2):
                    self.second(b, core, True)
            for zs in range(n_z):
                at = self.fin.at[zs]
                from_here = (cz == c) & (zs == z)
                pl.when(jnp.logical_not(from_here))(remote(at, at, self.f_send.at[0, 0], self.f_recv.at[zs], (d, z)).wait_recv)

        def sent(self):
            for b in range(2):
                for core in range(2):
                    for n in range(n_d - 1):
                        at = self.block(self.got.at[n], b, core)
                        remote(at, at, self.send.at[n, b, core], self.recv.at[n, b, core], (d, z)).wait_send()

    o_first = First(o_rows, o_cols, (o_base, o_got, o_put, o_fin), (o_s, o_r, of_s, of_r), 2)
    q_first = First(q_rows, q_cols, (q_base, q_got, q_put, q_fin), (q_s, q_r, qf_s, qf_r), 3)
    o_load = pltpu.make_async_copy(ot_ref, o_base, loc.at[4])
    wq_load = pltpu.make_async_copy(wq_ref, wq, loc.at[5])
    o_load.start()
    wq_load.start()
    greet_all(n_dp, n_z, d, z)
    o_load.wait()
    o_first.begin(0)
    o_first.begin(1)
    nothing = lambda: None

    def q_blocks(core):
        def one(k, carry):
            owner = pair ^ (n_d - 1 - k)
            rows_at = pl.ds(pl.multiple_of((2 * owner + core) * q_rows, q_rows), q_rows)
            q_base[rows_at] = dot_c(n_ref[:, rows_at], dq_ref[...]).astype(jnp.bfloat16)
            return carry

        lax.fori_loop(0, n_d, one, 0)

    def dn_blocks(low, high):
        def one(r, carry):
            rows_at = pl.ds(pl.multiple_of(r * 256, 256), 256)
            dn_ref[:, rows_at] = dot_t(dq_ref[...], wq[rows_at]).astype(jnp.bfloat16)
            return carry

        lax.fori_loop(low, high, one, 0)

    q_blocks(0)
    o_first.middle(0, lambda: q_blocks(1))
    q_first.begin(0)
    wq_load.wait()
    dn_tiles = width // 256
    dn_blocks(0, dn_tiles // 2)
    o_first.middle(1, nothing)
    q_first.begin(1)
    dn_blocks(dn_tiles // 2, dn_tiles)
    mine = pl.ds(pl.multiple_of(c * half, half), half)
    theirs = pl.ds(pl.multiple_of((1 - c) * half, half), half)
    swap = remote(dn_ref.at[theirs], got, p_s, p_r, (2 * pair + 1 - c, z))
    o_first.total(0, nothing)
    swap.start()

    g_src[pl.ds(0, 8)] = jnp.zeros((8, width), jnp.float32)
    g_src[pl.ds(8, 8)] = gain2_ref[...]
    swap.wait_recv()

    def rows_of(r, carry):
        at = pl.ds(pl.multiple_of(r * 16, 16), 16)
        src = pl.ds(pl.multiple_of(c * half + r * 16, 16), 16)
        d_normed = dn_ref[src].astype(jnp.float32) + got[at].astype(jnp.float32)
        value = x_ref[src].astype(jnp.float32)
        inverse = lax.rsqrt(jnp.mean(value * value, axis=-1, keepdims=True) + norm_eps)
        scaled = value * inverse
        d_scaled = d_normed * gain_ref[...]
        mean = jnp.mean(d_scaled * scaled, axis=-1, keepdims=True)
        out = dr_ref[src].astype(jnp.float32) + inverse * (d_scaled - scaled * mean)
        buf[at] = out.astype(jnp.bfloat16)
        prod = d_normed * scaled
        g_src[pl.ds(0, 8)] = g_src[pl.ds(0, 8)] + prod[:8] + prod[8:]
        return carry

    def row_send(b, wait):
        src = buf.at[pl.ds(b * quarter, quarter)]
        dst = ig.at[z % 2]
        zz = 2 * c + b
        here = (cz == c) & (zz == z)
        copy = remote(src, dst, i_s.at[b], i_r.at[z % 2], (2 * pair + cz, zz))
        keep = pltpu.make_async_copy(src, dst, loc.at[0])
        pl.when(jnp.logical_not(here))(copy.wait_send if wait else copy.start)
        pl.when(here)(keep.wait if wait else keep.start)

    q_first.middle(0, nothing)
    per = quarter // 16
    lax.fori_loop(0, per, rows_of, 0)
    o_first.total(1, lambda: row_send(0, False))
    lax.fori_loop(per, 2 * per, rows_of, 0)
    q_first.middle(1, lambda: row_send(1, False))

    each = width // total

    def gain_tile(o):
        return g_src.at[:, pl.ds(pl.multiple_of(o * each // 128 * 128, 128), 128)]

    own_gain = pltpu.make_async_copy(gain_tile(me), g_all.at[me], loc.at[1])
    own_gain.start()

    def send_gain(o, carry):
        other = lax.rem(me + o, total)
        remote(gain_tile(other), g_all.at[me], g_s, g_r, (other // n_z, lax.rem(other, n_z))).start()
        return carry

    lax.fori_loop(1, total, send_gain, 0)

    q_first.total(0, nothing)
    q_first.total(1, nothing)

    o_first.final()
    value = o_fin[0].astype(jnp.float32)
    for zs in range(1, n_z):
        value = value + o_fin[zs].astype(jnp.float32)
    go[...] = value.T

    many = g_all.at[pl.ds(0, total - 1)]
    gain_copy = remote(many, many, g_s, g_r, (d, z))
    gain_copy.wait_send()
    gain_copy.wait_recv()
    own_gain.wait()
    gains[...] = jnp.zeros_like(gains)

    def add_gain(o, carry):
        gains[...] = gains[...] + g_all[o]
        return carry

    lax.fori_loop(0, total, add_gain, 0)

    swap.wait_send()
    for b in range(2):
        row_send(b, True)
    for i in range(2):
        from_here = (cz == c) & (2 * c + i == z)
        at = ig.at[i]
        pl.when(jnp.logical_not(from_here))(remote(at, at, i_s.at[0], i_r.at[i], (d, z)).wait_recv)
    o_first.sent()
    q_first.sent()
    q_first.final()

    def last(r, carry):
        at = pl.ds(pl.multiple_of(r * 16, 16), 16)
        value = q_fin[0, at].astype(jnp.float32)
        for zs in range(1, n_z):
            value = value + q_fin[zs, at].astype(jnp.float32)
        gq[at] = value
        return carry

    lax.fori_loop(0, q_rows // 16, last, 0)


def hand_out(dq, normed, x, dr, gain, gain2, wq, ot, n_dp, n_z):
    full, width = x.shape
    n_d = n_dp // 2
    total = n_dp * n_z
    q_rows, q_cols = wq.shape[0] // n_dp, wq.shape[1] // 2
    o_rows, o_cols = ot.shape[0] // n_dp, ot.shape[1] // 2
    b16 = jnp.bfloat16
    f32 = jnp.float32

    def weight_bufs(rows, cols):
        return [
            pltpu.VMEM((n_dp * rows, 2 * cols), b16), pltpu.VMEM((n_d - 1, 2 * rows, 2 * cols), b16),
            pltpu.VMEM((2, 2, rows, cols), b16), pltpu.VMEM((n_z, rows, cols), b16),
        ]

    weight_sems = [DMA((n_d - 1, 2, 2)), DMA((n_d - 1, 2, 2)), DMA((2, 2)), DMA((n_z,))]
    return pl.pallas_call(
        functools.partial(hand_out_kernel, n_dp, n_z),
        in_specs=[VMEM_SPEC] * 6 + [ANY_SPEC] * 2,
        out_specs=[ANY_SPEC] + [VMEM_SPEC] * 3,
        out_shape=[
            jax.ShapeDtypeStruct((2, full // 4, width), b16),
            jax.ShapeDtypeStruct((q_rows, q_cols), f32),
            jax.ShapeDtypeStruct((o_cols, o_rows), f32),
            jax.ShapeDtypeStruct((16, 128), f32),
        ],
        scratch_shapes=[
            pltpu.VMEM((full, width), b16), pltpu.VMEM(wq.shape, b16),
            pltpu.VMEM((full // 2, width), b16), pltpu.VMEM((full // 2, width), b16),
            *weight_bufs(q_rows, q_cols), *weight_bufs(o_rows, o_cols),
            pltpu.VMEM((16, width), f32), pltpu.VMEM((total, 16, 128), f32),
            DMA, DMA, DMA((2,)), DMA((2,)), *weight_sems, *weight_sems, DMA, DMA,
            DMA((6,)),
        ],
        compiler_params=pltpu.CompilerParams(collective_id=5, has_side_effects=True, vmem_limit_bytes=58 * 1024 * 1024),
        cost_estimate=pl.CostEstimate(flops=0, bytes_accessed=300_000_000, transcendentals=0),
        name="hand_out",
    )(dq, normed, x, dr, gain, gain2, wq, ot)


def rms_forward(values, gain_wide):
    inverse = lax.rsqrt(jnp.mean(values * values, axis=-1, keepdims=True) + norm_eps)
    scaled = values * inverse
    return (scaled, inverse, (scaled * gain_wide).astype(jnp.bfloat16))


def adam_update(weight, grad, first, second):
    new_first = beta_one * first + (1.0 - beta_one) * grad
    new_second = beta_two * second + (1.0 - beta_two) * grad * grad
    first_hat = new_first / (1.0 - beta_one**step_count)
    second_hat = new_second / (1.0 - beta_two**step_count)
    new_weight = weight - learn_rate * (
        first_hat / (jnp.sqrt(second_hat) + adam_eps) + weight_decay * weight
    )
    return (new_weight, new_first, new_second)


def contract_rows(left, right):
    return lax.dot_general(
        left, right, (((0,), (0,)), ((), ())), preferred_element_type=jnp.float32
    )


def times_transpose(left, right):
    return lax.dot_general(
        left, right, (((1,), (1,)), ((), ())), preferred_element_type=jnp.float32
    )


def layer_step(
    block_input,
    segment_ids,
    cotangent,
    attn_gain,
    qkv_weight,
    out_weight,
    mlp_gain,
    gate_up_weight,
    down_weight,
    first_attn_gain,
    first_qkv,
    first_out,
    first_mlp_gain,
    first_gate_up,
    first_down,
    second_attn_gain,
    second_qkv,
    second_out,
    second_mlp_gain,
    second_gate_up,
    second_down,
):
    seqs_here, local_len, width = block_input.shape
    full_len = segment_ids.shape[1]
    n_dp = lax.axis_size("dp")
    n_z = lax.axis_size("seq")
    groups = HEADS // KV_HEADS
    unit_count = down_weight.shape[0]
    z_here = lax.axis_index("seq")
    owned = attn_gain.shape[0]
    gain_line = jnp.concatenate([attn_gain, mlp_gain]).astype(jnp.bfloat16).astype(jnp.float32)
    gain_tile = jnp.pad(gain_line[None], ((0, 7), (0, LANES - 2 * owned)))
    seg_tile = jnp.pad(segment_ids, ((0, 8 - seqs_here), (0, 0)))
    down_rows = lax.all_gather(down_weight.astype(jnp.bfloat16), "dp", axis=1, tiled=True)
    rows_in, qkv_cols, out_line, gain_all, seg_all, gate_up_here = gather_in(
        block_input,
        qkv_weight.astype(jnp.bfloat16),
        out_weight.astype(jnp.bfloat16).T,
        gain_tile,
        seg_tile,
        gate_up_weight,
        n_dp,
        n_z,
    )
    cot_late, _ = lax.optimization_barrier((cotangent, gain_all))
    cot_all = lax.all_gather(cot_late, "seq", axis=1, tiled=True)
    gain_one = gain_all[:, 0, :owned].reshape(1, width)
    gain_two = gain_all[:, 0, owned : 2 * owned].reshape(1, width)
    seg_here = lax.dynamic_slice(seg_all, (z_here // 2, z_here % 2, 0), (1, 1, full_len))[0]
    tables = attn_tables(seg_here)
    _, _, normed_one = rms_forward(rows_in.astype(jnp.float32), gain_one)
    qkv = jnp.dot(normed_one, qkv_cols, preferred_element_type=jnp.float32)
    turned, lse, attended16, out_rows = attn_forward(qkv, *tables, out_line, full_len, groups, n_dp)
    attn_part = times_transpose(attended16, out_rows)
    resid_all, gate_up_cols = share_resid(
        attn_part.astype(jnp.bfloat16), rows_in, gate_up_here, n_dp, n_z
    )
    total_rows = seqs_here * full_len
    resid = resid_all.reshape(total_rows, width).astype(jnp.float32)
    _, _, normed_two = rms_forward(resid, gain_two)
    gate_up = jnp.dot(normed_two, gate_up_cols, preferred_element_type=jnp.float32)
    gate_part = gate_up[:, :unit_count]
    up_part = gate_up[:, unit_count:]
    sigmoid_gate = jax.nn.sigmoid(gate_part)
    active = gate_part * sigmoid_gate
    hidden16 = (active * up_part).astype(jnp.bfloat16)
    cot_rows = cot_all.reshape(total_rows, width)
    d_hidden = times_transpose(cot_rows, down_rows)
    d_gate = d_hidden * up_part * sigmoid_gate * (1.0 + gate_part * (1.0 - sigmoid_gate))
    d_up = d_hidden * active
    d_gate_up16 = jnp.concatenate([d_gate, d_up], 1).astype(jnp.bfloat16)
    gate_up_term = contract_rows(normed_two, d_gate_up16).astype(jnp.bfloat16)
    gate_up_sum = lax.psum_scatter(gate_up_term, "dp", scatter_dimension=0, tiled=True)
    down_term = contract_rows(cot_rows, hidden16).astype(jnp.bfloat16)
    down_sum = lax.psum_scatter(down_term, "dp", scatter_dimension=0, tiled=True)
    d_normed_two = times_transpose(d_gate_up16, gate_up_cols).astype(jnp.bfloat16)
    d_resid16, gain_two_part, down_part = sum_line(
        d_normed_two.reshape(resid_all.shape), resid_all, cot_all, gain_two, hidden16, down_rows, n_z
    )
    down16 = down_part.reshape(resid_all.shape)
    pieces = [
        lax.dynamic_slice_in_dim(down16, (z_here + o) % n_z * local_len, local_len, 1)
        for o in range(n_z)
    ]
    for o in range(1, n_z):
        pieces[o] = lax.ppermute(pieces[o], "seq", [(i, (i + o) % n_z) for i in range(n_z)])
    down_here = sum(piece.astype(jnp.float32) for piece in pieces)
    resid_here = lax.dynamic_slice_in_dim(resid_all, z_here * local_len, local_len, 1)
    output = (resid_here.astype(jnp.float32) + down_here).astype(jnp.bfloat16)
    d_attended = jnp.dot(d_resid16, out_rows, preferred_element_type=jnp.float32).astype(jnp.bfloat16)
    d_qkv16 = attn_backward(turned, d_attended, lse, *tables, full_len, groups)
    out_term = contract_rows(d_resid16, attended16).astype(jnp.bfloat16)
    input_grad, grad_qkv, grad_out, gain_sums = hand_out(
        d_qkv16,
        normed_one,
        rows_in,
        d_resid16,
        gain_one,
        gain_two_part,
        qkv_cols,
        out_term,
        n_dp,
        n_z,
    )
    grad_gate_up, w_gu, m_gu, v_gu = adam_wide(
        gate_up_sum, gate_up_weight, first_gate_up, second_gate_up
    )
    grad_down, w_down, m_down, v_down = adam_turned(
        down_sum, down_weight, first_down, second_down
    )
    flat = lax.axis_index("dp") * n_z + z_here
    gain_sums = lax.dynamic_slice(
        jnp.sum(gain_sums.reshape(2, 8, LANES), axis=1), (0, flat * owned % LANES), (2, owned)
    )
    grad_gain_one = gain_sums[0]
    grad_gain_two = gain_sums[1]
    w_one, m_one, v_one = adam_update(attn_gain, grad_gain_one, first_attn_gain, second_attn_gain)
    w_qkv, m_qkv, v_qkv = adam_update(qkv_weight, grad_qkv, first_qkv, second_qkv)
    w_out, m_out, v_out = adam_update(out_weight, grad_out, first_out, second_out)
    w_two, m_two, v_two = adam_update(mlp_gain, grad_gain_two, first_mlp_gain, second_mlp_gain)
    return (
        output,
        input_grad,
        grad_gain_one,
        grad_qkv,
        grad_out,
        grad_gain_two,
        grad_gate_up,
        grad_down,
        w_one,
        w_qkv,
        w_out,
        w_two,
        w_gu,
        w_down,
        m_one,
        m_qkv,
        m_out,
        m_two,
        m_gu,
        m_down,
        v_one,
        v_qkv,
        v_out,
        v_two,
        v_gu,
        v_down,
    )


def solution(mesh):
    in_specs = (
        P("dp", "seq", None),
        P("dp", None),
        P("dp", "seq", None),
        P(("dp", "seq")),
        P("dp", "seq"),
        P("seq", "dp"),
        P(("dp", "seq")),
        P("dp", None, "seq"),
        P("seq", "dp"),
        P(("dp", "seq")),
        P("dp", "seq"),
        P("seq", "dp"),
        P(("dp", "seq")),
        P("dp", None, "seq"),
        P("seq", "dp"),
        P(("dp", "seq")),
        P("dp", "seq"),
        P("seq", "dp"),
        P(("dp", "seq")),
        P("dp", None, "seq"),
        P("seq", "dp"),
    )
    out_specs = (
        P("dp", "seq", None),
        P("dp", "seq", None),
        P(("dp", "seq")),
        P("dp", "seq"),
        P("seq", "dp"),
        P(("dp", "seq")),
        P("dp", None, "seq"),
        P("seq", "dp"),
        P(("dp", "seq")),
        P("dp", "seq"),
        P("seq", "dp"),
        P(("dp", "seq")),
        P("dp", None, "seq"),
        P("seq", "dp"),
        P(("dp", "seq")),
        P("dp", "seq"),
        P("seq", "dp"),
        P(("dp", "seq")),
        P("dp", None, "seq"),
        P("seq", "dp"),
        P(("dp", "seq")),
        P("dp", "seq"),
        P("seq", "dp"),
        P(("dp", "seq")),
        P("dp", None, "seq"),
        P("seq", "dp"),
    )
    return jax.shard_map(layer_step, mesh=mesh, in_specs=in_specs, out_specs=out_specs, check_vma=False)
```

```python
import functools

import jax
import jax.numpy as jnp
from jax import lax
from jax.experimental import pallas as pl
from jax.experimental.pallas import tpu as pltpu
from jax.sharding import PartitionSpec as P


HEADS = 32
KV_HEADS = 8
norm_eps = 1e-05
beta_one = 0.9
beta_two = 0.95
learn_rate = 0.01
weight_decay = 0.1
adam_eps = 1e-08
step_count = 10.0
masked_score = -1e30


HEAD_DIM = 64
LANES = 128


def dot_t(a, b):
    return lax.dot_general(a, b, (((1,), (1,)), ((), ())), preferred_element_type=jnp.float32)


def dot_n(a, b):
    return lax.dot_general(a, b, (((1,), (0,)), ((), ())), preferred_element_type=jnp.float32)


def dot_c(a, b):
    return lax.dot_general(a, b, (((0,), (0,)), ((), ())), preferred_element_type=jnp.float32)


def swap_halves(u):
    lane = lax.broadcasted_iota(jnp.int32, u.shape, 1)
    return jnp.where(lane % 64 < 32, pltpu.roll(u, 96, 1), pltpu.roll(u, 32, 1))


def turn(u, cos_wide, sin_wide):
    return u * cos_wide + swap_halves(u) * sin_wide


def key_start(block, q_rows, reach):
    return max(0, (block * q_rows - reach + 1) // q_rows * q_rows)


def attn_forward_kernel(pairs, q_rows, reach, qkv_ref, cos_ref, sin_ref, seg_col_ref, seg_row_ref,
                        turned_ref, lse_ref, out_ref):
    full_len = qkv_ref.shape[0]
    lane = lax.broadcasted_iota(jnp.int32, (full_len, LANES), 1)
    low = lane < HEAD_DIM
    cos_q = cos_ref[...]
    sin_q = sin_ref[...]
    kv = qkv_ref[:, pairs * LANES:].astype(jnp.float32)
    kv16 = turn(kv, jnp.where(low, cos_q, 1.0), jnp.where(low, sin_q, 0.0)).astype(jnp.bfloat16)
    turned_ref[:, pairs * LANES:] = kv16
    kv32 = kv16.astype(jnp.float32)
    rolled = pltpu.roll(kv32, HEAD_DIM, 1)
    zero = jnp.zeros_like(kv32)
    keys = (jnp.where(low, kv32, zero).astype(jnp.bfloat16), jnp.where(low, zero, rolled).astype(jnp.bfloat16))
    vals = (jnp.where(low, rolled, zero).astype(jnp.bfloat16), jnp.where(low, zero, kv32).astype(jnp.bfloat16))
    for pair in range(pairs):
        cols = slice(pair * LANES, (pair + 1) * LANES)
        query = turn(qkv_ref[:, cols].astype(jnp.float32), cos_q, sin_q) .astype(jnp.bfloat16)
        turned_ref[:, cols] = query
    for block in range(full_len // q_rows):
        first = key_start(block, q_rows, reach)
        last = (block + 1) * q_rows
        rows = slice(block * q_rows, last)
        span = slice(first, last)
        i = lax.broadcasted_iota(jnp.int32, (q_rows, last - first), 0) + block * q_rows
        j = lax.broadcasted_iota(jnp.int32, (q_rows, last - first), 1) + first
        allowed = (j <= i) & (seg_col_ref[rows, :1] == seg_row_ref[:1, span])
        for pair in range(pairs):
            cols = slice(pair * LANES, (pair + 1) * LANES)
            query = turned_ref[rows, cols]
            total = None
            for half in range(2):
                scores = dot_t(query, keys[half][span]) * (HEAD_DIM ** -0.5)
                scores = jnp.where(allowed, scores, masked_score)
                top = jnp.max(scores, axis=1, keepdims=True)
                lse = top + jnp.log(jnp.sum(jnp.exp(scores - top), axis=1, keepdims=True))
                probs = jnp.exp(scores - lse).astype(jnp.bfloat16)
                part = dot_n(probs, vals[half][span])
                total = part if total is None else total + part
                head = 2 * pair + half
                lse_ref[rows, head:head + 1] = lse
            out_ref[rows, cols] = total.astype(jnp.bfloat16)


def attn_backward_kernel(pairs, q_rows, reach, turned_ref, d_out_ref, lse_ref, cos_ref, sin_ref, seg_col_ref,
                         seg_row_ref, grad_ref, dk_ref, dv_ref):
    full_len = turned_ref.shape[0]
    lane = lax.broadcasted_iota(jnp.int32, (full_len, LANES), 1)
    low = lane < HEAD_DIM
    kv32 = turned_ref[:, pairs * LANES:].astype(jnp.float32)
    rolled = pltpu.roll(kv32, HEAD_DIM, 1)
    zero = jnp.zeros_like(kv32)
    keys = (jnp.where(low, kv32, zero).astype(jnp.bfloat16), jnp.where(low, zero, rolled).astype(jnp.bfloat16))
    vals = (jnp.where(low, rolled, zero).astype(jnp.bfloat16), jnp.where(low, zero, kv32).astype(jnp.bfloat16))
    dk_ref[...] = jnp.zeros_like(dk_ref)
    dv_ref[...] = jnp.zeros_like(dv_ref)
    low_rows = low[:q_rows]
    scale = HEAD_DIM ** -0.5
    for block in range(full_len // q_rows):
        first = key_start(block, q_rows, reach)
        last = (block + 1) * q_rows
        rows = slice(block * q_rows, last)
        span = slice(first, last)
        i = lax.broadcasted_iota(jnp.int32, (q_rows, last - first), 0) + block * q_rows
        j = lax.broadcasted_iota(jnp.int32, (q_rows, last - first), 1) + first
        allowed = (j <= i) & (seg_col_ref[rows, :1] == seg_row_ref[:1, span])
        cos_q = cos_ref[rows]
        sin_q = sin_ref[rows]
        for pair in range(pairs):
            cols = slice(pair * LANES, (pair + 1) * LANES)
            query = turned_ref[rows, cols]
            d_out = d_out_ref[rows, cols]
            q32 = query.astype(jnp.float32)
            o32 = d_out.astype(jnp.float32)
            d_query = None
            d_key = None
            d_val = None
            for half in range(2):
                keep = low_rows if half == 0 else ~low_rows
                q_only = jnp.where(keep, q32, 0.0).astype(jnp.bfloat16)
                o_only = jnp.where(keep, o32, 0.0).astype(jnp.bfloat16)
                head = 2 * pair + half
                scores = dot_t(query, keys[half][span]) * scale
                scores = jnp.where(allowed, scores, masked_score)
                probs = jnp.exp(scores - lse_ref[rows, head:head + 1])
                d_probs = dot_t(d_out, vals[half][span])
                delta = jnp.sum(probs * d_probs, axis=1, keepdims=True)
                d_scores = (probs * (d_probs - delta) * scale).astype(jnp.bfloat16)
                probs16 = probs.astype(jnp.bfloat16)
                dq = dot_n(d_scores, keys[half][span])
                dk = dot_c(d_scores, q_only)
                dv = dot_c(probs16, o_only)
                d_query = dq if d_query is None else d_query + dq
                d_key = dk if d_key is None else d_key + dk
                d_val = dv if d_val is None else d_val + dv
            dk_ref[span] = dk_ref[span] + d_key
            dv_ref[span] = dv_ref[span] + d_val
            grad_ref[rows, cols] = turn(d_query, cos_q, -sin_q).astype(jnp.bfloat16)
    d_key = dk_ref[...]
    d_val = dv_ref[...]
    d_key = d_key + pltpu.roll(d_key, HEAD_DIM, 1)
    d_val = d_val + pltpu.roll(d_val, HEAD_DIM, 1)
    d_key = turn(d_key, cos_ref[...], -sin_ref[...])
    grad_ref[:, pairs * LANES:] = jnp.where(low, d_key, d_val).astype(jnp.bfloat16)


def attn_specs(full_len, width):
    line = pl.BlockSpec((full_len, width), lambda s, g: (s, g))
    table = pl.BlockSpec((full_len, LANES), lambda s, g: (s, 0))
    row = pl.BlockSpec((8, full_len), lambda s, g: (s, 0))
    return line, table, row


Q_ROWS = 128
REACH = 256


def attn_gather_kernel(n_dp, pairs, q_rows, reach, qkv_ref, cos_ref, sin_ref, seg_col_ref, seg_row_ref, vo_ref,
                       turned_ref, lse_ref, out_ref, wo, d_s, d_r, loc):
    _, z, pair, c = place()
    n_d = n_dp // 2
    step = pl.program_id(1)
    steps = pl.num_programs(1)
    rows = vo_ref.shape[0]
    parts = 2
    part = rows // parts // 2

    def spot(owner, t, h):
        return wo.at[pl.ds(pl.multiple_of(owner * rows + (2 * t + h) * part, part), part)]

    spread = Spread(n_d, pair, c, z, parts, spot, d_s, d_r)
    keep = pltpu.make_async_copy(vo_ref, wo.at[pl.ds(pl.multiple_of(pair * rows, rows), rows)], loc)

    @pl.when(step == 0)
    def _():
        keep.start()
        barrier = pltpu.get_barrier_semaphore()
        for k in range(1, n_d):
            pl.semaphore_signal(barrier, inc=1, device_id=(2 * (pair ^ k) + c, z), device_id_type=MESH)
        pl.semaphore_wait(barrier, n_d - 1)
        keep.wait()
        for t in range(parts):
            spread.own(t)

    attn_forward_kernel(pairs, q_rows, reach, qkv_ref, cos_ref, sin_ref, seg_col_ref, seg_row_ref, turned_ref, lse_ref, out_ref)

    @pl.when(step == steps - 2)
    def _():
        spread.pass_on(0)

    @pl.when(step == steps - 1)
    def _():
        spread.pass_on(1)
        spread.finish()


def attn_forward(qkv, cos, sin, seg_col, seg_row, vo, full_len, groups, n_dp):
    pairs = groups // 2
    width = (groups + 2) * HEAD_DIM
    seqs = qkv.shape[0] // full_len
    kv = qkv.shape[1] // width
    n_d = n_dp // 2
    line, table, row = attn_specs(full_len, width)
    outw = pl.BlockSpec((full_len, groups * HEAD_DIM), lambda s, g: (s, g))
    rows = seqs * full_len
    return pl.pallas_call(
        functools.partial(attn_gather_kernel, n_dp, pairs, Q_ROWS, REACH),
        grid=(seqs, kv),
        in_specs=[line, table, table, table, row, VMEM_SPEC],
        out_specs=[line, pl.BlockSpec((full_len, LANES), lambda s, g: (s, g)), outw, ANY_SPEC],
        out_shape=[
            jax.ShapeDtypeStruct((rows, kv * width), jnp.bfloat16),
            jax.ShapeDtypeStruct((rows, kv * LANES), jnp.float32),
            jax.ShapeDtypeStruct((rows, kv * groups * HEAD_DIM), jnp.bfloat16),
            jax.ShapeDtypeStruct((n_d * vo.shape[0], vo.shape[1]), jnp.bfloat16),
        ],
        scratch_shapes=[DMA((n_d - 1, 2, 2)), DMA((n_d - 1, 2, 2)), DMA],
        compiler_params=pltpu.CompilerParams(collective_id=4, has_side_effects=True),
        cost_estimate=pl.CostEstimate(flops=4 * rows * full_len * kv * LANES * groups, bytes_accessed=150_000_000, transcendentals=0),
        name="attn_forward",
    )(qkv, cos, sin, seg_col, seg_row, vo)


def attn_backward(turned, d_out, lse, cos, sin, seg_col, seg_row, full_len, groups):
    pairs = groups // 2
    width = (groups + 2) * HEAD_DIM
    seqs = turned.shape[0] // full_len
    kv = turned.shape[1] // width
    line, table, row = attn_specs(full_len, width)
    outw = pl.BlockSpec((full_len, groups * HEAD_DIM), lambda s, g: (s, g))
    rows = seqs * full_len
    return pl.pallas_call(
        functools.partial(attn_backward_kernel, pairs, Q_ROWS, REACH),
        grid=(seqs, kv),
        in_specs=[line, outw, pl.BlockSpec((full_len, LANES), lambda s, g: (s, g)), table, table, table, row],
        out_specs=line,
        out_shape=jax.ShapeDtypeStruct((rows, kv * width), jnp.bfloat16),
        scratch_shapes=[pltpu.VMEM((full_len, LANES), jnp.float32)] * 2,
        cost_estimate=pl.CostEstimate(flops=10 * rows * full_len * kv * LANES * groups, bytes_accessed=rows * kv * width * 6, transcendentals=0),
        name="attn_backward",
    )(turned, d_out, lse, cos, sin, seg_col, seg_row)


def attn_tables(segment_ids):
    seqs, full_len = segment_ids.shape
    earlier = (segment_ids[..., None, :] < segment_ids[..., :, None]).astype(jnp.int32)
    positions = jnp.arange(full_len, dtype=jnp.int32) - jnp.sum(earlier, axis=-1, dtype=jnp.int32)
    inverse = 500000.0 ** (-2.0 * jnp.arange(HEAD_DIM // 2, dtype=jnp.float32) / HEAD_DIM)
    angles = positions.astype(jnp.float32)[..., None] * inverse
    cos = jnp.cos(angles)
    sin = jnp.sin(angles)
    cos = jnp.concatenate([cos] * 4, -1).reshape(seqs * full_len, LANES)
    sin = jnp.concatenate([-sin, sin] * 2, -1).reshape(seqs * full_len, LANES)
    seg_col = jnp.broadcast_to(segment_ids[:, :, None], (seqs, full_len, LANES)).reshape(seqs * full_len, LANES)
    seg_row = jnp.broadcast_to(segment_ids[:, None, :], (seqs, 8, full_len)).reshape(seqs * 8, full_len)
    return cos, sin, seg_col, seg_row


MESH = pl.DeviceIdType.MESH
VMEM_SPEC = pl.BlockSpec(memory_space=pltpu.VMEM)
ANY_SPEC = pl.BlockSpec(memory_space=pl.ANY)
DMA = pltpu.SemaphoreType.DMA


def place():
    d = lax.axis_index("dp")
    z = lax.axis_index("seq")
    return d, z, d // 2, d % 2


def remote(src, dst, send, recv, dev):
    return pltpu.make_async_remote_copy(
        src_ref=src, dst_ref=dst, send_sem=send, recv_sem=recv, device_id=dev, device_id_type=MESH
    )


def greet_all(n_dp, n_z, d, z):
    barrier = pltpu.get_barrier_semaphore()
    me = d * n_z + z

    def one(o, carry):
        other = lax.rem(me + o, n_dp * n_z)
        pl.semaphore_signal(barrier, inc=1, device_id=(other // n_z, lax.rem(other, n_z)), device_id_type=MESH)
        return carry

    lax.fori_loop(1, n_dp * n_z, one, 0)
    pl.semaphore_wait(barrier, n_dp * n_z - 1)


def greet_line(n_z, d, z, extra=()):
    barrier = pltpu.get_barrier_semaphore()
    c = d % 2
    for o in range(n_z):
        zz = lax.rem(z + o, n_z)
        for core in range(2):
            if o == 0 and core == 0:
                continue
            pl.semaphore_signal(barrier, inc=1, device_id=(d - c + lax.rem(c + core, 2), zz), device_id_type=MESH)
    for dev in extra:
        pl.semaphore_signal(barrier, inc=1, device_id=dev, device_id_type=MESH)
    pl.semaphore_wait(barrier, 2 * n_z - 1 + len(extra))


def block_at(ref, shape, row, col):
    return ref.at[pl.ds(pl.multiple_of(row * shape[0], shape[0]), shape[0]),
                  pl.ds(pl.multiple_of(col * shape[1], shape[1]), shape[1])]


class Spread:
    def __init__(self, n_d, pair, c, z, parts, spot, send, recv):
        self.n_d, self.pair, self.parts, self.spot = n_d, pair, parts, spot
        self.send, self.recv = send, recv
        self.dev = lambda k: (2 * (pair ^ k) + c, z)

    def copy(self, slot, owner, t, h, to):
        at = self.spot(owner, t, h)
        return remote(at, at, self.send.at[slot, t, h], self.recv.at[slot, t, h], self.dev(to))

    def own(self, t):
        if self.n_d == 4:
            for h in range(2):
                self.copy(0, self.pair, t, h, 1).start()
                self.copy(1, self.pair, t, 1 - h, 2).start()
        else:
            for k in range(1, self.n_d):
                for h in range(2):
                    self.copy(k - 1, self.pair, t, h, k).start()

    def pass_on(self, t):
        if self.n_d == 4:
            self.copy(0, self.pair ^ 1, t, 0, 1).wait_recv()
            self.copy(2, self.pair ^ 1, t, 0, 2).start()
            self.copy(1, self.pair ^ 2, t, 1, 2).wait_recv()
            self.copy(2, self.pair ^ 2, t, 1, 1).start()

    def rest(self, t):
        if self.n_d == 4:
            self.copy(0, self.pair ^ 1, t, 1, 1).wait_recv()
            self.copy(1, self.pair ^ 2, t, 0, 2).wait_recv()
        else:
            for k in range(1, self.n_d):
                for h in range(2):
                    self.copy(k - 1, self.pair ^ k, t, h, k).wait_recv()

    def far(self, t):
        if self.n_d == 4:
            for h in range(2):
                self.copy(2, self.pair ^ 3, t, h, 1).wait_recv()

    def sent(self):
        for t in range(self.parts):
            for h in range(2):
                for slot in range(self.n_d - 1):
                    self.copy(slot, self.pair, t, h, 1).wait_send()

    def finish(self):
        for t in range(self.parts):
            if self.n_d == 4:
                self.copy(0, self.pair ^ 1, t, 1, 1).wait_recv()
                self.copy(1, self.pair ^ 2, t, 0, 2).wait_recv()
                for h in range(2):
                    self.copy(2, self.pair ^ 3, t, h, 1).wait_recv()
                    for slot in range(3):
                        self.copy(slot, self.pair, t, h, 1).wait_send()
            else:
                for k in range(1, self.n_d):
                    for h in range(2):
                        self.copy(k - 1, self.pair ^ k, t, h, k).wait_recv()
                        self.copy(k - 1, self.pair, t, h, k).wait_send()


def gather_in_kernel(n_dp, n_z, x_ref, w_ref, v_ref, g_ref, s_ref, gu_ref, xs, wq, vo, ga, sg, gu16, gu_in, gu_out,
                     x_s, x_r, f_s, f_r, w_s, w_r, v_s, v_r, d_s, d_r, g_s, g_r, s_s, s_r, loc, gu_is, gu_os):
    d, z, pair, c = place()
    n_d = n_dp // 2
    me = d * n_z + z
    total = n_dp * n_z
    rows = x_ref.shape[1]
    half = rows // 2
    shape = w_ref.shape
    cz = z // 2
    chunks = gu_ref.shape[0] // WIDE_ROWS
    gu_width = gu_ref.shape[2]

    def chunk_in(i, slot):
        return pltpu.make_async_copy(gu_ref.at[pl.ds(pl.multiple_of(i * WIDE_ROWS, WIDE_ROWS), WIDE_ROWS)], gu_in.at[slot], gu_is.at[slot])

    def chunk_out(i, slot):
        return pltpu.make_async_copy(gu_out.at[slot], gu16.at[pl.ds(pl.multiple_of(i * WIDE_ROWS, WIDE_ROWS), WIDE_ROWS)], gu_os.at[slot])

    def round_chunks(low, high):
        def one(i, carry):
            slot = lax.rem(i, 2)
            pl.when(i + 1 < chunks)(chunk_in(i + 1, 1 - slot).start)
            chunk_in(i, slot).wait()
            pl.when(i >= 2)(chunk_out(i - 2, slot).wait)
            for n in range(2):
                gu_out[slot, :, n * gu_width : (n + 1) * gu_width] = gu_in[slot, :, n].astype(jnp.bfloat16)
            chunk_out(i, slot).start()
            return carry

        lax.fori_loop(low, high, one, 0)

    chunk_in(0, 0).start()
    greet_all(n_dp, n_z, d, z)

    def line_stage(src, dst, send, recv, spare, wait):
        for o in range(n_z):
            copy = remote(src, dst, send.at[o], recv.at[c, z % 2], (2 * pair + cz, lax.rem(z + o, n_z)))
            act = copy.wait_send if wait else copy.start
            if o == 0:
                pl.when(c != cz)(act)
                if not wait:
                    pl.when(c == cz)(pltpu.make_async_copy(src, dst, loc.at[spare]).start)
            else:
                act()

    my_block = block_at(wq, shape, d, z % 2)
    line_stage(w_ref, my_block, w_s, w_r, 0, False)

    for i in range(2):
        for h in range(2):
            src = x_ref.at[i, pl.ds(h * half, half)]
            dst = xs.at[pl.ds(pl.multiple_of(z * rows + h * half, half), half)]
            zz = 2 * c + i
            mine = (h == c) & (zz == z)
            copy = remote(src, dst, x_s.at[i, h], x_r.at[z], (2 * pair + h, zz))
            pl.when(jnp.logical_not(mine))(copy.start)
            pl.when(mine)(lambda src=src, dst=dst: pltpu.make_async_copy(src, dst, loc.at[1]).start())

    seg_copy = remote(s_ref, sg.at[c], s_s, s_r, (2 * pair + 1 - c, z))
    seg_copy.start()
    own_seg = pltpu.make_async_copy(s_ref, sg.at[c], loc.at[2])
    own_seg.start()
    own_gain = pltpu.make_async_copy(g_ref, ga.at[me], loc.at[3])
    own_gain.start()

    def send_gain(o, carry):
        other = lax.rem(me + o, total)
        remote(g_ref, ga.at[me], g_s, g_r, (other // n_z, lax.rem(other, n_z))).start()
        return carry

    lax.fori_loop(1, total, send_gain, 0)

    first = jnp.where(c == cz, z % 2, 1 - c)

    def turn_of(t):
        return t % 2, (first if t < 2 else 1 - first)

    def spot(owner, t, h):
        core, b = turn_of(t)
        part = shape[0] // 2
        return wq.at[pl.ds(pl.multiple_of((2 * owner + core) * shape[0] + h * part, part), part),
                     pl.ds(pl.multiple_of(b * shape[1], shape[1]), shape[1])]

    spread = Spread(n_d, pair, c, z, 4, spot, d_s, d_r)
    for t in range(4):
        core, b = turn_of(t)
        blk = block_at(wq, shape, 2 * pair + core, b)
        mine = (core == c) & (2 * c + b == z)
        arrive = remote(w_ref, blk, w_s.at[0], w_r.at[core, b], (d, z))
        pl.when(jnp.logical_not(mine))(arrive.wait_recv)
        pl.when(mine)(lambda blk=blk: pltpu.make_async_copy(w_ref, blk, loc.at[0]).wait())
        spread.own(t)
        if t == 1:
            line_stage(v_ref, block_at(vo, v_ref.shape, c, z % 2), v_s, v_r, 4, False)
        if t > 0:
            spread.pass_on(t - 1)
        round_chunks(t * chunks // 4, (t + 1) * chunks // 4)

    for o in range(n_z):
        zs = lax.rem(z + o, n_z)
        src = xs.at[pl.ds(pl.multiple_of(zs * rows + c * half, half), half)]
        mine = (cz == c) & (zs == z)
        arrive = remote(src, src, x_s.at[0, 0], x_r.at[zs], (d, z))
        pl.when(jnp.logical_not(mine))(arrive.wait_recv)
        pl.when(mine)(lambda src=src: pltpu.make_async_copy(src, src, loc.at[1]).wait())
        remote(src, src, f_s.at[zs], f_r.at[zs], (2 * pair + 1 - c, z)).start()
    spread.pass_on(3)

    line_stage(w_ref, my_block, w_s, w_r, 0, True)
    line_stage(v_ref, block_at(vo, v_ref.shape, c, z % 2), v_s, v_r, 4, True)
    for i in range(2):
        for h in range(2):
            src = x_ref.at[i, pl.ds(h * half, half)]
            mine = (h == c) & (2 * c + i == z)
            copy = remote(src, src, x_s.at[i, h], x_r.at[0], (d, z))
            pl.when(jnp.logical_not(mine))(copy.wait_send)
    for zs in range(n_z):
        src = xs.at[pl.ds(zs * rows, half)]
        copy = remote(src, src, f_s.at[zs], f_r.at[zs], (d, z))
        copy.wait_send()
        copy.wait_recv()
    for core in range(2):
        for b in range(2):
            blk = block_at(vo, v_ref.shape, core, b)
            mine = (core == c) & (2 * c + b == z)
            pl.when(jnp.logical_not(mine))(remote(blk, blk, v_s.at[0], v_r.at[core, b], (d, z)).wait_recv)
            pl.when(mine)(pltpu.make_async_copy(v_ref, blk, loc.at[4]).wait)
    for i in range(max(0, chunks - 2), chunks):
        chunk_out(i, i % 2).wait()
    seg_copy.wait_send()
    remote(s_ref, sg.at[1 - c], s_s, s_r, (d, z)).wait_recv()
    own_seg.wait()
    own_gain.wait()
    many = ga.at[pl.ds(0, total - 1)]
    gains = remote(many, many, g_s, g_r, (d, z))
    gains.wait_send()
    gains.wait_recv()
    spread.finish()


def gather_in(x_loc, w, v, gain_tile, seg_tile, wide, n_dp, n_z):
    _, rows, width = x_loc.shape
    n_d = n_dp // 2
    total = n_dp * n_z
    return pl.pallas_call(
        functools.partial(gather_in_kernel, n_dp, n_z),
        in_specs=[VMEM_SPEC] * 5 + [ANY_SPEC],
        out_specs=[ANY_SPEC] * 6,
        out_shape=[
            jax.ShapeDtypeStruct((rows * n_z, width), x_loc.dtype),
            jax.ShapeDtypeStruct((w.shape[0] * n_dp, 2 * w.shape[1]), w.dtype),
            jax.ShapeDtypeStruct((v.shape[0] * 2, 2 * v.shape[1]), v.dtype),
            jax.ShapeDtypeStruct((total,) + gain_tile.shape, gain_tile.dtype),
            jax.ShapeDtypeStruct((2,) + seg_tile.shape, seg_tile.dtype),
            jax.ShapeDtypeStruct((wide.shape[0], wide.shape[1] * wide.shape[2]), jnp.bfloat16),
        ],
        scratch_shapes=[
            pltpu.VMEM((2, WIDE_ROWS) + wide.shape[1:], jnp.float32),
            pltpu.VMEM((2, WIDE_ROWS, wide.shape[1] * wide.shape[2]), jnp.bfloat16),
            DMA((2, 2)), DMA((n_z,)), DMA((n_z,)), DMA((n_z,)), DMA((n_z,)), DMA((2, 2)), DMA((n_z,)), DMA((2, 2)),
            DMA((n_d - 1, 4, 2)), DMA((n_d - 1, 4, 2)), DMA, DMA, DMA, DMA, DMA((5,)), DMA((2,)), DMA((2,)),
        ],
        compiler_params=pltpu.CompilerParams(collective_id=1, has_side_effects=True),
        cost_estimate=pl.CostEstimate(flops=0, bytes_accessed=200_000_000, transcendentals=0),
        name="gather_in",
    )(x_loc, w, v, gain_tile, seg_tile, wide)


def share_resid_kernel(n_dp, n_z, part_ref, x_ref, w_ref, out, wall, got, buf, p_s, p_r, u_s, u_r, d_s, d_r, c_s, c_r, loc):
    d, z, pair, c = place()
    n_d = n_dp // 2
    cz = z // 2
    full = x_ref.shape[0]
    half = full // 2
    unit = half // 2
    w_rows = w_ref.shape[0]
    parts = 4
    piece = w_rows // parts
    own_copy = pltpu.make_async_copy(w_ref, wall.at[pl.ds(pl.multiple_of(d * w_rows, w_rows), w_rows)], loc.at[2])
    own_copy.start()
    greet_line(n_z, d, z, [(2 * (pair ^ k) + c, z) for k in range(1, n_d)])
    mine = pl.ds(pl.multiple_of(c * half, half), half)
    theirs = pl.ds(pl.multiple_of((1 - c) * half, half), half)
    swap = remote(part_ref.at[theirs], got, p_s, p_r, (2 * pair + 1 - c, z))
    swap.start()

    def spot_w(owner, t, h):
        sub = piece // 2
        return wall.at[pl.ds(pl.multiple_of((2 * owner + c) * w_rows + (2 * t + h) * sub, sub), sub)]

    def across(k, t, core):
        at = wall.at[pl.ds(pl.multiple_of((2 * (pair ^ k) + core) * w_rows + t * piece, piece), piece)]
        return remote(at, at, c_s.at[k, t], c_r.at[k, t], (2 * pair + 1 - c, z))

    spread = Spread(n_d, pair, c, z, parts, spot_w, d_s, d_r)
    own_copy.wait()
    for t in range(parts):
        spread.own(t)
        across(0, t, c).start()

    swap.wait_recv()

    def add(r, carry):
        at = pl.ds(pl.multiple_of(r * 16, 16), 16)
        src = pl.ds(pl.multiple_of(c * half + r * 16, 16), 16)
        total = x_ref[src].astype(jnp.float32) + part_ref[src].astype(jnp.float32) + got[at].astype(jnp.float32)
        buf[at] = total.astype(jnp.bfloat16)
        return carry

    def spot(jl, h, k):
        return out.at[jl, pl.ds(pl.multiple_of(h * half + k * unit, unit), unit)]

    def sends(k, wait):
        src = buf.at[pl.ds(k * unit, unit)]
        dst = spot(z % 2, c, k)
        for o, zz in ((1, z - 1), (2, z + 1), (0, z)):
            copy = remote(src, dst, u_s.at[o, k], u_r.at[z % 2, c, k], (2 * pair + cz, zz))
            act = copy.wait_send if wait else copy.start
            if o == 0:
                keep = pltpu.make_async_copy(src, dst, loc.at[k])
                pl.when(c != cz)(act)
                pl.when(c == cz)(keep.wait if wait else keep.start)
            elif o == 1:
                pl.when(z > 0)(act)
            else:
                pl.when(z < n_z - 1)(act)

    per = unit // 16
    lax.fori_loop(0, per, add, 0)
    lax.fori_loop(per, per + per // 2, add, 0)
    sends(0, False)
    lax.fori_loop(per + per // 2, 2 * per, add, 0)
    swap.wait_send()
    sends(1, False)

    def relay(dist, sign, k, h, begin):
        j = z + sign * dist
        ok = (j >= 2 * c) & (j <= 2 * c + 1)
        to = z - sign
        more = (to >= 0) & (to <= n_z - 1)
        jl = lax.rem(j + n_z, 2)
        at = spot(jl, h, k)
        copy = remote(at, at, u_s.at[3 + (0 if sign < 0 else 1), 4 * jl + 2 * h + k], u_r.at[jl, h, k], (2 * pair + c, to))
        if begin:

            @pl.when(ok)
            def _():
                copy.wait_recv()
                pl.when(more)(copy.start)
        else:
            pl.when(ok & more)(copy.wait_send)

    def take(t):
        spread.pass_on(t)

    def rest(t):
        spread.rest(t)
        for k in range(1, n_d):
            if n_d != 4 or k != 3:
                across(k, t, c).start()

    def far(t):
        if n_d == 4:
            spread.far(t)
            across(3, t, c).start()

    links = []
    for t in range(parts):
        links += [(take, t), (rest, t)]
    links += [(far, t) for t in range(parts)]
    line = [(dist, k, h) for dist in range(1, n_z) for k in range(2) for h in range(2)]
    for n in range(max(len(links), len(line))):
        if n < len(line):
            dist, k, h = line[n]
            for sign in (-1, 1):
                relay(dist, sign, k, h, True)
        if n < len(links):
            links[n][0](links[n][1])

    @pl.when(c == cz)
    def _():
        for k in range(2):
            at = spot(z % 2, 1 - c, k)
            remote(at, at, u_s.at[0, 0], u_r.at[z % 2, 1 - c, k], (d, z)).wait_recv()

    for dist, k, h in line:
        for sign in (-1, 1):
            relay(dist, sign, k, h, False)
    sends(0, True)
    sends(1, True)
    spread.sent()
    for k in range(n_d):
        for t in range(parts):
            across(k, t, c).wait_send()
            across(k, t, 1 - c).wait_recv()


def share_resid(part, x, w, n_dp, n_z):
    full, width = x.shape
    n_d = n_dp // 2
    return pl.pallas_call(
        functools.partial(share_resid_kernel, n_dp, n_z),
        in_specs=[VMEM_SPEC] * 3,
        out_specs=[ANY_SPEC] * 2,
        out_shape=[
            jax.ShapeDtypeStruct((2, full, width), jnp.bfloat16),
            jax.ShapeDtypeStruct((n_dp * w.shape[0], w.shape[1]), jnp.bfloat16),
        ],
        scratch_shapes=[
            pltpu.VMEM((full // 2, width), jnp.bfloat16), pltpu.VMEM((full // 2, width), jnp.bfloat16),
            DMA, DMA, DMA((5, 8)), DMA((2, 2, 2)), DMA((n_d - 1, 4, 2)), DMA((n_d - 1, 4, 2)), DMA((n_d, 4)), DMA((n_d, 4)),
            DMA((3,)),
        ],
        compiler_params=pltpu.CompilerParams(collective_id=2, has_side_effects=True),
        cost_estimate=pl.CostEstimate(flops=0, bytes_accessed=200_000_000, transcendentals=0),
        name="share_resid",
    )(part, x, w)


CHUNKS = 8
GROUPS = 4


def sum_line_kernel(n_z, d_gate_ref, d_up_ref, w_ref, resid_all, cot_all, gain_ref, hid_ref, down_ref, d_out, gain_out,
                    rows_out, left, w, part, got, buf, resid_ref, cot_ref, hid, down, rows_buf,
                    s_s, s_r, p_s, p_r, loc, rows_sem, mul_sem, out_sem, left_sem, w_sem):
    d, z, pair, c = place()
    cz = z // 2
    full, width = buf.shape
    inner = d_gate_ref.shape[1]
    rows = full // CHUNKS
    group = full // GROUPS
    per = CHUNKS // GROUPS
    tile = 256
    tiles = width // tile
    lefts = []
    for q in range(GROUPS):
        for jl in range(2):
            for n, src in enumerate((d_gate_ref, d_up_ref)):
                lefts.append(pltpu.make_async_copy(
                    src.at[pl.ds(jl * full + q * group, group)],
                    left.at[pl.ds((2 * q + jl) * group, group), pl.ds(n * inner, inner)],
                    left_sem.at[q, jl, n],
                ))

    def w_copy(n):
        at = pl.ds(pl.multiple_of(n * tile, tile), tile)
        return pltpu.make_async_copy(w_ref.at[at], w.at[at], w_sem.at[n])

    fetch = (
        pltpu.make_async_copy(resid_all.at[z % 2], resid_ref, rows_sem.at[0]),
        pltpu.make_async_copy(cot_all.at[z % 2], cot_ref, rows_sem.at[1]),
    )
    factors = (pltpu.make_async_copy(hid_ref, hid, mul_sem.at[0]), pltpu.make_async_copy(down_ref, down, mul_sem.at[1]))
    for one in lefts[:4]:
        one.start()
    for n in range(tiles):
        w_copy(n).start()
    for one in tuple(lefts[4:]) + factors + fetch:
        one.start()
    greet_line(n_z, d, z)
    gain_out[...] = jnp.zeros_like(gain_out)
    own = c == cz

    def compute(q, low, high):
        if low == 0:
            for one in lefts[4 * q : 4 * q + 4]:
                one.wait()

        def one_tile(n, carry):
            if q == 0:
                w_copy(n).wait()
            at = pl.ds(pl.multiple_of(n * tile, tile), tile)
            value = dot_t(left[pl.ds(2 * q * group, 2 * group)], w[at])
            part[pl.ds(2 * q * group, 2 * group), at] = value.astype(jnp.bfloat16)
            return carry

        lax.fori_loop(low, high, one_tile, 0)

    def tile_out(j):
        at = pl.ds(pl.multiple_of(j * tile, tile), tile)
        return pltpu.make_async_copy(rows_buf.at[lax.rem(j, 2)], rows_out.at[:, at], out_sem.at[lax.rem(j, 2)])

    def multiply(low, high):
        if low == 0:
            for one in factors:
                one.wait()

        def one_tile(j, carry):
            pl.when(j >= 2)(tile_out(j - 2).wait)
            at = pl.ds(pl.multiple_of(j * tile, tile), tile)
            rows_buf[lax.rem(j, 2)] = dot_n(hid[...], down[:, at]).astype(jnp.bfloat16)
            tile_out(j).start()
            return carry

        lax.fori_loop(low, high, one_tile, 0)

    def part_start(jl, k):
        return (2 * (k // per) + jl) * group + k % per * rows

    def part_at(jl, k, r):
        return pl.ds(pl.multiple_of(part_start(jl, k) + r * 16, 16), 16)

    def copy_on(k, t, side, src):
        jl = jnp.bitwise_xor(c, t)
        to = z + 1 if side == 0 else z - 1
        return remote(src, got.at[side, jl, pl.ds(k * rows, rows)], s_s.at[t, k], s_r.at[side, jl, k], (2 * pair + c, to))

    def arrived(side, jl, k):
        at = got.at[side, jl, pl.ds(k * rows, rows)]
        return remote(at, at, s_s.at[0, 0], s_r.at[side, jl, k], (d, z))

    def send_step(k, t, edge_only, inner_only, wait):
        jl = jnp.bitwise_xor(c, t)
        j = 2 * c + jl
        for side in range(2):
            going = (z < j) if side == 0 else (z > j)
            edge = (z == 0) if side == 0 else (z == n_z - 1)
            raw = copy_on(k, t, side, part.at[pl.ds(pl.multiple_of(part_start(jl, k), rows), rows)])
            passed = copy_on(k, t, side, got.at[side, jl, pl.ds(k * rows, rows)])
            if not inner_only:
                pl.when(going & edge)(raw.wait_send if wait else raw.start)
            if not edge_only:
                pl.when(going & jnp.logical_not(edge))(passed.wait_send if wait else passed.start)

    def add_in(side, jl, k):
        def one(r, carry):
            at = pl.ds(pl.multiple_of(k * rows + r * 16, 16), 16)
            got[side, jl, at] = (got[side, jl, at].astype(jnp.float32) + part[part_at(jl, k, r)].astype(jnp.float32)).astype(jnp.bfloat16)
            return carry

        lax.fori_loop(0, rows // 16, one, 0)

    def finish(jl, k):
        def one(r, carry):
            at = pl.ds(pl.multiple_of(k * rows + r * 16, 16), 16)
            total = part[part_at(jl, k, r)].astype(jnp.float32)
            low_side = got[0, jl, at].astype(jnp.float32)
            high_side = got[1, jl, at].astype(jnp.float32)
            total = total + jnp.where(z > 0, low_side, 0.0) + jnp.where(z < n_z - 1, high_side, 0.0)
            value = resid_ref[at].astype(jnp.float32)
            inverse = lax.rsqrt(jnp.mean(value * value, axis=-1, keepdims=True) + norm_eps)
            scaled = value * inverse
            d_scaled = total * gain_ref[...]
            mean = jnp.mean(d_scaled * scaled, axis=-1, keepdims=True)
            d_resid = cot_ref[at].astype(jnp.float32) + inverse * (d_scaled - scaled * mean)
            buf[at] = d_resid.astype(jnp.bfloat16)
            prod = total * scaled
            gain_out[...] = gain_out[...] + prod[:8] + prod[8:]
            return carry

        lax.fori_loop(0, rows // 16, one, 0)

    def to_partner(k):
        at = pl.ds(k * rows, rows)
        return remote(buf.at[at], d_out.at[at], p_s.at[k], p_r.at[k], (2 * pair + 1 - c, z))

    def keep(k):
        at = pl.ds(k * rows, rows)
        return pltpu.make_async_copy(buf.at[at], d_out.at[at], loc.at[k])

    def own_chunk(k):
        @pl.when(own)
        def _():
            jl = z % 2
            pl.when(z > 0)(arrived(0, jl, k).wait_recv)
            pl.when(z < n_z - 1)(arrived(1, jl, k).wait_recv)
            finish(jl, k)
            if k > 0:
                to_partner(k - 1).start()
                keep(k - 1).start()

    done = 0
    for q in range(GROUPS):
        compute(q, 0, 1)
        if q > 0:
            for k in range((q - 1) * per, q * per):
                for t in range(2):
                    send_step(k, t, True, False, False)
        compute(q, 1, tiles)
    multiply(done, done + 1)
    done += 1
    for k in range((GROUPS - 1) * per, CHUNKS):
        for t in range(2):
            send_step(k, t, True, False, False)
    for one in fetch:
        one.wait()

    steps = [(k, t) for k in range(CHUNKS) for t in range(2)]
    for n, (k, t) in enumerate(steps):
        jl = jnp.bitwise_xor(c, t)
        j = 2 * c + jl
        for side in range(2):
            going = (z < j) if side == 0 else (z > j)
            between = (z > 0) if side == 0 else (z < n_z - 1)

            @pl.when(going & between)
            def _():
                arrived(side, jl, k).wait_recv()
                add_in(side, jl, k)

        if n > 0:
            send_step(*steps[n - 1], False, True, False)
        if t == 0 and done < tiles:
            multiply(done, done + 1)
            done += 1
        if t == 1 and k > 0:
            own_chunk(k - 1)
    send_step(*steps[-1], False, True, False)
    own_chunk(CHUNKS - 1)
    if done < tiles:
        multiply(done, tiles)

    @pl.when(own)
    def _():
        to_partner(CHUNKS - 1).start()
        keep(CHUNKS - 1).start()

    for j in range(max(0, tiles - 2), tiles):
        tile_out(j).wait()
    for k, t in steps:
        send_step(k, t, False, False, True)
    for k in range(CHUNKS):
        at = d_out.at[pl.ds(k * rows, rows)]

        @pl.when(own)
        def _():
            to_partner(k).wait_send()
            keep(k).wait()

        pl.when(jnp.logical_not(own))(remote(at, at, p_s.at[k], p_r.at[k], (d, z)).wait_recv)


def sum_line(d_gate, d_up, w, resid, cot, gain, hidden, down, n_z):
    _, full, width = resid.shape
    b16 = jnp.bfloat16
    return pl.pallas_call(
        functools.partial(sum_line_kernel, n_z),
        in_specs=[ANY_SPEC] * 5 + [VMEM_SPEC] + [ANY_SPEC] * 2,
        out_specs=[ANY_SPEC, VMEM_SPEC, ANY_SPEC],
        out_shape=[
            jax.ShapeDtypeStruct((full, width), b16),
            jax.ShapeDtypeStruct((8, width), jnp.float32),
            jax.ShapeDtypeStruct((2 * full, width), b16),
        ],
        scratch_shapes=[
            pltpu.VMEM((2 * full, w.shape[1]), b16), pltpu.VMEM(w.shape, b16), pltpu.VMEM((2 * full, width), b16),
            pltpu.VMEM((2, 2, full, width), b16), pltpu.VMEM((full, width), b16),
            pltpu.VMEM((full, width), b16), pltpu.VMEM((full, width), b16),
            pltpu.VMEM(hidden.shape, b16), pltpu.VMEM(down.shape, b16), pltpu.VMEM((2, 2 * full, 256), b16),
            DMA((2, CHUNKS)), DMA((2, 2, CHUNKS)), DMA((CHUNKS,)), DMA((CHUNKS,)), DMA((CHUNKS,)), DMA((2,)), DMA((2,)), DMA((2,)),
            DMA((GROUPS, 2, 2)), DMA((width // 256,)),
        ],
        compiler_params=pltpu.CompilerParams(collective_id=3, has_side_effects=True, vmem_limit_bytes=63 * 1024 * 1024),
        cost_estimate=pl.CostEstimate(flops=0, bytes_accessed=200_000_000, transcendentals=0),
        name="sum_line",
    )(d_gate, d_up, w, resid, cot, gain, hidden, down)


WIDE_ROWS = 32
TURNED_ROWS = 512


def adam_wide_kernel(grad_ref, w_ref, m_ref, v_ref, g_out, w_out, m_out, v_out):
    width = w_ref.shape[-1]
    for n in range(2):
        grad = grad_ref[:, n * width : (n + 1) * width].astype(jnp.float32)
        weight, first, second = adam_update(w_ref[:, n], grad, m_ref[:, n], v_ref[:, n])
        g_out[:, n] = grad
        w_out[:, n] = weight
        m_out[:, n] = first
        v_out[:, n] = second


def adam_turned_kernel(grad_ref, w_ref, m_ref, v_ref, g_out, w_out, m_out, v_out):
    grad = grad_ref[...].astype(jnp.float32).T
    weight, first, second = adam_update(w_ref[...], grad, m_ref[...], v_ref[...])
    g_out[...] = grad
    w_out[...] = weight
    m_out[...] = first
    v_out[...] = second


def adam_call(kernel, grid, grad_spec, spec, arrays):
    shape = jax.ShapeDtypeStruct(arrays[1].shape, jnp.float32)
    return pl.pallas_call(
        kernel,
        grid=(grid,),
        in_specs=[grad_spec] + [spec] * 3,
        out_specs=[spec] * 4,
        out_shape=[shape] * 4,
        cost_estimate=pl.CostEstimate(flops=20 * shape.size, bytes_accessed=30 * shape.size, transcendentals=0),
    )(*arrays)


def adam_wide(*arrays):
    rows, _, width = arrays[1].shape
    return adam_call(
        adam_wide_kernel, rows // WIDE_ROWS,
        pl.BlockSpec((WIDE_ROWS, 2 * width), lambda i: (i, 0)),
        pl.BlockSpec((WIDE_ROWS, 2, width), lambda i: (i, 0, 0)),
        arrays,
    )


def adam_turned(*arrays):
    rows, cols = arrays[1].shape
    return adam_call(
        adam_turned_kernel, rows // TURNED_ROWS,
        pl.BlockSpec((cols, TURNED_ROWS), lambda i: (0, i)),
        pl.BlockSpec((TURNED_ROWS, cols), lambda i: (i, 0)),
        arrays,
    )


def hand_out_kernel(n_dp, n_z, dq_ref, n_ref, x_ref, dr_ref, gain_ref, gain2_ref, wq_ref, ot_ref, ig, gq, go, gains,
                    dn_ref, wq, got, buf, q_base, q_got, q_put, q_fin, o_base, o_got, o_put, o_fin, g_src, g_all,
                    p_s, p_r, i_s, i_r, q_s, q_r, qf_s, qf_r, o_s, o_r, of_s, of_r, g_s, g_r, loc):
    d, z, pair, c = place()
    n_d = n_dp // 2
    total = n_dp * n_z
    me = d * n_z + z
    cz = z // 2
    full, width = x_ref.shape
    half = full // 2
    quarter = half // 2
    q_rows, q_cols = q_fin.shape[1:]
    o_rows, o_cols = o_fin.shape[1:]
    relay = n_d == 4

    class First:
        def __init__(self, rows, cols, bufs, sems, spare):
            self.rows, self.cols, self.spare = rows, cols, spare
            self.base, self.got, self.put, self.fin = bufs
            self.send, self.recv, self.f_send, self.f_recv = sems

        def block(self, ref, b, core):
            return ref.at[pl.ds(core * self.rows, self.rows), pl.ds(b * self.cols, self.cols)]

        def source(self, owner, b, core):
            return self.base.at[pl.ds(pl.multiple_of((2 * owner + core) * self.rows, self.rows), self.rows), pl.ds(b * self.cols, self.cols)]

        def cut_of(self, owner, b, core, r):
            start = (2 * owner + core) * self.rows + r * 16
            return pl.ds(pl.multiple_of(start, 16), 16), pl.ds(b * self.cols, self.cols)

        def copy(self, n, b, core, owner, to):
            return remote(self.source(owner, b, core), self.block(self.got.at[n], b, core), self.send.at[n, b, core],
                          self.recv.at[n, b, core], (2 * (pair ^ to) + c, z))

        def begin(self, core):
            for b in range(2):
                if relay:
                    self.copy(1, b, core, pair ^ 3, 1 + b).start()
            for b in range(2):
                if relay:
                    self.copy(0, b, core, pair ^ (1 + b), 1 + b).start()
                else:
                    for k in range(1, n_d):
                        self.copy(k - 1, b, core, pair ^ k, k).start()

        def arrived(self, n, b, core):
            at = self.block(self.got.at[n], b, core)
            remote(at, at, self.send.at[n, b, core], self.recv.at[n, b, core], (d, z)).wait_recv()

        def cut(self, b, core, r):
            return pl.ds(pl.multiple_of(core * self.rows + r * 16, 16), 16), pl.ds(b * self.cols, self.cols)

        def middle_copy(self, b, core):
            return remote(self.source(pair ^ (2 >> b), b, core), self.block(self.got.at[2], b, core), self.send.at[2, b, core],
                          self.recv.at[2, b, core], (2 * (pair ^ (2 >> b)) + c, z))

        def middle(self, core, between):
            if not relay:
                return
            for b in range(2):
                self.arrived(1, b, core)

                def add(r, carry):
                    at = self.cut(b, core, r)
                    mid = self.cut_of(pair ^ (2 >> b), b, core, r)
                    self.base[mid] = (self.base[mid].astype(jnp.float32) + self.got[(1,) + at].astype(jnp.float32)).astype(jnp.bfloat16)
                    return carry

                lax.fori_loop(0, self.rows // 16, add, 0)
            self.middle_copy(0, core).start()
            between()
            self.middle_copy(1, core).start()

        def total(self, core, between):
            slots = (0, 2) if relay else range(n_d - 1)
            for b in range(2):
                for n in slots:
                    self.arrived(n, b, core)

                def add(r, carry):
                    at = self.cut(b, core, r)
                    value = self.base[self.cut_of(pair, b, core, r)].astype(jnp.float32)
                    for n in slots:
                        value = value + self.got[(n,) + at].astype(jnp.float32)
                    self.put[core, b, pl.ds(pl.multiple_of(r * 16, 16), 16)] = value.astype(jnp.bfloat16)
                    return carry

                lax.fori_loop(0, self.rows // 16, add, 0)
            self.second(0, core, False)
            between()
            self.second(1, core, False)

        def second(self, b, core, wait):
            here = (core == c) & (2 * c + b == z)
            src = self.put.at[core, b]
            copy = remote(src, self.fin.at[z], self.f_send.at[core, b], self.f_recv.at[z], (2 * pair + core, 2 * c + b))
            keep = pltpu.make_async_copy(src, self.fin.at[z], loc.at[self.spare])
            pl.when(jnp.logical_not(here))(copy.wait_send if wait else copy.start)
            pl.when(here)(keep.wait if wait else keep.start)

        def final(self):
            for core in range(2):
                for b in range(2):
                    self.second(b, core, True)
            for zs in range(n_z):
                at = self.fin.at[zs]
                from_here = (cz == c) & (zs == z)
                pl.when(jnp.logical_not(from_here))(remote(at, at, self.f_send.at[0, 0], self.f_recv.at[zs], (d, z)).wait_recv)

        def sent(self):
            for b in range(2):
                for core in range(2):
                    for n in range(n_d - 1):
                        at = self.block(self.got.at[n], b, core)
                        remote(at, at, self.send.at[n, b, core], self.recv.at[n, b, core], (d, z)).wait_send()

    o_first = First(o_rows, o_cols, (o_base, o_got, o_put, o_fin), (o_s, o_r, of_s, of_r), 2)
    q_first = First(q_rows, q_cols, (q_base, q_got, q_put, q_fin), (q_s, q_r, qf_s, qf_r), 3)
    o_load = pltpu.make_async_copy(ot_ref, o_base, loc.at[4])
    wq_load = pltpu.make_async_copy(wq_ref, wq, loc.at[5])
    o_load.start()
    wq_load.start()
    greet_all(n_dp, n_z, d, z)
    o_load.wait()
    o_first.begin(0)
    o_first.begin(1)
    nothing = lambda: None

    def q_blocks(core):
        def one(k, carry):
            owner = pair ^ (n_d - 1 - k)
            rows_at = pl.ds(pl.multiple_of((2 * owner + core) * q_rows, q_rows), q_rows)
            q_base[rows_at] = dot_c(n_ref[:, rows_at], dq_ref[...]).astype(jnp.bfloat16)
            return carry

        lax.fori_loop(0, n_d, one, 0)

    def dn_blocks(low, high):
        def one(r, carry):
            rows_at = pl.ds(pl.multiple_of(r * 256, 256), 256)
            dn_ref[:, rows_at] = dot_t(dq_ref[...], wq[rows_at]).astype(jnp.bfloat16)
            return carry

        lax.fori_loop(low, high, one, 0)

    q_blocks(0)
    o_first.middle(0, lambda: q_blocks(1))
    q_first.begin(0)
    wq_load.wait()
    dn_tiles = width // 256
    dn_blocks(0, dn_tiles // 2)
    o_first.middle(1, nothing)
    q_first.begin(1)
    dn_blocks(dn_tiles // 2, dn_tiles)
    mine = pl.ds(pl.multiple_of(c * half, half), half)
    theirs = pl.ds(pl.multiple_of((1 - c) * half, half), half)
    swap = remote(dn_ref.at[theirs], got, p_s, p_r, (2 * pair + 1 - c, z))
    o_first.total(0, nothing)
    swap.start()

    g_src[pl.ds(0, 8)] = jnp.zeros((8, width), jnp.float32)
    g_src[pl.ds(8, 8)] = gain2_ref[...]
    swap.wait_recv()

    def rows_of(r, carry):
        at = pl.ds(pl.multiple_of(r * 16, 16), 16)
        src = pl.ds(pl.multiple_of(c * half + r * 16, 16), 16)
        d_normed = dn_ref[src].astype(jnp.float32) + got[at].astype(jnp.float32)
        value = x_ref[src].astype(jnp.float32)
        inverse = lax.rsqrt(jnp.mean(value * value, axis=-1, keepdims=True) + norm_eps)
        scaled = value * inverse
        d_scaled = d_normed * gain_ref[...]
        mean = jnp.mean(d_scaled * scaled, axis=-1, keepdims=True)
        out = dr_ref[src].astype(jnp.float32) + inverse * (d_scaled - scaled * mean)
        buf[at] = out.astype(jnp.bfloat16)
        prod = d_normed * scaled
        g_src[pl.ds(0, 8)] = g_src[pl.ds(0, 8)] + prod[:8] + prod[8:]
        return carry

    def row_send(b, wait):
        src = buf.at[pl.ds(b * quarter, quarter)]
        dst = ig.at[z % 2]
        zz = 2 * c + b
        here = (cz == c) & (zz == z)
        copy = remote(src, dst, i_s.at[b], i_r.at[z % 2], (2 * pair + cz, zz))
        keep = pltpu.make_async_copy(src, dst, loc.at[0])
        pl.when(jnp.logical_not(here))(copy.wait_send if wait else copy.start)
        pl.when(here)(keep.wait if wait else keep.start)

    q_first.middle(0, nothing)
    per = quarter // 16
    lax.fori_loop(0, per, rows_of, 0)
    o_first.total(1, lambda: row_send(0, False))
    lax.fori_loop(per, 2 * per, rows_of, 0)
    q_first.middle(1, lambda: row_send(1, False))

    each = width // total

    def gain_tile(o):
        return g_src.at[:, pl.ds(pl.multiple_of(o * each // 128 * 128, 128), 128)]

    own_gain = pltpu.make_async_copy(gain_tile(me), g_all.at[me], loc.at[1])
    own_gain.start()

    def send_gain(o, carry):
        other = lax.rem(me + o, total)
        remote(gain_tile(other), g_all.at[me], g_s, g_r, (other // n_z, lax.rem(other, n_z))).start()
        return carry

    lax.fori_loop(1, total, send_gain, 0)

    q_first.total(0, nothing)
    q_first.total(1, nothing)

    o_first.final()
    value = o_fin[0].astype(jnp.float32)
    for zs in range(1, n_z):
        value = value + o_fin[zs].astype(jnp.float32)
    go[...] = value.T

    many = g_all.at[pl.ds(0, total - 1)]
    gain_copy = remote(many, many, g_s, g_r, (d, z))
    gain_copy.wait_send()
    gain_copy.wait_recv()
    own_gain.wait()
    gains[...] = jnp.zeros_like(gains)

    def add_gain(o, carry):
        gains[...] = gains[...] + g_all[o]
        return carry

    lax.fori_loop(0, total, add_gain, 0)

    swap.wait_send()
    for b in range(2):
        row_send(b, True)
    for i in range(2):
        from_here = (cz == c) & (2 * c + i == z)
        at = ig.at[i]
        pl.when(jnp.logical_not(from_here))(remote(at, at, i_s.at[0], i_r.at[i], (d, z)).wait_recv)
    o_first.sent()
    q_first.sent()
    q_first.final()

    def last(r, carry):
        at = pl.ds(pl.multiple_of(r * 16, 16), 16)
        value = q_fin[0, at].astype(jnp.float32)
        for zs in range(1, n_z):
            value = value + q_fin[zs, at].astype(jnp.float32)
        gq[at] = value
        return carry

    lax.fori_loop(0, q_rows // 16, last, 0)


def hand_out(dq, normed, x, dr, gain, gain2, wq, ot, n_dp, n_z):
    full, width = x.shape
    n_d = n_dp // 2
    total = n_dp * n_z
    q_rows, q_cols = wq.shape[0] // n_dp, wq.shape[1] // 2
    o_rows, o_cols = ot.shape[0] // n_dp, ot.shape[1] // 2
    b16 = jnp.bfloat16
    f32 = jnp.float32

    def weight_bufs(rows, cols):
        return [
            pltpu.VMEM((n_dp * rows, 2 * cols), b16), pltpu.VMEM((n_d - 1, 2 * rows, 2 * cols), b16),
            pltpu.VMEM((2, 2, rows, cols), b16), pltpu.VMEM((n_z, rows, cols), b16),
        ]

    weight_sems = [DMA((n_d - 1, 2, 2)), DMA((n_d - 1, 2, 2)), DMA((2, 2)), DMA((n_z,))]
    return pl.pallas_call(
        functools.partial(hand_out_kernel, n_dp, n_z),
        in_specs=[VMEM_SPEC] * 6 + [ANY_SPEC] * 2,
        out_specs=[ANY_SPEC] + [VMEM_SPEC] * 3,
        out_shape=[
            jax.ShapeDtypeStruct((2, full // 4, width), b16),
            jax.ShapeDtypeStruct((q_rows, q_cols), f32),
            jax.ShapeDtypeStruct((o_cols, o_rows), f32),
            jax.ShapeDtypeStruct((16, 128), f32),
        ],
        scratch_shapes=[
            pltpu.VMEM((full, width), b16), pltpu.VMEM(wq.shape, b16),
            pltpu.VMEM((full // 2, width), b16), pltpu.VMEM((full // 2, width), b16),
            *weight_bufs(q_rows, q_cols), *weight_bufs(o_rows, o_cols),
            pltpu.VMEM((16, width), f32), pltpu.VMEM((total, 16, 128), f32),
            DMA, DMA, DMA((2,)), DMA((2,)), *weight_sems, *weight_sems, DMA, DMA,
            DMA((6,)),
        ],
        compiler_params=pltpu.CompilerParams(collective_id=5, has_side_effects=True, vmem_limit_bytes=58 * 1024 * 1024),
        cost_estimate=pl.CostEstimate(flops=0, bytes_accessed=300_000_000, transcendentals=0),
        name="hand_out",
    )(dq, normed, x, dr, gain, gain2, wq, ot)


def rms_forward(values, gain_wide):
    inverse = lax.rsqrt(jnp.mean(values * values, axis=-1, keepdims=True) + norm_eps)
    scaled = values * inverse
    return (scaled, inverse, (scaled * gain_wide).astype(jnp.bfloat16))


def adam_update(weight, grad, first, second):
    new_first = beta_one * first + (1.0 - beta_one) * grad
    new_second = beta_two * second + (1.0 - beta_two) * grad * grad
    first_hat = new_first / (1.0 - beta_one**step_count)
    second_hat = new_second / (1.0 - beta_two**step_count)
    new_weight = weight - learn_rate * (
        first_hat / (jnp.sqrt(second_hat) + adam_eps) + weight_decay * weight
    )
    return (new_weight, new_first, new_second)


def contract_rows(left, right):
    return lax.dot_general(
        left, right, (((0,), (0,)), ((), ())), preferred_element_type=jnp.float32
    )


def times_transpose(left, right):
    return lax.dot_general(
        left, right, (((1,), (1,)), ((), ())), preferred_element_type=jnp.float32
    )


def layer_step(
    block_input,
    segment_ids,
    cotangent,
    attn_gain,
    qkv_weight,
    out_weight,
    mlp_gain,
    gate_up_weight,
    down_weight,
    first_attn_gain,
    first_qkv,
    first_out,
    first_mlp_gain,
    first_gate_up,
    first_down,
    second_attn_gain,
    second_qkv,
    second_out,
    second_mlp_gain,
    second_gate_up,
    second_down,
):
    seqs_here, local_len, width = block_input.shape
    full_len = segment_ids.shape[1]
    n_dp = lax.axis_size("dp")
    n_z = lax.axis_size("seq")
    groups = HEADS // KV_HEADS
    unit_count = down_weight.shape[0]
    z_here = lax.axis_index("seq")
    owned = attn_gain.shape[0]
    gain_line = jnp.concatenate([attn_gain, mlp_gain]).astype(jnp.bfloat16).astype(jnp.float32)
    gain_tile = jnp.pad(gain_line[None], ((0, 7), (0, LANES - 2 * owned)))
    seg_tile = jnp.pad(segment_ids, ((0, 8 - seqs_here), (0, 0)))
    down_rows = lax.all_gather(down_weight.astype(jnp.bfloat16), "dp", axis=1, tiled=True)
    rows_in, qkv_cols, out_line, gain_all, seg_all, gate_up_here = gather_in(
        block_input,
        qkv_weight.astype(jnp.bfloat16),
        out_weight.astype(jnp.bfloat16).T,
        gain_tile,
        seg_tile,
        gate_up_weight,
        n_dp,
        n_z,
    )
    cot_late, _ = lax.optimization_barrier((cotangent, gain_all))
    cot_all = lax.all_gather(cot_late, "seq", axis=1, tiled=True)
    gain_one = gain_all[:, 0, :owned].reshape(1, width)
    gain_two = gain_all[:, 0, owned : 2 * owned].reshape(1, width)
    seg_here = lax.dynamic_slice(seg_all, (z_here // 2, z_here % 2, 0), (1, 1, full_len))[0]
    tables = attn_tables(seg_here)
    _, _, normed_one = rms_forward(rows_in.astype(jnp.float32), gain_one)
    qkv = jnp.dot(normed_one, qkv_cols, preferred_element_type=jnp.float32)
    turned, lse, attended16, out_rows = attn_forward(qkv, *tables, out_line, full_len, groups, n_dp)
    attn_part = times_transpose(attended16, out_rows)
    resid_all, gate_up_cols = share_resid(
        attn_part.astype(jnp.bfloat16), rows_in, gate_up_here, n_dp, n_z
    )
    total_rows = seqs_here * full_len
    resid = resid_all.reshape(total_rows, width).astype(jnp.float32)
    _, _, normed_two = rms_forward(resid, gain_two)
    gate_up = jnp.dot(normed_two, gate_up_cols, preferred_element_type=jnp.float32)
    gate_part = gate_up[:, :unit_count]
    up_part = gate_up[:, unit_count:]
    sigmoid_gate = jax.nn.sigmoid(gate_part)
    active = gate_part * sigmoid_gate
    hidden16 = (active * up_part).astype(jnp.bfloat16)
    cot_rows = cot_all.reshape(total_rows, width)
    d_hidden = times_transpose(cot_rows, down_rows)
    d_gate = d_hidden * up_part * sigmoid_gate * (1.0 + gate_part * (1.0 - sigmoid_gate))
    d_up = d_hidden * active
    d_gate16 = d_gate.astype(jnp.bfloat16)
    d_up16 = d_up.astype(jnp.bfloat16)
    d_gate_up16 = jnp.concatenate([d_gate16, d_up16], 1)
    gate_up_term = contract_rows(normed_two, d_gate_up16).astype(jnp.bfloat16)
    gate_up_sum = lax.psum_scatter(gate_up_term, "dp", scatter_dimension=0, tiled=True)
    down_term = contract_rows(cot_rows, hidden16).astype(jnp.bfloat16)
    down_sum = lax.psum_scatter(down_term, "dp", scatter_dimension=0, tiled=True)
    d_resid16, gain_two_part, down_part = sum_line(
        d_gate16, d_up16, gate_up_cols, resid_all, cot_all, gain_two, hidden16, down_rows, n_z
    )
    down16 = down_part.reshape(resid_all.shape)
    pieces = [
        lax.dynamic_slice_in_dim(down16, (z_here + o) % n_z * local_len, local_len, 1)
        for o in range(n_z)
    ]
    for o in range(1, n_z):
        pieces[o] = lax.ppermute(pieces[o], "seq", [(i, (i + o) % n_z) for i in range(n_z)])
    down_here = sum(piece.astype(jnp.float32) for piece in pieces)
    resid_here = lax.dynamic_slice_in_dim(resid_all, z_here * local_len, local_len, 1)
    output = (resid_here.astype(jnp.float32) + down_here).astype(jnp.bfloat16)
    d_attended = jnp.dot(d_resid16, out_rows, preferred_element_type=jnp.float32).astype(jnp.bfloat16)
    d_qkv16 = attn_backward(turned, d_attended, lse, *tables, full_len, groups)
    out_term = contract_rows(d_resid16, attended16).astype(jnp.bfloat16)
    input_grad, grad_qkv, grad_out, gain_sums = hand_out(
        d_qkv16,
        normed_one,
        rows_in,
        d_resid16,
        gain_one,
        gain_two_part,
        qkv_cols,
        out_term,
        n_dp,
        n_z,
    )
    grad_gate_up, w_gu, m_gu, v_gu = adam_wide(
        gate_up_sum, gate_up_weight, first_gate_up, second_gate_up
    )
    grad_down, w_down, m_down, v_down = adam_turned(
        down_sum, down_weight, first_down, second_down
    )
    flat = lax.axis_index("dp") * n_z + z_here
    gain_sums = lax.dynamic_slice(
        jnp.sum(gain_sums.reshape(2, 8, LANES), axis=1), (0, flat * owned % LANES), (2, owned)
    )
    grad_gain_one = gain_sums[0]
    grad_gain_two = gain_sums[1]
    w_one, m_one, v_one = adam_update(attn_gain, grad_gain_one, first_attn_gain, second_attn_gain)
    w_qkv, m_qkv, v_qkv = adam_update(qkv_weight, grad_qkv, first_qkv, second_qkv)
    w_out, m_out, v_out = adam_update(out_weight, grad_out, first_out, second_out)
    w_two, m_two, v_two = adam_update(mlp_gain, grad_gain_two, first_mlp_gain, second_mlp_gain)
    return (
        output,
        input_grad,
        grad_gain_one,
        grad_qkv,
        grad_out,
        grad_gain_two,
        grad_gate_up,
        grad_down,
        w_one,
        w_qkv,
        w_out,
        w_two,
        w_gu,
        w_down,
        m_one,
        m_qkv,
        m_out,
        m_two,
        m_gu,
        m_down,
        v_one,
        v_qkv,
        v_out,
        v_two,
        v_gu,
        v_down,
    )


def solution(mesh):
    in_specs = (
        P("dp", "seq", None),
        P("dp", None),
        P("dp", "seq", None),
        P(("dp", "seq")),
        P("dp", "seq"),
        P("seq", "dp"),
        P(("dp", "seq")),
        P("dp", None, "seq"),
        P("seq", "dp"),
        P(("dp", "seq")),
        P("dp", "seq"),
        P("seq", "dp"),
        P(("dp", "seq")),
        P("dp", None, "seq"),
        P("seq", "dp"),
        P(("dp", "seq")),
        P("dp", "seq"),
        P("seq", "dp"),
        P(("dp", "seq")),
        P("dp", None, "seq"),
        P("seq", "dp"),
    )
    out_specs = (
        P("dp", "seq", None),
        P("dp", "seq", None),
        P(("dp", "seq")),
        P("dp", "seq"),
        P("seq", "dp"),
        P(("dp", "seq")),
        P("dp", None, "seq"),
        P("seq", "dp"),
        P(("dp", "seq")),
        P("dp", "seq"),
        P("seq", "dp"),
        P(("dp", "seq")),
        P("dp", None, "seq"),
        P("seq", "dp"),
        P(("dp", "seq")),
        P("dp", "seq"),
        P("seq", "dp"),
        P(("dp", "seq")),
        P("dp", None, "seq"),
        P("seq", "dp"),
        P(("dp", "seq")),
        P("dp", "seq"),
        P("seq", "dp"),
        P(("dp", "seq")),
        P("dp", None, "seq"),
        P("seq", "dp"),
    )
    return jax.shard_map(layer_step, mesh=mesh, in_specs=in_specs, out_specs=out_specs, check_vma=False)
```

```python
import functools

import jax
import jax.numpy as jnp
from jax import lax
from jax.experimental import pallas as pl
from jax.experimental.pallas import tpu as pltpu
from jax.sharding import PartitionSpec as P


HEADS = 32
KV_HEADS = 8
norm_eps = 1e-05
beta_one = 0.9
beta_two = 0.95
learn_rate = 0.01
weight_decay = 0.1
adam_eps = 1e-08
step_count = 10.0
masked_score = -1e30


HEAD_DIM = 64
LANES = 128


def dot_t(a, b):
    return lax.dot_general(a, b, (((1,), (1,)), ((), ())), preferred_element_type=jnp.float32)


def dot_n(a, b):
    return lax.dot_general(a, b, (((1,), (0,)), ((), ())), preferred_element_type=jnp.float32)


def dot_c(a, b):
    return lax.dot_general(a, b, (((0,), (0,)), ((), ())), preferred_element_type=jnp.float32)


def swap_halves(u):
    lane = lax.broadcasted_iota(jnp.int32, u.shape, 1)
    return jnp.where(lane % 64 < 32, pltpu.roll(u, 96, 1), pltpu.roll(u, 32, 1))


def turn(u, cos_wide, sin_wide):
    return u * cos_wide + swap_halves(u) * sin_wide


def key_start(block, q_rows, reach):
    return max(0, (block * q_rows - reach + 1) // q_rows * q_rows)


def attn_forward_kernel(pairs, q_rows, reach, qkv_ref, cos_ref, sin_ref, seg_col_ref, seg_row_ref,
                        turned_ref, lse_ref, out_ref):
    full_len = qkv_ref.shape[0]
    lane = lax.broadcasted_iota(jnp.int32, (full_len, LANES), 1)
    low = lane < HEAD_DIM
    cos_q = cos_ref[...]
    sin_q = sin_ref[...]
    kv = qkv_ref[:, pairs * LANES:].astype(jnp.float32)
    kv16 = turn(kv, jnp.where(low, cos_q, 1.0), jnp.where(low, sin_q, 0.0)).astype(jnp.bfloat16)
    turned_ref[:, pairs * LANES:] = kv16
    kv32 = kv16.astype(jnp.float32)
    rolled = pltpu.roll(kv32, HEAD_DIM, 1)
    zero = jnp.zeros_like(kv32)
    keys = (jnp.where(low, kv32, zero).astype(jnp.bfloat16), jnp.where(low, zero, rolled).astype(jnp.bfloat16))
    vals = (jnp.where(low, rolled, zero).astype(jnp.bfloat16), jnp.where(low, zero, kv32).astype(jnp.bfloat16))
    for pair in range(pairs):
        cols = slice(pair * LANES, (pair + 1) * LANES)
        query = turn(qkv_ref[:, cols].astype(jnp.float32), cos_q, sin_q) .astype(jnp.bfloat16)
        turned_ref[:, cols] = query
    for block in range(full_len // q_rows):
        first = key_start(block, q_rows, reach)
        last = (block + 1) * q_rows
        rows = slice(block * q_rows, last)
        span = slice(first, last)
        i = lax.broadcasted_iota(jnp.int32, (q_rows, last - first), 0) + block * q_rows
        j = lax.broadcasted_iota(jnp.int32, (q_rows, last - first), 1) + first
        allowed = (j <= i) & (seg_col_ref[rows, :1] == seg_row_ref[:1, span])
        for pair in range(pairs):
            cols = slice(pair * LANES, (pair + 1) * LANES)
            query = turned_ref[rows, cols]
            total = None
            for half in range(2):
                scores = dot_t(query, keys[half][span]) * (HEAD_DIM ** -0.5)
                scores = jnp.where(allowed, scores, masked_score)
                top = jnp.max(scores, axis=1, keepdims=True)
                lse = top + jnp.log(jnp.sum(jnp.exp(scores - top), axis=1, keepdims=True))
                probs = jnp.exp(scores - lse).astype(jnp.bfloat16)
                part = dot_n(probs, vals[half][span])
                total = part if total is None else total + part
                head = 2 * pair + half
                lse_ref[rows, head:head + 1] = lse
            out_ref[rows, cols] = total.astype(jnp.bfloat16)


def attn_backward_kernel(pairs, q_rows, reach, turned_ref, d_out_ref, lse_ref, cos_ref, sin_ref, seg_col_ref,
                         seg_row_ref, grad_ref, dk_ref, dv_ref):
    full_len = turned_ref.shape[0]
    lane = lax.broadcasted_iota(jnp.int32, (full_len, LANES), 1)
    low = lane < HEAD_DIM
    kv32 = turned_ref[:, pairs * LANES:].astype(jnp.float32)
    rolled = pltpu.roll(kv32, HEAD_DIM, 1)
    zero = jnp.zeros_like(kv32)
    keys = (jnp.where(low, kv32, zero).astype(jnp.bfloat16), jnp.where(low, zero, rolled).astype(jnp.bfloat16))
    vals = (jnp.where(low, rolled, zero).astype(jnp.bfloat16), jnp.where(low, zero, kv32).astype(jnp.bfloat16))
    dk_ref[...] = jnp.zeros_like(dk_ref)
    dv_ref[...] = jnp.zeros_like(dv_ref)
    low_rows = low[:q_rows]
    scale = HEAD_DIM ** -0.5
    for block in range(full_len // q_rows):
        first = key_start(block, q_rows, reach)
        last = (block + 1) * q_rows
        rows = slice(block * q_rows, last)
        span = slice(first, last)
        i = lax.broadcasted_iota(jnp.int32, (q_rows, last - first), 0) + block * q_rows
        j = lax.broadcasted_iota(jnp.int32, (q_rows, last - first), 1) + first
        allowed = (j <= i) & (seg_col_ref[rows, :1] == seg_row_ref[:1, span])
        cos_q = cos_ref[rows]
        sin_q = sin_ref[rows]
        for pair in range(pairs):
            cols = slice(pair * LANES, (pair + 1) * LANES)
            query = turned_ref[rows, cols]
            d_out = d_out_ref[rows, cols]
            q32 = query.astype(jnp.float32)
            o32 = d_out.astype(jnp.float32)
            d_query = None
            d_key = None
            d_val = None
            for half in range(2):
                keep = low_rows if half == 0 else ~low_rows
                q_only = jnp.where(keep, q32, 0.0).astype(jnp.bfloat16)
                o_only = jnp.where(keep, o32, 0.0).astype(jnp.bfloat16)
                head = 2 * pair + half
                scores = dot_t(query, keys[half][span]) * scale
                scores = jnp.where(allowed, scores, masked_score)
                probs = jnp.exp(scores - lse_ref[rows, head:head + 1])
                d_probs = dot_t(d_out, vals[half][span])
                delta = jnp.sum(probs * d_probs, axis=1, keepdims=True)
                d_scores = (probs * (d_probs - delta) * scale).astype(jnp.bfloat16)
                probs16 = probs.astype(jnp.bfloat16)
                dq = dot_n(d_scores, keys[half][span])
                dk = dot_c(d_scores, q_only)
                dv = dot_c(probs16, o_only)
                d_query = dq if d_query is None else d_query + dq
                d_key = dk if d_key is None else d_key + dk
                d_val = dv if d_val is None else d_val + dv
            dk_ref[span] = dk_ref[span] + d_key
            dv_ref[span] = dv_ref[span] + d_val
            grad_ref[rows, cols] = turn(d_query, cos_q, -sin_q).astype(jnp.bfloat16)
    d_key = dk_ref[...]
    d_val = dv_ref[...]
    d_key = d_key + pltpu.roll(d_key, HEAD_DIM, 1)
    d_val = d_val + pltpu.roll(d_val, HEAD_DIM, 1)
    d_key = turn(d_key, cos_ref[...], -sin_ref[...])
    grad_ref[:, pairs * LANES:] = jnp.where(low, d_key, d_val).astype(jnp.bfloat16)


def attn_specs(full_len, width):
    line = pl.BlockSpec((full_len, width), lambda s, g: (s, g))
    table = pl.BlockSpec((full_len, LANES), lambda s, g: (s, 0))
    row = pl.BlockSpec((8, full_len), lambda s, g: (s, 0))
    return line, table, row


Q_ROWS = 128
REACH = 256


def attn_gather_kernel(n_dp, pairs, q_rows, reach, qkv_ref, cos_ref, sin_ref, seg_col_ref, seg_row_ref, vo_ref,
                       turned_ref, lse_ref, out_ref, wo, d_s, d_r, loc):
    _, z, pair, c = place()
    n_d = n_dp // 2
    step = pl.program_id(1)
    steps = pl.num_programs(1)
    rows = vo_ref.shape[0]
    parts = 2
    part = rows // parts // 2

    def spot(owner, t, h):
        return wo.at[pl.ds(pl.multiple_of(owner * rows + (2 * t + h) * part, part), part)]

    spread = Spread(n_d, pair, c, z, parts, spot, d_s, d_r)
    keep = pltpu.make_async_copy(vo_ref, wo.at[pl.ds(pl.multiple_of(pair * rows, rows), rows)], loc)

    @pl.when(step == 0)
    def _():
        keep.start()
        barrier = pltpu.get_barrier_semaphore()
        for k in range(1, n_d):
            pl.semaphore_signal(barrier, inc=1, device_id=(2 * (pair ^ k) + c, z), device_id_type=MESH)
        pl.semaphore_wait(barrier, n_d - 1)
        keep.wait()
        for t in range(parts):
            spread.own(t)

    attn_forward_kernel(pairs, q_rows, reach, qkv_ref, cos_ref, sin_ref, seg_col_ref, seg_row_ref, turned_ref, lse_ref, out_ref)

    @pl.when(step == steps - 2)
    def _():
        spread.pass_on(0)

    @pl.when(step == steps - 1)
    def _():
        spread.pass_on(1)
        spread.finish()


def attn_forward(qkv, cos, sin, seg_col, seg_row, vo, full_len, groups, n_dp):
    pairs = groups // 2
    width = (groups + 2) * HEAD_DIM
    seqs = qkv.shape[0] // full_len
    kv = qkv.shape[1] // width
    n_d = n_dp // 2
    line, table, row = attn_specs(full_len, width)
    outw = pl.BlockSpec((full_len, groups * HEAD_DIM), lambda s, g: (s, g))
    rows = seqs * full_len
    return pl.pallas_call(
        functools.partial(attn_gather_kernel, n_dp, pairs, Q_ROWS, REACH),
        grid=(seqs, kv),
        in_specs=[line, table, table, table, row, VMEM_SPEC],
        out_specs=[line, pl.BlockSpec((full_len, LANES), lambda s, g: (s, g)), outw, ANY_SPEC],
        out_shape=[
            jax.ShapeDtypeStruct((rows, kv * width), jnp.bfloat16),
            jax.ShapeDtypeStruct((rows, kv * LANES), jnp.float32),
            jax.ShapeDtypeStruct((rows, kv * groups * HEAD_DIM), jnp.bfloat16),
            jax.ShapeDtypeStruct((n_d * vo.shape[0], vo.shape[1]), jnp.bfloat16),
        ],
        scratch_shapes=[DMA((n_d - 1, 2, 2)), DMA((n_d - 1, 2, 2)), DMA],
        compiler_params=pltpu.CompilerParams(collective_id=4, has_side_effects=True),
        cost_estimate=pl.CostEstimate(flops=4 * rows * full_len * kv * LANES * groups, bytes_accessed=150_000_000, transcendentals=0),
        name="attn_forward",
    )(qkv, cos, sin, seg_col, seg_row, vo)


def attn_backward(turned, d_out, lse, cos, sin, seg_col, seg_row, full_len, groups):
    pairs = groups // 2
    width = (groups + 2) * HEAD_DIM
    seqs = turned.shape[0] // full_len
    kv = turned.shape[1] // width
    line, table, row = attn_specs(full_len, width)
    outw = pl.BlockSpec((full_len, groups * HEAD_DIM), lambda s, g: (s, g))
    rows = seqs * full_len
    return pl.pallas_call(
        functools.partial(attn_backward_kernel, pairs, Q_ROWS, REACH),
        grid=(seqs, kv),
        in_specs=[line, outw, pl.BlockSpec((full_len, LANES), lambda s, g: (s, g)), table, table, table, row],
        out_specs=line,
        out_shape=jax.ShapeDtypeStruct((rows, kv * width), jnp.bfloat16),
        scratch_shapes=[pltpu.VMEM((full_len, LANES), jnp.float32)] * 2,
        cost_estimate=pl.CostEstimate(flops=10 * rows * full_len * kv * LANES * groups, bytes_accessed=rows * kv * width * 6, transcendentals=0),
        name="attn_backward",
    )(turned, d_out, lse, cos, sin, seg_col, seg_row)


def attn_tables(segment_ids):
    seqs, full_len = segment_ids.shape
    earlier = (segment_ids[..., None, :] < segment_ids[..., :, None]).astype(jnp.int32)
    positions = jnp.arange(full_len, dtype=jnp.int32) - jnp.sum(earlier, axis=-1, dtype=jnp.int32)
    inverse = 500000.0 ** (-2.0 * jnp.arange(HEAD_DIM // 2, dtype=jnp.float32) / HEAD_DIM)
    angles = positions.astype(jnp.float32)[..., None] * inverse
    cos = jnp.cos(angles)
    sin = jnp.sin(angles)
    cos = jnp.concatenate([cos] * 4, -1).reshape(seqs * full_len, LANES)
    sin = jnp.concatenate([-sin, sin] * 2, -1).reshape(seqs * full_len, LANES)
    seg_col = jnp.broadcast_to(segment_ids[:, :, None], (seqs, full_len, LANES)).reshape(seqs * full_len, LANES)
    seg_row = jnp.broadcast_to(segment_ids[:, None, :], (seqs, 8, full_len)).reshape(seqs * 8, full_len)
    return cos, sin, seg_col, seg_row


MESH = pl.DeviceIdType.MESH
VMEM_SPEC = pl.BlockSpec(memory_space=pltpu.VMEM)
ANY_SPEC = pl.BlockSpec(memory_space=pl.ANY)
DMA = pltpu.SemaphoreType.DMA


def place():
    d = lax.axis_index("dp")
    z = lax.axis_index("seq")
    return d, z, d // 2, d % 2


def remote(src, dst, send, recv, dev):
    return pltpu.make_async_remote_copy(
        src_ref=src, dst_ref=dst, send_sem=send, recv_sem=recv, device_id=dev, device_id_type=MESH
    )


def greet_all(n_dp, n_z, d, z):
    barrier = pltpu.get_barrier_semaphore()
    me = d * n_z + z

    def one(o, carry):
        other = lax.rem(me + o, n_dp * n_z)
        pl.semaphore_signal(barrier, inc=1, device_id=(other // n_z, lax.rem(other, n_z)), device_id_type=MESH)
        return carry

    lax.fori_loop(1, n_dp * n_z, one, 0)
    pl.semaphore_wait(barrier, n_dp * n_z - 1)


def greet_line(n_z, d, z, extra=()):
    barrier = pltpu.get_barrier_semaphore()
    c = d % 2
    for o in range(n_z):
        zz = lax.rem(z + o, n_z)
        for core in range(2):
            if o == 0 and core == 0:
                continue
            pl.semaphore_signal(barrier, inc=1, device_id=(d - c + lax.rem(c + core, 2), zz), device_id_type=MESH)
    for dev in extra:
        pl.semaphore_signal(barrier, inc=1, device_id=dev, device_id_type=MESH)
    pl.semaphore_wait(barrier, 2 * n_z - 1 + len(extra))


def block_at(ref, shape, row, col):
    return ref.at[pl.ds(pl.multiple_of(row * shape[0], shape[0]), shape[0]),
                  pl.ds(pl.multiple_of(col * shape[1], shape[1]), shape[1])]


class Spread:
    def __init__(self, n_d, pair, c, z, parts, spot, send, recv):
        self.n_d, self.pair, self.parts, self.spot = n_d, pair, parts, spot
        self.send, self.recv = send, recv
        self.dev = lambda k: (2 * (pair ^ k) + c, z)

    def copy(self, slot, owner, t, h, to):
        at = self.spot(owner, t, h)
        return remote(at, at, self.send.at[slot, t, h], self.recv.at[slot, t, h], self.dev(to))

    def own(self, t):
        if self.n_d == 4:
            for h in range(2):
                self.copy(0, self.pair, t, h, 1).start()
                self.copy(1, self.pair, t, 1 - h, 2).start()
        else:
            for k in range(1, self.n_d):
                for h in range(2):
                    self.copy(k - 1, self.pair, t, h, k).start()

    def pass_on(self, t):
        if self.n_d == 4:
            self.copy(0, self.pair ^ 1, t, 0, 1).wait_recv()
            self.copy(2, self.pair ^ 1, t, 0, 2).start()
            self.copy(1, self.pair ^ 2, t, 1, 2).wait_recv()
            self.copy(2, self.pair ^ 2, t, 1, 1).start()

    def rest(self, t):
        if self.n_d == 4:
            self.copy(0, self.pair ^ 1, t, 1, 1).wait_recv()
            self.copy(1, self.pair ^ 2, t, 0, 2).wait_recv()
        else:
            for k in range(1, self.n_d):
                for h in range(2):
                    self.copy(k - 1, self.pair ^ k, t, h, k).wait_recv()

    def far(self, t):
        if self.n_d == 4:
            for h in range(2):
                self.copy(2, self.pair ^ 3, t, h, 1).wait_recv()

    def sent(self):
        for t in range(self.parts):
            for h in range(2):
                for slot in range(self.n_d - 1):
                    self.copy(slot, self.pair, t, h, 1).wait_send()

    def finish(self):
        for t in range(self.parts):
            if self.n_d == 4:
                self.copy(0, self.pair ^ 1, t, 1, 1).wait_recv()
                self.copy(1, self.pair ^ 2, t, 0, 2).wait_recv()
                for h in range(2):
                    self.copy(2, self.pair ^ 3, t, h, 1).wait_recv()
                    for slot in range(3):
                        self.copy(slot, self.pair, t, h, 1).wait_send()
            else:
                for k in range(1, self.n_d):
                    for h in range(2):
                        self.copy(k - 1, self.pair ^ k, t, h, k).wait_recv()
                        self.copy(k - 1, self.pair, t, h, k).wait_send()


def gather_in_kernel(n_dp, n_z, x_ref, w_ref, v_ref, g_ref, s_ref, gu_ref, xs, wq, vo, ga, sg, gu16, gu_in, gu_out,
                     x_s, x_r, f_s, f_r, w_s, w_r, v_s, v_r, d_s, d_r, g_s, g_r, s_s, s_r, loc, gu_is, gu_os, w_f, v_f):
    d, z, pair, c = place()
    n_d = n_dp // 2
    me = d * n_z + z
    total = n_dp * n_z
    rows = x_ref.shape[1]
    half = rows // 2
    shape = w_ref.shape
    cz = z // 2
    chunks = gu_ref.shape[0] // WIDE_ROWS
    gu_width = gu_ref.shape[2]

    def chunk_in(i, slot):
        return pltpu.make_async_copy(gu_ref.at[pl.ds(pl.multiple_of(i * WIDE_ROWS, WIDE_ROWS), WIDE_ROWS)], gu_in.at[slot], gu_is.at[slot])

    def chunk_out(i, slot):
        return pltpu.make_async_copy(gu_out.at[slot], gu16.at[pl.ds(pl.multiple_of(i * WIDE_ROWS, WIDE_ROWS), WIDE_ROWS)], gu_os.at[slot])

    def round_chunks(low, high):
        def one(i, carry):
            slot = lax.rem(i, 2)
            pl.when(i + 1 < chunks)(chunk_in(i + 1, 1 - slot).start)
            chunk_in(i, slot).wait()
            pl.when(i >= 2)(chunk_out(i - 2, slot).wait)
            for n in range(2):
                gu_out[slot, :, n * gu_width : (n + 1) * gu_width] = gu_in[slot, :, n].astype(jnp.bfloat16)
            chunk_out(i, slot).start()
            return carry

        lax.fori_loop(low, high, one, 0)

    chunk_in(0, 0).start()
    greet_all(n_dp, n_z, d, z)

    def line_stage(src, dst, send, recv, spare, wait):
        for o, zz in ((0, z), (1, z - 1), (2, z + 1)):
            copy = remote(src, dst, send.at[o], recv.at[c, z % 2], (2 * pair + cz, zz))
            act = copy.wait_send if wait else copy.start
            if o == 0:
                pl.when(c != cz)(act)
                if not wait:
                    pl.when(c == cz)(pltpu.make_async_copy(src, dst, loc.at[spare]).start)
            else:
                pl.when(zz >= 0 if o == 1 else zz <= n_z - 1)(act)

    def line_relay(blk, send, recv, core, b, wait):
        j = 2 * c + b
        to = jnp.where(z > j, z + 1, z - 1)
        ok = (z != j) & (to >= 0) & (to <= n_z - 1)
        copy = remote(blk, blk, send, recv.at[core, b], (2 * pair + c, to))
        pl.when(ok)(copy.wait_send if wait else copy.start)

    my_block = block_at(wq, shape, d, z % 2)
    line_stage(w_ref, my_block, w_s, w_r, 0, False)

    for i in range(2):
        for h in range(2):
            src = x_ref.at[i, pl.ds(h * half, half)]
            dst = xs.at[pl.ds(pl.multiple_of(z * rows + h * half, half), half)]
            zz = 2 * c + i
            mine = (h == c) & (zz == z)
            copy = remote(src, dst, x_s.at[i, h], x_r.at[z], (2 * pair + h, zz))
            pl.when(jnp.logical_not(mine))(copy.start)
            pl.when(mine)(lambda src=src, dst=dst: pltpu.make_async_copy(src, dst, loc.at[1]).start())

    seg_copy = remote(s_ref, sg.at[c], s_s, s_r, (2 * pair + 1 - c, z))
    seg_copy.start()
    own_seg = pltpu.make_async_copy(s_ref, sg.at[c], loc.at[2])
    own_seg.start()
    own_gain = pltpu.make_async_copy(g_ref, ga.at[me], loc.at[3])
    own_gain.start()

    def send_gain(o, carry):
        other = lax.rem(me + o, total)
        remote(g_ref, ga.at[me], g_s, g_r, (other // n_z, lax.rem(other, n_z))).start()
        return carry

    lax.fori_loop(1, total, send_gain, 0)

    first = jnp.where(c == cz, z % 2, 1 - c)

    def turn_of(t):
        return t % 2, (first if t < 2 else 1 - first)

    def spot(owner, t, h):
        core, b = turn_of(t)
        part = shape[0] // 2
        return wq.at[pl.ds(pl.multiple_of((2 * owner + core) * shape[0] + h * part, part), part),
                     pl.ds(pl.multiple_of(b * shape[1], shape[1]), shape[1])]

    spread = Spread(n_d, pair, c, z, 4, spot, d_s, d_r)
    for t in range(4):
        core, b = turn_of(t)
        blk = block_at(wq, shape, 2 * pair + core, b)
        mine = (core == c) & (2 * c + b == z)
        arrive = remote(w_ref, blk, w_s.at[0], w_r.at[core, b], (d, z))
        pl.when(jnp.logical_not(mine))(arrive.wait_recv)
        pl.when(mine)(lambda blk=blk: pltpu.make_async_copy(w_ref, blk, loc.at[0]).wait())
        line_relay(blk, w_f.at[t], w_r, core, b, False)
        spread.own(t)
        if t == 0:
            line_stage(v_ref, block_at(vo, v_ref.shape, c, z % 2), v_s, v_r, 4, False)
        if t > 0:
            spread.pass_on(t - 1)
        round_chunks(t * chunks // 4, (t + 1) * chunks // 4)

    def out_unit(t, wait):
        core, b = turn_of(t)
        blk = block_at(vo, v_ref.shape, core, b)
        mine = (core == c) & (2 * c + b == z)
        if not wait:
            pl.when(jnp.logical_not(mine))(remote(blk, blk, v_s.at[0], v_r.at[core, b], (d, z)).wait_recv)
            pl.when(mine)(pltpu.make_async_copy(v_ref, blk, loc.at[4]).wait)
        line_relay(blk, v_f.at[t], v_r, core, b, wait)

    spread.pass_on(3)
    for o in range(n_z):
        zs = lax.rem(z + o, n_z)
        src = xs.at[pl.ds(pl.multiple_of(zs * rows + c * half, half), half)]
        mine = (cz == c) & (zs == z)
        arrive = remote(src, src, x_s.at[0, 0], x_r.at[zs], (d, z))
        pl.when(jnp.logical_not(mine))(arrive.wait_recv)
        pl.when(mine)(lambda src=src: pltpu.make_async_copy(src, src, loc.at[1]).wait())
        remote(src, src, f_s.at[zs], f_r.at[zs], (2 * pair + 1 - c, z)).start()
        out_unit(o, False)

    line_stage(w_ref, my_block, w_s, w_r, 0, True)
    line_stage(v_ref, block_at(vo, v_ref.shape, c, z % 2), v_s, v_r, 4, True)
    for i in range(2):
        for h in range(2):
            src = x_ref.at[i, pl.ds(h * half, half)]
            mine = (h == c) & (2 * c + i == z)
            copy = remote(src, src, x_s.at[i, h], x_r.at[0], (d, z))
            pl.when(jnp.logical_not(mine))(copy.wait_send)
    for zs in range(n_z):
        src = xs.at[pl.ds(zs * rows, half)]
        copy = remote(src, src, f_s.at[zs], f_r.at[zs], (d, z))
        copy.wait_send()
        copy.wait_recv()
    for t in range(4):
        core, b = turn_of(t)
        line_relay(block_at(wq, shape, 2 * pair + core, b), w_f.at[t], w_r, core, b, True)
        out_unit(t, True)
    for i in range(max(0, chunks - 2), chunks):
        chunk_out(i, i % 2).wait()
    seg_copy.wait_send()
    remote(s_ref, sg.at[1 - c], s_s, s_r, (d, z)).wait_recv()
    own_seg.wait()
    own_gain.wait()
    many = ga.at[pl.ds(0, total - 1)]
    gains = remote(many, many, g_s, g_r, (d, z))
    gains.wait_send()
    gains.wait_recv()
    spread.finish()


def gather_in(x_loc, w, v, gain_tile, seg_tile, wide, n_dp, n_z):
    _, rows, width = x_loc.shape
    n_d = n_dp // 2
    total = n_dp * n_z
    return pl.pallas_call(
        functools.partial(gather_in_kernel, n_dp, n_z),
        in_specs=[VMEM_SPEC] * 5 + [ANY_SPEC],
        out_specs=[ANY_SPEC] * 6,
        out_shape=[
            jax.ShapeDtypeStruct((rows * n_z, width), x_loc.dtype),
            jax.ShapeDtypeStruct((w.shape[0] * n_dp, 2 * w.shape[1]), w.dtype),
            jax.ShapeDtypeStruct((v.shape[0] * 2, 2 * v.shape[1]), v.dtype),
            jax.ShapeDtypeStruct((total,) + gain_tile.shape, gain_tile.dtype),
            jax.ShapeDtypeStruct((2,) + seg_tile.shape, seg_tile.dtype),
            jax.ShapeDtypeStruct((wide.shape[0], wide.shape[1] * wide.shape[2]), jnp.bfloat16),
        ],
        scratch_shapes=[
            pltpu.VMEM((2, WIDE_ROWS) + wide.shape[1:], jnp.float32),
            pltpu.VMEM((2, WIDE_ROWS, wide.shape[1] * wide.shape[2]), jnp.bfloat16),
            DMA((2, 2)), DMA((n_z,)), DMA((n_z,)), DMA((n_z,)), DMA((3,)), DMA((2, 2)), DMA((3,)), DMA((2, 2)),
            DMA((n_d - 1, 4, 2)), DMA((n_d - 1, 4, 2)), DMA, DMA, DMA, DMA, DMA((5,)), DMA((2,)), DMA((2,)), DMA((4,)), DMA((4,)),
        ],
        compiler_params=pltpu.CompilerParams(collective_id=1, has_side_effects=True),
        cost_estimate=pl.CostEstimate(flops=0, bytes_accessed=200_000_000, transcendentals=0),
        name="gather_in",
    )(x_loc, w, v, gain_tile, seg_tile, wide)


def share_resid_kernel(n_dp, n_z, part_ref, x_ref, w_ref, out, wall, got, buf, p_s, p_r, u_s, u_r, d_s, d_r, c_s, c_r, loc):
    d, z, pair, c = place()
    n_d = n_dp // 2
    cz = z // 2
    full = x_ref.shape[0]
    half = full // 2
    unit = half // 2
    w_rows = w_ref.shape[0]
    parts = 4
    piece = w_rows // parts
    own_copy = pltpu.make_async_copy(w_ref, wall.at[pl.ds(pl.multiple_of(d * w_rows, w_rows), w_rows)], loc.at[2])
    own_copy.start()
    greet_line(n_z, d, z, [(2 * (pair ^ k) + c, z) for k in range(1, n_d)])
    mine = pl.ds(pl.multiple_of(c * half, half), half)
    theirs = pl.ds(pl.multiple_of((1 - c) * half, half), half)
    swap = remote(part_ref.at[theirs], got, p_s, p_r, (2 * pair + 1 - c, z))
    swap.start()

    def spot_w(owner, t, h):
        sub = piece // 2
        return wall.at[pl.ds(pl.multiple_of((2 * owner + c) * w_rows + (2 * t + h) * sub, sub), sub)]

    def across(k, t, core):
        at = wall.at[pl.ds(pl.multiple_of((2 * (pair ^ k) + core) * w_rows + t * piece, piece), piece)]
        return remote(at, at, c_s.at[k, t], c_r.at[k, t], (2 * pair + 1 - c, z))

    spread = Spread(n_d, pair, c, z, parts, spot_w, d_s, d_r)
    own_copy.wait()
    for t in range(parts):
        spread.own(t)
        across(0, t, c).start()

    swap.wait_recv()

    def add(r, carry):
        at = pl.ds(pl.multiple_of(r * 16, 16), 16)
        src = pl.ds(pl.multiple_of(c * half + r * 16, 16), 16)
        total = x_ref[src].astype(jnp.float32) + part_ref[src].astype(jnp.float32) + got[at].astype(jnp.float32)
        buf[at] = total.astype(jnp.bfloat16)
        return carry

    def spot(jl, h, k):
        return out.at[jl, pl.ds(pl.multiple_of(h * half + k * unit, unit), unit)]

    def sends(k, wait):
        src = buf.at[pl.ds(k * unit, unit)]
        dst = spot(z % 2, c, k)
        for o, zz in ((1, z - 1), (2, z + 1), (0, z)):
            copy = remote(src, dst, u_s.at[o, k], u_r.at[z % 2, c, k], (2 * pair + cz, zz))
            act = copy.wait_send if wait else copy.start
            if o == 0:
                keep = pltpu.make_async_copy(src, dst, loc.at[k])
                pl.when(c != cz)(act)
                pl.when(c == cz)(keep.wait if wait else keep.start)
            elif o == 1:
                pl.when(z > 0)(act)
            else:
                pl.when(z < n_z - 1)(act)

    per = unit // 16
    lax.fori_loop(0, per, add, 0)
    lax.fori_loop(per, per + per // 2, add, 0)
    sends(0, False)
    lax.fori_loop(per + per // 2, 2 * per, add, 0)
    swap.wait_send()
    sends(1, False)

    def relay(dist, sign, k, h, begin):
        j = z + sign * dist
        ok = (j >= 2 * c) & (j <= 2 * c + 1)
        to = z - sign
        more = (to >= 0) & (to <= n_z - 1)
        jl = lax.rem(j + n_z, 2)
        at = spot(jl, h, k)
        copy = remote(at, at, u_s.at[3 + (0 if sign < 0 else 1), 4 * jl + 2 * h + k], u_r.at[jl, h, k], (2 * pair + c, to))
        if begin:

            @pl.when(ok)
            def _():
                copy.wait_recv()
                pl.when(more)(copy.start)
        else:
            pl.when(ok & more)(copy.wait_send)

    def take(t):
        spread.pass_on(t)

    def rest(t):
        spread.rest(t)
        for k in range(1, n_d):
            if n_d != 4 or k != 3:
                across(k, t, c).start()

    def far(t):
        if n_d == 4:
            spread.far(t)
            across(3, t, c).start()

    links = []
    for t in range(parts):
        links += [(take, t), (rest, t)]
    links += [(far, t) for t in range(parts)]
    line = [(dist, k, h) for dist in range(1, n_z) for k in range(2) for h in range(2)]
    for n in range(max(len(links), len(line))):
        if n < len(line):
            dist, k, h = line[n]
            for sign in (-1, 1):
                relay(dist, sign, k, h, True)
        if n < len(links):
            links[n][0](links[n][1])

    @pl.when(c == cz)
    def _():
        for k in range(2):
            at = spot(z % 2, 1 - c, k)
            remote(at, at, u_s.at[0, 0], u_r.at[z % 2, 1 - c, k], (d, z)).wait_recv()

    for dist, k, h in line:
        for sign in (-1, 1):
            relay(dist, sign, k, h, False)
    sends(0, True)
    sends(1, True)
    spread.sent()
    for k in range(n_d):
        for t in range(parts):
            across(k, t, c).wait_send()
            across(k, t, 1 - c).wait_recv()


def share_resid(part, x, w, n_dp, n_z):
    full, width = x.shape
    n_d = n_dp // 2
    return pl.pallas_call(
        functools.partial(share_resid_kernel, n_dp, n_z),
        in_specs=[VMEM_SPEC] * 3,
        out_specs=[ANY_SPEC] * 2,
        out_shape=[
            jax.ShapeDtypeStruct((2, full, width), jnp.bfloat16),
            jax.ShapeDtypeStruct((n_dp * w.shape[0], w.shape[1]), jnp.bfloat16),
        ],
        scratch_shapes=[
            pltpu.VMEM((full // 2, width), jnp.bfloat16), pltpu.VMEM((full // 2, width), jnp.bfloat16),
            DMA, DMA, DMA((5, 8)), DMA((2, 2, 2)), DMA((n_d - 1, 4, 2)), DMA((n_d - 1, 4, 2)), DMA((n_d, 4)), DMA((n_d, 4)),
            DMA((3,)),
        ],
        compiler_params=pltpu.CompilerParams(collective_id=2, has_side_effects=True),
        cost_estimate=pl.CostEstimate(flops=0, bytes_accessed=200_000_000, transcendentals=0),
        name="share_resid",
    )(part, x, w)


CHUNKS = 8
GROUPS = 4


def sum_line_kernel(n_z, d_gate_ref, d_up_ref, w_ref, resid_all, cot_all, gain_ref, hid_ref, down_ref, d_out, gain_out,
                    rows_out, left, w, part, got, buf, resid_ref, cot_ref, hid, down, rows_buf,
                    s_s, s_r, p_s, p_r, loc, rows_sem, mul_sem, out_sem, left_sem, w_sem):
    d, z, pair, c = place()
    cz = z // 2
    full, width = buf.shape
    inner = d_gate_ref.shape[1]
    rows = full // CHUNKS
    group = full // GROUPS
    per = CHUNKS // GROUPS
    tile = 256
    tiles = width // tile
    lefts = []
    for q in range(GROUPS):
        for jl in range(2):
            for n, src in enumerate((d_gate_ref, d_up_ref)):
                lefts.append(pltpu.make_async_copy(
                    src.at[pl.ds(jl * full + q * group, group)],
                    left.at[pl.ds((2 * q + jl) * group, group), pl.ds(n * inner, inner)],
                    left_sem.at[q, jl, n],
                ))

    def w_copy(n):
        at = pl.ds(pl.multiple_of(n * tile, tile), tile)
        return pltpu.make_async_copy(w_ref.at[at], w.at[at], w_sem.at[n])

    fetch = (
        pltpu.make_async_copy(resid_all.at[z % 2], resid_ref, rows_sem.at[0]),
        pltpu.make_async_copy(cot_all.at[z % 2], cot_ref, rows_sem.at[1]),
    )
    factors = (pltpu.make_async_copy(hid_ref, hid, mul_sem.at[0]), pltpu.make_async_copy(down_ref, down, mul_sem.at[1]))
    for one in lefts[:4]:
        one.start()
    for n in range(tiles):
        w_copy(n).start()
    for one in tuple(lefts[4:]) + factors + fetch:
        one.start()
    greet_line(n_z, d, z)
    gain_out[...] = jnp.zeros_like(gain_out)
    own = c == cz

    def compute(q, low, high):
        if low == 0:
            for one in lefts[4 * q : 4 * q + 4]:
                one.wait()

        def one_tile(n, carry):
            if q == 0:
                w_copy(n).wait()
            at = pl.ds(pl.multiple_of(n * tile, tile), tile)
            value = dot_t(left[pl.ds(2 * q * group, 2 * group)], w[at])
            part[pl.ds(2 * q * group, 2 * group), at] = value.astype(jnp.bfloat16)
            return carry

        lax.fori_loop(low, high, one_tile, 0)

    def tile_out(j):
        at = pl.ds(pl.multiple_of(j * tile, tile), tile)
        return pltpu.make_async_copy(rows_buf.at[lax.rem(j, 2)], rows_out.at[:, at], out_sem.at[lax.rem(j, 2)])

    def multiply(low, high):
        if low == 0:
            for one in factors:
                one.wait()

        def one_tile(j, carry):
            pl.when(j >= 2)(tile_out(j - 2).wait)
            at = pl.ds(pl.multiple_of(j * tile, tile), tile)
            rows_buf[lax.rem(j, 2)] = dot_n(hid[...], down[:, at]).astype(jnp.bfloat16)
            tile_out(j).start()
            return carry

        lax.fori_loop(low, high, one_tile, 0)

    def part_start(jl, k):
        return (2 * (k // per) + jl) * group + k % per * rows

    def part_at(jl, k, r):
        return pl.ds(pl.multiple_of(part_start(jl, k) + r * 16, 16), 16)

    def copy_on(k, t, side, src):
        jl = jnp.bitwise_xor(c, t)
        to = z + 1 if side == 0 else z - 1
        return remote(src, got.at[side, jl, pl.ds(k * rows, rows)], s_s.at[t, k], s_r.at[side, jl, k], (2 * pair + c, to))

    def arrived(side, jl, k):
        at = got.at[side, jl, pl.ds(k * rows, rows)]
        return remote(at, at, s_s.at[0, 0], s_r.at[side, jl, k], (d, z))

    def send_step(k, t, edge_only, inner_only, wait):
        jl = jnp.bitwise_xor(c, t)
        j = 2 * c + jl
        for side in range(2):
            going = (z < j) if side == 0 else (z > j)
            edge = (z == 0) if side == 0 else (z == n_z - 1)
            raw = copy_on(k, t, side, part.at[pl.ds(pl.multiple_of(part_start(jl, k), rows), rows)])
            passed = copy_on(k, t, side, got.at[side, jl, pl.ds(k * rows, rows)])
            if not inner_only:
                pl.when(going & edge)(raw.wait_send if wait else raw.start)
            if not edge_only:
                pl.when(going & jnp.logical_not(edge))(passed.wait_send if wait else passed.start)

    def add_in(side, jl, k):
        def one(r, carry):
            at = pl.ds(pl.multiple_of(k * rows + r * 16, 16), 16)
            got[side, jl, at] = (got[side, jl, at].astype(jnp.float32) + part[part_at(jl, k, r)].astype(jnp.float32)).astype(jnp.bfloat16)
            return carry

        lax.fori_loop(0, rows // 16, one, 0)

    def finish(jl, k):
        def one(r, carry):
            at = pl.ds(pl.multiple_of(k * rows + r * 16, 16), 16)
            total = part[part_at(jl, k, r)].astype(jnp.float32)
            low_side = got[0, jl, at].astype(jnp.float32)
            high_side = got[1, jl, at].astype(jnp.float32)
            total = total + jnp.where(z > 0, low_side, 0.0) + jnp.where(z < n_z - 1, high_side, 0.0)
            value = resid_ref[at].astype(jnp.float32)
            inverse = lax.rsqrt(jnp.mean(value * value, axis=-1, keepdims=True) + norm_eps)
            scaled = value * inverse
            d_scaled = total * gain_ref[...]
            mean = jnp.mean(d_scaled * scaled, axis=-1, keepdims=True)
            d_resid = cot_ref[at].astype(jnp.float32) + inverse * (d_scaled - scaled * mean)
            buf[at] = d_resid.astype(jnp.bfloat16)
            prod = total * scaled
            gain_out[...] = gain_out[...] + prod[:8] + prod[8:]
            return carry

        lax.fori_loop(0, rows // 16, one, 0)

    def to_partner(k):
        at = pl.ds(k * rows, rows)
        return remote(buf.at[at], d_out.at[at], p_s.at[k], p_r.at[k], (2 * pair + 1 - c, z))

    def keep(k):
        at = pl.ds(k * rows, rows)
        return pltpu.make_async_copy(buf.at[at], d_out.at[at], loc.at[k])

    def own_chunk(k):
        @pl.when(own)
        def _():
            jl = z % 2
            pl.when(z > 0)(arrived(0, jl, k).wait_recv)
            pl.when(z < n_z - 1)(arrived(1, jl, k).wait_recv)
            finish(jl, k)
            if k > 0:
                to_partner(k - 1).start()
                keep(k - 1).start()

    done = 0
    for q in range(GROUPS):
        compute(q, 0, 1)
        if q > 0:
            for k in range((q - 1) * per, q * per):
                for t in range(2):
                    send_step(k, t, True, False, False)
        compute(q, 1, tiles)
    multiply(done, done + 1)
    done += 1
    for k in range((GROUPS - 1) * per, CHUNKS):
        for t in range(2):
            send_step(k, t, True, False, False)
    for one in fetch:
        one.wait()

    steps = [(k, t) for k in range(CHUNKS) for t in range(2)]
    for n, (k, t) in enumerate(steps):
        jl = jnp.bitwise_xor(c, t)
        j = 2 * c + jl
        for side in range(2):
            going = (z < j) if side == 0 else (z > j)
            between = (z > 0) if side == 0 else (z < n_z - 1)

            @pl.when(going & between)
            def _():
                arrived(side, jl, k).wait_recv()
                add_in(side, jl, k)

        if n > 0:
            send_step(*steps[n - 1], False, True, False)
        if t == 0 and done < tiles:
            multiply(done, done + 1)
            done += 1
        if t == 1 and k > 0:
            own_chunk(k - 1)
    send_step(*steps[-1], False, True, False)
    own_chunk(CHUNKS - 1)
    if done < tiles:
        multiply(done, tiles)

    @pl.when(own)
    def _():
        to_partner(CHUNKS - 1).start()
        keep(CHUNKS - 1).start()

    for j in range(max(0, tiles - 2), tiles):
        tile_out(j).wait()
    for k, t in steps:
        send_step(k, t, False, False, True)
    for k in range(CHUNKS):
        at = d_out.at[pl.ds(k * rows, rows)]

        @pl.when(own)
        def _():
            to_partner(k).wait_send()
            keep(k).wait()

        pl.when(jnp.logical_not(own))(remote(at, at, p_s.at[k], p_r.at[k], (d, z)).wait_recv)


def sum_line(d_gate, d_up, w, resid, cot, gain, hidden, down, n_z):
    _, full, width = resid.shape
    b16 = jnp.bfloat16
    return pl.pallas_call(
        functools.partial(sum_line_kernel, n_z),
        in_specs=[ANY_SPEC] * 5 + [VMEM_SPEC] + [ANY_SPEC] * 2,
        out_specs=[ANY_SPEC, VMEM_SPEC, ANY_SPEC],
        out_shape=[
            jax.ShapeDtypeStruct((full, width), b16),
            jax.ShapeDtypeStruct((8, width), jnp.float32),
            jax.ShapeDtypeStruct((2 * full, width), b16),
        ],
        scratch_shapes=[
            pltpu.VMEM((2 * full, w.shape[1]), b16), pltpu.VMEM(w.shape, b16), pltpu.VMEM((2 * full, width), b16),
            pltpu.VMEM((2, 2, full, width), b16), pltpu.VMEM((full, width), b16),
            pltpu.VMEM((full, width), b16), pltpu.VMEM((full, width), b16),
            pltpu.VMEM(hidden.shape, b16), pltpu.VMEM(down.shape, b16), pltpu.VMEM((2, 2 * full, 256), b16),
            DMA((2, CHUNKS)), DMA((2, 2, CHUNKS)), DMA((CHUNKS,)), DMA((CHUNKS,)), DMA((CHUNKS,)), DMA((2,)), DMA((2,)), DMA((2,)),
            DMA((GROUPS, 2, 2)), DMA((width // 256,)),
        ],
        compiler_params=pltpu.CompilerParams(collective_id=3, has_side_effects=True, vmem_limit_bytes=63 * 1024 * 1024),
        cost_estimate=pl.CostEstimate(flops=0, bytes_accessed=200_000_000, transcendentals=0),
        name="sum_line",
    )(d_gate, d_up, w, resid, cot, gain, hidden, down)


WIDE_ROWS = 32
TURNED_ROWS = 512


def adam_wide_kernel(grad_ref, w_ref, m_ref, v_ref, g_out, w_out, m_out, v_out):
    width = w_ref.shape[-1]
    for n in range(2):
        grad = grad_ref[:, n * width : (n + 1) * width].astype(jnp.float32)
        weight, first, second = adam_update(w_ref[:, n], grad, m_ref[:, n], v_ref[:, n])
        g_out[:, n] = grad
        w_out[:, n] = weight
        m_out[:, n] = first
        v_out[:, n] = second


def adam_turned_kernel(grad_ref, w_ref, m_ref, v_ref, g_out, w_out, m_out, v_out):
    grad = grad_ref[...].astype(jnp.float32).T
    weight, first, second = adam_update(w_ref[...], grad, m_ref[...], v_ref[...])
    g_out[...] = grad
    w_out[...] = weight
    m_out[...] = first
    v_out[...] = second


def adam_call(kernel, grid, grad_spec, spec, arrays):
    shape = jax.ShapeDtypeStruct(arrays[1].shape, jnp.float32)
    return pl.pallas_call(
        kernel,
        grid=(grid,),
        in_specs=[grad_spec] + [spec] * 3,
        out_specs=[spec] * 4,
        out_shape=[shape] * 4,
        cost_estimate=pl.CostEstimate(flops=20 * shape.size, bytes_accessed=30 * shape.size, transcendentals=0),
    )(*arrays)


def adam_wide(*arrays):
    rows, _, width = arrays[1].shape
    return adam_call(
        adam_wide_kernel, rows // WIDE_ROWS,
        pl.BlockSpec((WIDE_ROWS, 2 * width), lambda i: (i, 0)),
        pl.BlockSpec((WIDE_ROWS, 2, width), lambda i: (i, 0, 0)),
        arrays,
    )


def adam_turned(*arrays):
    rows, cols = arrays[1].shape
    return adam_call(
        adam_turned_kernel, rows // TURNED_ROWS,
        pl.BlockSpec((cols, TURNED_ROWS), lambda i: (0, i)),
        pl.BlockSpec((TURNED_ROWS, cols), lambda i: (i, 0)),
        arrays,
    )


def hand_out_kernel(n_dp, n_z, dq_ref, n_ref, x_ref, dr_ref, gain_ref, gain2_ref, wq_ref, ot_ref, ig, gq, go, gains,
                    dn_ref, wq, got, buf, q_base, q_got, q_put, q_fin, o_base, o_got, o_put, o_fin, g_src, g_all,
                    p_s, p_r, i_s, i_r, q_s, q_r, qf_s, qf_r, o_s, o_r, of_s, of_r, g_s, g_r, loc):
    d, z, pair, c = place()
    n_d = n_dp // 2
    total = n_dp * n_z
    me = d * n_z + z
    cz = z // 2
    full, width = x_ref.shape
    half = full // 2
    quarter = half // 2
    q_rows, q_cols = q_fin.shape[1:]
    o_rows, o_cols = o_fin.shape[1:]
    relay = n_d == 4

    class First:
        def __init__(self, rows, cols, bufs, sems, spare):
            self.rows, self.cols, self.spare = rows, cols, spare
            self.base, self.got, self.put, self.fin = bufs
            self.send, self.recv, self.f_send, self.f_recv = sems

        def block(self, ref, b, core):
            return ref.at[pl.ds(core * self.rows, self.rows), pl.ds(b * self.cols, self.cols)]

        def source(self, owner, b, core):
            return self.base.at[pl.ds(pl.multiple_of((2 * owner + core) * self.rows, self.rows), self.rows), pl.ds(b * self.cols, self.cols)]

        def cut_of(self, owner, b, core, r):
            start = (2 * owner + core) * self.rows + r * 16
            return pl.ds(pl.multiple_of(start, 16), 16), pl.ds(b * self.cols, self.cols)

        def copy(self, n, b, core, owner, to):
            return remote(self.source(owner, b, core), self.block(self.got.at[n], b, core), self.send.at[n, b, core],
                          self.recv.at[n, b, core], (2 * (pair ^ to) + c, z))

        def begin(self, core):
            for b in range(2):
                if relay:
                    self.copy(1, b, core, pair ^ 3, 1 + b).start()
            for b in range(2):
                if relay:
                    self.copy(0, b, core, pair ^ (1 + b), 1 + b).start()
                else:
                    for k in range(1, n_d):
                        self.copy(k - 1, b, core, pair ^ k, k).start()

        def arrived(self, n, b, core):
            at = self.block(self.got.at[n], b, core)
            remote(at, at, self.send.at[n, b, core], self.recv.at[n, b, core], (d, z)).wait_recv()

        def cut(self, b, core, r):
            return pl.ds(pl.multiple_of(core * self.rows + r * 16, 16), 16), pl.ds(b * self.cols, self.cols)

        def middle_copy(self, b, core):
            return remote(self.source(pair ^ (2 >> b), b, core), self.block(self.got.at[2], b, core), self.send.at[2, b, core],
                          self.recv.at[2, b, core], (2 * (pair ^ (2 >> b)) + c, z))

        def middle(self, core, between):
            if not relay:
                return
            for b in range(2):
                self.arrived(1, b, core)

                def add(r, carry):
                    at = self.cut(b, core, r)
                    mid = self.cut_of(pair ^ (2 >> b), b, core, r)
                    self.base[mid] = (self.base[mid].astype(jnp.float32) + self.got[(1,) + at].astype(jnp.float32)).astype(jnp.bfloat16)
                    return carry

                lax.fori_loop(0, self.rows // 16, add, 0)
            self.middle_copy(0, core).start()
            between()
            self.middle_copy(1, core).start()

        def total(self, core, between):
            slots = (0, 2) if relay else range(n_d - 1)
            for b in range(2):
                for n in slots:
                    self.arrived(n, b, core)

                def add(r, carry):
                    at = self.cut(b, core, r)
                    value = self.base[self.cut_of(pair, b, core, r)].astype(jnp.float32)
                    for n in slots:
                        value = value + self.got[(n,) + at].astype(jnp.float32)
                    self.put[core, b, pl.ds(pl.multiple_of(r * 16, 16), 16)] = value.astype(jnp.bfloat16)
                    return carry

                lax.fori_loop(0, self.rows // 16, add, 0)
            self.second(0, core, False)
            between()
            self.second(1, core, False)

        def second(self, b, core, wait):
            here = (core == c) & (2 * c + b == z)
            src = self.put.at[core, b]
            copy = remote(src, self.fin.at[z], self.f_send.at[core, b], self.f_recv.at[z], (2 * pair + core, 2 * c + b))
            keep = pltpu.make_async_copy(src, self.fin.at[z], loc.at[self.spare])
            pl.when(jnp.logical_not(here))(copy.wait_send if wait else copy.start)
            pl.when(here)(keep.wait if wait else keep.start)

        def final(self):
            for core in range(2):
                for b in range(2):
                    self.second(b, core, True)
            for zs in range(n_z):
                at = self.fin.at[zs]
                from_here = (cz == c) & (zs == z)
                pl.when(jnp.logical_not(from_here))(remote(at, at, self.f_send.at[0, 0], self.f_recv.at[zs], (d, z)).wait_recv)

        def sent(self):
            for b in range(2):
                for core in range(2):
                    for n in range(n_d - 1):
                        at = self.block(self.got.at[n], b, core)
                        remote(at, at, self.send.at[n, b, core], self.recv.at[n, b, core], (d, z)).wait_send()

    o_first = First(o_rows, o_cols, (o_base, o_got, o_put, o_fin), (o_s, o_r, of_s, of_r), 2)
    q_first = First(q_rows, q_cols, (q_base, q_got, q_put, q_fin), (q_s, q_r, qf_s, qf_r), 3)
    o_load = pltpu.make_async_copy(ot_ref, o_base, loc.at[4])
    wq_load = pltpu.make_async_copy(wq_ref, wq, loc.at[5])
    o_load.start()
    wq_load.start()
    greet_all(n_dp, n_z, d, z)
    o_load.wait()
    o_first.begin(0)
    o_first.begin(1)
    nothing = lambda: None

    def q_blocks(core):
        def one(k, carry):
            owner = pair ^ (n_d - 1 - k)
            rows_at = pl.ds(pl.multiple_of((2 * owner + core) * q_rows, q_rows), q_rows)
            q_base[rows_at] = dot_c(n_ref[:, rows_at], dq_ref[...]).astype(jnp.bfloat16)
            return carry

        lax.fori_loop(0, n_d, one, 0)

    def dn_blocks(low, high):
        def one(r, carry):
            rows_at = pl.ds(pl.multiple_of(r * 256, 256), 256)
            dn_ref[:, rows_at] = dot_t(dq_ref[...], wq[rows_at]).astype(jnp.bfloat16)
            return carry

        lax.fori_loop(low, high, one, 0)

    q_blocks(0)
    o_first.middle(0, lambda: q_blocks(1))
    q_first.begin(0)
    wq_load.wait()
    dn_tiles = width // 256
    dn_blocks(0, dn_tiles // 2)
    o_first.middle(1, nothing)
    q_first.begin(1)
    dn_blocks(dn_tiles // 2, dn_tiles)
    mine = pl.ds(pl.multiple_of(c * half, half), half)
    theirs = pl.ds(pl.multiple_of((1 - c) * half, half), half)
    swap = remote(dn_ref.at[theirs], got, p_s, p_r, (2 * pair + 1 - c, z))
    o_first.total(0, nothing)
    swap.start()

    g_src[pl.ds(0, 8)] = jnp.zeros((8, width), jnp.float32)
    g_src[pl.ds(8, 8)] = gain2_ref[...]
    swap.wait_recv()

    def rows_of(r, carry):
        at = pl.ds(pl.multiple_of(r * 16, 16), 16)
        src = pl.ds(pl.multiple_of(c * half + r * 16, 16), 16)
        d_normed = dn_ref[src].astype(jnp.float32) + got[at].astype(jnp.float32)
        value = x_ref[src].astype(jnp.float32)
        inverse = lax.rsqrt(jnp.mean(value * value, axis=-1, keepdims=True) + norm_eps)
        scaled = value * inverse
        d_scaled = d_normed * gain_ref[...]
        mean = jnp.mean(d_scaled * scaled, axis=-1, keepdims=True)
        out = dr_ref[src].astype(jnp.float32) + inverse * (d_scaled - scaled * mean)
        buf[at] = out.astype(jnp.bfloat16)
        prod = d_normed * scaled
        g_src[pl.ds(0, 8)] = g_src[pl.ds(0, 8)] + prod[:8] + prod[8:]
        return carry

    def row_send(b, wait):
        src = buf.at[pl.ds(b * quarter, quarter)]
        dst = ig.at[z % 2]
        zz = 2 * c + b
        here = (cz == c) & (zz == z)
        copy = remote(src, dst, i_s.at[b], i_r.at[z % 2], (2 * pair + cz, zz))
        keep = pltpu.make_async_copy(src, dst, loc.at[0])
        pl.when(jnp.logical_not(here))(copy.wait_send if wait else copy.start)
        pl.when(here)(keep.wait if wait else keep.start)

    q_first.middle(0, nothing)
    per = quarter // 16
    lax.fori_loop(0, per, rows_of, 0)
    o_first.total(1, lambda: row_send(0, False))
    lax.fori_loop(per, 2 * per, rows_of, 0)
    q_first.middle(1, lambda: row_send(1, False))

    each = width // total

    def gain_tile(o):
        return g_src.at[:, pl.ds(pl.multiple_of(o * each // 128 * 128, 128), 128)]

    own_gain = pltpu.make_async_copy(gain_tile(me), g_all.at[me], loc.at[1])
    own_gain.start()

    def send_gain(o, carry):
        other = lax.rem(me + o, total)
        remote(gain_tile(other), g_all.at[me], g_s, g_r, (other // n_z, lax.rem(other, n_z))).start()
        return carry

    lax.fori_loop(1, total, send_gain, 0)

    q_first.total(0, nothing)
    q_first.total(1, nothing)

    o_first.final()
    value = o_fin[0].astype(jnp.float32)
    for zs in range(1, n_z):
        value = value + o_fin[zs].astype(jnp.float32)
    go[...] = value.T

    many = g_all.at[pl.ds(0, total - 1)]
    gain_copy = remote(many, many, g_s, g_r, (d, z))
    gain_copy.wait_send()
    gain_copy.wait_recv()
    own_gain.wait()
    gains[...] = jnp.zeros_like(gains)

    def add_gain(o, carry):
        gains[...] = gains[...] + g_all[o]
        return carry

    lax.fori_loop(0, total, add_gain, 0)

    swap.wait_send()
    for b in range(2):
        row_send(b, True)
    for i in range(2):
        from_here = (cz == c) & (2 * c + i == z)
        at = ig.at[i]
        pl.when(jnp.logical_not(from_here))(remote(at, at, i_s.at[0], i_r.at[i], (d, z)).wait_recv)
    o_first.sent()
    q_first.sent()
    q_first.final()

    def last(r, carry):
        at = pl.ds(pl.multiple_of(r * 16, 16), 16)
        value = q_fin[0, at].astype(jnp.float32)
        for zs in range(1, n_z):
            value = value + q_fin[zs, at].astype(jnp.float32)
        gq[at] = value
        return carry

    lax.fori_loop(0, q_rows // 16, last, 0)


def hand_out(dq, normed, x, dr, gain, gain2, wq, ot, n_dp, n_z):
    full, width = x.shape
    n_d = n_dp // 2
    total = n_dp * n_z
    q_rows, q_cols = wq.shape[0] // n_dp, wq.shape[1] // 2
    o_rows, o_cols = ot.shape[0] // n_dp, ot.shape[1] // 2
    b16 = jnp.bfloat16
    f32 = jnp.float32

    def weight_bufs(rows, cols):
        return [
            pltpu.VMEM((n_dp * rows, 2 * cols), b16), pltpu.VMEM((n_d - 1, 2 * rows, 2 * cols), b16),
            pltpu.VMEM((2, 2, rows, cols), b16), pltpu.VMEM((n_z, rows, cols), b16),
        ]

    weight_sems = [DMA((n_d - 1, 2, 2)), DMA((n_d - 1, 2, 2)), DMA((2, 2)), DMA((n_z,))]
    return pl.pallas_call(
        functools.partial(hand_out_kernel, n_dp, n_z),
        in_specs=[VMEM_SPEC] * 6 + [ANY_SPEC] * 2,
        out_specs=[ANY_SPEC] + [VMEM_SPEC] * 3,
        out_shape=[
            jax.ShapeDtypeStruct((2, full // 4, width), b16),
            jax.ShapeDtypeStruct((q_rows, q_cols), f32),
            jax.ShapeDtypeStruct((o_cols, o_rows), f32),
            jax.ShapeDtypeStruct((16, 128), f32),
        ],
        scratch_shapes=[
            pltpu.VMEM((full, width), b16), pltpu.VMEM(wq.shape, b16),
            pltpu.VMEM((full // 2, width), b16), pltpu.VMEM((full // 2, width), b16),
            *weight_bufs(q_rows, q_cols), *weight_bufs(o_rows, o_cols),
            pltpu.VMEM((16, width), f32), pltpu.VMEM((total, 16, 128), f32),
            DMA, DMA, DMA((2,)), DMA((2,)), *weight_sems, *weight_sems, DMA, DMA,
            DMA((6,)),
        ],
        compiler_params=pltpu.CompilerParams(collective_id=5, has_side_effects=True, vmem_limit_bytes=58 * 1024 * 1024),
        cost_estimate=pl.CostEstimate(flops=0, bytes_accessed=300_000_000, transcendentals=0),
        name="hand_out",
    )(dq, normed, x, dr, gain, gain2, wq, ot)


def rms_forward(values, gain_wide):
    inverse = lax.rsqrt(jnp.mean(values * values, axis=-1, keepdims=True) + norm_eps)
    scaled = values * inverse
    return (scaled, inverse, (scaled * gain_wide).astype(jnp.bfloat16))


def adam_update(weight, grad, first, second):
    new_first = beta_one * first + (1.0 - beta_one) * grad
    new_second = beta_two * second + (1.0 - beta_two) * grad * grad
    first_hat = new_first / (1.0 - beta_one**step_count)
    second_hat = new_second / (1.0 - beta_two**step_count)
    new_weight = weight - learn_rate * (
        first_hat / (jnp.sqrt(second_hat) + adam_eps) + weight_decay * weight
    )
    return (new_weight, new_first, new_second)


def contract_rows(left, right):
    return lax.dot_general(
        left, right, (((0,), (0,)), ((), ())), preferred_element_type=jnp.float32
    )


def times_transpose(left, right):
    return lax.dot_general(
        left, right, (((1,), (1,)), ((), ())), preferred_element_type=jnp.float32
    )


def layer_step(
    block_input,
    segment_ids,
    cotangent,
    attn_gain,
    qkv_weight,
    out_weight,
    mlp_gain,
    gate_up_weight,
    down_weight,
    first_attn_gain,
    first_qkv,
    first_out,
    first_mlp_gain,
    first_gate_up,
    first_down,
    second_attn_gain,
    second_qkv,
    second_out,
    second_mlp_gain,
    second_gate_up,
    second_down,
):
    seqs_here, local_len, width = block_input.shape
    full_len = segment_ids.shape[1]
    n_dp = lax.axis_size("dp")
    n_z = lax.axis_size("seq")
    groups = HEADS // KV_HEADS
    unit_count = down_weight.shape[0]
    z_here = lax.axis_index("seq")
    owned = attn_gain.shape[0]
    gain_line = jnp.concatenate([attn_gain, mlp_gain]).astype(jnp.bfloat16).astype(jnp.float32)
    gain_tile = jnp.pad(gain_line[None], ((0, 7), (0, LANES - 2 * owned)))
    seg_tile = jnp.pad(segment_ids, ((0, 8 - seqs_here), (0, 0)))
    down_rows = lax.all_gather(down_weight.astype(jnp.bfloat16), "dp", axis=1, tiled=True)
    rows_in, qkv_cols, out_line, gain_all, seg_all, gate_up_here = gather_in(
        block_input,
        qkv_weight.astype(jnp.bfloat16),
        out_weight.astype(jnp.bfloat16).T,
        gain_tile,
        seg_tile,
        gate_up_weight,
        n_dp,
        n_z,
    )
    cot_late, _ = lax.optimization_barrier((cotangent, gain_all))
    cot_all = lax.all_gather(cot_late, "seq", axis=1, tiled=True)
    gain_one = gain_all[:, 0, :owned].reshape(1, width)
    gain_two = gain_all[:, 0, owned : 2 * owned].reshape(1, width)
    seg_here = lax.dynamic_slice(seg_all, (z_here // 2, z_here % 2, 0), (1, 1, full_len))[0]
    tables = attn_tables(seg_here)
    _, _, normed_one = rms_forward(rows_in.astype(jnp.float32), gain_one)
    qkv = jnp.dot(normed_one, qkv_cols, preferred_element_type=jnp.float32)
    turned, lse, attended16, out_rows = attn_forward(qkv, *tables, out_line, full_len, groups, n_dp)
    attn_part = times_transpose(attended16, out_rows)
    resid_all, gate_up_cols = share_resid(
        attn_part.astype(jnp.bfloat16), rows_in, gate_up_here, n_dp, n_z
    )
    total_rows = seqs_here * full_len
    resid = resid_all.reshape(total_rows, width).astype(jnp.float32)
    _, _, normed_two = rms_forward(resid, gain_two)
    gate_up = jnp.dot(normed_two, gate_up_cols, preferred_element_type=jnp.float32)
    gate_part = gate_up[:, :unit_count]
    up_part = gate_up[:, unit_count:]
    sigmoid_gate = jax.nn.sigmoid(gate_part)
    active = gate_part * sigmoid_gate
    hidden16 = (active * up_part).astype(jnp.bfloat16)
    cot_rows = cot_all.reshape(total_rows, width)
    d_hidden = times_transpose(cot_rows, down_rows)
    d_gate = d_hidden * up_part * sigmoid_gate * (1.0 + gate_part * (1.0 - sigmoid_gate))
    d_up = d_hidden * active
    d_gate16 = d_gate.astype(jnp.bfloat16)
    d_up16 = d_up.astype(jnp.bfloat16)
    d_gate_up16 = jnp.concatenate([d_gate16, d_up16], 1)
    gate_up_term = contract_rows(normed_two, d_gate_up16).astype(jnp.bfloat16)
    gate_up_sum = lax.psum_scatter(gate_up_term, "dp", scatter_dimension=0, tiled=True)
    down_term = contract_rows(cot_rows, hidden16).astype(jnp.bfloat16)
    down_sum = lax.psum_scatter(down_term, "dp", scatter_dimension=0, tiled=True)
    d_resid16, gain_two_part, down_part = sum_line(
        d_gate16, d_up16, gate_up_cols, resid_all, cot_all, gain_two, hidden16, down_rows, n_z
    )
    down16 = down_part.reshape(resid_all.shape)
    pieces = [
        lax.dynamic_slice_in_dim(down16, (z_here + o) % n_z * local_len, local_len, 1)
        for o in range(n_z)
    ]
    for o in range(1, n_z):
        pieces[o] = lax.ppermute(pieces[o], "seq", [(i, (i + o) % n_z) for i in range(n_z)])
    down_here = sum(piece.astype(jnp.float32) for piece in pieces)
    resid_here = lax.dynamic_slice_in_dim(resid_all, z_here * local_len, local_len, 1)
    output = (resid_here.astype(jnp.float32) + down_here).astype(jnp.bfloat16)
    d_attended = jnp.dot(d_resid16, out_rows, preferred_element_type=jnp.float32).astype(jnp.bfloat16)
    d_qkv16 = attn_backward(turned, d_attended, lse, *tables, full_len, groups)
    out_term = contract_rows(d_resid16, attended16).astype(jnp.bfloat16)
    input_grad, grad_qkv, grad_out, gain_sums = hand_out(
        d_qkv16,
        normed_one,
        rows_in,
        d_resid16,
        gain_one,
        gain_two_part,
        qkv_cols,
        out_term,
        n_dp,
        n_z,
    )
    grad_gate_up, w_gu, m_gu, v_gu = adam_wide(
        gate_up_sum, gate_up_weight, first_gate_up, second_gate_up
    )
    grad_down, w_down, m_down, v_down = adam_turned(
        down_sum, down_weight, first_down, second_down
    )
    flat = lax.axis_index("dp") * n_z + z_here
    gain_sums = lax.dynamic_slice(
        jnp.sum(gain_sums.reshape(2, 8, LANES), axis=1), (0, flat * owned % LANES), (2, owned)
    )
    grad_gain_one = gain_sums[0]
    grad_gain_two = gain_sums[1]
    w_one, m_one, v_one = adam_update(attn_gain, grad_gain_one, first_attn_gain, second_attn_gain)
    w_qkv, m_qkv, v_qkv = adam_update(qkv_weight, grad_qkv, first_qkv, second_qkv)
    w_out, m_out, v_out = adam_update(out_weight, grad_out, first_out, second_out)
    w_two, m_two, v_two = adam_update(mlp_gain, grad_gain_two, first_mlp_gain, second_mlp_gain)
    return (
        output,
        input_grad,
        grad_gain_one,
        grad_qkv,
        grad_out,
        grad_gain_two,
        grad_gate_up,
        grad_down,
        w_one,
        w_qkv,
        w_out,
        w_two,
        w_gu,
        w_down,
        m_one,
        m_qkv,
        m_out,
        m_two,
        m_gu,
        m_down,
        v_one,
        v_qkv,
        v_out,
        v_two,
        v_gu,
        v_down,
    )


def solution(mesh):
    in_specs = (
        P("dp", "seq", None),
        P("dp", None),
        P("dp", "seq", None),
        P(("dp", "seq")),
        P("dp", "seq"),
        P("seq", "dp"),
        P(("dp", "seq")),
        P("dp", None, "seq"),
        P("seq", "dp"),
        P(("dp", "seq")),
        P("dp", "seq"),
        P("seq", "dp"),
        P(("dp", "seq")),
        P("dp", None, "seq"),
        P("seq", "dp"),
        P(("dp", "seq")),
        P("dp", "seq"),
        P("seq", "dp"),
        P(("dp", "seq")),
        P("dp", None, "seq"),
        P("seq", "dp"),
    )
    out_specs = (
        P("dp", "seq", None),
        P("dp", "seq", None),
        P(("dp", "seq")),
        P("dp", "seq"),
        P("seq", "dp"),
        P(("dp", "seq")),
        P("dp", None, "seq"),
        P("seq", "dp"),
        P(("dp", "seq")),
        P("dp", "seq"),
        P("seq", "dp"),
        P(("dp", "seq")),
        P("dp", None, "seq"),
        P("seq", "dp"),
        P(("dp", "seq")),
        P("dp", "seq"),
        P("seq", "dp"),
        P(("dp", "seq")),
        P("dp", None, "seq"),
        P("seq", "dp"),
        P(("dp", "seq")),
        P("dp", "seq"),
        P("seq", "dp"),
        P(("dp", "seq")),
        P("dp", None, "seq"),
        P("seq", "dp"),
    )
    return jax.shard_map(layer_step, mesh=mesh, in_specs=in_specs, out_specs=out_specs, check_vma=False)
```

```python
import functools

import jax
import jax.numpy as jnp
from jax import lax
from jax.experimental import pallas as pl
from jax.experimental.pallas import tpu as pltpu
from jax.sharding import PartitionSpec as P


HEADS = 32
KV_HEADS = 8
norm_eps = 1e-05
beta_one = 0.9
beta_two = 0.95
learn_rate = 0.01
weight_decay = 0.1
adam_eps = 1e-08
step_count = 10.0
masked_score = -1e30


HEAD_DIM = 64
LANES = 128


def dot_t(a, b):
    return lax.dot_general(a, b, (((1,), (1,)), ((), ())), preferred_element_type=jnp.float32)


def dot_n(a, b):
    return lax.dot_general(a, b, (((1,), (0,)), ((), ())), preferred_element_type=jnp.float32)


def dot_c(a, b):
    return lax.dot_general(a, b, (((0,), (0,)), ((), ())), preferred_element_type=jnp.float32)


def swap_halves(u):
    lane = lax.broadcasted_iota(jnp.int32, u.shape, 1)
    return jnp.where(lane % 64 < 32, pltpu.roll(u, 96, 1), pltpu.roll(u, 32, 1))


def turn(u, cos_wide, sin_wide):
    return u * cos_wide + swap_halves(u) * sin_wide


def key_start(block, q_rows, reach):
    return max(0, (block * q_rows - reach + 1) // q_rows * q_rows)


def attn_forward_kernel(pairs, q_rows, reach, qkv_ref, cos_ref, sin_ref, seg_col_ref, seg_row_ref,
                        turned_ref, lse_ref, out_ref):
    full_len = qkv_ref.shape[0]
    lane = lax.broadcasted_iota(jnp.int32, (full_len, LANES), 1)
    low = lane < HEAD_DIM
    cos_q = cos_ref[...]
    sin_q = sin_ref[...]
    kv = qkv_ref[:, pairs * LANES:].astype(jnp.float32)
    kv16 = turn(kv, jnp.where(low, cos_q, 1.0), jnp.where(low, sin_q, 0.0)).astype(jnp.bfloat16)
    turned_ref[:, pairs * LANES:] = kv16
    kv32 = kv16.astype(jnp.float32)
    rolled = pltpu.roll(kv32, HEAD_DIM, 1)
    zero = jnp.zeros_like(kv32)
    keys = (jnp.where(low, kv32, zero).astype(jnp.bfloat16), jnp.where(low, zero, rolled).astype(jnp.bfloat16))
    vals = (jnp.where(low, rolled, zero).astype(jnp.bfloat16), jnp.where(low, zero, kv32).astype(jnp.bfloat16))
    for pair in range(pairs):
        cols = slice(pair * LANES, (pair + 1) * LANES)
        query = turn(qkv_ref[:, cols].astype(jnp.float32), cos_q, sin_q) .astype(jnp.bfloat16)
        turned_ref[:, cols] = query
    for block in range(full_len // q_rows):
        first = key_start(block, q_rows, reach)
        last = (block + 1) * q_rows
        rows = slice(block * q_rows, last)
        span = slice(first, last)
        i = lax.broadcasted_iota(jnp.int32, (q_rows, last - first), 0) + block * q_rows
        j = lax.broadcasted_iota(jnp.int32, (q_rows, last - first), 1) + first
        allowed = (j <= i) & (seg_col_ref[rows, :1] == seg_row_ref[:1, span])
        for pair in range(pairs):
            cols = slice(pair * LANES, (pair + 1) * LANES)
            query = turned_ref[rows, cols]
            total = None
            for half in range(2):
                scores = dot_t(query, keys[half][span]) * (HEAD_DIM ** -0.5)
                scores = jnp.where(allowed, scores, masked_score)
                top = jnp.max(scores, axis=1, keepdims=True)
                lse = top + jnp.log(jnp.sum(jnp.exp(scores - top), axis=1, keepdims=True))
                probs = jnp.exp(scores - lse).astype(jnp.bfloat16)
                part = dot_n(probs, vals[half][span])
                total = part if total is None else total + part
                head = 2 * pair + half
                lse_ref[rows, head:head + 1] = lse
            out_ref[rows, cols] = total.astype(jnp.bfloat16)


def attn_backward_kernel(pairs, q_rows, reach, turned_ref, d_out_ref, lse_ref, cos_ref, sin_ref, seg_col_ref,
                         seg_row_ref, grad_ref, dk_ref, dv_ref):
    full_len = turned_ref.shape[0]
    lane = lax.broadcasted_iota(jnp.int32, (full_len, LANES), 1)
    low = lane < HEAD_DIM
    kv32 = turned_ref[:, pairs * LANES:].astype(jnp.float32)
    rolled = pltpu.roll(kv32, HEAD_DIM, 1)
    zero = jnp.zeros_like(kv32)
    keys = (jnp.where(low, kv32, zero).astype(jnp.bfloat16), jnp.where(low, zero, rolled).astype(jnp.bfloat16))
    vals = (jnp.where(low, rolled, zero).astype(jnp.bfloat16), jnp.where(low, zero, kv32).astype(jnp.bfloat16))
    dk_ref[...] = jnp.zeros_like(dk_ref)
    dv_ref[...] = jnp.zeros_like(dv_ref)
    low_rows = low[:q_rows]
    scale = HEAD_DIM ** -0.5
    for block in range(full_len // q_rows):
        first = key_start(block, q_rows, reach)
        last = (block + 1) * q_rows
        rows = slice(block * q_rows, last)
        span = slice(first, last)
        i = lax.broadcasted_iota(jnp.int32, (q_rows, last - first), 0) + block * q_rows
        j = lax.broadcasted_iota(jnp.int32, (q_rows, last - first), 1) + first
        allowed = (j <= i) & (seg_col_ref[rows, :1] == seg_row_ref[:1, span])
        cos_q = cos_ref[rows]
        sin_q = sin_ref[rows]
        for pair in range(pairs):
            cols = slice(pair * LANES, (pair + 1) * LANES)
            query = turned_ref[rows, cols]
            d_out = d_out_ref[rows, cols]
            q32 = query.astype(jnp.float32)
            o32 = d_out.astype(jnp.float32)
            d_query = None
            d_key = None
            d_val = None
            for half in range(2):
                keep = low_rows if half == 0 else ~low_rows
                q_only = jnp.where(keep, q32, 0.0).astype(jnp.bfloat16)
                o_only = jnp.where(keep, o32, 0.0).astype(jnp.bfloat16)
                head = 2 * pair + half
                scores = dot_t(query, keys[half][span]) * scale
                scores = jnp.where(allowed, scores, masked_score)
                probs = jnp.exp(scores - lse_ref[rows, head:head + 1])
                d_probs = dot_t(d_out, vals[half][span])
                delta = jnp.sum(probs * d_probs, axis=1, keepdims=True)
                d_scores = (probs * (d_probs - delta) * scale).astype(jnp.bfloat16)
                probs16 = probs.astype(jnp.bfloat16)
                dq = dot_n(d_scores, keys[half][span])
                dk = dot_c(d_scores, q_only)
                dv = dot_c(probs16, o_only)
                d_query = dq if d_query is None else d_query + dq
                d_key = dk if d_key is None else d_key + dk
                d_val = dv if d_val is None else d_val + dv
            dk_ref[span] = dk_ref[span] + d_key
            dv_ref[span] = dv_ref[span] + d_val
            grad_ref[rows, cols] = turn(d_query, cos_q, -sin_q).astype(jnp.bfloat16)
    d_key = dk_ref[...]
    d_val = dv_ref[...]
    d_key = d_key + pltpu.roll(d_key, HEAD_DIM, 1)
    d_val = d_val + pltpu.roll(d_val, HEAD_DIM, 1)
    d_key = turn(d_key, cos_ref[...], -sin_ref[...])
    grad_ref[:, pairs * LANES:] = jnp.where(low, d_key, d_val).astype(jnp.bfloat16)


def attn_specs(full_len, width):
    line = pl.BlockSpec((full_len, width), lambda s, g: (s, g))
    table = pl.BlockSpec((full_len, LANES), lambda s, g: (s, 0))
    row = pl.BlockSpec((8, full_len), lambda s, g: (s, 0))
    return line, table, row


Q_ROWS = 128
REACH = 256


def attn_gather_kernel(n_dp, pairs, q_rows, reach, qkv_ref, cos_ref, sin_ref, seg_col_ref, seg_row_ref, vo_ref,
                       turned_ref, lse_ref, out_ref, wo, d_s, d_r, loc):
    _, z, pair, c = place()
    n_d = n_dp // 2
    step = pl.program_id(1)
    steps = pl.num_programs(1)
    rows = vo_ref.shape[0]
    parts = 2
    part = rows // parts // 2

    def spot(owner, t, h):
        return wo.at[pl.ds(pl.multiple_of(owner * rows + (2 * t + h) * part, part), part)]

    spread = Spread(n_d, pair, c, z, parts, spot, d_s, d_r)
    keep = pltpu.make_async_copy(vo_ref, wo.at[pl.ds(pl.multiple_of(pair * rows, rows), rows)], loc)

    @pl.when(step == 0)
    def _():
        keep.start()
        barrier = pltpu.get_barrier_semaphore()
        for k in range(1, n_d):
            pl.semaphore_signal(barrier, inc=1, device_id=(2 * (pair ^ k) + c, z), device_id_type=MESH)
        pl.semaphore_wait(barrier, n_d - 1)
        keep.wait()
        for t in range(parts):
            spread.own(t)

    attn_forward_kernel(pairs, q_rows, reach, qkv_ref, cos_ref, sin_ref, seg_col_ref, seg_row_ref, turned_ref, lse_ref, out_ref)

    @pl.when(step == steps - 2)
    def _():
        spread.pass_on(0)

    @pl.when(step == steps - 1)
    def _():
        spread.pass_on(1)
        spread.finish()


def attn_forward(qkv, cos, sin, seg_col, seg_row, vo, full_len, groups, n_dp):
    pairs = groups // 2
    width = (groups + 2) * HEAD_DIM
    seqs = qkv.shape[0] // full_len
    kv = qkv.shape[1] // width
    n_d = n_dp // 2
    line, table, row = attn_specs(full_len, width)
    outw = pl.BlockSpec((full_len, groups * HEAD_DIM), lambda s, g: (s, g))
    rows = seqs * full_len
    return pl.pallas_call(
        functools.partial(attn_gather_kernel, n_dp, pairs, Q_ROWS, REACH),
        grid=(seqs, kv),
        in_specs=[line, table, table, table, row, VMEM_SPEC],
        out_specs=[line, pl.BlockSpec((full_len, LANES), lambda s, g: (s, g)), outw, ANY_SPEC],
        out_shape=[
            jax.ShapeDtypeStruct((rows, kv * width), jnp.bfloat16),
            jax.ShapeDtypeStruct((rows, kv * LANES), jnp.float32),
            jax.ShapeDtypeStruct((rows, kv * groups * HEAD_DIM), jnp.bfloat16),
            jax.ShapeDtypeStruct((n_d * vo.shape[0], vo.shape[1]), jnp.bfloat16),
        ],
        scratch_shapes=[DMA((n_d - 1, 2, 2)), DMA((n_d - 1, 2, 2)), DMA],
        compiler_params=pltpu.CompilerParams(collective_id=4, has_side_effects=True),
        cost_estimate=pl.CostEstimate(flops=4 * rows * full_len * kv * LANES * groups, bytes_accessed=150_000_000, transcendentals=0),
        name="attn_forward",
    )(qkv, cos, sin, seg_col, seg_row, vo)


def attn_backward(turned, d_out, lse, cos, sin, seg_col, seg_row, full_len, groups):
    pairs = groups // 2
    width = (groups + 2) * HEAD_DIM
    seqs = turned.shape[0] // full_len
    kv = turned.shape[1] // width
    line, table, row = attn_specs(full_len, width)
    outw = pl.BlockSpec((full_len, groups * HEAD_DIM), lambda s, g: (s, g))
    rows = seqs * full_len
    return pl.pallas_call(
        functools.partial(attn_backward_kernel, pairs, Q_ROWS, REACH),
        grid=(seqs, kv),
        in_specs=[line, outw, pl.BlockSpec((full_len, LANES), lambda s, g: (s, g)), table, table, table, row],
        out_specs=line,
        out_shape=jax.ShapeDtypeStruct((rows, kv * width), jnp.bfloat16),
        scratch_shapes=[pltpu.VMEM((full_len, LANES), jnp.float32)] * 2,
        cost_estimate=pl.CostEstimate(flops=10 * rows * full_len * kv * LANES * groups, bytes_accessed=rows * kv * width * 6, transcendentals=0),
        name="attn_backward",
    )(turned, d_out, lse, cos, sin, seg_col, seg_row)


def attn_tables(segment_ids):
    seqs, full_len = segment_ids.shape
    earlier = (segment_ids[..., None, :] < segment_ids[..., :, None]).astype(jnp.int32)
    positions = jnp.arange(full_len, dtype=jnp.int32) - jnp.sum(earlier, axis=-1, dtype=jnp.int32)
    inverse = 500000.0 ** (-2.0 * jnp.arange(HEAD_DIM // 2, dtype=jnp.float32) / HEAD_DIM)
    angles = positions.astype(jnp.float32)[..., None] * inverse
    cos = jnp.cos(angles)
    sin = jnp.sin(angles)
    cos = jnp.concatenate([cos] * 4, -1).reshape(seqs * full_len, LANES)
    sin = jnp.concatenate([-sin, sin] * 2, -1).reshape(seqs * full_len, LANES)
    seg_col = jnp.broadcast_to(segment_ids[:, :, None], (seqs, full_len, LANES)).reshape(seqs * full_len, LANES)
    seg_row = jnp.broadcast_to(segment_ids[:, None, :], (seqs, 8, full_len)).reshape(seqs * 8, full_len)
    return cos, sin, seg_col, seg_row


MESH = pl.DeviceIdType.MESH
VMEM_SPEC = pl.BlockSpec(memory_space=pltpu.VMEM)
ANY_SPEC = pl.BlockSpec(memory_space=pl.ANY)
DMA = pltpu.SemaphoreType.DMA


def place():
    d = lax.axis_index("dp")
    z = lax.axis_index("seq")
    return d, z, d // 2, d % 2


def remote(src, dst, send, recv, dev):
    return pltpu.make_async_remote_copy(
        src_ref=src, dst_ref=dst, send_sem=send, recv_sem=recv, device_id=dev, device_id_type=MESH
    )


def greet_all(n_dp, n_z, d, z):
    barrier = pltpu.get_barrier_semaphore()
    me = d * n_z + z

    def one(o, carry):
        other = lax.rem(me + o, n_dp * n_z)
        pl.semaphore_signal(barrier, inc=1, device_id=(other // n_z, lax.rem(other, n_z)), device_id_type=MESH)
        return carry

    lax.fori_loop(1, n_dp * n_z, one, 0)
    pl.semaphore_wait(barrier, n_dp * n_z - 1)


def greet_line(n_z, d, z, extra=()):
    barrier = pltpu.get_barrier_semaphore()
    c = d % 2
    for o in range(n_z):
        zz = lax.rem(z + o, n_z)
        for core in range(2):
            if o == 0 and core == 0:
                continue
            pl.semaphore_signal(barrier, inc=1, device_id=(d - c + lax.rem(c + core, 2), zz), device_id_type=MESH)
    for dev in extra:
        pl.semaphore_signal(barrier, inc=1, device_id=dev, device_id_type=MESH)
    pl.semaphore_wait(barrier, 2 * n_z - 1 + len(extra))


def block_at(ref, shape, row, col):
    return ref.at[pl.ds(pl.multiple_of(row * shape[0], shape[0]), shape[0]),
                  pl.ds(pl.multiple_of(col * shape[1], shape[1]), shape[1])]


class Spread:
    def __init__(self, n_d, pair, c, z, parts, spot, send, recv):
        self.n_d, self.pair, self.parts, self.spot = n_d, pair, parts, spot
        self.send, self.recv = send, recv
        self.dev = lambda k: (2 * (pair ^ k) + c, z)

    def copy(self, slot, owner, t, h, to):
        at = self.spot(owner, t, h)
        return remote(at, at, self.send.at[slot, t, h], self.recv.at[slot, t, h], self.dev(to))

    def own(self, t):
        if self.n_d == 4:
            for h in range(2):
                self.copy(0, self.pair, t, h, 1).start()
                self.copy(1, self.pair, t, 1 - h, 2).start()
        else:
            for k in range(1, self.n_d):
                for h in range(2):
                    self.copy(k - 1, self.pair, t, h, k).start()

    def pass_on(self, t):
        if self.n_d == 4:
            self.copy(0, self.pair ^ 1, t, 0, 1).wait_recv()
            self.copy(2, self.pair ^ 1, t, 0, 2).start()
            self.copy(1, self.pair ^ 2, t, 1, 2).wait_recv()
            self.copy(2, self.pair ^ 2, t, 1, 1).start()

    def rest(self, t):
        if self.n_d == 4:
            self.copy(0, self.pair ^ 1, t, 1, 1).wait_recv()
            self.copy(1, self.pair ^ 2, t, 0, 2).wait_recv()
        else:
            for k in range(1, self.n_d):
                for h in range(2):
                    self.copy(k - 1, self.pair ^ k, t, h, k).wait_recv()

    def far(self, t):
        if self.n_d == 4:
            for h in range(2):
                self.copy(2, self.pair ^ 3, t, h, 1).wait_recv()

    def sent(self):
        for t in range(self.parts):
            for h in range(2):
                for slot in range(self.n_d - 1):
                    self.copy(slot, self.pair, t, h, 1).wait_send()

    def finish(self):
        for t in range(self.parts):
            if self.n_d == 4:
                self.copy(0, self.pair ^ 1, t, 1, 1).wait_recv()
                self.copy(1, self.pair ^ 2, t, 0, 2).wait_recv()
                for h in range(2):
                    self.copy(2, self.pair ^ 3, t, h, 1).wait_recv()
                    for slot in range(3):
                        self.copy(slot, self.pair, t, h, 1).wait_send()
            else:
                for k in range(1, self.n_d):
                    for h in range(2):
                        self.copy(k - 1, self.pair ^ k, t, h, k).wait_recv()
                        self.copy(k - 1, self.pair, t, h, k).wait_send()


def gather_in_kernel(n_dp, n_z, x_ref, w_wide, v_wide, g_ref, s_ref, gu_ref, dw_ref, xs, wq, vo, ga, sg, gu16, dw16,
                     w_ref, v_ref, gu_in, gu_out, dw_in, dw_out,
                     x_s, x_r, f_s, f_r, w_s, w_r, v_s, v_r, d_s, d_r, g_s, g_r, s_s, s_r, loc, gu_is, gu_os, dw_is, dw_os, w_f, v_f):
    d, z, pair, c = place()
    n_d = n_dp // 2
    me = d * n_z + z
    total = n_dp * n_z
    rows = x_ref.shape[1]
    half = rows // 2
    shape = w_ref.shape
    cz = z // 2
    chunks = gu_ref.shape[0] // WIDE_ROWS
    gu_width = gu_ref.shape[2]

    def chunk_in(i, slot):
        return pltpu.make_async_copy(gu_ref.at[pl.ds(pl.multiple_of(i * WIDE_ROWS, WIDE_ROWS), WIDE_ROWS)], gu_in.at[slot], gu_is.at[slot])

    def chunk_out(i, slot):
        return pltpu.make_async_copy(gu_out.at[slot], gu16.at[pl.ds(pl.multiple_of(i * WIDE_ROWS, WIDE_ROWS), WIDE_ROWS)], gu_os.at[slot])

    dw_rows = dw_in.shape[1]

    def dw_chunk_in(i, slot):
        return pltpu.make_async_copy(dw_ref.at[pl.ds(pl.multiple_of(i * dw_rows, dw_rows), dw_rows)], dw_in.at[slot], dw_is.at[slot])

    def dw_chunk_out(i, slot):
        return pltpu.make_async_copy(dw_out.at[slot], dw16.at[pl.ds(pl.multiple_of(i * dw_rows, dw_rows), dw_rows)], dw_os.at[slot])

    def round_chunks(low, high):
        def one(i, carry):
            slot = lax.rem(i, 2)

            @pl.when(i + 1 < chunks)
            def _():
                chunk_in(i + 1, 1 - slot).start()
                dw_chunk_in(i + 1, 1 - slot).start()

            chunk_in(i, slot).wait()
            dw_chunk_in(i, slot).wait()

            @pl.when(i >= 2)
            def _():
                chunk_out(i - 2, slot).wait()
                dw_chunk_out(i - 2, slot).wait()

            for n in range(2):
                gu_out[slot, :, n * gu_width : (n + 1) * gu_width] = gu_in[slot, :, n].astype(jnp.bfloat16)
            dw_out[slot] = dw_in[slot].astype(jnp.bfloat16)
            chunk_out(i, slot).start()
            dw_chunk_out(i, slot).start()
            return carry

        lax.fori_loop(low, high, one, 0)

    chunk_in(0, 0).start()
    dw_chunk_in(0, 0).start()
    w_ref[...] = w_wide[...].astype(jnp.bfloat16)
    v_ref[...] = v_wide[...].T.astype(jnp.bfloat16)
    greet_all(n_dp, n_z, d, z)

    def line_stage(src, dst, send, recv, spare, wait):
        for o, zz in ((0, z), (1, z - 1), (2, z + 1)):
            copy = remote(src, dst, send.at[o], recv.at[c, z % 2], (2 * pair + cz, zz))
            act = copy.wait_send if wait else copy.start
            if o == 0:
                pl.when(c != cz)(act)
                if not wait:
                    pl.when(c == cz)(pltpu.make_async_copy(src, dst, loc.at[spare]).start)
            else:
                pl.when(zz >= 0 if o == 1 else zz <= n_z - 1)(act)

    def line_relay(blk, send, recv, core, b, wait):
        j = 2 * c + b
        to = jnp.where(z > j, z + 1, z - 1)
        ok = (z != j) & (to >= 0) & (to <= n_z - 1)
        copy = remote(blk, blk, send, recv.at[core, b], (2 * pair + c, to))
        pl.when(ok)(copy.wait_send if wait else copy.start)

    my_block = block_at(wq, shape, d, z % 2)
    line_stage(w_ref, my_block, w_s, w_r, 0, False)

    for i in range(2):
        for h in range(2):
            src = x_ref.at[i, pl.ds(h * half, half)]
            dst = xs.at[pl.ds(pl.multiple_of(z * rows + h * half, half), half)]
            zz = 2 * c + i
            mine = (h == c) & (zz == z)
            copy = remote(src, dst, x_s.at[i, h], x_r.at[z], (2 * pair + h, zz))
            pl.when(jnp.logical_not(mine))(copy.start)
            pl.when(mine)(lambda src=src, dst=dst: pltpu.make_async_copy(src, dst, loc.at[1]).start())

    seg_copy = remote(s_ref, sg.at[c], s_s, s_r, (2 * pair + 1 - c, z))
    seg_copy.start()
    own_seg = pltpu.make_async_copy(s_ref, sg.at[c], loc.at[2])
    own_seg.start()
    own_gain = pltpu.make_async_copy(g_ref, ga.at[me], loc.at[3])
    own_gain.start()

    def send_gain(o, carry):
        other = lax.rem(me + o, total)
        remote(g_ref, ga.at[me], g_s, g_r, (other // n_z, lax.rem(other, n_z))).start()
        return carry

    lax.fori_loop(1, total, send_gain, 0)

    first = jnp.where(c == cz, z % 2, 1 - c)

    def turn_of(t):
        return t % 2, (first if t < 2 else 1 - first)

    def spot(owner, t, h):
        core, b = turn_of(t)
        part = shape[0] // 2
        return wq.at[pl.ds(pl.multiple_of((2 * owner + core) * shape[0] + h * part, part), part),
                     pl.ds(pl.multiple_of(b * shape[1], shape[1]), shape[1])]

    spread = Spread(n_d, pair, c, z, 4, spot, d_s, d_r)
    for t in range(4):
        core, b = turn_of(t)
        blk = block_at(wq, shape, 2 * pair + core, b)
        mine = (core == c) & (2 * c + b == z)
        arrive = remote(w_ref, blk, w_s.at[0], w_r.at[core, b], (d, z))
        pl.when(jnp.logical_not(mine))(arrive.wait_recv)
        pl.when(mine)(lambda blk=blk: pltpu.make_async_copy(w_ref, blk, loc.at[0]).wait())
        line_relay(blk, w_f.at[t], w_r, core, b, False)
        spread.own(t)
        if t == 0:
            line_stage(v_ref, block_at(vo, v_ref.shape, c, z % 2), v_s, v_r, 4, False)
        if t > 0:
            spread.pass_on(t - 1)
        round_chunks(t * chunks // 4, (t + 1) * chunks // 4)

    def out_unit(t, wait):
        core, b = turn_of(t)
        blk = block_at(vo, v_ref.shape, core, b)
        mine = (core == c) & (2 * c + b == z)
        if not wait:
            pl.when(jnp.logical_not(mine))(remote(blk, blk, v_s.at[0], v_r.at[core, b], (d, z)).wait_recv)
            pl.when(mine)(pltpu.make_async_copy(v_ref, blk, loc.at[4]).wait)
        line_relay(blk, v_f.at[t], v_r, core, b, wait)

    spread.pass_on(3)
    for o in range(n_z):
        zs = lax.rem(z + o, n_z)
        src = xs.at[pl.ds(pl.multiple_of(zs * rows + c * half, half), half)]
        mine = (cz == c) & (zs == z)
        arrive = remote(src, src, x_s.at[0, 0], x_r.at[zs], (d, z))
        pl.when(jnp.logical_not(mine))(arrive.wait_recv)
        pl.when(mine)(lambda src=src: pltpu.make_async_copy(src, src, loc.at[1]).wait())
        remote(src, src, f_s.at[zs], f_r.at[zs], (2 * pair + 1 - c, z)).start()
        out_unit(o, False)

    line_stage(w_ref, my_block, w_s, w_r, 0, True)
    line_stage(v_ref, block_at(vo, v_ref.shape, c, z % 2), v_s, v_r, 4, True)
    for i in range(2):
        for h in range(2):
            src = x_ref.at[i, pl.ds(h * half, half)]
            mine = (h == c) & (2 * c + i == z)
            copy = remote(src, src, x_s.at[i, h], x_r.at[0], (d, z))
            pl.when(jnp.logical_not(mine))(copy.wait_send)
    for zs in range(n_z):
        src = xs.at[pl.ds(zs * rows, half)]
        copy = remote(src, src, f_s.at[zs], f_r.at[zs], (d, z))
        copy.wait_send()
        copy.wait_recv()
    for t in range(4):
        core, b = turn_of(t)
        line_relay(block_at(wq, shape, 2 * pair + core, b), w_f.at[t], w_r, core, b, True)
        out_unit(t, True)
    for i in range(max(0, chunks - 2), chunks):
        chunk_out(i, i % 2).wait()
        dw_chunk_out(i, i % 2).wait()
    seg_copy.wait_send()
    remote(s_ref, sg.at[1 - c], s_s, s_r, (d, z)).wait_recv()
    own_seg.wait()
    own_gain.wait()
    many = ga.at[pl.ds(0, total - 1)]
    gains = remote(many, many, g_s, g_r, (d, z))
    gains.wait_send()
    gains.wait_recv()
    spread.finish()


def gather_in(x_loc, w, v, gain_tile, seg_tile, wide, down, n_dp, n_z):
    _, rows, width = x_loc.shape
    n_d = n_dp // 2
    total = n_dp * n_z
    b16 = jnp.bfloat16
    down_rows = down.shape[0] * WIDE_ROWS // wide.shape[0]
    return pl.pallas_call(
        functools.partial(gather_in_kernel, n_dp, n_z),
        in_specs=[VMEM_SPEC] * 5 + [ANY_SPEC] * 2,
        out_specs=[ANY_SPEC] * 7,
        out_shape=[
            jax.ShapeDtypeStruct((rows * n_z, width), x_loc.dtype),
            jax.ShapeDtypeStruct((w.shape[0] * n_dp, 2 * w.shape[1]), b16),
            jax.ShapeDtypeStruct((v.shape[1] * 2, 2 * v.shape[0]), b16),
            jax.ShapeDtypeStruct((total,) + gain_tile.shape, gain_tile.dtype),
            jax.ShapeDtypeStruct((2,) + seg_tile.shape, seg_tile.dtype),
            jax.ShapeDtypeStruct((wide.shape[0], wide.shape[1] * wide.shape[2]), b16),
            jax.ShapeDtypeStruct(down.shape, b16),
        ],
        scratch_shapes=[
            pltpu.VMEM(w.shape, b16), pltpu.VMEM(v.shape[::-1], b16),
            pltpu.VMEM((2, WIDE_ROWS) + wide.shape[1:], jnp.float32),
            pltpu.VMEM((2, WIDE_ROWS, wide.shape[1] * wide.shape[2]), b16),
            pltpu.VMEM((2, down_rows, down.shape[1]), jnp.float32), pltpu.VMEM((2, down_rows, down.shape[1]), b16),
            DMA((2, 2)), DMA((n_z,)), DMA((n_z,)), DMA((n_z,)), DMA((3,)), DMA((2, 2)), DMA((3,)), DMA((2, 2)),
            DMA((n_d - 1, 4, 2)), DMA((n_d - 1, 4, 2)), DMA, DMA, DMA, DMA, DMA((5,)), DMA((2,)), DMA((2,)), DMA((2,)), DMA((2,)), DMA((4,)), DMA((4,)),
        ],
        compiler_params=pltpu.CompilerParams(collective_id=1, has_side_effects=True),
        cost_estimate=pl.CostEstimate(flops=0, bytes_accessed=200_000_000, transcendentals=0),
        name="gather_in",
    )(x_loc, w, v, gain_tile, seg_tile, wide, down)


def share_resid_kernel(n_dp, n_z, part_ref, x_ref, w_ref, out, wall, got, buf, p_s, p_r, u_s, u_r, d_s, d_r, c_s, c_r, loc):
    d, z, pair, c = place()
    n_d = n_dp // 2
    cz = z // 2
    full = x_ref.shape[0]
    half = full // 2
    unit = half // 2
    w_rows = w_ref.shape[0]
    parts = 4
    piece = w_rows // parts
    own_copy = pltpu.make_async_copy(w_ref, wall.at[pl.ds(pl.multiple_of(d * w_rows, w_rows), w_rows)], loc.at[2])
    own_copy.start()
    greet_line(n_z, d, z, [(2 * (pair ^ k) + c, z) for k in range(1, n_d)])
    mine = pl.ds(pl.multiple_of(c * half, half), half)
    theirs = pl.ds(pl.multiple_of((1 - c) * half, half), half)
    swap = remote(part_ref.at[theirs], got, p_s, p_r, (2 * pair + 1 - c, z))
    swap.start()

    def spot_w(owner, t, h):
        sub = piece // 2
        return wall.at[pl.ds(pl.multiple_of((2 * owner + c) * w_rows + (2 * t + h) * sub, sub), sub)]

    def across(k, t, core):
        at = wall.at[pl.ds(pl.multiple_of((2 * (pair ^ k) + core) * w_rows + t * piece, piece), piece)]
        return remote(at, at, c_s.at[k, t], c_r.at[k, t], (2 * pair + 1 - c, z))

    spread = Spread(n_d, pair, c, z, parts, spot_w, d_s, d_r)
    own_copy.wait()
    for t in range(parts):
        spread.own(t)
        across(0, t, c).start()

    swap.wait_recv()

    def add(r, carry):
        at = pl.ds(pl.multiple_of(r * 16, 16), 16)
        src = pl.ds(pl.multiple_of(c * half + r * 16, 16), 16)
        total = x_ref[src].astype(jnp.float32) + part_ref[src].astype(jnp.float32) + got[at].astype(jnp.float32)
        buf[at] = total.astype(jnp.bfloat16)
        return carry

    def spot(jl, h, k):
        return out.at[jl, pl.ds(pl.multiple_of(h * half + k * unit, unit), unit)]

    def sends(k, wait):
        src = buf.at[pl.ds(k * unit, unit)]
        dst = spot(z % 2, c, k)
        for o, zz in ((1, z - 1), (2, z + 1), (0, z)):
            copy = remote(src, dst, u_s.at[o, k], u_r.at[z % 2, c, k], (2 * pair + cz, zz))
            act = copy.wait_send if wait else copy.start
            if o == 0:
                keep = pltpu.make_async_copy(src, dst, loc.at[k])
                pl.when(c != cz)(act)
                pl.when(c == cz)(keep.wait if wait else keep.start)
            elif o == 1:
                pl.when(z > 0)(act)
            else:
                pl.when(z < n_z - 1)(act)

    per = unit // 16
    lax.fori_loop(0, per, add, 0)
    lax.fori_loop(per, per + per // 2, add, 0)
    sends(0, False)
    lax.fori_loop(per + per // 2, 2 * per, add, 0)
    swap.wait_send()
    sends(1, False)

    def relay(dist, sign, k, h, begin):
        j = z + sign * dist
        ok = (j >= 2 * c) & (j <= 2 * c + 1)
        to = z - sign
        more = (to >= 0) & (to <= n_z - 1)
        jl = lax.rem(j + n_z, 2)
        at = spot(jl, h, k)
        copy = remote(at, at, u_s.at[3 + (0 if sign < 0 else 1), 4 * jl + 2 * h + k], u_r.at[jl, h, k], (2 * pair + c, to))
        if begin:

            @pl.when(ok)
            def _():
                copy.wait_recv()
                pl.when(more)(copy.start)
        else:
            pl.when(ok & more)(copy.wait_send)

    def take(t):
        spread.pass_on(t)

    def rest(t):
        spread.rest(t)
        for k in range(1, n_d):
            if n_d != 4 or k != 3:
                across(k, t, c).start()

    def far(t):
        if n_d == 4:
            spread.far(t)
            across(3, t, c).start()

    links = []
    for t in range(parts):
        links += [(take, t), (rest, t)]
    links += [(far, t) for t in range(parts)]
    line = [(dist, k, h) for dist in range(1, n_z) for k in range(2) for h in range(2)]
    for n in range(max(len(links), len(line))):
        if n < len(line):
            dist, k, h = line[n]
            for sign in (-1, 1):
                relay(dist, sign, k, h, True)
        if n < len(links):
            links[n][0](links[n][1])

    @pl.when(c == cz)
    def _():
        for k in range(2):
            at = spot(z % 2, 1 - c, k)
            remote(at, at, u_s.at[0, 0], u_r.at[z % 2, 1 - c, k], (d, z)).wait_recv()

    for dist, k, h in line:
        for sign in (-1, 1):
            relay(dist, sign, k, h, False)
    sends(0, True)
    sends(1, True)
    spread.sent()
    for k in range(n_d):
        for t in range(parts):
            across(k, t, c).wait_send()
            across(k, t, 1 - c).wait_recv()


def share_resid(part, x, w, n_dp, n_z):
    full, width = x.shape
    n_d = n_dp // 2
    return pl.pallas_call(
        functools.partial(share_resid_kernel, n_dp, n_z),
        in_specs=[VMEM_SPEC] * 3,
        out_specs=[ANY_SPEC] * 2,
        out_shape=[
            jax.ShapeDtypeStruct((2, full, width), jnp.bfloat16),
            jax.ShapeDtypeStruct((n_dp * w.shape[0], w.shape[1]), jnp.bfloat16),
        ],
        scratch_shapes=[
            pltpu.VMEM((full // 2, width), jnp.bfloat16), pltpu.VMEM((full // 2, width), jnp.bfloat16),
            DMA, DMA, DMA((5, 8)), DMA((2, 2, 2)), DMA((n_d - 1, 4, 2)), DMA((n_d - 1, 4, 2)), DMA((n_d, 4)), DMA((n_d, 4)),
            DMA((3,)),
        ],
        compiler_params=pltpu.CompilerParams(collective_id=2, has_side_effects=True),
        cost_estimate=pl.CostEstimate(flops=0, bytes_accessed=200_000_000, transcendentals=0),
        name="share_resid",
    )(part, x, w)


CHUNKS = 8
GROUPS = 4


def sum_line_kernel(n_z, d_gate_ref, d_up_ref, w_ref, resid_all, cot_all, gain_ref, hid_ref, down_ref, d_out, gain_out,
                    rows_out, left, w, part, got, buf, resid_ref, cot_ref, hid, down, rows_buf,
                    s_s, s_r, p_s, p_r, loc, rows_sem, mul_sem, out_sem, left_sem, w_sem):
    d, z, pair, c = place()
    cz = z // 2
    full, width = buf.shape
    inner = d_gate_ref.shape[1]
    rows = full // CHUNKS
    group = full // GROUPS
    per = CHUNKS // GROUPS
    tile = 256
    tiles = width // tile
    lefts = []
    for q in range(GROUPS):
        for jl in range(2):
            for n, src in enumerate((d_gate_ref, d_up_ref)):
                lefts.append(pltpu.make_async_copy(
                    src.at[pl.ds(jl * full + q * group, group)],
                    left.at[pl.ds((2 * q + jl) * group, group), pl.ds(n * inner, inner)],
                    left_sem.at[q, jl, n],
                ))

    def w_copy(n):
        at = pl.ds(pl.multiple_of(n * tile, tile), tile)
        return pltpu.make_async_copy(w_ref.at[at], w.at[at], w_sem.at[n])

    fetch = (
        pltpu.make_async_copy(resid_all.at[z % 2], resid_ref, rows_sem.at[0]),
        pltpu.make_async_copy(cot_all.at[z % 2], cot_ref, rows_sem.at[1]),
    )
    factors = (pltpu.make_async_copy(hid_ref, hid, mul_sem.at[0]), pltpu.make_async_copy(down_ref, down, mul_sem.at[1]))
    for one in lefts[:4]:
        one.start()
    for n in range(tiles):
        w_copy(n).start()
    for one in tuple(lefts[4:]) + factors + fetch:
        one.start()
    greet_line(n_z, d, z)
    gain_out[...] = jnp.zeros_like(gain_out)
    own = c == cz

    def compute(q, low, high):
        if low == 0:
            for one in lefts[4 * q : 4 * q + 4]:
                one.wait()

        def one_tile(n, carry):
            if q == 0:
                w_copy(n).wait()
            at = pl.ds(pl.multiple_of(n * tile, tile), tile)
            value = dot_t(left[pl.ds(2 * q * group, 2 * group)], w[at])
            part[pl.ds(2 * q * group, 2 * group), at] = value.astype(jnp.bfloat16)
            return carry

        lax.fori_loop(low, high, one_tile, 0)

    def tile_out(j):
        at = pl.ds(pl.multiple_of(j * tile, tile), tile)
        return pltpu.make_async_copy(rows_buf.at[lax.rem(j, 2)], rows_out.at[:, at], out_sem.at[lax.rem(j, 2)])

    def multiply(low, high):
        if low == 0:
            for one in factors:
                one.wait()

        def one_tile(j, carry):
            pl.when(j >= 2)(tile_out(j - 2).wait)
            at = pl.ds(pl.multiple_of(j * tile, tile), tile)
            rows_buf[lax.rem(j, 2)] = dot_n(hid[...], down[:, at]).astype(jnp.bfloat16)
            tile_out(j).start()
            return carry

        lax.fori_loop(low, high, one_tile, 0)

    def part_start(jl, k):
        return (2 * (k // per) + jl) * group + k % per * rows

    def part_at(jl, k, r):
        return pl.ds(pl.multiple_of(part_start(jl, k) + r * 16, 16), 16)

    def copy_on(k, t, side, src):
        jl = jnp.bitwise_xor(c, t)
        to = z + 1 if side == 0 else z - 1
        return remote(src, got.at[side, jl, pl.ds(k * rows, rows)], s_s.at[t, k], s_r.at[side, jl, k], (2 * pair + c, to))

    def arrived(side, jl, k):
        at = got.at[side, jl, pl.ds(k * rows, rows)]
        return remote(at, at, s_s.at[0, 0], s_r.at[side, jl, k], (d, z))

    def send_step(k, t, edge_only, inner_only, wait):
        jl = jnp.bitwise_xor(c, t)
        j = 2 * c + jl
        for side in range(2):
            going = (z < j) if side == 0 else (z > j)
            edge = (z == 0) if side == 0 else (z == n_z - 1)
            raw = copy_on(k, t, side, part.at[pl.ds(pl.multiple_of(part_start(jl, k), rows), rows)])
            passed = copy_on(k, t, side, got.at[side, jl, pl.ds(k * rows, rows)])
            if not inner_only:
                pl.when(going & edge)(raw.wait_send if wait else raw.start)
            if not edge_only:
                pl.when(going & jnp.logical_not(edge))(passed.wait_send if wait else passed.start)

    def add_in(side, jl, k):
        def one(r, carry):
            at = pl.ds(pl.multiple_of(k * rows + r * 16, 16), 16)
            got[side, jl, at] = (got[side, jl, at].astype(jnp.float32) + part[part_at(jl, k, r)].astype(jnp.float32)).astype(jnp.bfloat16)
            return carry

        lax.fori_loop(0, rows // 16, one, 0)

    def finish(jl, k):
        def one(r, carry):
            at = pl.ds(pl.multiple_of(k * rows + r * 16, 16), 16)
            total = part[part_at(jl, k, r)].astype(jnp.float32)
            low_side = got[0, jl, at].astype(jnp.float32)
            high_side = got[1, jl, at].astype(jnp.float32)
            total = total + jnp.where(z > 0, low_side, 0.0) + jnp.where(z < n_z - 1, high_side, 0.0)
            value = resid_ref[at].astype(jnp.float32)
            inverse = lax.rsqrt(jnp.mean(value * value, axis=-1, keepdims=True) + norm_eps)
            scaled = value * inverse
            d_scaled = total * gain_ref[...]
            mean = jnp.mean(d_scaled * scaled, axis=-1, keepdims=True)
            d_resid = cot_ref[at].astype(jnp.float32) + inverse * (d_scaled - scaled * mean)
            buf[at] = d_resid.astype(jnp.bfloat16)
            prod = total * scaled
            gain_out[...] = gain_out[...] + prod[:8] + prod[8:]
            return carry

        lax.fori_loop(0, rows // 16, one, 0)

    def to_partner(k):
        at = pl.ds(k * rows, rows)
        return remote(buf.at[at], d_out.at[at], p_s.at[k], p_r.at[k], (2 * pair + 1 - c, z))

    def keep(k):
        at = pl.ds(k * rows, rows)
        return pltpu.make_async_copy(buf.at[at], d_out.at[at], loc.at[k])

    def own_chunk(k):
        @pl.when(own)
        def _():
            jl = z % 2
            pl.when(z > 0)(arrived(0, jl, k).wait_recv)
            pl.when(z < n_z - 1)(arrived(1, jl, k).wait_recv)
            finish(jl, k)
            if k > 0:
                to_partner(k - 1).start()
                keep(k - 1).start()

    done = 0
    for q in range(GROUPS):
        compute(q, 0, 1)
        if q > 0:
            for k in range((q - 1) * per, q * per):
                for t in range(2):
                    send_step(k, t, True, False, False)
        compute(q, 1, tiles)
    multiply(done, done + 1)
    done += 1
    for k in range((GROUPS - 1) * per, CHUNKS):
        for t in range(2):
            send_step(k, t, True, False, False)
    for one in fetch:
        one.wait()

    steps = [(k, t) for k in range(CHUNKS) for t in range(2)]
    for n, (k, t) in enumerate(steps):
        jl = jnp.bitwise_xor(c, t)
        j = 2 * c + jl
        for side in range(2):
            going = (z < j) if side == 0 else (z > j)
            between = (z > 0) if side == 0 else (z < n_z - 1)

            @pl.when(going & between)
            def _():
                arrived(side, jl, k).wait_recv()
                add_in(side, jl, k)

        if n > 0:
            send_step(*steps[n - 1], False, True, False)
        if t == 0 and done < tiles:
            multiply(done, done + 1)
            done += 1
        if t == 1 and k > 0:
            own_chunk(k - 1)
    send_step(*steps[-1], False, True, False)
    own_chunk(CHUNKS - 1)
    if done < tiles:
        multiply(done, tiles)

    @pl.when(own)
    def _():
        to_partner(CHUNKS - 1).start()
        keep(CHUNKS - 1).start()

    for j in range(max(0, tiles - 2), tiles):
        tile_out(j).wait()
    for k, t in steps:
        send_step(k, t, False, False, True)
    for k in range(CHUNKS):
        at = d_out.at[pl.ds(k * rows, rows)]

        @pl.when(own)
        def _():
            to_partner(k).wait_send()
            keep(k).wait()

        pl.when(jnp.logical_not(own))(remote(at, at, p_s.at[k], p_r.at[k], (d, z)).wait_recv)


def sum_line(d_gate, d_up, w, resid, cot, gain, hidden, down, n_z):
    _, full, width = resid.shape
    b16 = jnp.bfloat16
    return pl.pallas_call(
        functools.partial(sum_line_kernel, n_z),
        in_specs=[ANY_SPEC] * 5 + [VMEM_SPEC] + [ANY_SPEC] * 2,
        out_specs=[ANY_SPEC, VMEM_SPEC, ANY_SPEC],
        out_shape=[
            jax.ShapeDtypeStruct((full, width), b16),
            jax.ShapeDtypeStruct((8, width), jnp.float32),
            jax.ShapeDtypeStruct((2 * full, width), b16),
        ],
        scratch_shapes=[
            pltpu.VMEM((2 * full, w.shape[1]), b16), pltpu.VMEM(w.shape, b16), pltpu.VMEM((2 * full, width), b16),
            pltpu.VMEM((2, 2, full, width), b16), pltpu.VMEM((full, width), b16),
            pltpu.VMEM((full, width), b16), pltpu.VMEM((full, width), b16),
            pltpu.VMEM(hidden.shape, b16), pltpu.VMEM(down.shape, b16), pltpu.VMEM((2, 2 * full, 256), b16),
            DMA((2, CHUNKS)), DMA((2, 2, CHUNKS)), DMA((CHUNKS,)), DMA((CHUNKS,)), DMA((CHUNKS,)), DMA((2,)), DMA((2,)), DMA((2,)),
            DMA((GROUPS, 2, 2)), DMA((width // 256,)),
        ],
        compiler_params=pltpu.CompilerParams(collective_id=3, has_side_effects=True, vmem_limit_bytes=63 * 1024 * 1024),
        cost_estimate=pl.CostEstimate(flops=0, bytes_accessed=200_000_000, transcendentals=0),
        name="sum_line",
    )(d_gate, d_up, w, resid, cot, gain, hidden, down)


def hidden_kernel(resid_ref, gain_ref, gate_w, up_w, normed_ref, gate_ref, up_ref, hidden_ref):
    @pl.when(pl.program_id(0) == 0)
    def _():
        def one(r, carry):
            at = pl.ds(pl.multiple_of(r * 16, 16), 16)
            value = resid_ref[at].astype(jnp.float32)
            inverse = lax.rsqrt(jnp.mean(value * value, axis=-1, keepdims=True) + norm_eps)
            normed_ref[at] = (value * inverse * gain_ref[...]).astype(jnp.bfloat16)
            return carry

        lax.fori_loop(0, resid_ref.shape[0] // 16, one, 0, unroll=2)

    half = resid_ref.shape[0] // 4
    for h in range(4):
        at = slice(h * half, (h + 1) * half)
        gate = dot_n(normed_ref[at], gate_w[...])
        up = dot_n(normed_ref[at], up_w[...])
        gate_ref[at] = gate.astype(jnp.bfloat16)
        up_ref[at] = up.astype(jnp.bfloat16)
        hidden_ref[at] = (gate * jax.nn.sigmoid(gate) * up).astype(jnp.bfloat16)


HIDDEN_TILE = 256


def hidden_forward(resid, gain, weights):
    rows, width = resid.shape
    units = weights.shape[1] // 2
    tiles = units // HIDDEN_TILE
    whole = lambda shape: pl.BlockSpec(shape, lambda j: (0, 0))
    tile = pl.BlockSpec((rows, HIDDEN_TILE), lambda j: (0, j))
    return pl.pallas_call(
        hidden_kernel,
        grid=(tiles,),
        in_specs=[
            whole((rows, width)), whole((1, width)),
            pl.BlockSpec((width, HIDDEN_TILE), lambda j: (0, j)),
            pl.BlockSpec((width, HIDDEN_TILE), lambda j: (0, j + tiles)),
        ],
        out_specs=[whole((rows, width)), tile, tile, tile],
        out_shape=[jax.ShapeDtypeStruct((rows, width), jnp.bfloat16)] + [jax.ShapeDtypeStruct((rows, units), jnp.bfloat16)] * 3,
        cost_estimate=pl.CostEstimate(flops=4 * rows * width * units, bytes_accessed=40_000_000, transcendentals=0),
        name="hidden_forward",
    )(resid, gain, weights, weights)


WIDE_ROWS = 32
TURNED_ROWS = 512


def adam_wide_kernel(grad_ref, w_ref, m_ref, v_ref, g_out, w_out, m_out, v_out):
    width = w_ref.shape[-1]
    for n in range(2):
        grad = grad_ref[:, n * width : (n + 1) * width].astype(jnp.float32)
        weight, first, second = adam_update(w_ref[:, n], grad, m_ref[:, n], v_ref[:, n])
        g_out[:, n] = grad
        w_out[:, n] = weight
        m_out[:, n] = first
        v_out[:, n] = second


def adam_turned_kernel(grad_ref, w_ref, m_ref, v_ref, g_out, w_out, m_out, v_out):
    grad = grad_ref[...].astype(jnp.float32).T
    weight, first, second = adam_update(w_ref[...], grad, m_ref[...], v_ref[...])
    g_out[...] = grad
    w_out[...] = weight
    m_out[...] = first
    v_out[...] = second


def adam_call(kernel, grid, grad_spec, spec, arrays):
    shape = jax.ShapeDtypeStruct(arrays[1].shape, jnp.float32)
    return pl.pallas_call(
        kernel,
        grid=(grid,),
        in_specs=[grad_spec] + [spec] * 3,
        out_specs=[spec] * 4,
        out_shape=[shape] * 4,
        cost_estimate=pl.CostEstimate(flops=20 * shape.size, bytes_accessed=30 * shape.size, transcendentals=0),
    )(*arrays)


def adam_wide(*arrays):
    rows, _, width = arrays[1].shape
    return adam_call(
        adam_wide_kernel, rows // WIDE_ROWS,
        pl.BlockSpec((WIDE_ROWS, 2 * width), lambda i: (i, 0)),
        pl.BlockSpec((WIDE_ROWS, 2, width), lambda i: (i, 0, 0)),
        arrays,
    )


def adam_turned(*arrays):
    rows, cols = arrays[1].shape
    return adam_call(
        adam_turned_kernel, rows // TURNED_ROWS,
        pl.BlockSpec((cols, TURNED_ROWS), lambda i: (0, i)),
        pl.BlockSpec((TURNED_ROWS, cols), lambda i: (i, 0)),
        arrays,
    )


def hand_out_kernel(n_dp, n_z, dq_ref, n_ref, x_ref, dr_ref, gain_ref, gain2_ref, wq_ref, ot_ref, ig, gq, go, gains,
                    dn_ref, wq, got, buf, q_base, q_got, q_put, q_fin, o_base, o_got, o_put, o_fin, g_src, g_all,
                    p_s, p_r, i_s, i_r, q_s, q_r, qf_s, qf_r, o_s, o_r, of_s, of_r, g_s, g_r, loc):
    d, z, pair, c = place()
    n_d = n_dp // 2
    total = n_dp * n_z
    me = d * n_z + z
    cz = z // 2
    full, width = x_ref.shape
    half = full // 2
    quarter = half // 2
    q_rows, q_cols = q_fin.shape[1:]
    o_rows, o_cols = o_fin.shape[1:]
    relay = n_d == 4

    class First:
        def __init__(self, rows, cols, bufs, sems, spare):
            self.rows, self.cols, self.spare = rows, cols, spare
            self.base, self.got, self.put, self.fin = bufs
            self.send, self.recv, self.f_send, self.f_recv = sems

        def block(self, ref, b, core):
            return ref.at[pl.ds(core * self.rows, self.rows), pl.ds(b * self.cols, self.cols)]

        def source(self, owner, b, core):
            return self.base.at[pl.ds(pl.multiple_of((2 * owner + core) * self.rows, self.rows), self.rows), pl.ds(b * self.cols, self.cols)]

        def cut_of(self, owner, b, core, r):
            start = (2 * owner + core) * self.rows + r * 16
            return pl.ds(pl.multiple_of(start, 16), 16), pl.ds(b * self.cols, self.cols)

        def copy(self, n, b, core, owner, to):
            return remote(self.source(owner, b, core), self.block(self.got.at[n], b, core), self.send.at[n, b, core],
                          self.recv.at[n, b, core], (2 * (pair ^ to) + c, z))

        def begin(self, core):
            for b in range(2):
                if relay:
                    self.copy(1, b, core, pair ^ 3, 1 + b).start()
            for b in range(2):
                if relay:
                    self.copy(0, b, core, pair ^ (1 + b), 1 + b).start()
                else:
                    for k in range(1, n_d):
                        self.copy(k - 1, b, core, pair ^ k, k).start()

        def arrived(self, n, b, core):
            at = self.block(self.got.at[n], b, core)
            remote(at, at, self.send.at[n, b, core], self.recv.at[n, b, core], (d, z)).wait_recv()

        def cut(self, b, core, r):
            return pl.ds(pl.multiple_of(core * self.rows + r * 16, 16), 16), pl.ds(b * self.cols, self.cols)

        def middle_copy(self, b, core):
            return remote(self.source(pair ^ (2 >> b), b, core), self.block(self.got.at[2], b, core), self.send.at[2, b, core],
                          self.recv.at[2, b, core], (2 * (pair ^ (2 >> b)) + c, z))

        def middle(self, core, between):
            if not relay:
                return
            for b in range(2):
                self.arrived(1, b, core)

                def add(r, carry):
                    at = self.cut(b, core, r)
                    mid = self.cut_of(pair ^ (2 >> b), b, core, r)
                    self.base[mid] = (self.base[mid].astype(jnp.float32) + self.got[(1,) + at].astype(jnp.float32)).astype(jnp.bfloat16)
                    return carry

                lax.fori_loop(0, self.rows // 16, add, 0)
            self.middle_copy(0, core).start()
            between()
            self.middle_copy(1, core).start()

        def total(self, core, between):
            slots = (0, 2) if relay else range(n_d - 1)
            for b in range(2):
                for n in slots:
                    self.arrived(n, b, core)

                def add(r, carry):
                    at = self.cut(b, core, r)
                    value = self.base[self.cut_of(pair, b, core, r)].astype(jnp.float32)
                    for n in slots:
                        value = value + self.got[(n,) + at].astype(jnp.float32)
                    self.put[core, b, pl.ds(pl.multiple_of(r * 16, 16), 16)] = value.astype(jnp.bfloat16)
                    return carry

                lax.fori_loop(0, self.rows // 16, add, 0)
            self.second(0, core, False)
            between()
            self.second(1, core, False)

        def second(self, b, core, wait):
            here = (core == c) & (2 * c + b == z)
            src = self.put.at[core, b]
            copy = remote(src, self.fin.at[z], self.f_send.at[core, b], self.f_recv.at[z], (2 * pair + core, 2 * c + b))
            keep = pltpu.make_async_copy(src, self.fin.at[z], loc.at[self.spare])
            pl.when(jnp.logical_not(here))(copy.wait_send if wait else copy.start)
            pl.when(here)(keep.wait if wait else keep.start)

        def final(self):
            for core in range(2):
                for b in range(2):
                    self.second(b, core, True)
            for zs in range(n_z):
                at = self.fin.at[zs]
                from_here = (cz == c) & (zs == z)
                pl.when(jnp.logical_not(from_here))(remote(at, at, self.f_send.at[0, 0], self.f_recv.at[zs], (d, z)).wait_recv)

        def sent(self):
            for b in range(2):
                for core in range(2):
                    for n in range(n_d - 1):
                        at = self.block(self.got.at[n], b, core)
                        remote(at, at, self.send.at[n, b, core], self.recv.at[n, b, core], (d, z)).wait_send()

    o_first = First(o_rows, o_cols, (o_base, o_got, o_put, o_fin), (o_s, o_r, of_s, of_r), 2)
    q_first = First(q_rows, q_cols, (q_base, q_got, q_put, q_fin), (q_s, q_r, qf_s, qf_r), 3)
    o_load = pltpu.make_async_copy(ot_ref, o_base, loc.at[4])
    wq_load = pltpu.make_async_copy(wq_ref, wq, loc.at[5])
    o_load.start()
    wq_load.start()
    greet_all(n_dp, n_z, d, z)
    o_load.wait()
    o_first.begin(0)
    o_first.begin(1)
    nothing = lambda: None

    def q_blocks(core):
        def one(k, carry):
            owner = pair ^ (n_d - 1 - k)
            rows_at = pl.ds(pl.multiple_of((2 * owner + core) * q_rows, q_rows), q_rows)
            q_base[rows_at] = dot_c(n_ref[:, rows_at], dq_ref[...]).astype(jnp.bfloat16)
            return carry

        lax.fori_loop(0, n_d, one, 0)

    def dn_blocks(low, high):
        def one(r, carry):
            rows_at = pl.ds(pl.multiple_of(r * 256, 256), 256)
            dn_ref[:, rows_at] = dot_t(dq_ref[...], wq[rows_at]).astype(jnp.bfloat16)
            return carry

        lax.fori_loop(low, high, one, 0)

    q_blocks(0)
    o_first.middle(0, lambda: q_blocks(1))
    q_first.begin(0)
    wq_load.wait()
    dn_tiles = width // 256
    dn_blocks(0, dn_tiles // 2)
    o_first.middle(1, nothing)
    q_first.begin(1)
    dn_blocks(dn_tiles // 2, dn_tiles)
    mine = pl.ds(pl.multiple_of(c * half, half), half)
    theirs = pl.ds(pl.multiple_of((1 - c) * half, half), half)
    swap = remote(dn_ref.at[theirs], got, p_s, p_r, (2 * pair + 1 - c, z))
    o_first.total(0, nothing)
    swap.start()

    g_src[pl.ds(0, 8)] = jnp.zeros((8, width), jnp.float32)
    g_src[pl.ds(8, 8)] = gain2_ref[...]
    swap.wait_recv()

    def rows_of(r, carry):
        at = pl.ds(pl.multiple_of(r * 16, 16), 16)
        src = pl.ds(pl.multiple_of(c * half + r * 16, 16), 16)
        d_normed = dn_ref[src].astype(jnp.float32) + got[at].astype(jnp.float32)
        value = x_ref[src].astype(jnp.float32)
        inverse = lax.rsqrt(jnp.mean(value * value, axis=-1, keepdims=True) + norm_eps)
        scaled = value * inverse
        d_scaled = d_normed * gain_ref[...]
        mean = jnp.mean(d_scaled * scaled, axis=-1, keepdims=True)
        out = dr_ref[src].astype(jnp.float32) + inverse * (d_scaled - scaled * mean)
        buf[at] = out.astype(jnp.bfloat16)
        prod = d_normed * scaled
        g_src[pl.ds(0, 8)] = g_src[pl.ds(0, 8)] + prod[:8] + prod[8:]
        return carry

    def row_send(b, wait):
        src = buf.at[pl.ds(b * quarter, quarter)]
        dst = ig.at[z % 2]
        zz = 2 * c + b
        here = (cz == c) & (zz == z)
        copy = remote(src, dst, i_s.at[b], i_r.at[z % 2], (2 * pair + cz, zz))
        keep = pltpu.make_async_copy(src, dst, loc.at[0])
        pl.when(jnp.logical_not(here))(copy.wait_send if wait else copy.start)
        pl.when(here)(keep.wait if wait else keep.start)

    q_first.middle(0, nothing)
    per = quarter // 16
    lax.fori_loop(0, per, rows_of, 0)
    o_first.total(1, lambda: row_send(0, False))
    lax.fori_loop(per, 2 * per, rows_of, 0)
    q_first.middle(1, lambda: row_send(1, False))

    each = width // total

    def gain_tile(o):
        return g_src.at[:, pl.ds(pl.multiple_of(o * each // 128 * 128, 128), 128)]

    own_gain = pltpu.make_async_copy(gain_tile(me), g_all.at[me], loc.at[1])
    own_gain.start()

    def send_gain(o, carry):
        other = lax.rem(me + o, total)
        remote(gain_tile(other), g_all.at[me], g_s, g_r, (other // n_z, lax.rem(other, n_z))).start()
        return carry

    lax.fori_loop(1, total, send_gain, 0)

    q_first.total(0, nothing)
    q_first.total(1, nothing)

    o_first.final()
    value = o_fin[0].astype(jnp.float32)
    for zs in range(1, n_z):
        value = value + o_fin[zs].astype(jnp.float32)
    go[...] = value.T

    many = g_all.at[pl.ds(0, total - 1)]
    gain_copy = remote(many, many, g_s, g_r, (d, z))
    gain_copy.wait_send()
    gain_copy.wait_recv()
    own_gain.wait()
    gains[...] = jnp.zeros_like(gains)

    def add_gain(o, carry):
        gains[...] = gains[...] + g_all[o]
        return carry

    lax.fori_loop(0, total, add_gain, 0)

    swap.wait_send()
    for b in range(2):
        row_send(b, True)
    for i in range(2):
        from_here = (cz == c) & (2 * c + i == z)
        at = ig.at[i]
        pl.when(jnp.logical_not(from_here))(remote(at, at, i_s.at[0], i_r.at[i], (d, z)).wait_recv)
    o_first.sent()
    q_first.sent()
    q_first.final()

    def last(r, carry):
        at = pl.ds(pl.multiple_of(r * 16, 16), 16)
        value = q_fin[0, at].astype(jnp.float32)
        for zs in range(1, n_z):
            value = value + q_fin[zs, at].astype(jnp.float32)
        gq[at] = value
        return carry

    lax.fori_loop(0, q_rows // 16, last, 0)


def hand_out(dq, normed, x, dr, gain, gain2, wq, ot, n_dp, n_z):
    full, width = x.shape
    n_d = n_dp // 2
    total = n_dp * n_z
    q_rows, q_cols = wq.shape[0] // n_dp, wq.shape[1] // 2
    o_rows, o_cols = ot.shape[0] // n_dp, ot.shape[1] // 2
    b16 = jnp.bfloat16
    f32 = jnp.float32

    def weight_bufs(rows, cols):
        return [
            pltpu.VMEM((n_dp * rows, 2 * cols), b16), pltpu.VMEM((n_d - 1, 2 * rows, 2 * cols), b16),
            pltpu.VMEM((2, 2, rows, cols), b16), pltpu.VMEM((n_z, rows, cols), b16),
        ]

    weight_sems = [DMA((n_d - 1, 2, 2)), DMA((n_d - 1, 2, 2)), DMA((2, 2)), DMA((n_z,))]
    return pl.pallas_call(
        functools.partial(hand_out_kernel, n_dp, n_z),
        in_specs=[VMEM_SPEC] * 6 + [ANY_SPEC] * 2,
        out_specs=[ANY_SPEC] + [VMEM_SPEC] * 3,
        out_shape=[
            jax.ShapeDtypeStruct((2, full // 4, width), b16),
            jax.ShapeDtypeStruct((q_rows, q_cols), f32),
            jax.ShapeDtypeStruct((o_cols, o_rows), f32),
            jax.ShapeDtypeStruct((16, 128), f32),
        ],
        scratch_shapes=[
            pltpu.VMEM((full, width), b16), pltpu.VMEM(wq.shape, b16),
            pltpu.VMEM((full // 2, width), b16), pltpu.VMEM((full // 2, width), b16),
            *weight_bufs(q_rows, q_cols), *weight_bufs(o_rows, o_cols),
            pltpu.VMEM((16, width), f32), pltpu.VMEM((total, 16, 128), f32),
            DMA, DMA, DMA((2,)), DMA((2,)), *weight_sems, *weight_sems, DMA, DMA,
            DMA((6,)),
        ],
        compiler_params=pltpu.CompilerParams(collective_id=5, has_side_effects=True, vmem_limit_bytes=58 * 1024 * 1024),
        cost_estimate=pl.CostEstimate(flops=0, bytes_accessed=300_000_000, transcendentals=0),
        name="hand_out",
    )(dq, normed, x, dr, gain, gain2, wq, ot)


def rms_forward(values, gain_wide):
    inverse = lax.rsqrt(jnp.mean(values * values, axis=-1, keepdims=True) + norm_eps)
    scaled = values * inverse
    return (scaled, inverse, (scaled * gain_wide).astype(jnp.bfloat16))


def adam_update(weight, grad, first, second):
    new_first = beta_one * first + (1.0 - beta_one) * grad
    new_second = beta_two * second + (1.0 - beta_two) * grad * grad
    first_hat = new_first / (1.0 - beta_one**step_count)
    second_hat = new_second / (1.0 - beta_two**step_count)
    new_weight = weight - learn_rate * (
        first_hat / (jnp.sqrt(second_hat) + adam_eps) + weight_decay * weight
    )
    return (new_weight, new_first, new_second)


def contract_rows(left, right):
    return lax.dot_general(
        left, right, (((0,), (0,)), ((), ())), preferred_element_type=jnp.float32
    )


def times_transpose(left, right):
    return lax.dot_general(
        left, right, (((1,), (1,)), ((), ())), preferred_element_type=jnp.float32
    )


def layer_step(
    block_input,
    segment_ids,
    cotangent,
    attn_gain,
    qkv_weight,
    out_weight,
    mlp_gain,
    gate_up_weight,
    down_weight,
    first_attn_gain,
    first_qkv,
    first_out,
    first_mlp_gain,
    first_gate_up,
    first_down,
    second_attn_gain,
    second_qkv,
    second_out,
    second_mlp_gain,
    second_gate_up,
    second_down,
):
    seqs_here, local_len, width = block_input.shape
    full_len = segment_ids.shape[1]
    n_dp = lax.axis_size("dp")
    n_z = lax.axis_size("seq")
    groups = HEADS // KV_HEADS
    z_here = lax.axis_index("seq")
    owned = attn_gain.shape[0]
    gain_line = jnp.concatenate([attn_gain, mlp_gain]).astype(jnp.bfloat16).astype(jnp.float32)
    gain_tile = jnp.pad(gain_line[None], ((0, 7), (0, LANES - 2 * owned)))
    seg_tile = jnp.pad(segment_ids, ((0, 8 - seqs_here), (0, 0)))
    rows_in, qkv_cols, out_line, gain_all, seg_all, gate_up_here, down_here16 = gather_in(
        block_input,
        qkv_weight,
        out_weight,
        gain_tile,
        seg_tile,
        gate_up_weight,
        down_weight,
        n_dp,
        n_z,
    )
    cot_late, _ = lax.optimization_barrier((cotangent, gain_all))
    cot_all = lax.all_gather(cot_late, "seq", axis=1, tiled=True)
    gain_one = gain_all[:, 0, :owned].reshape(1, width)
    gain_two = gain_all[:, 0, owned : 2 * owned].reshape(1, width)
    seg_here = lax.dynamic_slice(seg_all, (z_here // 2, z_here % 2, 0), (1, 1, full_len))[0]
    tables = attn_tables(seg_here)
    _, _, normed_one = rms_forward(rows_in.astype(jnp.float32), gain_one)
    qkv = jnp.dot(normed_one, qkv_cols, preferred_element_type=jnp.float32)
    turned, lse, attended16, out_rows = attn_forward(qkv, *tables, out_line, full_len, groups, n_dp)
    attn_part = times_transpose(attended16, out_rows)
    resid_all, gate_up_cols = share_resid(
        attn_part.astype(jnp.bfloat16), rows_in, gate_up_here, n_dp, n_z
    )
    total_rows = seqs_here * full_len
    down_late, _ = lax.optimization_barrier((down_here16, resid_all))
    down_rows = lax.all_gather(down_late, "dp", axis=1, tiled=True)
    normed_two, gate16, up16, hidden16 = hidden_forward(resid_all.reshape(total_rows, width), gain_two, gate_up_cols)
    gate_part = gate16.astype(jnp.float32)
    up_part = up16.astype(jnp.float32)
    sigmoid_gate = jax.nn.sigmoid(gate_part)
    active = gate_part * sigmoid_gate
    cot_rows = cot_all.reshape(total_rows, width)
    d_hidden = times_transpose(cot_rows, down_rows)
    d_gate = d_hidden * up_part * sigmoid_gate * (1.0 + gate_part * (1.0 - sigmoid_gate))
    d_up = d_hidden * active
    d_gate16 = d_gate.astype(jnp.bfloat16)
    d_up16 = d_up.astype(jnp.bfloat16)
    d_gate_up16 = jnp.concatenate([d_gate16, d_up16], 1)
    gate_up_term = contract_rows(normed_two, d_gate_up16).astype(jnp.bfloat16)
    gate_up_sum = lax.psum_scatter(gate_up_term, "dp", scatter_dimension=0, tiled=True)
    down_term = contract_rows(cot_rows, hidden16).astype(jnp.bfloat16)
    down_sum = lax.psum_scatter(down_term, "dp", scatter_dimension=0, tiled=True)
    d_resid16, gain_two_part, down_part = sum_line(
        d_gate16, d_up16, gate_up_cols, resid_all, cot_all, gain_two, hidden16, down_rows, n_z
    )
    down_here = lax.psum_scatter(
        down_part.reshape(resid_all.shape), "seq", scatter_dimension=1, tiled=True
    )
    down_here = down_here.astype(jnp.float32)
    resid_here = lax.dynamic_slice_in_dim(resid_all, z_here * local_len, local_len, 1)
    output = (resid_here.astype(jnp.float32) + down_here).astype(jnp.bfloat16)
    d_attended = jnp.dot(d_resid16, out_rows, preferred_element_type=jnp.float32).astype(jnp.bfloat16)
    d_qkv16 = attn_backward(turned, d_attended, lse, *tables, full_len, groups)
    out_term = contract_rows(d_resid16, attended16).astype(jnp.bfloat16)
    input_grad, grad_qkv, grad_out, gain_sums = hand_out(
        d_qkv16,
        normed_one,
        rows_in,
        d_resid16,
        gain_one,
        gain_two_part,
        qkv_cols,
        out_term,
        n_dp,
        n_z,
    )
    grad_gate_up, w_gu, m_gu, v_gu = adam_wide(
        gate_up_sum, gate_up_weight, first_gate_up, second_gate_up
    )
    grad_down, w_down, m_down, v_down = adam_turned(
        down_sum, down_weight, first_down, second_down
    )
    flat = lax.axis_index("dp") * n_z + z_here
    gain_sums = lax.dynamic_slice(
        jnp.sum(gain_sums.reshape(2, 8, LANES), axis=1), (0, flat * owned % LANES), (2, owned)
    )
    grad_gain_one = gain_sums[0]
    grad_gain_two = gain_sums[1]
    w_one, m_one, v_one = adam_update(attn_gain, grad_gain_one, first_attn_gain, second_attn_gain)
    w_qkv, m_qkv, v_qkv = adam_update(qkv_weight, grad_qkv, first_qkv, second_qkv)
    w_out, m_out, v_out = adam_update(out_weight, grad_out, first_out, second_out)
    w_two, m_two, v_two = adam_update(mlp_gain, grad_gain_two, first_mlp_gain, second_mlp_gain)
    return (
        output,
        input_grad,
        grad_gain_one,
        grad_qkv,
        grad_out,
        grad_gain_two,
        grad_gate_up,
        grad_down,
        w_one,
        w_qkv,
        w_out,
        w_two,
        w_gu,
        w_down,
        m_one,
        m_qkv,
        m_out,
        m_two,
        m_gu,
        m_down,
        v_one,
        v_qkv,
        v_out,
        v_two,
        v_gu,
        v_down,
    )


def solution(mesh):
    in_specs = (
        P("dp", "seq", None),
        P("dp", None),
        P("dp", "seq", None),
        P(("dp", "seq")),
        P("dp", "seq"),
        P("seq", "dp"),
        P(("dp", "seq")),
        P("dp", None, "seq"),
        P("seq", "dp"),
        P(("dp", "seq")),
        P("dp", "seq"),
        P("seq", "dp"),
        P(("dp", "seq")),
        P("dp", None, "seq"),
        P("seq", "dp"),
        P(("dp", "seq")),
        P("dp", "seq"),
        P("seq", "dp"),
        P(("dp", "seq")),
        P("dp", None, "seq"),
        P("seq", "dp"),
    )
    out_specs = (
        P("dp", "seq", None),
        P("dp", "seq", None),
        P(("dp", "seq")),
        P("dp", "seq"),
        P("seq", "dp"),
        P(("dp", "seq")),
        P("dp", None, "seq"),
        P("seq", "dp"),
        P(("dp", "seq")),
        P("dp", "seq"),
        P("seq", "dp"),
        P(("dp", "seq")),
        P("dp", None, "seq"),
        P("seq", "dp"),
        P(("dp", "seq")),
        P("dp", "seq"),
        P("seq", "dp"),
        P(("dp", "seq")),
        P("dp", None, "seq"),
        P("seq", "dp"),
        P(("dp", "seq")),
        P("dp", "seq"),
        P("seq", "dp"),
        P(("dp", "seq")),
        P("dp", None, "seq"),
        P("seq", "dp"),
    )
    return jax.shard_map(layer_step, mesh=mesh, in_specs=in_specs, out_specs=out_specs, check_vma=False)
```

```python
import functools

import jax
import jax.numpy as jnp
from jax import lax
from jax.experimental import pallas as pl
from jax.experimental.pallas import tpu as pltpu
from jax.sharding import PartitionSpec as P


HEADS = 32
KV_HEADS = 8
norm_eps = 1e-05
beta_one = 0.9
beta_two = 0.95
learn_rate = 0.01
weight_decay = 0.1
adam_eps = 1e-08
step_count = 10.0
masked_score = -1e30


HEAD_DIM = 64
LANES = 128


def dot_t(a, b):
    return lax.dot_general(a, b, (((1,), (1,)), ((), ())), preferred_element_type=jnp.float32)


def dot_n(a, b):
    return lax.dot_general(a, b, (((1,), (0,)), ((), ())), preferred_element_type=jnp.float32)


def dot_c(a, b):
    return lax.dot_general(a, b, (((0,), (0,)), ((), ())), preferred_element_type=jnp.float32)


def swap_halves(u):
    lane = lax.broadcasted_iota(jnp.int32, u.shape, 1)
    return jnp.where(lane % 64 < 32, pltpu.roll(u, 96, 1), pltpu.roll(u, 32, 1))


def turn(u, cos_wide, sin_wide):
    return u * cos_wide + swap_halves(u) * sin_wide


def key_start(block, q_rows, reach):
    return max(0, (block * q_rows - reach + 1) // q_rows * q_rows)


def attn_forward_kernel(pairs, q_rows, reach, qkv_ref, cos_ref, sin_ref, seg_col_ref, seg_row_ref,
                        turned_ref, lse_ref, out_ref):
    full_len = qkv_ref.shape[0]
    lane = lax.broadcasted_iota(jnp.int32, (full_len, LANES), 1)
    low = lane < HEAD_DIM
    cos_q = cos_ref[...]
    sin_q = sin_ref[...]
    kv = qkv_ref[:, pairs * LANES:].astype(jnp.float32)
    kv16 = turn(kv, jnp.where(low, cos_q, 1.0), jnp.where(low, sin_q, 0.0)).astype(jnp.bfloat16)
    turned_ref[:, pairs * LANES:] = kv16
    kv32 = kv16.astype(jnp.float32)
    rolled = pltpu.roll(kv32, HEAD_DIM, 1)
    zero = jnp.zeros_like(kv32)
    keys = (jnp.where(low, kv32, zero).astype(jnp.bfloat16), jnp.where(low, zero, rolled).astype(jnp.bfloat16))
    vals = (jnp.where(low, rolled, zero).astype(jnp.bfloat16), jnp.where(low, zero, kv32).astype(jnp.bfloat16))
    for pair in range(pairs):
        cols = slice(pair * LANES, (pair + 1) * LANES)
        query = turn(qkv_ref[:, cols].astype(jnp.float32), cos_q, sin_q) .astype(jnp.bfloat16)
        turned_ref[:, cols] = query
    for block in range(full_len // q_rows):
        first = key_start(block, q_rows, reach)
        last = (block + 1) * q_rows
        rows = slice(block * q_rows, last)
        span = slice(first, last)
        i = lax.broadcasted_iota(jnp.int32, (q_rows, last - first), 0) + block * q_rows
        j = lax.broadcasted_iota(jnp.int32, (q_rows, last - first), 1) + first
        allowed = (j <= i) & (seg_col_ref[rows, :1] == seg_row_ref[:1, span])
        for pair in range(pairs):
            cols = slice(pair * LANES, (pair + 1) * LANES)
            query = turned_ref[rows, cols]
            total = None
            for half in range(2):
                scores = dot_t(query, keys[half][span]) * (HEAD_DIM ** -0.5)
                scores = jnp.where(allowed, scores, masked_score)
                top = jnp.max(scores, axis=1, keepdims=True)
                lse = top + jnp.log(jnp.sum(jnp.exp(scores - top), axis=1, keepdims=True))
                probs = jnp.exp(scores - lse).astype(jnp.bfloat16)
                part = dot_n(probs, vals[half][span])
                total = part if total is None else total + part
                head = 2 * pair + half
                lse_ref[rows, head:head + 1] = lse
            out_ref[rows, cols] = total.astype(jnp.bfloat16)


def attn_backward_kernel(pairs, q_rows, reach, turned_ref, d_out_ref, lse_ref, cos_ref, sin_ref, seg_col_ref,
                         seg_row_ref, grad_ref, dk_ref, dv_ref):
    full_len = turned_ref.shape[0]
    lane = lax.broadcasted_iota(jnp.int32, (full_len, LANES), 1)
    low = lane < HEAD_DIM
    kv32 = turned_ref[:, pairs * LANES:].astype(jnp.float32)
    rolled = pltpu.roll(kv32, HEAD_DIM, 1)
    zero = jnp.zeros_like(kv32)
    keys = (jnp.where(low, kv32, zero).astype(jnp.bfloat16), jnp.where(low, zero, rolled).astype(jnp.bfloat16))
    vals = (jnp.where(low, rolled, zero).astype(jnp.bfloat16), jnp.where(low, zero, kv32).astype(jnp.bfloat16))
    dk_ref[...] = jnp.zeros_like(dk_ref)
    dv_ref[...] = jnp.zeros_like(dv_ref)
    low_rows = low[:q_rows]
    scale = HEAD_DIM ** -0.5
    for block in range(full_len // q_rows):
        first = key_start(block, q_rows, reach)
        last = (block + 1) * q_rows
        rows = slice(block * q_rows, last)
        span = slice(first, last)
        i = lax.broadcasted_iota(jnp.int32, (q_rows, last - first), 0) + block * q_rows
        j = lax.broadcasted_iota(jnp.int32, (q_rows, last - first), 1) + first
        allowed = (j <= i) & (seg_col_ref[rows, :1] == seg_row_ref[:1, span])
        cos_q = cos_ref[rows]
        sin_q = sin_ref[rows]
        for pair in range(pairs):
            cols = slice(pair * LANES, (pair + 1) * LANES)
            query = turned_ref[rows, cols]
            d_out = d_out_ref[rows, cols]
            q32 = query.astype(jnp.float32)
            o32 = d_out.astype(jnp.float32)
            d_query = None
            d_key = None
            d_val = None
            for half in range(2):
                keep = low_rows if half == 0 else ~low_rows
                q_only = jnp.where(keep, q32, 0.0).astype(jnp.bfloat16)
                o_only = jnp.where(keep, o32, 0.0).astype(jnp.bfloat16)
                head = 2 * pair + half
                scores = dot_t(query, keys[half][span]) * scale
                scores = jnp.where(allowed, scores, masked_score)
                probs = jnp.exp(scores - lse_ref[rows, head:head + 1])
                d_probs = dot_t(d_out, vals[half][span])
                delta = jnp.sum(probs * d_probs, axis=1, keepdims=True)
                d_scores = (probs * (d_probs - delta) * scale).astype(jnp.bfloat16)
                probs16 = probs.astype(jnp.bfloat16)
                dq = dot_n(d_scores, keys[half][span])
                dk = dot_c(d_scores, q_only)
                dv = dot_c(probs16, o_only)
                d_query = dq if d_query is None else d_query + dq
                d_key = dk if d_key is None else d_key + dk
                d_val = dv if d_val is None else d_val + dv
            dk_ref[span] = dk_ref[span] + d_key
            dv_ref[span] = dv_ref[span] + d_val
            grad_ref[rows, cols] = turn(d_query, cos_q, -sin_q).astype(jnp.bfloat16)
    d_key = dk_ref[...]
    d_val = dv_ref[...]
    d_key = d_key + pltpu.roll(d_key, HEAD_DIM, 1)
    d_val = d_val + pltpu.roll(d_val, HEAD_DIM, 1)
    d_key = turn(d_key, cos_ref[...], -sin_ref[...])
    grad_ref[:, pairs * LANES:] = jnp.where(low, d_key, d_val).astype(jnp.bfloat16)


def attn_specs(full_len, width):
    line = pl.BlockSpec((full_len, width), lambda s, g: (s, g))
    table = pl.BlockSpec((full_len, LANES), lambda s, g: (s, 0))
    row = pl.BlockSpec((8, full_len), lambda s, g: (s, 0))
    return line, table, row


Q_ROWS = 128
REACH = 256


def attn_gather_kernel(n_dp, pairs, q_rows, reach, qkv_ref, cos_ref, sin_ref, seg_col_ref, seg_row_ref, vo_ref,
                       turned_ref, lse_ref, out_ref, wo, d_s, d_r, loc):
    _, z, pair, c = place()
    n_d = n_dp // 2
    step = pl.program_id(1)
    steps = pl.num_programs(1)
    rows = vo_ref.shape[0]
    parts = 2
    part = rows // parts // 2

    def spot(owner, t, h):
        return wo.at[pl.ds(pl.multiple_of(owner * rows + (2 * t + h) * part, part), part)]

    spread = Spread(n_d, pair, c, z, parts, spot, d_s, d_r)
    keep = pltpu.make_async_copy(vo_ref, wo.at[pl.ds(pl.multiple_of(pair * rows, rows), rows)], loc)

    @pl.when(step == 0)
    def _():
        keep.start()
        barrier = pltpu.get_barrier_semaphore()
        for k in range(1, n_d):
            pl.semaphore_signal(barrier, inc=1, device_id=(2 * (pair ^ k) + c, z), device_id_type=MESH)
        pl.semaphore_wait(barrier, n_d - 1)
        keep.wait()
        for t in range(parts):
            spread.own(t)

    attn_forward_kernel(pairs, q_rows, reach, qkv_ref, cos_ref, sin_ref, seg_col_ref, seg_row_ref, turned_ref, lse_ref, out_ref)

    @pl.when(step == steps - 2)
    def _():
        spread.pass_on(0)

    @pl.when(step == steps - 1)
    def _():
        spread.pass_on(1)
        spread.finish()


def attn_forward(qkv, cos, sin, seg_col, seg_row, vo, full_len, groups, n_dp):
    pairs = groups // 2
    width = (groups + 2) * HEAD_DIM
    seqs = qkv.shape[0] // full_len
    kv = qkv.shape[1] // width
    n_d = n_dp // 2
    line, table, row = attn_specs(full_len, width)
    outw = pl.BlockSpec((full_len, groups * HEAD_DIM), lambda s, g: (s, g))
    rows = seqs * full_len
    return pl.pallas_call(
        functools.partial(attn_gather_kernel, n_dp, pairs, Q_ROWS, REACH),
        grid=(seqs, kv),
        in_specs=[line, table, table, table, row, VMEM_SPEC],
        out_specs=[line, pl.BlockSpec((full_len, LANES), lambda s, g: (s, g)), outw, ANY_SPEC],
        out_shape=[
            jax.ShapeDtypeStruct((rows, kv * width), jnp.bfloat16),
            jax.ShapeDtypeStruct((rows, kv * LANES), jnp.float32),
            jax.ShapeDtypeStruct((rows, kv * groups * HEAD_DIM), jnp.bfloat16),
            jax.ShapeDtypeStruct((n_d * vo.shape[0], vo.shape[1]), jnp.bfloat16),
        ],
        scratch_shapes=[DMA((n_d - 1, 2, 2)), DMA((n_d - 1, 2, 2)), DMA],
        compiler_params=pltpu.CompilerParams(collective_id=4, has_side_effects=True),
        cost_estimate=pl.CostEstimate(flops=4 * rows * full_len * kv * LANES * groups, bytes_accessed=150_000_000, transcendentals=0),
        name="attn_forward",
    )(qkv, cos, sin, seg_col, seg_row, vo)


def attn_backward(turned, d_out, lse, cos, sin, seg_col, seg_row, full_len, groups):
    pairs = groups // 2
    width = (groups + 2) * HEAD_DIM
    seqs = turned.shape[0] // full_len
    kv = turned.shape[1] // width
    line, table, row = attn_specs(full_len, width)
    outw = pl.BlockSpec((full_len, groups * HEAD_DIM), lambda s, g: (s, g))
    rows = seqs * full_len
    return pl.pallas_call(
        functools.partial(attn_backward_kernel, pairs, Q_ROWS, REACH),
        grid=(seqs, kv),
        in_specs=[line, outw, pl.BlockSpec((full_len, LANES), lambda s, g: (s, g)), table, table, table, row],
        out_specs=line,
        out_shape=jax.ShapeDtypeStruct((rows, kv * width), jnp.bfloat16),
        scratch_shapes=[pltpu.VMEM((full_len, LANES), jnp.float32)] * 2,
        cost_estimate=pl.CostEstimate(flops=10 * rows * full_len * kv * LANES * groups, bytes_accessed=rows * kv * width * 6, transcendentals=0),
        name="attn_backward",
    )(turned, d_out, lse, cos, sin, seg_col, seg_row)


def attn_tables(segment_ids):
    seqs, full_len = segment_ids.shape
    earlier = (segment_ids[..., None, :] < segment_ids[..., :, None]).astype(jnp.int32)
    positions = jnp.arange(full_len, dtype=jnp.int32) - jnp.sum(earlier, axis=-1, dtype=jnp.int32)
    inverse = 500000.0 ** (-2.0 * jnp.arange(HEAD_DIM // 2, dtype=jnp.float32) / HEAD_DIM)
    angles = positions.astype(jnp.float32)[..., None] * inverse
    cos = jnp.cos(angles)
    sin = jnp.sin(angles)
    cos = jnp.concatenate([cos] * 4, -1).reshape(seqs * full_len, LANES)
    sin = jnp.concatenate([-sin, sin] * 2, -1).reshape(seqs * full_len, LANES)
    seg_col = jnp.broadcast_to(segment_ids[:, :, None], (seqs, full_len, LANES)).reshape(seqs * full_len, LANES)
    seg_row = jnp.broadcast_to(segment_ids[:, None, :], (seqs, 8, full_len)).reshape(seqs * 8, full_len)
    return cos, sin, seg_col, seg_row


MESH = pl.DeviceIdType.MESH
VMEM_SPEC = pl.BlockSpec(memory_space=pltpu.VMEM)
ANY_SPEC = pl.BlockSpec(memory_space=pl.ANY)
DMA = pltpu.SemaphoreType.DMA


def place():
    d = lax.axis_index("dp")
    z = lax.axis_index("seq")
    return d, z, d // 2, d % 2


def remote(src, dst, send, recv, dev):
    return pltpu.make_async_remote_copy(
        src_ref=src, dst_ref=dst, send_sem=send, recv_sem=recv, device_id=dev, device_id_type=MESH
    )


def greet_all(n_dp, n_z, d, z):
    barrier = pltpu.get_barrier_semaphore()
    me = d * n_z + z

    def one(o, carry):
        other = lax.rem(me + o, n_dp * n_z)
        pl.semaphore_signal(barrier, inc=1, device_id=(other // n_z, lax.rem(other, n_z)), device_id_type=MESH)
        return carry

    lax.fori_loop(1, n_dp * n_z, one, 0)
    pl.semaphore_wait(barrier, n_dp * n_z - 1)


def greet_line(n_z, d, z, extra=()):
    barrier = pltpu.get_barrier_semaphore()
    c = d % 2
    for o in range(n_z):
        zz = lax.rem(z + o, n_z)
        for core in range(2):
            if o == 0 and core == 0:
                continue
            pl.semaphore_signal(barrier, inc=1, device_id=(d - c + lax.rem(c + core, 2), zz), device_id_type=MESH)
    for dev in extra:
        pl.semaphore_signal(barrier, inc=1, device_id=dev, device_id_type=MESH)
    pl.semaphore_wait(barrier, 2 * n_z - 1 + len(extra))


def block_at(ref, shape, row, col):
    return ref.at[pl.ds(pl.multiple_of(row * shape[0], shape[0]), shape[0]),
                  pl.ds(pl.multiple_of(col * shape[1], shape[1]), shape[1])]


class Spread:
    def __init__(self, n_d, pair, c, z, parts, spot, send, recv):
        self.n_d, self.pair, self.parts, self.spot = n_d, pair, parts, spot
        self.send, self.recv = send, recv
        self.dev = lambda k: (2 * (pair ^ k) + c, z)

    def copy(self, slot, owner, t, h, to):
        at = self.spot(owner, t, h)
        return remote(at, at, self.send.at[slot, t, h], self.recv.at[slot, t, h], self.dev(to))

    def own(self, t):
        if self.n_d == 4:
            for h in range(2):
                self.copy(0, self.pair, t, h, 1).start()
                self.copy(1, self.pair, t, 1 - h, 2).start()
        else:
            for k in range(1, self.n_d):
                for h in range(2):
                    self.copy(k - 1, self.pair, t, h, k).start()

    def pass_on(self, t):
        if self.n_d == 4:
            self.copy(0, self.pair ^ 1, t, 0, 1).wait_recv()
            self.copy(2, self.pair ^ 1, t, 0, 2).start()
            self.copy(1, self.pair ^ 2, t, 1, 2).wait_recv()
            self.copy(2, self.pair ^ 2, t, 1, 1).start()

    def rest(self, t):
        if self.n_d == 4:
            self.copy(0, self.pair ^ 1, t, 1, 1).wait_recv()
            self.copy(1, self.pair ^ 2, t, 0, 2).wait_recv()
        else:
            for k in range(1, self.n_d):
                for h in range(2):
                    self.copy(k - 1, self.pair ^ k, t, h, k).wait_recv()

    def far(self, t):
        if self.n_d == 4:
            for h in range(2):
                self.copy(2, self.pair ^ 3, t, h, 1).wait_recv()

    def sent(self):
        for t in range(self.parts):
            for h in range(2):
                for slot in range(self.n_d - 1):
                    self.copy(slot, self.pair, t, h, 1).wait_send()

    def finish(self):
        for t in range(self.parts):
            if self.n_d == 4:
                self.copy(0, self.pair ^ 1, t, 1, 1).wait_recv()
                self.copy(1, self.pair ^ 2, t, 0, 2).wait_recv()
                for h in range(2):
                    self.copy(2, self.pair ^ 3, t, h, 1).wait_recv()
                    for slot in range(3):
                        self.copy(slot, self.pair, t, h, 1).wait_send()
            else:
                for k in range(1, self.n_d):
                    for h in range(2):
                        self.copy(k - 1, self.pair ^ k, t, h, k).wait_recv()
                        self.copy(k - 1, self.pair, t, h, k).wait_send()


def gather_in_kernel(n_dp, n_z, x_ref, w_wide, v_wide, g_ref, s_ref, gu_ref, dw_ref, xs, wq, vo, ga, sg, gu16, dw16,
                     w_ref, v_ref, gu_in, gu_out, dw_in, dw_out,
                     x_s, x_r, f_s, f_r, w_s, w_r, v_s, v_r, d_s, d_r, g_s, g_r, s_s, s_r, loc, gu_is, gu_os, dw_is, dw_os, w_f, v_f):
    d, z, pair, c = place()
    n_d = n_dp // 2
    me = d * n_z + z
    total = n_dp * n_z
    rows = x_ref.shape[1]
    half = rows // 2
    shape = w_ref.shape
    cz = z // 2
    chunks = gu_ref.shape[0] // WIDE_ROWS
    gu_width = gu_ref.shape[2]

    def chunk_in(i, slot):
        return pltpu.make_async_copy(gu_ref.at[pl.ds(pl.multiple_of(i * WIDE_ROWS, WIDE_ROWS), WIDE_ROWS)], gu_in.at[slot], gu_is.at[slot])

    def chunk_out(i, slot):
        return pltpu.make_async_copy(gu_out.at[slot], gu16.at[pl.ds(pl.multiple_of(i * WIDE_ROWS, WIDE_ROWS), WIDE_ROWS)], gu_os.at[slot])

    dw_rows = dw_in.shape[1]

    def dw_chunk_in(i, slot):
        return pltpu.make_async_copy(dw_ref.at[pl.ds(pl.multiple_of(i * dw_rows, dw_rows), dw_rows)], dw_in.at[slot], dw_is.at[slot])

    def dw_chunk_out(i, slot):
        return pltpu.make_async_copy(dw_out.at[slot], dw16.at[pl.ds(pl.multiple_of(i * dw_rows, dw_rows), dw_rows)], dw_os.at[slot])

    def round_chunks(low, high):
        def one(i, carry):
            slot = lax.rem(i, 2)

            @pl.when(i + 1 < chunks)
            def _():
                chunk_in(i + 1, 1 - slot).start()
                dw_chunk_in(i + 1, 1 - slot).start()

            chunk_in(i, slot).wait()
            dw_chunk_in(i, slot).wait()

            @pl.when(i >= 2)
            def _():
                chunk_out(i - 2, slot).wait()
                dw_chunk_out(i - 2, slot).wait()

            for n in range(2):
                gu_out[slot, :, n * gu_width : (n + 1) * gu_width] = gu_in[slot, :, n].astype(jnp.bfloat16)
            dw_out[slot] = dw_in[slot].astype(jnp.bfloat16)
            chunk_out(i, slot).start()
            dw_chunk_out(i, slot).start()
            return carry

        lax.fori_loop(low, high, one, 0)

    chunk_in(0, 0).start()
    dw_chunk_in(0, 0).start()
    w_ref[...] = w_wide[...].astype(jnp.bfloat16)
    v_ref[...] = v_wide[...].T.astype(jnp.bfloat16)
    greet_all(n_dp, n_z, d, z)

    def line_stage(src, dst, send, recv, spare, wait):
        for o, zz in ((0, z), (1, z - 1), (2, z + 1)):
            copy = remote(src, dst, send.at[o], recv.at[c, z % 2], (2 * pair + cz, zz))
            act = copy.wait_send if wait else copy.start
            if o == 0:
                pl.when(c != cz)(act)
                if not wait:
                    pl.when(c == cz)(pltpu.make_async_copy(src, dst, loc.at[spare]).start)
            else:
                pl.when(zz >= 0 if o == 1 else zz <= n_z - 1)(act)

    def line_relay(blk, send, recv, core, b, wait):
        j = 2 * c + b
        to = jnp.where(z > j, z + 1, z - 1)
        ok = (z != j) & (to >= 0) & (to <= n_z - 1)
        copy = remote(blk, blk, send, recv.at[core, b], (2 * pair + c, to))
        pl.when(ok)(copy.wait_send if wait else copy.start)

    my_block = block_at(wq, shape, d, z % 2)
    line_stage(w_ref, my_block, w_s, w_r, 0, False)

    for i in range(2):
        for h in range(2):
            src = x_ref.at[i, pl.ds(h * half, half)]
            dst = xs.at[pl.ds(pl.multiple_of(z * rows + h * half, half), half)]
            zz = 2 * c + i
            mine = (h == c) & (zz == z)
            copy = remote(src, dst, x_s.at[i, h], x_r.at[z], (2 * pair + h, zz))
            pl.when(jnp.logical_not(mine))(copy.start)
            pl.when(mine)(lambda src=src, dst=dst: pltpu.make_async_copy(src, dst, loc.at[1]).start())

    seg_copy = remote(s_ref, sg.at[c], s_s, s_r, (2 * pair + 1 - c, z))
    seg_copy.start()
    own_seg = pltpu.make_async_copy(s_ref, sg.at[c], loc.at[2])
    own_seg.start()
    own_gain = pltpu.make_async_copy(g_ref, ga.at[me], loc.at[3])
    own_gain.start()

    def send_gain(o, carry):
        other = lax.rem(me + o, total)
        remote(g_ref, ga.at[me], g_s, g_r, (other // n_z, lax.rem(other, n_z))).start()
        return carry

    lax.fori_loop(1, total, send_gain, 0)

    first = jnp.where(c == cz, z % 2, 1 - c)

    def turn_of(t):
        return t % 2, (first if t < 2 else 1 - first)

    def spot(owner, t, h):
        core, b = turn_of(t)
        part = shape[0] // 2
        return wq.at[pl.ds(pl.multiple_of((2 * owner + core) * shape[0] + h * part, part), part),
                     pl.ds(pl.multiple_of(b * shape[1], shape[1]), shape[1])]

    spread = Spread(n_d, pair, c, z, 4, spot, d_s, d_r)
    for t in range(4):
        core, b = turn_of(t)
        blk = block_at(wq, shape, 2 * pair + core, b)
        mine = (core == c) & (2 * c + b == z)
        arrive = remote(w_ref, blk, w_s.at[0], w_r.at[core, b], (d, z))
        pl.when(jnp.logical_not(mine))(arrive.wait_recv)
        pl.when(mine)(lambda blk=blk: pltpu.make_async_copy(w_ref, blk, loc.at[0]).wait())
        line_relay(blk, w_f.at[t], w_r, core, b, False)
        spread.own(t)
        if t == 0:
            line_stage(v_ref, block_at(vo, v_ref.shape, c, z % 2), v_s, v_r, 4, False)
        if t > 0:
            spread.pass_on(t - 1)
        round_chunks(t * chunks // 4, (t + 1) * chunks // 4)

    def out_unit(t, wait):
        core, b = turn_of(t)
        blk = block_at(vo, v_ref.shape, core, b)
        mine = (core == c) & (2 * c + b == z)
        if not wait:
            pl.when(jnp.logical_not(mine))(remote(blk, blk, v_s.at[0], v_r.at[core, b], (d, z)).wait_recv)
            pl.when(mine)(pltpu.make_async_copy(v_ref, blk, loc.at[4]).wait)
        line_relay(blk, v_f.at[t], v_r, core, b, wait)

    spread.pass_on(3)
    for o in range(n_z):
        zs = lax.rem(z + o, n_z)
        src = xs.at[pl.ds(pl.multiple_of(zs * rows + c * half, half), half)]
        mine = (cz == c) & (zs == z)
        arrive = remote(src, src, x_s.at[0, 0], x_r.at[zs], (d, z))
        pl.when(jnp.logical_not(mine))(arrive.wait_recv)
        pl.when(mine)(lambda src=src: pltpu.make_async_copy(src, src, loc.at[1]).wait())
        remote(src, src, f_s.at[zs], f_r.at[zs], (2 * pair + 1 - c, z)).start()
        out_unit(o, False)

    line_stage(w_ref, my_block, w_s, w_r, 0, True)
    line_stage(v_ref, block_at(vo, v_ref.shape, c, z % 2), v_s, v_r, 4, True)
    for i in range(2):
        for h in range(2):
            src = x_ref.at[i, pl.ds(h * half, half)]
            mine = (h == c) & (2 * c + i == z)
            copy = remote(src, src, x_s.at[i, h], x_r.at[0], (d, z))
            pl.when(jnp.logical_not(mine))(copy.wait_send)
    for zs in range(n_z):
        src = xs.at[pl.ds(zs * rows, half)]
        copy = remote(src, src, f_s.at[zs], f_r.at[zs], (d, z))
        copy.wait_send()
        copy.wait_recv()
    for t in range(4):
        core, b = turn_of(t)
        line_relay(block_at(wq, shape, 2 * pair + core, b), w_f.at[t], w_r, core, b, True)
        out_unit(t, True)
    for i in range(max(0, chunks - 2), chunks):
        chunk_out(i, i % 2).wait()
        dw_chunk_out(i, i % 2).wait()
    seg_copy.wait_send()
    remote(s_ref, sg.at[1 - c], s_s, s_r, (d, z)).wait_recv()
    own_seg.wait()
    own_gain.wait()
    many = ga.at[pl.ds(0, total - 1)]
    gains = remote(many, many, g_s, g_r, (d, z))
    gains.wait_send()
    gains.wait_recv()
    spread.finish()


def gather_in(x_loc, w, v, gain_tile, seg_tile, wide, down, n_dp, n_z):
    _, rows, width = x_loc.shape
    n_d = n_dp // 2
    total = n_dp * n_z
    b16 = jnp.bfloat16
    down_rows = down.shape[0] * WIDE_ROWS // wide.shape[0]
    return pl.pallas_call(
        functools.partial(gather_in_kernel, n_dp, n_z),
        in_specs=[VMEM_SPEC] * 5 + [ANY_SPEC] * 2,
        out_specs=[ANY_SPEC] * 7,
        out_shape=[
            jax.ShapeDtypeStruct((rows * n_z, width), x_loc.dtype),
            jax.ShapeDtypeStruct((w.shape[0] * n_dp, 2 * w.shape[1]), b16),
            jax.ShapeDtypeStruct((v.shape[1] * 2, 2 * v.shape[0]), b16),
            jax.ShapeDtypeStruct((total,) + gain_tile.shape, gain_tile.dtype),
            jax.ShapeDtypeStruct((2,) + seg_tile.shape, seg_tile.dtype),
            jax.ShapeDtypeStruct((wide.shape[0], wide.shape[1] * wide.shape[2]), b16),
            jax.ShapeDtypeStruct(down.shape, b16),
        ],
        scratch_shapes=[
            pltpu.VMEM(w.shape, b16), pltpu.VMEM(v.shape[::-1], b16),
            pltpu.VMEM((2, WIDE_ROWS) + wide.shape[1:], jnp.float32),
            pltpu.VMEM((2, WIDE_ROWS, wide.shape[1] * wide.shape[2]), b16),
            pltpu.VMEM((2, down_rows, down.shape[1]), jnp.float32), pltpu.VMEM((2, down_rows, down.shape[1]), b16),
            DMA((2, 2)), DMA((n_z,)), DMA((n_z,)), DMA((n_z,)), DMA((3,)), DMA((2, 2)), DMA((3,)), DMA((2, 2)),
            DMA((n_d - 1, 4, 2)), DMA((n_d - 1, 4, 2)), DMA, DMA, DMA, DMA, DMA((5,)), DMA((2,)), DMA((2,)), DMA((2,)), DMA((2,)), DMA((4,)), DMA((4,)),
        ],
        compiler_params=pltpu.CompilerParams(collective_id=1, has_side_effects=True),
        cost_estimate=pl.CostEstimate(flops=0, bytes_accessed=200_000_000, transcendentals=0),
        name="gather_in",
    )(x_loc, w, v, gain_tile, seg_tile, wide, down)


def share_resid_kernel(n_dp, n_z, part_ref, x_ref, w_ref, out, wall, got, buf, p_s, p_r, u_s, u_r, d_s, d_r, c_s, c_r, loc):
    d, z, pair, c = place()
    n_d = n_dp // 2
    cz = z // 2
    full = x_ref.shape[0]
    half = full // 2
    unit = half // 2
    w_rows = w_ref.shape[0]
    parts = 4
    piece = w_rows // parts
    own_copy = pltpu.make_async_copy(w_ref, wall.at[pl.ds(pl.multiple_of(d * w_rows, w_rows), w_rows)], loc.at[2])
    own_copy.start()
    greet_line(n_z, d, z, [(2 * (pair ^ k) + c, z) for k in range(1, n_d)])
    mine = pl.ds(pl.multiple_of(c * half, half), half)
    theirs = pl.ds(pl.multiple_of((1 - c) * half, half), half)
    swap = remote(part_ref.at[theirs], got, p_s, p_r, (2 * pair + 1 - c, z))
    swap.start()

    def spot_w(owner, t, h):
        sub = piece // 2
        return wall.at[pl.ds(pl.multiple_of((2 * owner + c) * w_rows + (2 * t + h) * sub, sub), sub)]

    def across(k, t, core):
        at = wall.at[pl.ds(pl.multiple_of((2 * (pair ^ k) + core) * w_rows + t * piece, piece), piece)]
        return remote(at, at, c_s.at[k, t], c_r.at[k, t], (2 * pair + 1 - c, z))

    spread = Spread(n_d, pair, c, z, parts, spot_w, d_s, d_r)
    own_copy.wait()
    for t in range(parts):
        spread.own(t)
        across(0, t, c).start()

    swap.wait_recv()

    def add(r, carry):
        at = pl.ds(pl.multiple_of(r * 16, 16), 16)
        src = pl.ds(pl.multiple_of(c * half + r * 16, 16), 16)
        total = x_ref[src].astype(jnp.float32) + part_ref[src].astype(jnp.float32) + got[at].astype(jnp.float32)
        buf[at] = total.astype(jnp.bfloat16)
        return carry

    def spot(jl, h, k):
        return out.at[jl, pl.ds(pl.multiple_of(h * half + k * unit, unit), unit)]

    def sends(k, wait):
        src = buf.at[pl.ds(k * unit, unit)]
        dst = spot(z % 2, c, k)
        for o, zz in ((1, z - 1), (2, z + 1), (0, z)):
            copy = remote(src, dst, u_s.at[o, k], u_r.at[z % 2, c, k], (2 * pair + cz, zz))
            act = copy.wait_send if wait else copy.start
            if o == 0:
                keep = pltpu.make_async_copy(src, dst, loc.at[k])
                pl.when(c != cz)(act)
                pl.when(c == cz)(keep.wait if wait else keep.start)
            elif o == 1:
                pl.when(z > 0)(act)
            else:
                pl.when(z < n_z - 1)(act)

    per = unit // 16
    lax.fori_loop(0, per, add, 0)
    lax.fori_loop(per, per + per // 2, add, 0)
    sends(0, False)
    lax.fori_loop(per + per // 2, 2 * per, add, 0)
    swap.wait_send()
    sends(1, False)

    def relay(dist, sign, k, h, begin):
        j = z + sign * dist
        ok = (j >= 2 * c) & (j <= 2 * c + 1)
        to = z - sign
        more = (to >= 0) & (to <= n_z - 1)
        jl = lax.rem(j + n_z, 2)
        at = spot(jl, h, k)
        copy = remote(at, at, u_s.at[3 + (0 if sign < 0 else 1), 4 * jl + 2 * h + k], u_r.at[jl, h, k], (2 * pair + c, to))
        if begin:

            @pl.when(ok)
            def _():
                copy.wait_recv()
                pl.when(more)(copy.start)
        else:
            pl.when(ok & more)(copy.wait_send)

    def take(t):
        spread.pass_on(t)

    def rest(t):
        spread.rest(t)
        for k in range(1, n_d):
            if n_d != 4 or k != 3:
                across(k, t, c).start()

    def far(t):
        if n_d == 4:
            spread.far(t)
            across(3, t, c).start()

    links = []
    for t in range(parts):
        links += [(take, t), (rest, t)]
    links += [(far, t) for t in range(parts)]
    line = [(dist, k, h) for dist in range(1, n_z) for k in range(2) for h in range(2)]
    for n in range(max(len(links), len(line))):
        if n < len(line):
            dist, k, h = line[n]
            for sign in (-1, 1):
                relay(dist, sign, k, h, True)
        if n < len(links):
            links[n][0](links[n][1])

    @pl.when(c == cz)
    def _():
        for k in range(2):
            at = spot(z % 2, 1 - c, k)
            remote(at, at, u_s.at[0, 0], u_r.at[z % 2, 1 - c, k], (d, z)).wait_recv()

    for dist, k, h in line:
        for sign in (-1, 1):
            relay(dist, sign, k, h, False)
    sends(0, True)
    sends(1, True)
    spread.sent()
    for k in range(n_d):
        for t in range(parts):
            across(k, t, c).wait_send()
            across(k, t, 1 - c).wait_recv()


def share_resid(part, x, w, n_dp, n_z):
    full, width = x.shape
    n_d = n_dp // 2
    return pl.pallas_call(
        functools.partial(share_resid_kernel, n_dp, n_z),
        in_specs=[VMEM_SPEC] * 3,
        out_specs=[ANY_SPEC] * 2,
        out_shape=[
            jax.ShapeDtypeStruct((2, full, width), jnp.bfloat16),
            jax.ShapeDtypeStruct((n_dp * w.shape[0], w.shape[1]), jnp.bfloat16),
        ],
        scratch_shapes=[
            pltpu.VMEM((full // 2, width), jnp.bfloat16), pltpu.VMEM((full // 2, width), jnp.bfloat16),
            DMA, DMA, DMA((5, 8)), DMA((2, 2, 2)), DMA((n_d - 1, 4, 2)), DMA((n_d - 1, 4, 2)), DMA((n_d, 4)), DMA((n_d, 4)),
            DMA((3,)),
        ],
        compiler_params=pltpu.CompilerParams(collective_id=2, has_side_effects=True),
        cost_estimate=pl.CostEstimate(flops=0, bytes_accessed=200_000_000, transcendentals=0),
        name="share_resid",
    )(part, x, w)


CHUNKS = 8
GROUPS = 4


def sum_line_kernel(n_z, d_gate_ref, d_up_ref, w_ref, resid_all, cot_all, gain_ref, hid_ref, down_ref, d_out, gain_out,
                    rows_out, left, w, part, got, buf, resid_ref, cot_ref, hid, down, rows_buf,
                    s_s, s_r, p_s, p_r, loc, rows_sem, mul_sem, out_sem, left_sem, w_sem):
    d, z, pair, c = place()
    cz = z // 2
    full, width = buf.shape
    inner = d_gate_ref.shape[1]
    rows = full // CHUNKS
    group = full // GROUPS
    per = CHUNKS // GROUPS
    tile = 256
    tiles = width // tile
    lefts = []
    for q in range(GROUPS):
        for jl in range(2):
            for n, src in enumerate((d_gate_ref, d_up_ref)):
                lefts.append(pltpu.make_async_copy(
                    src.at[pl.ds(jl * full + q * group, group)],
                    left.at[pl.ds((2 * q + jl) * group, group), pl.ds(n * inner, inner)],
                    left_sem.at[q, jl, n],
                ))

    def w_copy(n):
        at = pl.ds(pl.multiple_of(n * tile, tile), tile)
        return pltpu.make_async_copy(w_ref.at[at], w.at[at], w_sem.at[n])

    fetch = (
        pltpu.make_async_copy(resid_all.at[z % 2], resid_ref, rows_sem.at[0]),
        pltpu.make_async_copy(cot_all.at[z % 2], cot_ref, rows_sem.at[1]),
    )
    factors = (pltpu.make_async_copy(hid_ref, hid, mul_sem.at[0]), pltpu.make_async_copy(down_ref, down, mul_sem.at[1]))
    for one in lefts[:4]:
        one.start()
    for n in range(tiles):
        w_copy(n).start()
    for one in tuple(lefts[4:]) + factors + fetch:
        one.start()
    greet_line(n_z, d, z)
    gain_out[...] = jnp.zeros_like(gain_out)
    own = c == cz

    def compute(q, low, high):
        if low == 0:
            for one in lefts[4 * q : 4 * q + 4]:
                one.wait()

        def one_tile(n, carry):
            if q == 0:
                w_copy(n).wait()
            at = pl.ds(pl.multiple_of(n * tile, tile), tile)
            value = dot_t(left[pl.ds(2 * q * group, 2 * group)], w[at])
            part[pl.ds(2 * q * group, 2 * group), at] = value.astype(jnp.bfloat16)
            return carry

        lax.fori_loop(low, high, one_tile, 0)

    def tile_out(j):
        at = pl.ds(pl.multiple_of(j * tile, tile), tile)
        return pltpu.make_async_copy(rows_buf.at[lax.rem(j, 2)], rows_out.at[:, at], out_sem.at[lax.rem(j, 2)])

    def multiply(low, high):
        if low == 0:
            for one in factors:
                one.wait()

        def one_tile(j, carry):
            pl.when(j >= 2)(tile_out(j - 2).wait)
            at = pl.ds(pl.multiple_of(j * tile, tile), tile)
            rows_buf[lax.rem(j, 2)] = dot_n(hid[...], down[:, at]).astype(jnp.bfloat16)
            tile_out(j).start()
            return carry

        lax.fori_loop(low, high, one_tile, 0)

    def part_start(jl, k):
        return (2 * (k // per) + jl) * group + k % per * rows

    def part_at(jl, k, r):
        return pl.ds(pl.multiple_of(part_start(jl, k) + r * 16, 16), 16)

    def copy_on(k, t, side, src):
        jl = jnp.bitwise_xor(c, t)
        to = z + 1 if side == 0 else z - 1
        return remote(src, got.at[side, jl, pl.ds(k * rows, rows)], s_s.at[t, k], s_r.at[side, jl, k], (2 * pair + c, to))

    def arrived(side, jl, k):
        at = got.at[side, jl, pl.ds(k * rows, rows)]
        return remote(at, at, s_s.at[0, 0], s_r.at[side, jl, k], (d, z))

    def send_step(k, t, edge_only, inner_only, wait):
        jl = jnp.bitwise_xor(c, t)
        j = 2 * c + jl
        for side in range(2):
            going = (z < j) if side == 0 else (z > j)
            edge = (z == 0) if side == 0 else (z == n_z - 1)
            raw = copy_on(k, t, side, part.at[pl.ds(pl.multiple_of(part_start(jl, k), rows), rows)])
            passed = copy_on(k, t, side, got.at[side, jl, pl.ds(k * rows, rows)])
            if not inner_only:
                pl.when(going & edge)(raw.wait_send if wait else raw.start)
            if not edge_only:
                pl.when(going & jnp.logical_not(edge))(passed.wait_send if wait else passed.start)

    def add_in(side, jl, k):
        def one(r, carry):
            at = pl.ds(pl.multiple_of(k * rows + r * 16, 16), 16)
            got[side, jl, at] = (got[side, jl, at].astype(jnp.float32) + part[part_at(jl, k, r)].astype(jnp.float32)).astype(jnp.bfloat16)
            return carry

        lax.fori_loop(0, rows // 16, one, 0)

    def finish(jl, k):
        def one(r, carry):
            at = pl.ds(pl.multiple_of(k * rows + r * 16, 16), 16)
            total = part[part_at(jl, k, r)].astype(jnp.float32)
            low_side = got[0, jl, at].astype(jnp.float32)
            high_side = got[1, jl, at].astype(jnp.float32)
            total = total + jnp.where(z > 0, low_side, 0.0) + jnp.where(z < n_z - 1, high_side, 0.0)
            value = resid_ref[at].astype(jnp.float32)
            inverse = lax.rsqrt(jnp.mean(value * value, axis=-1, keepdims=True) + norm_eps)
            scaled = value * inverse
            d_scaled = total * gain_ref[...]
            mean = jnp.mean(d_scaled * scaled, axis=-1, keepdims=True)
            d_resid = cot_ref[at].astype(jnp.float32) + inverse * (d_scaled - scaled * mean)
            buf[at] = d_resid.astype(jnp.bfloat16)
            prod = total * scaled
            gain_out[...] = gain_out[...] + prod[:8] + prod[8:]
            return carry

        lax.fori_loop(0, rows // 16, one, 0)

    def to_partner(k):
        at = pl.ds(k * rows, rows)
        return remote(buf.at[at], d_out.at[at], p_s.at[k], p_r.at[k], (2 * pair + 1 - c, z))

    def keep(k):
        at = pl.ds(k * rows, rows)
        return pltpu.make_async_copy(buf.at[at], d_out.at[at], loc.at[k])

    def own_chunk(k):
        @pl.when(own)
        def _():
            jl = z % 2
            pl.when(z > 0)(arrived(0, jl, k).wait_recv)
            pl.when(z < n_z - 1)(arrived(1, jl, k).wait_recv)
            finish(jl, k)
            if k > 0:
                to_partner(k - 1).start()
                keep(k - 1).start()

    done = 0
    for q in range(GROUPS):
        compute(q, 0, 1)
        if q > 0:
            for k in range((q - 1) * per, q * per):
                for t in range(2):
                    send_step(k, t, True, False, False)
        compute(q, 1, tiles)
    multiply(done, done + 1)
    done += 1
    for k in range((GROUPS - 1) * per, CHUNKS):
        for t in range(2):
            send_step(k, t, True, False, False)
    for one in fetch:
        one.wait()

    steps = [(k, t) for k in range(CHUNKS) for t in range(2)]
    for n, (k, t) in enumerate(steps):
        jl = jnp.bitwise_xor(c, t)
        j = 2 * c + jl
        for side in range(2):
            going = (z < j) if side == 0 else (z > j)
            between = (z > 0) if side == 0 else (z < n_z - 1)

            @pl.when(going & between)
            def _():
                arrived(side, jl, k).wait_recv()
                add_in(side, jl, k)

        if n > 0:
            send_step(*steps[n - 1], False, True, False)
        if t == 0 and done < tiles:
            multiply(done, done + 1)
            done += 1
        if t == 1 and k > 0:
            own_chunk(k - 1)
    send_step(*steps[-1], False, True, False)
    own_chunk(CHUNKS - 1)
    if done < tiles:
        multiply(done, tiles)

    @pl.when(own)
    def _():
        to_partner(CHUNKS - 1).start()
        keep(CHUNKS - 1).start()

    for j in range(max(0, tiles - 2), tiles):
        tile_out(j).wait()
    for k, t in steps:
        send_step(k, t, False, False, True)
    for k in range(CHUNKS):
        at = d_out.at[pl.ds(k * rows, rows)]

        @pl.when(own)
        def _():
            to_partner(k).wait_send()
            keep(k).wait()

        pl.when(jnp.logical_not(own))(remote(at, at, p_s.at[k], p_r.at[k], (d, z)).wait_recv)


def sum_line(d_gate, d_up, w, resid, cot, gain, hidden, down, n_z):
    _, full, width = resid.shape
    b16 = jnp.bfloat16
    return pl.pallas_call(
        functools.partial(sum_line_kernel, n_z),
        in_specs=[ANY_SPEC] * 5 + [VMEM_SPEC] + [ANY_SPEC] * 2,
        out_specs=[ANY_SPEC, VMEM_SPEC, ANY_SPEC],
        out_shape=[
            jax.ShapeDtypeStruct((full, width), b16),
            jax.ShapeDtypeStruct((8, width), jnp.float32),
            jax.ShapeDtypeStruct((2 * full, width), b16),
        ],
        scratch_shapes=[
            pltpu.VMEM((2 * full, w.shape[1]), b16), pltpu.VMEM(w.shape, b16), pltpu.VMEM((2 * full, width), b16),
            pltpu.VMEM((2, 2, full, width), b16), pltpu.VMEM((full, width), b16),
            pltpu.VMEM((full, width), b16), pltpu.VMEM((full, width), b16),
            pltpu.VMEM(hidden.shape, b16), pltpu.VMEM(down.shape, b16), pltpu.VMEM((2, 2 * full, 256), b16),
            DMA((2, CHUNKS)), DMA((2, 2, CHUNKS)), DMA((CHUNKS,)), DMA((CHUNKS,)), DMA((CHUNKS,)), DMA((2,)), DMA((2,)), DMA((2,)),
            DMA((GROUPS, 2, 2)), DMA((width // 256,)),
        ],
        compiler_params=pltpu.CompilerParams(collective_id=3, has_side_effects=True, vmem_limit_bytes=63 * 1024 * 1024),
        cost_estimate=pl.CostEstimate(flops=0, bytes_accessed=200_000_000, transcendentals=0),
        name="sum_line",
    )(d_gate, d_up, w, resid, cot, gain, hidden, down)


def hidden_kernel(resid_ref, gain_ref, gate_w, up_w, normed_ref, gate_ref, up_ref, hidden_ref):
    @pl.when(pl.program_id(0) == 0)
    def _():
        def one(r, carry):
            at = pl.ds(pl.multiple_of(r * 16, 16), 16)
            value = resid_ref[at].astype(jnp.float32)
            inverse = lax.rsqrt(jnp.mean(value * value, axis=-1, keepdims=True) + norm_eps)
            normed_ref[at] = (value * inverse * gain_ref[...]).astype(jnp.bfloat16)
            return carry

        lax.fori_loop(0, resid_ref.shape[0] // 16, one, 0, unroll=2)

    half = resid_ref.shape[0] // 4
    for h in range(4):
        at = slice(h * half, (h + 1) * half)
        gate = dot_n(normed_ref[at], gate_w[...])
        up = dot_n(normed_ref[at], up_w[...])
        gate_ref[at] = gate.astype(jnp.bfloat16)
        up_ref[at] = up.astype(jnp.bfloat16)
        hidden_ref[at] = (gate * jax.nn.sigmoid(gate) * up).astype(jnp.bfloat16)


HIDDEN_TILE = 256


def hidden_forward(resid, gain, weights):
    rows, width = resid.shape
    units = weights.shape[1] // 2
    tiles = units // HIDDEN_TILE
    whole = lambda shape: pl.BlockSpec(shape, lambda j: (0, 0))
    tile = pl.BlockSpec((rows, HIDDEN_TILE), lambda j: (0, j))
    return pl.pallas_call(
        hidden_kernel,
        grid=(tiles,),
        in_specs=[
            whole((rows, width)), whole((1, width)),
            pl.BlockSpec((width, HIDDEN_TILE), lambda j: (0, j)),
            pl.BlockSpec((width, HIDDEN_TILE), lambda j: (0, j + tiles)),
        ],
        out_specs=[whole((rows, width)), tile, tile, tile],
        out_shape=[jax.ShapeDtypeStruct((rows, width), jnp.bfloat16)] + [jax.ShapeDtypeStruct((rows, units), jnp.bfloat16)] * 3,
        cost_estimate=pl.CostEstimate(flops=4 * rows * width * units, bytes_accessed=40_000_000, transcendentals=0),
        name="hidden_forward",
    )(resid, gain, weights, weights)


WIDE_ROWS = 32
TURNED_ROWS = 512


def adam_wide_kernel(grad_ref, w_ref, m_ref, v_ref, g_out, w_out, m_out, v_out):
    width = w_ref.shape[-1]
    for n in range(2):
        grad = grad_ref[:, n * width : (n + 1) * width].astype(jnp.float32)
        weight, first, second = adam_update(w_ref[:, n], grad, m_ref[:, n], v_ref[:, n])
        g_out[:, n] = grad
        w_out[:, n] = weight
        m_out[:, n] = first
        v_out[:, n] = second


def adam_turned_kernel(grad_ref, w_ref, m_ref, v_ref, g_out, w_out, m_out, v_out):
    grad = grad_ref[...].astype(jnp.float32).T
    weight, first, second = adam_update(w_ref[...], grad, m_ref[...], v_ref[...])
    g_out[...] = grad
    w_out[...] = weight
    m_out[...] = first
    v_out[...] = second


def adam_call(kernel, grid, grad_spec, spec, arrays):
    shape = jax.ShapeDtypeStruct(arrays[1].shape, jnp.float32)
    return pl.pallas_call(
        kernel,
        grid=(grid,),
        in_specs=[grad_spec] + [spec] * 3,
        out_specs=[spec] * 4,
        out_shape=[shape] * 4,
        cost_estimate=pl.CostEstimate(flops=20 * shape.size, bytes_accessed=30 * shape.size, transcendentals=0),
    )(*arrays)


def adam_wide(*arrays):
    rows, _, width = arrays[1].shape
    return adam_call(
        adam_wide_kernel, rows // WIDE_ROWS,
        pl.BlockSpec((WIDE_ROWS, 2 * width), lambda i: (i, 0)),
        pl.BlockSpec((WIDE_ROWS, 2, width), lambda i: (i, 0, 0)),
        arrays,
    )


def adam_turned(*arrays):
    rows, cols = arrays[1].shape
    return adam_call(
        adam_turned_kernel, rows // TURNED_ROWS,
        pl.BlockSpec((cols, TURNED_ROWS), lambda i: (0, i)),
        pl.BlockSpec((TURNED_ROWS, cols), lambda i: (i, 0)),
        arrays,
    )


def hand_out_kernel(n_dp, n_z, dq_ref, n_ref, x_ref, dr_ref, gain_ref, gain2_ref, wq_ref, ot_ref, ig, gq, go, gains,
                    dn_ref, wq, got, buf, q_base, q_got, q_put, q_fin, o_base, o_got, o_put, o_fin, g_src, g_all,
                    p_s, p_r, i_s, i_r, q_s, q_r, qf_s, qf_r, o_s, o_r, of_s, of_r, g_s, g_r, loc):
    d, z, pair, c = place()
    n_d = n_dp // 2
    total = n_dp * n_z
    me = d * n_z + z
    cz = z // 2
    full, width = x_ref.shape
    half = full // 2
    quarter = half // 2
    q_rows, q_cols = q_fin.shape[1:]
    o_rows, o_cols = o_fin.shape[1:]
    relay = n_d == 4

    class First:
        def __init__(self, rows, cols, bufs, sems, spare):
            self.rows, self.cols, self.spare = rows, cols, spare
            self.base, self.got, self.put, self.fin = bufs
            self.send, self.recv, self.f_send, self.f_recv = sems

        def block(self, ref, b, core):
            return ref.at[pl.ds(core * self.rows, self.rows), pl.ds(b * self.cols, self.cols)]

        def source(self, owner, b, core):
            return self.base.at[pl.ds(pl.multiple_of((2 * owner + core) * self.rows, self.rows), self.rows), pl.ds(b * self.cols, self.cols)]

        def cut_of(self, owner, b, core, r):
            start = (2 * owner + core) * self.rows + r * 16
            return pl.ds(pl.multiple_of(start, 16), 16), pl.ds(b * self.cols, self.cols)

        def copy(self, n, b, core, owner, to):
            return remote(self.source(owner, b, core), self.block(self.got.at[n], b, core), self.send.at[n, b, core],
                          self.recv.at[n, b, core], (2 * (pair ^ to) + c, z))

        def begin(self, core):
            for b in range(2):
                if relay:
                    self.copy(1, b, core, pair ^ 3, 1 + b).start()
            for b in range(2):
                if relay:
                    self.copy(0, b, core, pair ^ (1 + b), 1 + b).start()
                else:
                    for k in range(1, n_d):
                        self.copy(k - 1, b, core, pair ^ k, k).start()

        def arrived(self, n, b, core):
            at = self.block(self.got.at[n], b, core)
            remote(at, at, self.send.at[n, b, core], self.recv.at[n, b, core], (d, z)).wait_recv()

        def cut(self, b, core, r):
            return pl.ds(pl.multiple_of(core * self.rows + r * 16, 16), 16), pl.ds(b * self.cols, self.cols)

        def middle_copy(self, b, core):
            return remote(self.source(pair ^ (2 >> b), b, core), self.block(self.got.at[2], b, core), self.send.at[2, b, core],
                          self.recv.at[2, b, core], (2 * (pair ^ (2 >> b)) + c, z))

        def middle(self, core, between):
            if not relay:
                return
            for b in range(2):
                self.arrived(1, b, core)

                def add(r, carry):
                    at = self.cut(b, core, r)
                    mid = self.cut_of(pair ^ (2 >> b), b, core, r)
                    self.base[mid] = (self.base[mid].astype(jnp.float32) + self.got[(1,) + at].astype(jnp.float32)).astype(jnp.bfloat16)
                    return carry

                lax.fori_loop(0, self.rows // 16, add, 0)
            self.middle_copy(0, core).start()
            between()
            self.middle_copy(1, core).start()

        def total(self, core, between):
            slots = (0, 2) if relay else range(n_d - 1)
            for b in range(2):
                for n in slots:
                    self.arrived(n, b, core)

                def add(r, carry):
                    at = self.cut(b, core, r)
                    value = self.base[self.cut_of(pair, b, core, r)].astype(jnp.float32)
                    for n in slots:
                        value = value + self.got[(n,) + at].astype(jnp.float32)
                    self.put[core, b, pl.ds(pl.multiple_of(r * 16, 16), 16)] = value.astype(jnp.bfloat16)
                    return carry

                lax.fori_loop(0, self.rows // 16, add, 0)
            self.second(0, core, False)
            between()
            self.second(1, core, False)

        def second(self, b, core, wait):
            here = (core == c) & (2 * c + b == z)
            src = self.put.at[core, b]
            copy = remote(src, self.fin.at[z], self.f_send.at[core, b], self.f_recv.at[z], (2 * pair + core, 2 * c + b))
            keep = pltpu.make_async_copy(src, self.fin.at[z], loc.at[self.spare])
            pl.when(jnp.logical_not(here))(copy.wait_send if wait else copy.start)
            pl.when(here)(keep.wait if wait else keep.start)

        def final(self):
            for core in range(2):
                for b in range(2):
                    self.second(b, core, True)
            for zs in range(n_z):
                at = self.fin.at[zs]
                from_here = (cz == c) & (zs == z)
                pl.when(jnp.logical_not(from_here))(remote(at, at, self.f_send.at[0, 0], self.f_recv.at[zs], (d, z)).wait_recv)

        def sent(self):
            for b in range(2):
                for core in range(2):
                    for n in range(n_d - 1):
                        at = self.block(self.got.at[n], b, core)
                        remote(at, at, self.send.at[n, b, core], self.recv.at[n, b, core], (d, z)).wait_send()

    o_first = First(o_rows, o_cols, (o_base, o_got, o_put, o_fin), (o_s, o_r, of_s, of_r), 2)
    q_first = First(q_rows, q_cols, (q_base, q_got, q_put, q_fin), (q_s, q_r, qf_s, qf_r), 3)
    o_load = pltpu.make_async_copy(ot_ref, o_base, loc.at[4])
    wq_load = pltpu.make_async_copy(wq_ref, wq, loc.at[5])
    o_load.start()
    wq_load.start()
    greet_all(n_dp, n_z, d, z)
    o_load.wait()
    o_first.begin(0)
    o_first.begin(1)
    nothing = lambda: None

    def q_blocks(core):
        def one(k, carry):
            owner = pair ^ (n_d - 1 - k)
            rows_at = pl.ds(pl.multiple_of((2 * owner + core) * q_rows, q_rows), q_rows)
            q_base[rows_at] = dot_c(n_ref[:, rows_at], dq_ref[...]).astype(jnp.bfloat16)
            return carry

        lax.fori_loop(0, n_d, one, 0)

    def dn_blocks(low, high):
        def one(r, carry):
            rows_at = pl.ds(pl.multiple_of(r * 256, 256), 256)
            dn_ref[:, rows_at] = dot_t(dq_ref[...], wq[rows_at]).astype(jnp.bfloat16)
            return carry

        lax.fori_loop(low, high, one, 0)

    q_blocks(0)
    o_first.middle(0, lambda: q_blocks(1))
    q_first.begin(0)
    wq_load.wait()
    dn_tiles = width // 256
    dn_blocks(0, dn_tiles // 2)
    o_first.middle(1, nothing)
    q_first.begin(1)
    dn_blocks(dn_tiles // 2, dn_tiles)
    mine = pl.ds(pl.multiple_of(c * half, half), half)
    theirs = pl.ds(pl.multiple_of((1 - c) * half, half), half)
    swap = remote(dn_ref.at[theirs], got, p_s, p_r, (2 * pair + 1 - c, z))
    o_first.total(0, nothing)
    swap.start()

    g_src[pl.ds(0, 8)] = jnp.zeros((8, width), jnp.float32)
    g_src[pl.ds(8, 8)] = gain2_ref[...]
    swap.wait_recv()

    def rows_of(r, carry):
        at = pl.ds(pl.multiple_of(r * 16, 16), 16)
        src = pl.ds(pl.multiple_of(c * half + r * 16, 16), 16)
        d_normed = dn_ref[src].astype(jnp.float32) + got[at].astype(jnp.float32)
        value = x_ref[src].astype(jnp.float32)
        inverse = lax.rsqrt(jnp.mean(value * value, axis=-1, keepdims=True) + norm_eps)
        scaled = value * inverse
        d_scaled = d_normed * gain_ref[...]
        mean = jnp.mean(d_scaled * scaled, axis=-1, keepdims=True)
        out = dr_ref[src].astype(jnp.float32) + inverse * (d_scaled - scaled * mean)
        buf[at] = out.astype(jnp.bfloat16)
        prod = d_normed * scaled
        g_src[pl.ds(0, 8)] = g_src[pl.ds(0, 8)] + prod[:8] + prod[8:]
        return carry

    def row_send(b, wait):
        src = buf.at[pl.ds(b * quarter, quarter)]
        dst = ig.at[z % 2]
        zz = 2 * c + b
        here = (cz == c) & (zz == z)
        copy = remote(src, dst, i_s.at[b], i_r.at[z % 2], (2 * pair + cz, zz))
        keep = pltpu.make_async_copy(src, dst, loc.at[0])
        pl.when(jnp.logical_not(here))(copy.wait_send if wait else copy.start)
        pl.when(here)(keep.wait if wait else keep.start)

    q_first.middle(0, nothing)
    per = quarter // 16
    lax.fori_loop(0, per, rows_of, 0)
    o_first.total(1, lambda: row_send(0, False))
    lax.fori_loop(per, 2 * per, rows_of, 0)
    q_first.middle(1, lambda: row_send(1, False))

    each = width // total

    def gain_tile(o):
        return g_src.at[:, pl.ds(pl.multiple_of(o * each // 128 * 128, 128), 128)]

    own_gain = pltpu.make_async_copy(gain_tile(me), g_all.at[me], loc.at[1])
    own_gain.start()

    def send_gain(o, carry):
        other = lax.rem(me + o, total)
        remote(gain_tile(other), g_all.at[me], g_s, g_r, (other // n_z, lax.rem(other, n_z))).start()
        return carry

    lax.fori_loop(1, total, send_gain, 0)

    q_first.total(0, nothing)
    q_first.total(1, nothing)

    o_first.final()
    value = o_fin[0].astype(jnp.float32)
    for zs in range(1, n_z):
        value = value + o_fin[zs].astype(jnp.float32)
    go[...] = value.T

    many = g_all.at[pl.ds(0, total - 1)]
    gain_copy = remote(many, many, g_s, g_r, (d, z))
    gain_copy.wait_send()
    gain_copy.wait_recv()
    own_gain.wait()
    gains[...] = jnp.zeros_like(gains)

    def add_gain(o, carry):
        gains[...] = gains[...] + g_all[o]
        return carry

    lax.fori_loop(0, total, add_gain, 0)

    swap.wait_send()
    for b in range(2):
        row_send(b, True)
    for i in range(2):
        from_here = (cz == c) & (2 * c + i == z)
        at = ig.at[i]
        pl.when(jnp.logical_not(from_here))(remote(at, at, i_s.at[0], i_r.at[i], (d, z)).wait_recv)
    o_first.sent()
    q_first.sent()
    q_first.final()

    def last(r, carry):
        at = pl.ds(pl.multiple_of(r * 16, 16), 16)
        value = q_fin[0, at].astype(jnp.float32)
        for zs in range(1, n_z):
            value = value + q_fin[zs, at].astype(jnp.float32)
        gq[at] = value
        return carry

    lax.fori_loop(0, q_rows // 16, last, 0)


def hand_out(dq, normed, x, dr, gain, gain2, wq, ot, n_dp, n_z):
    full, width = x.shape
    n_d = n_dp // 2
    total = n_dp * n_z
    q_rows, q_cols = wq.shape[0] // n_dp, wq.shape[1] // 2
    o_rows, o_cols = ot.shape[0] // n_dp, ot.shape[1] // 2
    b16 = jnp.bfloat16
    f32 = jnp.float32

    def weight_bufs(rows, cols):
        return [
            pltpu.VMEM((n_dp * rows, 2 * cols), b16), pltpu.VMEM((n_d - 1, 2 * rows, 2 * cols), b16),
            pltpu.VMEM((2, 2, rows, cols), b16), pltpu.VMEM((n_z, rows, cols), b16),
        ]

    weight_sems = [DMA((n_d - 1, 2, 2)), DMA((n_d - 1, 2, 2)), DMA((2, 2)), DMA((n_z,))]
    return pl.pallas_call(
        functools.partial(hand_out_kernel, n_dp, n_z),
        in_specs=[VMEM_SPEC] * 6 + [ANY_SPEC] * 2,
        out_specs=[ANY_SPEC] + [VMEM_SPEC] * 3,
        out_shape=[
            jax.ShapeDtypeStruct((2, full // 4, width), b16),
            jax.ShapeDtypeStruct((q_rows, q_cols), f32),
            jax.ShapeDtypeStruct((o_cols, o_rows), f32),
            jax.ShapeDtypeStruct((16, 128), f32),
        ],
        scratch_shapes=[
            pltpu.VMEM((full, width), b16), pltpu.VMEM(wq.shape, b16),
            pltpu.VMEM((full // 2, width), b16), pltpu.VMEM((full // 2, width), b16),
            *weight_bufs(q_rows, q_cols), *weight_bufs(o_rows, o_cols),
            pltpu.VMEM((16, width), f32), pltpu.VMEM((total, 16, 128), f32),
            DMA, DMA, DMA((2,)), DMA((2,)), *weight_sems, *weight_sems, DMA, DMA,
            DMA((6,)),
        ],
        compiler_params=pltpu.CompilerParams(collective_id=5, has_side_effects=True, vmem_limit_bytes=58 * 1024 * 1024),
        cost_estimate=pl.CostEstimate(flops=0, bytes_accessed=300_000_000, transcendentals=0),
        name="hand_out",
    )(dq, normed, x, dr, gain, gain2, wq, ot)


def rms_forward(values, gain_wide):
    inverse = lax.rsqrt(jnp.mean(values * values, axis=-1, keepdims=True) + norm_eps)
    scaled = values * inverse
    return (scaled, inverse, (scaled * gain_wide).astype(jnp.bfloat16))


def adam_update(weight, grad, first, second):
    new_first = beta_one * first + (1.0 - beta_one) * grad
    new_second = beta_two * second + (1.0 - beta_two) * grad * grad
    first_hat = new_first / (1.0 - beta_one**step_count)
    second_hat = new_second / (1.0 - beta_two**step_count)
    new_weight = weight - learn_rate * (
        first_hat / (jnp.sqrt(second_hat) + adam_eps) + weight_decay * weight
    )
    return (new_weight, new_first, new_second)


def contract_rows(left, right):
    return lax.dot_general(
        left, right, (((0,), (0,)), ((), ())), preferred_element_type=jnp.float32
    )


def times_transpose(left, right):
    return lax.dot_general(
        left, right, (((1,), (1,)), ((), ())), preferred_element_type=jnp.float32
    )


def layer_step(
    block_input,
    segment_ids,
    cotangent,
    attn_gain,
    qkv_weight,
    out_weight,
    mlp_gain,
    gate_up_weight,
    down_weight,
    first_attn_gain,
    first_qkv,
    first_out,
    first_mlp_gain,
    first_gate_up,
    first_down,
    second_attn_gain,
    second_qkv,
    second_out,
    second_mlp_gain,
    second_gate_up,
    second_down,
):
    seqs_here, local_len, width = block_input.shape
    full_len = segment_ids.shape[1]
    n_dp = lax.axis_size("dp")
    n_z = lax.axis_size("seq")
    groups = HEADS // KV_HEADS
    z_here = lax.axis_index("seq")
    owned = attn_gain.shape[0]
    gain_line = jnp.concatenate([attn_gain, mlp_gain]).astype(jnp.bfloat16).astype(jnp.float32)
    gain_tile = jnp.pad(gain_line[None], ((0, 7), (0, LANES - 2 * owned)))
    seg_tile = jnp.pad(segment_ids, ((0, 8 - seqs_here), (0, 0)))
    rows_in, qkv_cols, out_line, gain_all, seg_all, gate_up_here, down_here16 = gather_in(
        block_input,
        qkv_weight,
        out_weight,
        gain_tile,
        seg_tile,
        gate_up_weight,
        down_weight,
        n_dp,
        n_z,
    )
    cot_late, _ = lax.optimization_barrier((cotangent, gain_all))
    cot_all = lax.all_gather(cot_late, "seq", axis=1, tiled=True)
    gain_one = gain_all[:, 0, :owned].reshape(1, width)
    gain_two = gain_all[:, 0, owned : 2 * owned].reshape(1, width)
    seg_here = lax.dynamic_slice(seg_all, (z_here // 2, z_here % 2, 0), (1, 1, full_len))[0]
    tables = attn_tables(seg_here)
    _, _, normed_one = rms_forward(rows_in.astype(jnp.float32), gain_one)
    qkv = jnp.dot(normed_one, qkv_cols, preferred_element_type=jnp.float32)
    turned, lse, attended16, out_rows = attn_forward(qkv, *tables, out_line, full_len, groups, n_dp)
    attn_part = times_transpose(attended16, out_rows)
    resid_all, gate_up_cols = share_resid(
        attn_part.astype(jnp.bfloat16), rows_in, gate_up_here, n_dp, n_z
    )
    total_rows = seqs_here * full_len
    down_late, _ = lax.optimization_barrier((down_here16, resid_all))
    down_rows = lax.all_gather(down_late, "dp", axis=1, tiled=True)
    normed_two, gate16, up16, hidden16 = hidden_forward(resid_all.reshape(total_rows, width), gain_two, gate_up_cols)
    gate_part = gate16.astype(jnp.float32)
    up_part = up16.astype(jnp.float32)
    sigmoid_gate = jax.nn.sigmoid(gate_part)
    active = gate_part * sigmoid_gate
    cot_rows = cot_all.reshape(total_rows, width)
    d_hidden = times_transpose(cot_rows, down_rows)
    d_gate = d_hidden * up_part * sigmoid_gate * (1.0 + gate_part * (1.0 - sigmoid_gate))
    d_up = d_hidden * active
    d_gate16 = d_gate.astype(jnp.bfloat16)
    d_up16 = d_up.astype(jnp.bfloat16)
    d_gate_up16 = jnp.concatenate([d_gate16, d_up16], 1)
    gate_up_term = contract_rows(normed_two, d_gate_up16).astype(jnp.bfloat16)
    gate_up_sum = lax.psum_scatter(gate_up_term, "dp", scatter_dimension=0, tiled=True)
    down_term = contract_rows(cot_rows, hidden16).astype(jnp.bfloat16)
    down_sum = lax.psum_scatter(down_term, "dp", scatter_dimension=0, tiled=True)
    d_resid16, gain_two_part, down_part = sum_line(
        d_gate16, d_up16, gate_up_cols, resid_all, cot_all, gain_two, hidden16, down_rows, n_z
    )
    down16 = down_part.reshape(resid_all.shape)
    pieces = [
        lax.dynamic_slice_in_dim(down16, (z_here + o) % n_z * local_len, local_len, 1)
        for o in range(n_z)
    ]
    for o in range(1, n_z):
        pieces[o] = lax.ppermute(pieces[o], "seq", [(i, (i + o) % n_z) for i in range(n_z)])
    down_here = sum(piece.astype(jnp.float32) for piece in pieces)
    resid_here = lax.dynamic_slice_in_dim(resid_all, z_here * local_len, local_len, 1)
    output = (resid_here.astype(jnp.float32) + down_here).astype(jnp.bfloat16)
    d_attended = jnp.dot(d_resid16, out_rows, preferred_element_type=jnp.float32).astype(jnp.bfloat16)
    d_qkv16 = attn_backward(turned, d_attended, lse, *tables, full_len, groups)
    out_term = contract_rows(d_resid16, attended16).astype(jnp.bfloat16)
    input_grad, grad_qkv, grad_out, gain_sums = hand_out(
        d_qkv16,
        normed_one,
        rows_in,
        d_resid16,
        gain_one,
        gain_two_part,
        qkv_cols,
        out_term,
        n_dp,
        n_z,
    )
    grad_gate_up, w_gu, m_gu, v_gu = adam_wide(
        gate_up_sum, gate_up_weight, first_gate_up, second_gate_up
    )
    grad_down, w_down, m_down, v_down = adam_turned(
        down_sum, down_weight, first_down, second_down
    )
    flat = lax.axis_index("dp") * n_z + z_here
    gain_sums = lax.dynamic_slice(
        jnp.sum(gain_sums.reshape(2, 8, LANES), axis=1), (0, flat * owned % LANES), (2, owned)
    )
    grad_gain_one = gain_sums[0]
    grad_gain_two = gain_sums[1]
    w_one, m_one, v_one = adam_update(attn_gain, grad_gain_one, first_attn_gain, second_attn_gain)
    w_qkv, m_qkv, v_qkv = adam_update(qkv_weight, grad_qkv, first_qkv, second_qkv)
    w_out, m_out, v_out = adam_update(out_weight, grad_out, first_out, second_out)
    w_two, m_two, v_two = adam_update(mlp_gain, grad_gain_two, first_mlp_gain, second_mlp_gain)
    return (
        output,
        input_grad,
        grad_gain_one,
        grad_qkv,
        grad_out,
        grad_gain_two,
        grad_gate_up,
        grad_down,
        w_one,
        w_qkv,
        w_out,
        w_two,
        w_gu,
        w_down,
        m_one,
        m_qkv,
        m_out,
        m_two,
        m_gu,
        m_down,
        v_one,
        v_qkv,
        v_out,
        v_two,
        v_gu,
        v_down,
    )


def solution(mesh):
    in_specs = (
        P("dp", "seq", None),
        P("dp", None),
        P("dp", "seq", None),
        P(("dp", "seq")),
        P("dp", "seq"),
        P("seq", "dp"),
        P(("dp", "seq")),
        P("dp", None, "seq"),
        P("seq", "dp"),
        P(("dp", "seq")),
        P("dp", "seq"),
        P("seq", "dp"),
        P(("dp", "seq")),
        P("dp", None, "seq"),
        P("seq", "dp"),
        P(("dp", "seq")),
        P("dp", "seq"),
        P("seq", "dp"),
        P(("dp", "seq")),
        P("dp", None, "seq"),
        P("seq", "dp"),
    )
    out_specs = (
        P("dp", "seq", None),
        P("dp", "seq", None),
        P(("dp", "seq")),
        P("dp", "seq"),
        P("seq", "dp"),
        P(("dp", "seq")),
        P("dp", None, "seq"),
        P("seq", "dp"),
        P(("dp", "seq")),
        P("dp", "seq"),
        P("seq", "dp"),
        P(("dp", "seq")),
        P("dp", None, "seq"),
        P("seq", "dp"),
        P(("dp", "seq")),
        P("dp", "seq"),
        P("seq", "dp"),
        P(("dp", "seq")),
        P("dp", None, "seq"),
        P("seq", "dp"),
        P(("dp", "seq")),
        P("dp", "seq"),
        P("seq", "dp"),
        P(("dp", "seq")),
        P("dp", None, "seq"),
        P("seq", "dp"),
    )
    return jax.shard_map(layer_step, mesh=mesh, in_specs=in_specs, out_specs=out_specs, check_vma=False)
```
